32 devices in a mesh: wide: 16 (over z, x, core), narrow: 2 (over y).
Axes of the slice: x: 2, y: 2, z: 4, core: 2. Of those that a mesh axis runs over, the one named last changes fastest.
Arguments:
- layer_in: bfloat16 [16384, 768], P(('wide', 'narrow')), may hold values from -6 to 6
- doc_ids: int32 [32, 512], P('wide'), may hold values from 0 to 3, never falling along the last dimension, each value on 1 to 256 neighbouring positions
- query_weight: bfloat16 [768, 768], P(('wide', 'narrow')), may hold values from -0.21875 to 0.21875
- query_bias: bfloat16 [768], P(('wide', 'narrow')), may hold values from -2 to 2
- key_weight: bfloat16 [768, 768], P(('wide', 'narrow')), may hold values from -0.21875 to 0.21875
- key_bias: bfloat16 [768], P(('wide', 'narrow')), may hold values from -2 to 2
- value_weight: bfloat16 [768, 768], P(('wide', 'narrow')), may hold values from -0.21875 to 0.21875
- value_bias: bfloat16 [768], P(('wide', 'narrow')), may hold values from -2 to 2
- output_weight: bfloat16 [768, 768], P(('wide', 'narrow')), may hold values from -0.875 to 0.875
- output_bias: bfloat16 [768], P(('wide', 'narrow')), may hold values from -2 to 2
- attn_gain: bfloat16 [768], P(('wide', 'narrow')), may hold values from 0.25 to 1.75
- attn_shift: bfloat16 [768], P(('wide', 'narrow')), may hold values from -2 to 2
- inner_weight: bfloat16 [768, 3072], P('wide', 'narrow'), may hold values from -0.21875 to 0.21875
- inner_bias: bfloat16 [3072], P(('narrow', 'wide')), may hold values from -2 to 2
- outer_weight: bfloat16 [3072, 768], P('narrow', 'wide'), may hold values from -0.109375 to 0.109375
- outer_bias: bfloat16 [768], P(('wide', 'narrow')), may hold values from -2 to 2
- ffn_gain: bfloat16 [768], P(('wide', 'narrow')), may hold values from 0.25 to 1.75
- ffn_shift: bfloat16 [768], P(('wide', 'narrow')), may hold values from -2 to 2
- cotangent: bfloat16 [16384, 768], P(('wide', 'narrow')), may hold values from -6 to 6
Outputs:
- layer_out: float32 [16384, 768], P(('wide', 'narrow'))
- input_grad: float32 [16384, 768], P(('wide', 'narrow'))
- query_wgrad: float32 [768, 768], P(('wide', 'narrow'))
- query_bgrad: float32 [768], P(('wide', 'narrow'))
- key_wgrad: float32 [768, 768], P(('wide', 'narrow'))
- key_bgrad: float32 [768], P(('wide', 'narrow'))
- value_wgrad: float32 [768, 768], P(('wide', 'narrow'))
- value_bgrad: float32 [768], P(('wide', 'narrow'))
- output_wgrad: float32 [768, 768], P(('wide', 'narrow'))
- output_bgrad: float32 [768], P(('wide', 'narrow'))
- attn_ggrad: float32 [768], P(('wide', 'narrow'))
- attn_sgrad: float32 [768], P(('wide', 'narrow'))
- inner_wgrad: float32 [768, 3072], P('wide', 'narrow')
- inner_bgrad: float32 [3072], P(('narrow', 'wide'))
- outer_wgrad: float32 [3072, 768], P('narrow', 'wide')
- outer_bgrad: float32 [768], P(('wide', 'narrow'))
- ffn_ggrad: float32 [768], P(('wide', 'narrow'))
- ffn_sgrad: float32 [768], P(('wide', 'narrow'))
The draws below stay inside these ranges and needn't reach their ends.
Inputs may be any that keep to these rules, and one draw needn't show every extreme that they name: `doc_ids`: within each pack the ids never fall, so each document is one run of 1 to 256 tokens.
All inputs are finite; a program needn't handle non-finite values.
Results may differ from the reference program's by a relative error of at most 0.018.
Values may be sent and summed in bfloat16 or wider, within the bound.
A program may use at most 192 MiB of HBM per device.

```python
import math
import jax
import jax.numpy as jnp
import numpy as np
from jax import lax

D = 768
HEADS = 12
HEAD_DIM = 64
FF = 3072
PACK = 512
DOCS = 4
PACKS_PAIR = 2
HALF = 256
PACKS = 32
TOKENS = 16384


def shard_levels(rng, shape, pieces, low, largest):
    level, own = 1.0, jax.random.fold_in(rng, 6)
    for axis_at, parts in pieces:
        draws = jnp.exp(jax.random.uniform(jax.random.fold_in(own, axis_at), (parts,), jnp.float32, low / len(pieces), largest / len(pieces)))
        level = level * jnp.repeat(draws, shape[axis_at] // parts).reshape([-1 if axis == axis_at else 1 for axis in range(len(shape))])
    return level


def split_up(number_of, total, reach, slope):
    loads = [(1 << 20) // math.isqrt(rank ** slope) + 1 for rank in range(2, number_of + 1)]
    rest, given = total - reach - (number_of - 1), [1] * (number_of - 1)
    while rest > 0:
        candidates = [i for i in range(number_of - 1) if given[i] < reach]
        pool, remaining = sum([loads[i] for i in candidates]), rest
        for i in candidates:
            more = min(reach - given[i], max(1, remaining * loads[i] // pool), rest)
            given[i] = given[i] + more
            rest = rest - more
    return np.array([reach] + given)


def uneven(rng, amount, total, reach, slope):
    if amount == 2:
        one = jax.random.randint(rng, (), max(1, total - reach), min(reach, total - 1) + 1)
        return jnp.stack([one, total - one])
    sizes = jnp.asarray(split_up(amount, total, reach, slope), jnp.int32)
    twos = (amount - 1) // 2
    source_of, taker = sizes[1:1 + 2 * twos:2], sizes[2:2 + 2 * twos:2]
    room = jnp.minimum(source_of - 1, reach - taker)
    moved = jax.random.randint(jax.random.fold_in(rng, 1), (twos,), 0, 1 << 20) % (room + 1)
    sizes = sizes.at[1:1 + 2 * twos:2].set(source_of - moved).at[2:2 + 2 * twos:2].set(taker + moved)
    return sizes[jax.random.permutation(jax.random.fold_in(rng, 2), amount)]


def bell_draw(own_key, extent, deviation, most, pieces=(), held_as=jnp.bfloat16):
    entries = deviation * jax.random.normal(own_key, extent, jnp.float32)
    if pieces:
        entries = entries * shard_levels(own_key, extent, pieces, -0.22, 0.18)
    return jnp.clip(entries, -most, most).astype(held_as)


def setup_inputs(seed: int = 0) -> dict:
    keys = jax.random.split(jax.random.key(seed), 20)
    return {
        "layer_in": bell_draw(keys[0], (TOKENS, D), 1.0, 6.0, ((0, 32),)),
        "doc_ids": jax.vmap(lambda own: jnp.searchsorted(jnp.cumsum(uneven(own, DOCS, PACK, PACK // 2, 1)), jnp.arange(PACK), side="right"))(jax.random.split(keys[1], PACKS)).reshape((PACKS, PACK)).astype(jnp.int32),
        "query_weight": bell_draw(keys[2], (D, D), D ** -0.5, 0.21875, ((0, 32),)),
        "query_bias": bell_draw(keys[3], (D,), 0.3, 2.0, ((0, 32),)),
        "key_weight": bell_draw(keys[4], (D, D), D ** -0.5, 0.21875, ((0, 32),)),
        "key_bias": bell_draw(keys[5], (D,), 0.3, 2.0, ((0, 32),)),
        "value_weight": bell_draw(keys[6], (D, D), D ** -0.5, 0.21875, ((0, 32),)),
        "value_bias": bell_draw(keys[7], (D,), 0.3, 2.0, ((0, 32),)),
        "output_weight": bell_draw(keys[8], (D, D), (D // 16) ** -0.5, 0.875, ((0, 32),)),
        "output_bias": bell_draw(keys[9], (D,), 0.3, 2.0, ((0, 32),)),
        "attn_gain": jnp.clip(1.0 + 0.15 * jax.random.normal(keys[10], (D,), jnp.float32), 0.25, 1.75).astype(jnp.bfloat16),
        "attn_shift": bell_draw(keys[11], (D,), 0.3, 2.0, ((0, 32),)),
        "inner_weight": bell_draw(keys[12], (D, FF), D ** -0.5, 0.21875, ((0, 16), (1, 2))),
        "inner_bias": bell_draw(keys[13], (FF,), 0.3, 2.0, ((0, 32),)),
        "outer_weight": bell_draw(keys[14], (FF, D), FF ** -0.5, 0.109375, ((0, 2), (1, 16))),
        "outer_bias": bell_draw(keys[15], (D,), 0.3, 2.0, ((0, 32),)),
        "ffn_gain": jnp.clip(1.0 + 0.15 * jax.random.normal(keys[16], (D,), jnp.float32), 0.25, 1.75).astype(jnp.bfloat16),
        "ffn_shift": bell_draw(keys[17], (D,), 0.3, 2.0, ((0, 32),)),
        "cotangent": bell_draw(keys[18], (TOKENS, D), 1.0, 6.0, ((0, 32),)),
    }


@jax.custom_vjp
def low(v):
    return lax.optimization_barrier(v.astype(jnp.bfloat16)).astype(jnp.float32)

@jax.custom_vjp
def low_back(v):
    return v

def low_keep(v):
    return (low(v), None)

def low_pass(kept, grad):
    return (grad,)

def back_keep(v):
    return (v, None)

def back_low(kept, grad):
    return (low(grad),)
low.defvjp(low_keep, low_pass)
low_back.defvjp(back_keep, back_low)
layer_eps = 1e-12
masked_score = -1e+30

def matmul(left_op, right_op):
    return jnp.dot(left_op, right_op, precision=lax.Precision.HIGHEST)

def layer_norm(values, gain_vec, shift_vec):
    center = values - lax.optimization_barrier(jnp.mean(values, axis=-1, keepdims=True))
    spread = lax.optimization_barrier(jnp.mean(center * center, axis=-1, keepdims=True))
    return center * lax.rsqrt(spread + layer_eps) * gain_vec + shift_vec

def rotary_tables(doc_row):
    places = jnp.arange(doc_row.shape[0], dtype=jnp.int32)
    before = lax.optimization_barrier(jnp.sum((doc_row[None, :] < doc_row[:, None]).astype(jnp.int32), axis=1))
    position = (places - before).astype(jnp.float32)
    frequency = 10000.0 ** (-2.0 * jnp.arange(HEAD_DIM // 2, dtype=jnp.float32) / HEAD_DIM)
    angles = position[:, None] * frequency[None, :]
    return (jnp.cos(angles), jnp.sin(angles))

def rotate(values, cosine, sine_tab):
    half_dim = values.shape[-1] // 2
    first_half = values[..., :half_dim]
    second = values[..., half_dim:]
    return jnp.concatenate([first_half * cosine - second * sine_tab, second * cosine + first_half * sine_tab], axis=-1)

def attend_pack(packed):
    query_rot, key_rot, value_low, doc_row = packed
    scores = jnp.einsum('qhd,khd->hqk', query_rot, key_rot, precision=lax.Precision.HIGHEST) * HEAD_DIM ** (-0.5)
    same_doc = doc_row[:, None] == doc_row[None, :]
    scores = low_back(jnp.where(same_doc[None], scores, masked_score))
    probability = low(jax.nn.softmax(scores, axis=-1))
    return jnp.einsum('hqk,khd->qhd', probability, value_low, precision=lax.Precision.HIGHEST)

def forward(params, all_rows, all_docs):
    query_weight, query_bias, key_weight, key_bias, value_weight, value_bias, output_weight, output_bias, attn_gain, attn_shift, inner_weight, inner_bias, outer_weight, outer_bias, ffn_gain, ffn_shift = params
    pack_count = all_docs.shape[0]
    cosine, sine_tab = jax.vmap(rotary_tables)(all_docs)
    cosine = cosine[:, :, None, :]
    sine_tab = sine_tab[:, :, None, :]

    def heads_of(values):
        return values.reshape(pack_count, PACK, HEADS, HEAD_DIM)
    query_rot = low(rotate(heads_of(low_back(matmul(all_rows, query_weight) + query_bias)), cosine, sine_tab))
    key_rot = low(rotate(heads_of(low_back(matmul(all_rows, key_weight) + key_bias)), cosine, sine_tab))
    value_low = low(low_back(heads_of(matmul(all_rows, value_weight) + value_bias)))
    mixed_out = lax.map(jax.checkpoint(attend_pack), (query_rot, key_rot, value_low, all_docs))
    mixed_out = low(low_back(mixed_out.reshape(all_rows.shape)))
    attn_out = low_back(matmul(mixed_out, output_weight) + output_bias)
    norm_one = layer_norm(all_rows + attn_out, attn_gain, attn_shift)
    inner_pre = low_back(matmul(low(norm_one), inner_weight) + inner_bias)
    act_low = low(jax.nn.gelu(inner_pre, approximate=False))
    outer_out = low_back(matmul(act_low, outer_weight) + outer_bias)
    return layer_norm(norm_one + outer_out, ffn_gain, ffn_shift)

def to_packs(values):
    pair_count = PACKS // PACKS_PAIR
    return values.reshape(pair_count, 2, PACKS_PAIR, HALF, D).transpose(0, 2, 1, 3, 4).reshape(TOKENS, D)

def from_packs(values):
    pair_count = PACKS // PACKS_PAIR
    return values.reshape(pair_count, PACKS_PAIR, 2, HALF, D).transpose(0, 2, 1, 3, 4).reshape(TOKENS, D)

def reference(layer_in, doc_ids, query_weight, query_bias, key_weight, key_bias, value_weight, value_bias, output_weight, output_bias, attn_gain, attn_shift, inner_weight, inner_bias, outer_weight, outer_bias, ffn_gain, ffn_shift, cotangent):
    params = tuple((weight.astype(jnp.float32) for weight in (query_weight, query_bias, key_weight, key_bias, value_weight, value_bias, output_weight, output_bias, attn_gain, attn_shift, inner_weight, inner_bias, outer_weight, outer_bias, ffn_gain, ffn_shift)))
    group_size = math.gcd(PACKS, max(1, 4096 // PACK))
    rounds = PACKS // group_size
    all_rows = to_packs(layer_in.astype(jnp.float32)).reshape(rounds, group_size * PACK, D)
    all_docs = doc_ids.reshape(rounds, group_size, PACK)
    all_cots = to_packs(cotangent.astype(jnp.float32)).reshape(rounds, group_size * PACK, D)

    def advance(totals, blocks):
        block_rows, block_docs, block_cots = blocks

        def apply_layer(weights, inputs):
            return forward(weights, inputs, block_docs)
        result, pullback = jax.vjp(apply_layer, params, block_rows)
        weight_grads, row_grads = pullback(block_cots)
        return (jax.tree.map(jnp.add, totals, weight_grads), (result, row_grads))
    zero_grads = tuple((jnp.zeros_like(weight) for weight in params))
    totals, (results, row_grads) = lax.scan(advance, zero_grads, (all_rows, all_docs, all_cots))
    return (from_packs(results.reshape(TOKENS, D)), from_packs(row_grads.reshape(TOKENS, D)), totals[0], totals[1], totals[2], totals[3], totals[4], totals[5], totals[6], totals[7], totals[8], totals[9], totals[10], totals[11], totals[12], totals[13], totals[14], totals[15])
```

```python
import jax
import jax.numpy as jnp
from jax import lax
from jax.sharding import PartitionSpec as P

D = 768
HEADS = 12
HEAD_DIM = 64

ALL = ("wide", "narrow")
layer_eps = 1e-12
masked_score = -1e30


def swapped(shard, axis, bit):
    return lax.ppermute(shard, axis, [(i, i ^ 1 << bit) for i in range(lax.axis_size(axis))])


def bit_order(total, narrow_n):
    bits = total.bit_length() - 1
    core_bit = narrow_n.bit_length() - 1
    return [b for b in reversed(range(bits)) if b != core_bit] + [core_bit]


def is_pow2(n):
    return n & (n - 1) == 0


def gather_all(shard):
    total = lax.axis_size("wide") * lax.axis_size("narrow")
    narrow_n = lax.axis_size("narrow")
    if not (is_pow2(total) and is_pow2(narrow_n)):
        return lax.all_gather(shard, ALL, axis=0, tiled=False)
    me = lax.axis_index(ALL)
    order = bit_order(total, narrow_n)
    cur = shard
    for b in order:
        other = lax.ppermute(cur, ALL, [(i, i ^ (1 << b)) for i in range(total)])
        bit = (me >> b) & 1
        pick = (jnp.arange(2) == bit).reshape((2,) + (1,) * cur.ndim)
        cur = jnp.where(pick, cur[None], other[None])
    k = len(order)
    perm = [k - 1 - order.index(b) for b in reversed(range(k))]
    cur = cur.transpose(perm + list(range(k, cur.ndim)))
    return cur.reshape((total,) + shard.shape)


def scatter_sum_all(parts):
    total = lax.axis_size("wide") * lax.axis_size("narrow")
    narrow_n = lax.axis_size("narrow")
    if not (is_pow2(total) and is_pow2(narrow_n)):
        return lax.psum_scatter(
            parts.astype(jnp.bfloat16), ALL, scatter_dimension=0, tiled=False
        ).astype(jnp.float32)
    me = lax.axis_index(ALL)
    nbits = total.bit_length() - 1
    cur = parts.reshape((2,) * nbits + parts.shape[1:])
    axes = list(reversed(range(nbits)))
    for b in reversed(bit_order(total, narrow_n)):
        a = axes.index(b)
        bit = (me >> b) & 1
        mine = lax.dynamic_index_in_dim(cur, bit, axis=a, keepdims=False)
        theirs = lax.dynamic_index_in_dim(cur, 1 - bit, axis=a, keepdims=False)
        got = lax.ppermute(
            theirs.astype(jnp.bfloat16), ALL, [(i, i ^ (1 << b)) for i in range(total)]
        )
        cur = mine + got.astype(jnp.float32)
        axes.pop(a)
    return cur


def narrow_gather(rows):
    n = lax.axis_size("narrow")
    if n != 2:
        return lax.all_gather(rows, "narrow", axis=0, tiled=True)
    other = swapped(rows, "narrow", 0)
    first = lax.axis_index("narrow") == 0
    return jnp.where(first, jnp.concatenate([rows, other]), jnp.concatenate([other, rows]))


def narrow_scatter_sum(part):
    n = lax.axis_size("narrow")
    if n != 2:
        return lax.psum_scatter(
            part.astype(jnp.bfloat16), "narrow", scatter_dimension=0, tiled=True
        ).astype(jnp.float32)
    rows = part.shape[0] // 2
    me = lax.axis_index("narrow")
    mine = lax.dynamic_slice_in_dim(part, me * rows, rows, 0)
    theirs = lax.dynamic_slice_in_dim(part, (1 - me) * rows, rows, 0)
    return mine + swapped(theirs.astype(jnp.bfloat16), "narrow", 0).astype(jnp.float32)


def layer_norm(values, gain_vec, shift_vec):
    center = values - jnp.mean(values, axis=-1, keepdims=True)
    spread = jnp.mean(center * center, axis=-1, keepdims=True)
    return center * lax.rsqrt(spread + layer_eps) * gain_vec + shift_vec


def gelu_exact(values):
    return jax.nn.gelu(values, approximate=False)


def rotary_tables(doc_row):
    places = jnp.arange(doc_row.shape[0], dtype=jnp.int32)
    before = jnp.sum((doc_row[None, :] < doc_row[:, None]).astype(jnp.int32), axis=1)
    position = (places - before).astype(jnp.float32)
    frequency = 10000.0 ** (-2.0 * jnp.arange(HEAD_DIM // 2, dtype=jnp.float32) / HEAD_DIM)
    angles = position[:, None] * frequency[None, :]
    return (jnp.cos(angles), jnp.sin(angles))


def rotate(values, cosine, sine_tab):
    half_dim = values.shape[-1] // 2
    first_half = values[..., :half_dim]
    second = values[..., half_dim:]
    return jnp.concatenate(
        [first_half * cosine - second * sine_tab, second * cosine + first_half * sine_tab], axis=-1
    )


def unrotate(values, cosine, sine_tab):
    half_dim = values.shape[-1] // 2
    first_half = values[..., :half_dim]
    second = values[..., half_dim:]
    return jnp.concatenate(
        [first_half * cosine + second * sine_tab, second * cosine - first_half * sine_tab], axis=-1
    )


def contract_rows(left_op, right_op):
    return lax.dot_general(
        left_op, right_op, (((0,), (0,)), ((), ())), preferred_element_type=jnp.float32
    )


def contract_cols(left_op, right_op):
    return lax.dot_general(
        left_op, right_op, (((1,), (1,)), ((), ())), preferred_element_type=jnp.float32
    )


def score_block(query_rot, key_rot, query_docs, key_docs):
    scores = jnp.einsum(
        "pqhd,pkhd->phqk", query_rot, key_rot, preferred_element_type=jnp.float32
    ) * HEAD_DIM ** (-0.5)
    same_doc = query_docs[:, :, None] == key_docs[:, None, :]
    return jnp.where(same_doc[:, None], scores, masked_score)


def attend(query_rot, key_rot, value_low, query_docs, key_docs):
    scores = score_block(query_rot, key_rot, query_docs, key_docs)
    row_peak = jnp.max(scores, axis=-1, keepdims=True)
    exponent = jnp.exp(scores - row_peak)
    totals = jnp.sum(exponent, axis=-1, keepdims=True)
    probability = (exponent / totals).astype(jnp.bfloat16)
    mixed_out = jnp.einsum(
        "phqk,pkhd->pqhd", probability, value_low, preferred_element_type=jnp.float32
    )
    return (mixed_out, row_peak + jnp.log(totals))


def attend_back(query_rot, key_rot, value_low, query_docs, key_docs, logsum, grad_mixed):
    probability = jnp.exp(score_block(query_rot, key_rot, query_docs, key_docs) - logsum)
    grad_values = jnp.einsum(
        "phqk,pqhd->pkhd",
        probability.astype(jnp.bfloat16),
        grad_mixed,
        preferred_element_type=jnp.float32,
    )
    grad_probs = jnp.einsum(
        "pqhd,pkhd->phqk", grad_mixed, value_low, preferred_element_type=jnp.float32
    )
    inner_sum = jnp.sum(probability * grad_probs, axis=-1, keepdims=True)
    grad_scores = (probability * (grad_probs - inner_sum)).astype(jnp.bfloat16)
    grad_query = jnp.einsum(
        "phqk,pkhd->pqhd", grad_scores, key_rot, preferred_element_type=jnp.float32
    ) * HEAD_DIM ** (-0.5)
    grad_keys = jnp.einsum(
        "phqk,pqhd->pkhd", grad_scores, query_rot, preferred_element_type=jnp.float32
    ) * HEAD_DIM ** (-0.5)
    return (grad_query, grad_keys, grad_values)


def local(
    layer_in,
    doc_ids,
    query_weight,
    query_bias,
    key_weight,
    key_bias,
    value_weight,
    value_bias,
    output_weight,
    output_bias,
    attn_gain,
    attn_shift,
    inner_weight,
    inner_bias,
    outer_weight,
    outer_bias,
    ffn_gain,
    ffn_shift,
    cotangent,
):
    wide_n = lax.axis_size("wide")
    total = wide_n * lax.axis_size("narrow")
    share = query_weight.shape[0]
    small_list = (
        query_bias,
        key_bias,
        value_bias,
        output_bias,
        attn_gain,
        attn_shift,
        outer_bias,
        ffn_gain,
        ffn_shift,
    )
    small = jnp.stack(small_list, axis=1)
    small = jnp.pad(small, ((0, 0), (0, 128 - len(small_list))))
    shard = jnp.concatenate([query_weight, key_weight, value_weight, output_weight, small], axis=1)
    full = gather_all(shard).reshape(total * share, shard.shape[1])
    qkv_full = full[:, : 3 * D]
    output_full = full[:, 3 * D : 4 * D]
    vecs = full[:, 4 * D :].astype(jnp.float32)
    (
        query_offset,
        key_offset,
        value_offset,
        output_offset,
        attn_scale,
        attn_offset,
        outer_offset,
        ffn_scale,
        ffn_offset,
    ) = [vecs[:, i] for i in range(len(small_list))]
    qkv_offset = jnp.concatenate([query_offset, key_offset, value_offset])

    ffn_rows, ffn_cols = inner_weight.shape
    bias_n = inner_bias.shape[0]
    bias_k = -(-bias_n // ffn_rows)
    bias_rows = jnp.pad(inner_bias, (0, ffn_rows * bias_k - bias_n)).reshape(ffn_rows, bias_k)
    ffn_shard = jnp.concatenate([inner_weight, outer_weight.T, bias_rows], axis=1)
    ffn_all = lax.all_gather(ffn_shard, "wide", axis=0, tiled=True)
    inner_cols = ffn_all[:, :ffn_cols]
    outer_cols = ffn_all[:, ffn_cols : 2 * ffn_cols]
    inner_offset = ffn_all[:, 2 * ffn_cols :].reshape(wide_n, ffn_rows * bias_k)[:, :bias_n]
    inner_offset = inner_offset.reshape(-1).astype(jnp.float32)

    rows_dev = layer_in.shape[0]
    half_len = doc_ids.shape[1] // 2
    pack_count = rows_dev // half_len
    narrow_place = lax.axis_index("narrow")
    half_bit = narrow_place % 2
    pair_slot = narrow_place // 2
    pack_docs = lax.dynamic_slice_in_dim(doc_ids, pair_slot * pack_count, pack_count, 0)
    cosine, sine_tab = jax.vmap(rotary_tables)(pack_docs)
    cosine = cosine[:, :, None, :]
    sine_tab = sine_tab[:, :, None, :]
    own_start = half_bit * half_len
    far_start = (1 - half_bit) * half_len
    own_cos = lax.dynamic_slice_in_dim(cosine, own_start, half_len, 1)
    own_sin = lax.dynamic_slice_in_dim(sine_tab, own_start, half_len, 1)
    own_docs = lax.dynamic_slice_in_dim(pack_docs, own_start, half_len, 1)
    far_docs = lax.dynamic_slice_in_dim(pack_docs, far_start, half_len, 1)
    key_docs = jnp.concatenate([own_docs, far_docs], axis=1)

    def heads_of(values):
        return values.reshape(pack_count, half_len, HEADS, HEAD_DIM)

    qkv = jnp.dot(layer_in, qkv_full, preferred_element_type=jnp.float32) + qkv_offset
    query_rot = rotate(heads_of(qkv[:, :D]), own_cos, own_sin).astype(jnp.bfloat16)
    key_rot = rotate(heads_of(qkv[:, D : 2 * D]), own_cos, own_sin).astype(jnp.bfloat16)
    value_low = heads_of(qkv[:, 2 * D :]).astype(jnp.bfloat16)
    far_keys, far_values = swapped((key_rot, value_low), "narrow", 0)
    all_keys = jnp.concatenate([key_rot, far_keys], axis=1)
    all_values = jnp.concatenate([value_low, far_values], axis=1)
    mixed_out, logsum = attend(query_rot, all_keys, all_values, own_docs, key_docs)
    mixed_low = mixed_out.reshape(rows_dev, D).astype(jnp.bfloat16)
    attn_out = jnp.dot(mixed_low, output_full, preferred_element_type=jnp.float32) + output_offset
    res_one = layer_in.astype(jnp.float32) + attn_out
    norm_one, norm_pull = jax.vjp(layer_norm, res_one, attn_scale, attn_offset)
    norm_low = norm_one.astype(jnp.bfloat16)
    group_rows = narrow_gather(norm_low)
    inner_pre = jnp.dot(group_rows, inner_cols, preferred_element_type=jnp.float32) + inner_offset
    act_value, gelu_pull = jax.vjp(gelu_exact, inner_pre)
    act_low = act_value.astype(jnp.bfloat16)
    outer_out = narrow_scatter_sum(contract_cols(act_low, outer_cols)) + outer_offset
    res_two = norm_one + outer_out
    layer_out, ffn_pull = jax.vjp(layer_norm, res_two, ffn_scale, ffn_offset)
    grad_two, ffn_gsum, ffn_ssum = ffn_pull(cotangent.astype(jnp.float32))
    grad_outer = grad_two.astype(jnp.bfloat16)
    outer_bsum = jnp.sum(grad_outer.astype(jnp.float32), axis=0)
    group_grads = narrow_gather(grad_outer)
    grad_act = jnp.dot(group_grads, outer_cols, preferred_element_type=jnp.float32)
    grad_inner = gelu_pull(grad_act)[0].astype(jnp.bfloat16)
    outer_wsum_t = contract_rows(group_grads, act_low)
    inner_wsum = contract_rows(group_rows, grad_inner)
    inner_bsum = jnp.sum(grad_inner.astype(jnp.float32), axis=0)
    grad_part = narrow_scatter_sum(contract_cols(grad_inner, inner_cols))
    bsum_rows = jnp.pad(
        inner_bsum.reshape(wide_n, bias_n), ((0, 0), (0, ffn_rows * bias_k - bias_n))
    ).reshape(wide_n * ffn_rows, bias_k)
    ffn_sums = jnp.concatenate([inner_wsum, outer_wsum_t, bsum_rows], axis=1).astype(jnp.bfloat16)
    ffn_mine = lax.psum_scatter(ffn_sums, "wide", scatter_dimension=0, tiled=True)
    ffn_mine = ffn_mine.astype(jnp.float32)
    inner_wgrad = ffn_mine[:, :ffn_cols]
    outer_wgrad = ffn_mine[:, ffn_cols : 2 * ffn_cols].T
    inner_bgrad = ffn_mine[:, 2 * ffn_cols :].reshape(-1)[:bias_n]

    grad_norm = grad_two + grad_part
    grad_one, attn_gsum, attn_ssum = norm_pull(grad_norm)
    grad_attn = grad_one.astype(jnp.bfloat16)
    output_bsum = jnp.sum(grad_attn.astype(jnp.float32), axis=0)
    output_wsum = contract_rows(mixed_low, grad_attn)
    early_small = jnp.stack(
        [output_bsum, attn_gsum, attn_ssum, outer_bsum, ffn_gsum, ffn_ssum], axis=1
    )
    early = jnp.concatenate(
        [output_wsum.reshape(total, share, D), early_small.reshape(total, share, -1)], axis=2
    )
    early_mine = scatter_sum_all(early)

    grad_mixed = heads_of(contract_cols(grad_attn, output_full).astype(jnp.bfloat16))
    grad_qrot, grad_kall, grad_vall = attend_back(
        query_rot, all_keys, all_values, own_docs, key_docs, logsum, grad_mixed
    )
    back_keys, back_values = swapped(
        (
            grad_kall[:, half_len:].astype(jnp.bfloat16),
            grad_vall[:, half_len:].astype(jnp.bfloat16),
        ),
        "narrow",
        0,
    )
    grad_krot = grad_kall[:, :half_len] + back_keys.astype(jnp.float32)
    grad_values = (grad_vall[:, :half_len] + back_values.astype(jnp.float32)).astype(jnp.bfloat16)
    grad_query = unrotate(grad_qrot, own_cos, own_sin).astype(jnp.bfloat16)
    grad_keys = unrotate(grad_krot, own_cos, own_sin).astype(jnp.bfloat16)
    grad_qkv = jnp.concatenate(
        [
            grad_query.reshape(rows_dev, D),
            grad_keys.reshape(rows_dev, D),
            grad_values.reshape(rows_dev, D),
        ],
        axis=1,
    )
    qkv_wsum = contract_rows(layer_in, grad_qkv)
    qkv_bsum = jnp.sum(grad_qkv.astype(jnp.float32), axis=0).reshape(3, D)
    input_grad = grad_one + contract_cols(grad_qkv, qkv_full)
    late = jnp.concatenate(
        [
            qkv_wsum.reshape(total, share, 3 * D),
            qkv_bsum.T.reshape(total, share, 3),
        ],
        axis=2,
    )
    late_mine = scatter_sum_all(late)
    query_wgrad = late_mine[:, :D]
    key_wgrad = late_mine[:, D : 2 * D]
    value_wgrad = late_mine[:, 2 * D : 3 * D]
    query_bgrad = late_mine[:, 3 * D]
    key_bgrad = late_mine[:, 3 * D + 1]
    value_bgrad = late_mine[:, 3 * D + 2]
    output_wgrad = early_mine[:, :D]
    output_bgrad = early_mine[:, D]
    attn_ggrad = early_mine[:, D + 1]
    attn_sgrad = early_mine[:, D + 2]
    outer_bgrad = early_mine[:, D + 3]
    ffn_ggrad = early_mine[:, D + 4]
    ffn_sgrad = early_mine[:, D + 5]
    return (
        layer_out,
        input_grad,
        query_wgrad,
        query_bgrad,
        key_wgrad,
        key_bgrad,
        value_wgrad,
        value_bgrad,
        output_wgrad,
        output_bgrad,
        attn_ggrad,
        attn_sgrad,
        inner_wgrad,
        inner_bgrad,
        outer_wgrad,
        outer_bgrad,
        ffn_ggrad,
        ffn_sgrad,
    )


def solution(mesh):
    return jax.shard_map(
        local,
        mesh=mesh,
        in_specs=(
            P(("wide", "narrow"), None),
            P("wide", None),
            P(("wide", "narrow"), None),
            P(("wide", "narrow")),
            P(("wide", "narrow"), None),
            P(("wide", "narrow")),
            P(("wide", "narrow"), None),
            P(("wide", "narrow")),
            P(("wide", "narrow"), None),
            P(("wide", "narrow")),
            P(("wide", "narrow")),
            P(("wide", "narrow")),
            P("wide", "narrow"),
            P(("narrow", "wide")),
            P("narrow", "wide"),
            P(("wide", "narrow")),
            P(("wide", "narrow")),
            P(("wide", "narrow")),
            P(("wide", "narrow"), None),
        ),
        out_specs=(
            P(("wide", "narrow"), None),
            P(("wide", "narrow"), None),
            P(("wide", "narrow"), None),
            P(("wide", "narrow")),
            P(("wide", "narrow"), None),
            P(("wide", "narrow")),
            P(("wide", "narrow"), None),
            P(("wide", "narrow")),
            P(("wide", "narrow"), None),
            P(("wide", "narrow")),
            P(("wide", "narrow")),
            P(("wide", "narrow")),
            P("wide", "narrow"),
            P(("narrow", "wide")),
            P("narrow", "wide"),
            P(("wide", "narrow")),
            P(("wide", "narrow")),
            P(("wide", "narrow")),
        ),
        check_vma=False,
    )
```

```python
import jax
import jax.numpy as jnp
from jax import lax
from jax.sharding import PartitionSpec as P

D = 768
HEADS = 12
HEAD_DIM = 64

ALL = ("wide", "narrow")
layer_eps = 1e-12
masked_score = -1e30


def swapped(shard, axis, bit):
    return lax.ppermute(shard, axis, [(i, i ^ 1 << bit) for i in range(lax.axis_size(axis))])


def part_orders(total, narrow_n, parts):
    bits = total.bit_length() - 1
    core_bit = narrow_n.bit_length() - 1
    narrow_bits = list(range(core_bit))
    wide_bits = [b for b in reversed(range(core_bit + 1, bits))]
    orders = []
    for p in range(parts):
        k = p % max(1, len(wide_bits))
        orders.append(narrow_bits + wide_bits[k:] + wide_bits[:k] + [core_bit])
    return orders


def is_pow2(n):
    return n & (n - 1) == 0


def column_splits(cols, parts):
    step = -(-cols // (parts * 128)) * 128
    edges = [min(cols, i * step) for i in range(parts + 1)]
    return [(a, b) for a, b in zip(edges[:-1], edges[1:]) if b > a]


def doubling_gather(shard, order, total):
    me = lax.axis_index(ALL)
    cur = shard
    for b in order:
        other = lax.ppermute(cur, ALL, [(i, i ^ (1 << b)) for i in range(total)])
        bit = (me >> b) & 1
        pick = (jnp.arange(2) == bit).reshape((2,) + (1,) * cur.ndim)
        cur = jnp.where(pick, cur[None], other[None])
    k = len(order)
    perm = [k - 1 - order.index(b) for b in reversed(range(k))]
    cur = cur.transpose(perm + list(range(k, cur.ndim)))
    return cur.reshape((total,) + shard.shape)


def gather_all(shard, parts=3):
    total = lax.axis_size("wide") * lax.axis_size("narrow")
    narrow_n = lax.axis_size("narrow")
    if not (is_pow2(total) and is_pow2(narrow_n)):
        return lax.all_gather(shard, ALL, axis=0, tiled=False)
    splits = column_splits(shard.shape[-1], parts)
    orders = part_orders(total, narrow_n, len(splits))
    pieces = [
        doubling_gather(shard[..., a:b], order, total) for (a, b), order in zip(splits, orders)
    ]
    return jnp.concatenate(pieces, axis=-1)


def halving_scatter(parts_in, order, total):
    me = lax.axis_index(ALL)
    nbits = total.bit_length() - 1
    cur = parts_in.reshape((2,) * nbits + parts_in.shape[1:])
    axes = list(reversed(range(nbits)))
    for b in order:
        a = axes.index(b)
        bit = (me >> b) & 1
        mine = lax.dynamic_index_in_dim(cur, bit, axis=a, keepdims=False)
        theirs = lax.dynamic_index_in_dim(cur, 1 - bit, axis=a, keepdims=False)
        got = lax.ppermute(
            theirs.astype(jnp.bfloat16), ALL, [(i, i ^ (1 << b)) for i in range(total)]
        )
        cur = mine + got.astype(jnp.float32)
        axes.pop(a)
    return cur


def scatter_sum_all(parts_in, parts=3):
    total = lax.axis_size("wide") * lax.axis_size("narrow")
    narrow_n = lax.axis_size("narrow")
    if not (is_pow2(total) and is_pow2(narrow_n)):
        return lax.psum_scatter(
            parts_in.astype(jnp.bfloat16), ALL, scatter_dimension=0, tiled=False
        ).astype(jnp.float32)
    splits = column_splits(parts_in.shape[-1], parts)
    orders = part_orders(total, narrow_n, len(splits))
    pieces = [
        halving_scatter(parts_in[..., a:b], list(reversed(order)), total)
        for (a, b), order in zip(splits, orders)
    ]
    return jnp.concatenate(pieces, axis=-1)


def narrow_gather(rows):
    n = lax.axis_size("narrow")
    if n != 2:
        return lax.all_gather(rows, "narrow", axis=0, tiled=True)
    other = swapped(rows, "narrow", 0)
    first = lax.axis_index("narrow") == 0
    return jnp.where(first, jnp.concatenate([rows, other]), jnp.concatenate([other, rows]))


def narrow_scatter_sum(part):
    n = lax.axis_size("narrow")
    if n != 2:
        return lax.psum_scatter(
            part.astype(jnp.bfloat16), "narrow", scatter_dimension=0, tiled=True
        ).astype(jnp.float32)
    rows = part.shape[0] // 2
    me = lax.axis_index("narrow")
    mine = lax.dynamic_slice_in_dim(part, me * rows, rows, 0)
    theirs = lax.dynamic_slice_in_dim(part, (1 - me) * rows, rows, 0)
    return mine + swapped(theirs.astype(jnp.bfloat16), "narrow", 0).astype(jnp.float32)


def layer_norm(values, gain_vec, shift_vec):
    center = values - jnp.mean(values, axis=-1, keepdims=True)
    spread = jnp.mean(center * center, axis=-1, keepdims=True)
    return center * lax.rsqrt(spread + layer_eps) * gain_vec + shift_vec


def gelu_exact(values):
    return jax.nn.gelu(values, approximate=False)


def rotary_tables(doc_row):
    places = jnp.arange(doc_row.shape[0], dtype=jnp.int32)
    before = jnp.sum((doc_row[None, :] < doc_row[:, None]).astype(jnp.int32), axis=1)
    position = (places - before).astype(jnp.float32)
    frequency = 10000.0 ** (-2.0 * jnp.arange(HEAD_DIM // 2, dtype=jnp.float32) / HEAD_DIM)
    angles = position[:, None] * frequency[None, :]
    return (jnp.cos(angles), jnp.sin(angles))


def rotate(values, cosine, sine_tab):
    half_dim = values.shape[-1] // 2
    first_half = values[..., :half_dim]
    second = values[..., half_dim:]
    return jnp.concatenate(
        [first_half * cosine - second * sine_tab, second * cosine + first_half * sine_tab], axis=-1
    )


def unrotate(values, cosine, sine_tab):
    half_dim = values.shape[-1] // 2
    first_half = values[..., :half_dim]
    second = values[..., half_dim:]
    return jnp.concatenate(
        [first_half * cosine + second * sine_tab, second * cosine - first_half * sine_tab], axis=-1
    )


def contract_rows(left_op, right_op):
    return lax.dot_general(
        left_op, right_op, (((0,), (0,)), ((), ())), preferred_element_type=jnp.float32
    )


def contract_cols(left_op, right_op):
    return lax.dot_general(
        left_op, right_op, (((1,), (1,)), ((), ())), preferred_element_type=jnp.float32
    )


def score_block(query_rot, key_rot, query_docs, key_docs):
    scores = jnp.einsum(
        "pqhd,pkhd->phqk", query_rot, key_rot, preferred_element_type=jnp.float32
    ) * HEAD_DIM ** (-0.5)
    same_doc = query_docs[:, :, None] == key_docs[:, None, :]
    return jnp.where(same_doc[:, None], scores, masked_score)


def attend(query_rot, key_rot, value_low, query_docs, key_docs):
    scores = score_block(query_rot, key_rot, query_docs, key_docs)
    row_peak = jnp.max(scores, axis=-1, keepdims=True)
    exponent = jnp.exp(scores - row_peak)
    totals = jnp.sum(exponent, axis=-1, keepdims=True)
    probability = (exponent / totals).astype(jnp.bfloat16)
    mixed_out = jnp.einsum(
        "phqk,pkhd->pqhd", probability, value_low, preferred_element_type=jnp.float32
    )
    return (mixed_out, row_peak + jnp.log(totals))


def attend_back(query_rot, key_rot, value_low, query_docs, key_docs, logsum, grad_mixed):
    probability = jnp.exp(score_block(query_rot, key_rot, query_docs, key_docs) - logsum)
    grad_values = jnp.einsum(
        "phqk,pqhd->pkhd",
        probability.astype(jnp.bfloat16),
        grad_mixed,
        preferred_element_type=jnp.float32,
    )
    grad_probs = jnp.einsum(
        "pqhd,pkhd->phqk", grad_mixed, value_low, preferred_element_type=jnp.float32
    )
    inner_sum = jnp.sum(probability * grad_probs, axis=-1, keepdims=True)
    grad_scores = (probability * (grad_probs - inner_sum)).astype(jnp.bfloat16)
    grad_query = jnp.einsum(
        "phqk,pkhd->pqhd", grad_scores, key_rot, preferred_element_type=jnp.float32
    ) * HEAD_DIM ** (-0.5)
    grad_keys = jnp.einsum(
        "phqk,pqhd->pkhd", grad_scores, query_rot, preferred_element_type=jnp.float32
    ) * HEAD_DIM ** (-0.5)
    return (grad_query, grad_keys, grad_values)


def ffn_forward(rows, inner_cols, inner_offset, outer_cols):
    inner_pre = jnp.dot(rows, inner_cols, preferred_element_type=jnp.float32) + inner_offset
    act_value, gelu_pull = jax.vjp(gelu_exact, inner_pre)
    act_low = act_value.astype(jnp.bfloat16)
    return act_low, gelu_pull, contract_cols(act_low, outer_cols)


def ffn_backward(grads, gelu_pull, inner_cols, outer_cols):
    grad_act = jnp.dot(grads, outer_cols, preferred_element_type=jnp.float32)
    grad_inner = gelu_pull(grad_act)[0].astype(jnp.bfloat16)
    return grad_inner, contract_cols(grad_inner, inner_cols)


def local(
    layer_in,
    doc_ids,
    query_weight,
    query_bias,
    key_weight,
    key_bias,
    value_weight,
    value_bias,
    output_weight,
    output_bias,
    attn_gain,
    attn_shift,
    inner_weight,
    inner_bias,
    outer_weight,
    outer_bias,
    ffn_gain,
    ffn_shift,
    cotangent,
):
    wide_n = lax.axis_size("wide")
    narrow_n = lax.axis_size("narrow")
    total = wide_n * narrow_n
    share = query_weight.shape[0]
    small_list = (
        query_bias,
        key_bias,
        value_bias,
        output_bias,
        attn_gain,
        attn_shift,
        outer_bias,
        ffn_gain,
        ffn_shift,
    )
    small = jnp.stack(small_list, axis=1)
    small = jnp.pad(small, ((0, 0), (0, 128 - len(small_list))))
    shard = jnp.concatenate([query_weight, key_weight, value_weight, output_weight, small], axis=1)
    full = gather_all(shard).reshape(total * share, shard.shape[1])
    qkv_full = full[:, : 3 * D]
    output_full = full[:, 3 * D : 4 * D]
    vecs = full[:, 4 * D :].astype(jnp.float32)
    (
        query_offset,
        key_offset,
        value_offset,
        output_offset,
        attn_scale,
        attn_offset,
        outer_offset,
        ffn_scale,
        ffn_offset,
    ) = [vecs[:, i] for i in range(len(small_list))]
    qkv_offset = jnp.concatenate([query_offset, key_offset, value_offset])

    ffn_rows, ffn_cols = inner_weight.shape
    bias_n = inner_bias.shape[0]
    bias_k = -(-bias_n // ffn_rows)
    bias_rows = jnp.pad(inner_bias, (0, ffn_rows * bias_k - bias_n)).reshape(ffn_rows, bias_k)
    ffn_shard = jnp.concatenate([inner_weight, outer_weight.T, bias_rows], axis=1)
    ffn_all = lax.all_gather(ffn_shard, "wide", axis=0, tiled=True)
    inner_cols = ffn_all[:, :ffn_cols]
    outer_cols = ffn_all[:, ffn_cols : 2 * ffn_cols]
    inner_offset = ffn_all[:, 2 * ffn_cols :].reshape(wide_n, ffn_rows * bias_k)[:, :bias_n]
    inner_offset = inner_offset.reshape(-1).astype(jnp.float32)

    rows_dev = layer_in.shape[0]
    half_len = doc_ids.shape[1] // 2
    pack_count = rows_dev // half_len
    narrow_place = lax.axis_index("narrow")
    half_bit = narrow_place % 2
    pair_slot = narrow_place // 2
    pack_docs = lax.dynamic_slice_in_dim(doc_ids, pair_slot * pack_count, pack_count, 0)
    cosine, sine_tab = jax.vmap(rotary_tables)(pack_docs)
    cosine = cosine[:, :, None, :]
    sine_tab = sine_tab[:, :, None, :]
    own_start = half_bit * half_len
    far_start = (1 - half_bit) * half_len
    own_cos = lax.dynamic_slice_in_dim(cosine, own_start, half_len, 1)
    own_sin = lax.dynamic_slice_in_dim(sine_tab, own_start, half_len, 1)
    own_docs = lax.dynamic_slice_in_dim(pack_docs, own_start, half_len, 1)
    far_docs = lax.dynamic_slice_in_dim(pack_docs, far_start, half_len, 1)
    key_docs = jnp.concatenate([own_docs, far_docs], axis=1)

    def heads_of(values):
        return values.reshape(pack_count, half_len, HEADS, HEAD_DIM)

    qkv = jnp.dot(layer_in, qkv_full, preferred_element_type=jnp.float32) + qkv_offset
    query_rot = rotate(heads_of(qkv[:, :D]), own_cos, own_sin).astype(jnp.bfloat16)
    key_rot = rotate(heads_of(qkv[:, D : 2 * D]), own_cos, own_sin).astype(jnp.bfloat16)
    value_low = heads_of(qkv[:, 2 * D :]).astype(jnp.bfloat16)
    far_keys, far_values = swapped((key_rot, value_low), "narrow", 0)
    all_keys = jnp.concatenate([key_rot, far_keys], axis=1)
    all_values = jnp.concatenate([value_low, far_values], axis=1)
    mixed_out, logsum = attend(query_rot, all_keys, all_values, own_docs, key_docs)
    mixed_low = mixed_out.reshape(rows_dev, D).astype(jnp.bfloat16)
    attn_out = jnp.dot(mixed_low, output_full, preferred_element_type=jnp.float32) + output_offset
    res_one = layer_in.astype(jnp.float32) + attn_out
    norm_one, norm_pull = jax.vjp(layer_norm, res_one, attn_scale, attn_offset)
    norm_low = norm_one.astype(jnp.bfloat16)

    if narrow_n == 2:
        far_rows = swapped(norm_low, "narrow", 0)
        own_act, own_pull, own_part = ffn_forward(norm_low, inner_cols, inner_offset, outer_cols)
        far_act, far_pull, far_part = ffn_forward(far_rows, inner_cols, inner_offset, outer_cols)
        outer_sum = own_part + swapped(far_part.astype(jnp.bfloat16), "narrow", 0).astype(
            jnp.float32
        )
    else:
        group_rows = lax.all_gather(norm_low, "narrow", axis=0, tiled=True)
        all_act, all_pull, all_part = ffn_forward(group_rows, inner_cols, inner_offset, outer_cols)
        outer_sum = narrow_scatter_sum(all_part)
    outer_out = outer_sum + outer_offset
    res_two = norm_one + outer_out
    layer_out, ffn_pull = jax.vjp(layer_norm, res_two, ffn_scale, ffn_offset)
    grad_two, ffn_gsum, ffn_ssum = ffn_pull(cotangent.astype(jnp.float32))
    grad_outer = grad_two.astype(jnp.bfloat16)
    outer_bsum = jnp.sum(grad_outer.astype(jnp.float32), axis=0)
    if narrow_n == 2:
        far_grads = swapped(grad_outer, "narrow", 0)
        own_inner, own_back = ffn_backward(grad_outer, own_pull, inner_cols, outer_cols)
        far_inner, far_back = ffn_backward(far_grads, far_pull, inner_cols, outer_cols)
        grad_part = own_back + swapped(far_back.astype(jnp.bfloat16), "narrow", 0).astype(
            jnp.float32
        )
        outer_wsum_t = contract_rows(grad_outer, own_act) + contract_rows(far_grads, far_act)
        inner_wsum = contract_rows(norm_low, own_inner) + contract_rows(far_rows, far_inner)
        inner_bsum = jnp.sum(own_inner.astype(jnp.float32), axis=0) + jnp.sum(
            far_inner.astype(jnp.float32), axis=0
        )
    else:
        group_grads = lax.all_gather(grad_outer, "narrow", axis=0, tiled=True)
        all_inner, all_back = ffn_backward(group_grads, all_pull, inner_cols, outer_cols)
        grad_part = narrow_scatter_sum(all_back)
        outer_wsum_t = contract_rows(group_grads, all_act)
        inner_wsum = contract_rows(group_rows, all_inner)
        inner_bsum = jnp.sum(all_inner.astype(jnp.float32), axis=0)
    bsum_rows = jnp.pad(
        inner_bsum.reshape(wide_n, bias_n), ((0, 0), (0, ffn_rows * bias_k - bias_n))
    ).reshape(wide_n * ffn_rows, bias_k)
    ffn_sums = jnp.concatenate([inner_wsum, outer_wsum_t, bsum_rows], axis=1).astype(jnp.bfloat16)
    ffn_mine = lax.psum_scatter(ffn_sums, "wide", scatter_dimension=0, tiled=True)
    ffn_mine = ffn_mine.astype(jnp.float32)
    inner_wgrad = ffn_mine[:, :ffn_cols]
    outer_wgrad = ffn_mine[:, ffn_cols : 2 * ffn_cols].T
    inner_bgrad = ffn_mine[:, 2 * ffn_cols :].reshape(-1)[:bias_n]

    grad_norm = grad_two + grad_part
    grad_one, attn_gsum, attn_ssum = norm_pull(grad_norm)
    grad_attn = grad_one.astype(jnp.bfloat16)
    output_bsum = jnp.sum(grad_attn.astype(jnp.float32), axis=0)
    output_wsum = contract_rows(mixed_low, grad_attn)
    early_small = jnp.stack(
        [output_bsum, attn_gsum, attn_ssum, outer_bsum, ffn_gsum, ffn_ssum], axis=1
    )
    early = jnp.concatenate(
        [output_wsum.reshape(total, share, D), early_small.reshape(total, share, -1)], axis=2
    )
    early_mine = scatter_sum_all(early)

    grad_mixed = heads_of(contract_cols(grad_attn, output_full).astype(jnp.bfloat16))
    grad_qrot, grad_kall, grad_vall = attend_back(
        query_rot, all_keys, all_values, own_docs, key_docs, logsum, grad_mixed
    )
    back_keys, back_values = swapped(
        (
            grad_kall[:, half_len:].astype(jnp.bfloat16),
            grad_vall[:, half_len:].astype(jnp.bfloat16),
        ),
        "narrow",
        0,
    )
    grad_krot = grad_kall[:, :half_len] + back_keys.astype(jnp.float32)
    grad_values = (grad_vall[:, :half_len] + back_values.astype(jnp.float32)).astype(jnp.bfloat16)
    grad_query = unrotate(grad_qrot, own_cos, own_sin).astype(jnp.bfloat16)
    grad_keys = unrotate(grad_krot, own_cos, own_sin).astype(jnp.bfloat16)
    grad_qkv = jnp.concatenate(
        [
            grad_query.reshape(rows_dev, D),
            grad_keys.reshape(rows_dev, D),
            grad_values.reshape(rows_dev, D),
        ],
        axis=1,
    )
    qkv_wsum = contract_rows(layer_in, grad_qkv)
    qkv_bsum = jnp.sum(grad_qkv.astype(jnp.float32), axis=0).reshape(3, D)
    input_grad = grad_one + contract_cols(grad_qkv, qkv_full)
    late = jnp.concatenate(
        [
            qkv_wsum.reshape(total, share, 3 * D),
            qkv_bsum.T.reshape(total, share, 3),
        ],
        axis=2,
    )
    late_mine = scatter_sum_all(late)
    query_wgrad = late_mine[:, :D]
    key_wgrad = late_mine[:, D : 2 * D]
    value_wgrad = late_mine[:, 2 * D : 3 * D]
    query_bgrad = late_mine[:, 3 * D]
    key_bgrad = late_mine[:, 3 * D + 1]
    value_bgrad = late_mine[:, 3 * D + 2]
    output_wgrad = early_mine[:, :D]
    output_bgrad = early_mine[:, D]
    attn_ggrad = early_mine[:, D + 1]
    attn_sgrad = early_mine[:, D + 2]
    outer_bgrad = early_mine[:, D + 3]
    ffn_ggrad = early_mine[:, D + 4]
    ffn_sgrad = early_mine[:, D + 5]
    return (
        layer_out,
        input_grad,
        query_wgrad,
        query_bgrad,
        key_wgrad,
        key_bgrad,
        value_wgrad,
        value_bgrad,
        output_wgrad,
        output_bgrad,
        attn_ggrad,
        attn_sgrad,
        inner_wgrad,
        inner_bgrad,
        outer_wgrad,
        outer_bgrad,
        ffn_ggrad,
        ffn_sgrad,
    )


def solution(mesh):
    return jax.shard_map(
        local,
        mesh=mesh,
        in_specs=(
            P(("wide", "narrow"), None),
            P("wide", None),
            P(("wide", "narrow"), None),
            P(("wide", "narrow")),
            P(("wide", "narrow"), None),
            P(("wide", "narrow")),
            P(("wide", "narrow"), None),
            P(("wide", "narrow")),
            P(("wide", "narrow"), None),
            P(("wide", "narrow")),
            P(("wide", "narrow")),
            P(("wide", "narrow")),
            P("wide", "narrow"),
            P(("narrow", "wide")),
            P("narrow", "wide"),
            P(("wide", "narrow")),
            P(("wide", "narrow")),
            P(("wide", "narrow")),
            P(("wide", "narrow"), None),
        ),
        out_specs=(
            P(("wide", "narrow"), None),
            P(("wide", "narrow"), None),
            P(("wide", "narrow"), None),
            P(("wide", "narrow")),
            P(("wide", "narrow"), None),
            P(("wide", "narrow")),
            P(("wide", "narrow"), None),
            P(("wide", "narrow")),
            P(("wide", "narrow"), None),
            P(("wide", "narrow")),
            P(("wide", "narrow")),
            P(("wide", "narrow")),
            P("wide", "narrow"),
            P(("narrow", "wide")),
            P("narrow", "wide"),
            P(("wide", "narrow")),
            P(("wide", "narrow")),
            P(("wide", "narrow")),
        ),
        check_vma=False,
    )
```

```python
import jax
import jax.numpy as jnp
from jax import lax
from jax.sharding import PartitionSpec as P

D = 768
HEADS = 12
HEAD_DIM = 64

ALL = ("wide", "narrow")
layer_eps = 1e-12
masked_score = -1e30


def swapped(shard, axis, bit):
    return lax.ppermute(shard, axis, [(i, i ^ 1 << bit) for i in range(lax.axis_size(axis))])


def part_orders(total, narrow_n, parts):
    bits = total.bit_length() - 1
    core_bit = narrow_n.bit_length() - 1
    narrow_bits = list(range(core_bit))
    wide_bits = [b for b in reversed(range(core_bit + 1, bits))]
    orders = []
    for p in range(parts):
        k = p % max(1, len(wide_bits))
        orders.append(narrow_bits + wide_bits[k:] + wide_bits[:k] + [core_bit])
    return orders


def is_pow2(n):
    return n & (n - 1) == 0


def column_splits(cols, parts):
    tiles = -(-cols // 128)
    parts = max(1, min(parts, tiles))
    edges = [min(cols, (tiles * i // parts) * 128) for i in range(parts)] + [cols]
    return [(a, b) for a, b in zip(edges[:-1], edges[1:]) if b > a]


def doubling_gather(shard, order, total):
    me = lax.axis_index(ALL)
    cur = shard
    for b in order:
        other = lax.ppermute(cur, ALL, [(i, i ^ (1 << b)) for i in range(total)])
        bit = (me >> b) & 1
        pick = (jnp.arange(2) == bit).reshape((2,) + (1,) * cur.ndim)
        cur = jnp.where(pick, cur[None], other[None])
    k = len(order)
    perm = [k - 1 - order.index(b) for b in reversed(range(k))]
    cur = cur.transpose(perm + list(range(k, cur.ndim)))
    return cur.reshape((total,) + shard.shape)


def gather_all(shard, parts=3):
    total = lax.axis_size("wide") * lax.axis_size("narrow")
    narrow_n = lax.axis_size("narrow")
    if not (is_pow2(total) and is_pow2(narrow_n)):
        return lax.all_gather(shard, ALL, axis=0, tiled=False)
    splits = column_splits(shard.shape[-1], parts)
    orders = part_orders(total, narrow_n, len(splits))
    pieces = [
        doubling_gather(shard[..., a:b], order, total) for (a, b), order in zip(splits, orders)
    ]
    return jnp.concatenate(pieces, axis=-1)


def halving_scatter(parts_in, order, total):
    me = lax.axis_index(ALL)
    nbits = total.bit_length() - 1
    cur = parts_in.reshape((2,) * nbits + parts_in.shape[1:])
    axes = list(reversed(range(nbits)))
    for b in order:
        a = axes.index(b)
        bit = (me >> b) & 1
        mine = lax.dynamic_index_in_dim(cur, bit, axis=a, keepdims=False)
        theirs = lax.dynamic_index_in_dim(cur, 1 - bit, axis=a, keepdims=False)
        got = lax.ppermute(
            theirs.astype(jnp.bfloat16), ALL, [(i, i ^ (1 << b)) for i in range(total)]
        )
        cur = mine + got.astype(jnp.float32)
        axes.pop(a)
    return cur


def scatter_sum_all(parts_in, parts=3):
    total = lax.axis_size("wide") * lax.axis_size("narrow")
    narrow_n = lax.axis_size("narrow")
    if not (is_pow2(total) and is_pow2(narrow_n)):
        return lax.psum_scatter(
            parts_in.astype(jnp.bfloat16), ALL, scatter_dimension=0, tiled=False
        ).astype(jnp.float32)
    splits = column_splits(parts_in.shape[-1], parts)
    orders = part_orders(total, narrow_n, len(splits))
    pieces = [
        halving_scatter(parts_in[..., a:b], list(reversed(order)), total)
        for (a, b), order in zip(splits, orders)
    ]
    return jnp.concatenate(pieces, axis=-1)


def narrow_gather(rows):
    n = lax.axis_size("narrow")
    if n != 2:
        return lax.all_gather(rows, "narrow", axis=0, tiled=True)
    other = swapped(rows, "narrow", 0)
    first = lax.axis_index("narrow") == 0
    return jnp.where(first, jnp.concatenate([rows, other]), jnp.concatenate([other, rows]))


def narrow_scatter_sum(part):
    n = lax.axis_size("narrow")
    if n != 2:
        return lax.psum_scatter(
            part.astype(jnp.bfloat16), "narrow", scatter_dimension=0, tiled=True
        ).astype(jnp.float32)
    rows = part.shape[0] // 2
    me = lax.axis_index("narrow")
    mine = lax.dynamic_slice_in_dim(part, me * rows, rows, 0)
    theirs = lax.dynamic_slice_in_dim(part, (1 - me) * rows, rows, 0)
    return mine + swapped(theirs.astype(jnp.bfloat16), "narrow", 0).astype(jnp.float32)


def narrow_sum_rows(blocks):
    n = lax.axis_size("narrow")
    me = lax.axis_index("narrow")
    if n != 2:
        return lax.psum_scatter(
            blocks.astype(jnp.bfloat16), "narrow", scatter_dimension=0, tiled=False
        ).astype(jnp.float32)
    mine = lax.dynamic_index_in_dim(blocks, me, axis=0, keepdims=False)
    theirs = lax.dynamic_index_in_dim(blocks, 1 - me, axis=0, keepdims=False)
    return mine + swapped(theirs.astype(jnp.bfloat16), "narrow", 0).astype(jnp.float32)


def layer_norm(values, gain_vec, shift_vec):
    center = values - jnp.mean(values, axis=-1, keepdims=True)
    spread = jnp.mean(center * center, axis=-1, keepdims=True)
    return center * lax.rsqrt(spread + layer_eps) * gain_vec + shift_vec


def gelu_exact(values):
    return jax.nn.gelu(values, approximate=False)


def rotary_tables(doc_row):
    places = jnp.arange(doc_row.shape[0], dtype=jnp.int32)
    before = jnp.sum((doc_row[None, :] < doc_row[:, None]).astype(jnp.int32), axis=1)
    position = (places - before).astype(jnp.float32)
    frequency = 10000.0 ** (-2.0 * jnp.arange(HEAD_DIM // 2, dtype=jnp.float32) / HEAD_DIM)
    angles = position[:, None] * frequency[None, :]
    return (jnp.cos(angles), jnp.sin(angles))


def rotate(values, cosine, sine_tab):
    half_dim = values.shape[-1] // 2
    first_half = values[..., :half_dim]
    second = values[..., half_dim:]
    return jnp.concatenate(
        [first_half * cosine - second * sine_tab, second * cosine + first_half * sine_tab], axis=-1
    )


def unrotate(values, cosine, sine_tab):
    half_dim = values.shape[-1] // 2
    first_half = values[..., :half_dim]
    second = values[..., half_dim:]
    return jnp.concatenate(
        [first_half * cosine + second * sine_tab, second * cosine - first_half * sine_tab], axis=-1
    )


def contract_rows(left_op, right_op):
    return lax.dot_general(
        left_op, right_op, (((0,), (0,)), ((), ())), preferred_element_type=jnp.float32
    )


def contract_cols(left_op, right_op):
    return lax.dot_general(
        left_op, right_op, (((1,), (1,)), ((), ())), preferred_element_type=jnp.float32
    )


def score_block(query_rot, key_rot, query_docs, key_docs):
    scores = jnp.einsum(
        "pqhd,pkhd->phqk", query_rot, key_rot, preferred_element_type=jnp.float32
    ) * HEAD_DIM ** (-0.5)
    same_doc = query_docs[:, :, None] == key_docs[:, None, :]
    return jnp.where(same_doc[:, None], scores, masked_score)


def attend(query_rot, key_rot, value_low, query_docs, key_docs):
    scores = score_block(query_rot, key_rot, query_docs, key_docs)
    row_peak = jnp.max(scores, axis=-1, keepdims=True)
    exponent = jnp.exp(scores - row_peak)
    totals = jnp.sum(exponent, axis=-1, keepdims=True)
    probability = (exponent / totals).astype(jnp.bfloat16)
    mixed_out = jnp.einsum(
        "phqk,pkhd->pqhd", probability, value_low, preferred_element_type=jnp.float32
    )
    return (mixed_out, row_peak + jnp.log(totals))


def attend_back(query_rot, key_rot, value_low, query_docs, key_docs, logsum, grad_mixed):
    probability = jnp.exp(score_block(query_rot, key_rot, query_docs, key_docs) - logsum)
    grad_values = jnp.einsum(
        "phqk,pqhd->pkhd",
        probability.astype(jnp.bfloat16),
        grad_mixed,
        preferred_element_type=jnp.float32,
    )
    grad_probs = jnp.einsum(
        "pqhd,pkhd->phqk", grad_mixed, value_low, preferred_element_type=jnp.float32
    )
    inner_sum = jnp.sum(probability * grad_probs, axis=-1, keepdims=True)
    grad_scores = (probability * (grad_probs - inner_sum)).astype(jnp.bfloat16)
    grad_query = jnp.einsum(
        "phqk,pkhd->pqhd", grad_scores, key_rot, preferred_element_type=jnp.float32
    ) * HEAD_DIM ** (-0.5)
    grad_keys = jnp.einsum(
        "phqk,pqhd->pkhd", grad_scores, query_rot, preferred_element_type=jnp.float32
    ) * HEAD_DIM ** (-0.5)
    return (grad_query, grad_keys, grad_values)


def ffn_forward(rows, inner_cols, inner_offset, outer_cols):
    inner_pre = jnp.dot(rows, inner_cols, preferred_element_type=jnp.float32) + inner_offset
    act_value, gelu_pull = jax.vjp(gelu_exact, inner_pre)
    act_low = act_value.astype(jnp.bfloat16)
    return act_low, gelu_pull, contract_cols(act_low, outer_cols)


def ffn_backward(grads, gelu_pull, inner_cols, outer_cols):
    grad_act = jnp.dot(grads, outer_cols, preferred_element_type=jnp.float32)
    grad_inner = gelu_pull(grad_act)[0].astype(jnp.bfloat16)
    return grad_inner, contract_cols(grad_inner, inner_cols)


def local(
    layer_in,
    doc_ids,
    query_weight,
    query_bias,
    key_weight,
    key_bias,
    value_weight,
    value_bias,
    output_weight,
    output_bias,
    attn_gain,
    attn_shift,
    inner_weight,
    inner_bias,
    outer_weight,
    outer_bias,
    ffn_gain,
    ffn_shift,
    cotangent,
):
    wide_n = lax.axis_size("wide")
    narrow_n = lax.axis_size("narrow")
    total = wide_n * narrow_n
    share = query_weight.shape[0]
    small_list = (
        query_bias,
        key_bias,
        value_bias,
        output_bias,
        attn_gain,
        attn_shift,
        outer_bias,
        ffn_gain,
        ffn_shift,
    )
    small = jnp.stack(small_list, axis=1)
    small = jnp.pad(small, ((0, 0), (0, 128 - len(small_list))))
    shard = jnp.concatenate([query_weight, key_weight, value_weight, output_weight, small], axis=1)
    full = gather_all(shard).reshape(total * share, shard.shape[1])
    qkv_full = full[:, : 3 * D]
    output_full = full[:, 3 * D : 4 * D]
    vecs = full[:, 4 * D :].astype(jnp.float32)
    (
        query_offset,
        key_offset,
        value_offset,
        output_offset,
        attn_scale,
        attn_offset,
        outer_offset,
        ffn_scale,
        ffn_offset,
    ) = [vecs[:, i] for i in range(len(small_list))]
    qkv_offset = jnp.concatenate([query_offset, key_offset, value_offset])

    ffn_rows, ffn_cols = inner_weight.shape
    bias_n = inner_bias.shape[0]
    bias_k = -(-bias_n // ffn_rows)
    bias_rows = jnp.pad(inner_bias, (0, ffn_rows * bias_k - bias_n)).reshape(ffn_rows, bias_k)
    ffn_shard = jnp.concatenate([inner_weight, outer_weight.T, bias_rows], axis=1)
    ffn_all = lax.all_gather(ffn_shard, "wide", axis=0, tiled=True)
    inner_cols = ffn_all[:, :ffn_cols]
    outer_cols = ffn_all[:, ffn_cols : 2 * ffn_cols]
    inner_offset = ffn_all[:, 2 * ffn_cols :].reshape(wide_n, ffn_rows * bias_k)[:, :bias_n]
    inner_offset = inner_offset.reshape(-1).astype(jnp.float32)

    rows_dev = layer_in.shape[0]
    half_len = doc_ids.shape[1] // 2
    pack_count = rows_dev // half_len
    narrow_place = lax.axis_index("narrow")
    half_bit = narrow_place % 2
    pair_slot = narrow_place // 2
    pack_docs = lax.dynamic_slice_in_dim(doc_ids, pair_slot * pack_count, pack_count, 0)
    cosine, sine_tab = jax.vmap(rotary_tables)(pack_docs)
    cosine = cosine[:, :, None, :]
    sine_tab = sine_tab[:, :, None, :]
    own_start = half_bit * half_len
    far_start = (1 - half_bit) * half_len
    own_cos = lax.dynamic_slice_in_dim(cosine, own_start, half_len, 1)
    own_sin = lax.dynamic_slice_in_dim(sine_tab, own_start, half_len, 1)
    own_docs = lax.dynamic_slice_in_dim(pack_docs, own_start, half_len, 1)
    far_docs = lax.dynamic_slice_in_dim(pack_docs, far_start, half_len, 1)
    key_docs = jnp.concatenate([own_docs, far_docs], axis=1)

    def heads_of(values):
        return values.reshape(pack_count, half_len, HEADS, HEAD_DIM)

    qkv = jnp.dot(layer_in, qkv_full, preferred_element_type=jnp.float32) + qkv_offset
    query_rot = rotate(heads_of(qkv[:, :D]), own_cos, own_sin).astype(jnp.bfloat16)
    key_rot = rotate(heads_of(qkv[:, D : 2 * D]), own_cos, own_sin).astype(jnp.bfloat16)
    value_low = heads_of(qkv[:, 2 * D :]).astype(jnp.bfloat16)
    far_keys, far_values = swapped((key_rot, value_low), "narrow", 0)
    all_keys = jnp.concatenate([key_rot, far_keys], axis=1)
    all_values = jnp.concatenate([value_low, far_values], axis=1)
    mixed_out, logsum = attend(query_rot, all_keys, all_values, own_docs, key_docs)
    mixed_low = mixed_out.reshape(rows_dev, D).astype(jnp.bfloat16)
    attn_out = jnp.dot(mixed_low, output_full, preferred_element_type=jnp.float32) + output_offset
    res_one = layer_in.astype(jnp.float32) + attn_out
    norm_one, norm_pull = jax.vjp(layer_norm, res_one, attn_scale, attn_offset)
    norm_low = norm_one.astype(jnp.bfloat16)

    if narrow_n == 2:
        far_rows = swapped(norm_low, "narrow", 0)
        own_act, own_pull, own_part = ffn_forward(norm_low, inner_cols, inner_offset, outer_cols)
        own_act, own_part, far_rows = lax.optimization_barrier((own_act, own_part, far_rows))
        far_act, far_pull, far_part = ffn_forward(far_rows, inner_cols, inner_offset, outer_cols)
        outer_sum = own_part + swapped(far_part.astype(jnp.bfloat16), "narrow", 0).astype(
            jnp.float32
        )
    else:
        group_rows = lax.all_gather(norm_low, "narrow", axis=0, tiled=True)
        all_act, all_pull, all_part = ffn_forward(group_rows, inner_cols, inner_offset, outer_cols)
        outer_sum = narrow_scatter_sum(all_part)
    outer_out = outer_sum + outer_offset
    res_two = norm_one + outer_out
    layer_out, ffn_pull = jax.vjp(layer_norm, res_two, ffn_scale, ffn_offset)
    grad_two, ffn_gsum, ffn_ssum = ffn_pull(cotangent.astype(jnp.float32))
    grad_outer = grad_two.astype(jnp.bfloat16)
    outer_bsum = jnp.sum(grad_outer.astype(jnp.float32), axis=0)
    if narrow_n == 2:
        far_grads = swapped(grad_outer, "narrow", 0)
        own_inner, own_back = ffn_backward(grad_outer, own_pull, inner_cols, outer_cols)
        own_inner, own_back, far_grads = lax.optimization_barrier((own_inner, own_back, far_grads))
        far_inner, far_back = ffn_backward(far_grads, far_pull, inner_cols, outer_cols)
        grad_part = own_back + swapped(far_back.astype(jnp.bfloat16), "narrow", 0).astype(
            jnp.float32
        )
        outer_wsum_t = contract_rows(grad_outer, own_act) + contract_rows(far_grads, far_act)
        inner_wsum = contract_rows(norm_low, own_inner) + contract_rows(far_rows, far_inner)
        inner_bsum = jnp.sum(own_inner.astype(jnp.float32), axis=0) + jnp.sum(
            far_inner.astype(jnp.float32), axis=0
        )
    else:
        group_grads = lax.all_gather(grad_outer, "narrow", axis=0, tiled=True)
        all_inner, all_back = ffn_backward(group_grads, all_pull, inner_cols, outer_cols)
        grad_part = narrow_scatter_sum(all_back)
        outer_wsum_t = contract_rows(group_grads, all_act)
        inner_wsum = contract_rows(group_rows, all_inner)
        inner_bsum = jnp.sum(all_inner.astype(jnp.float32), axis=0)
    grad_norm = grad_two + grad_part
    grad_one, attn_gsum, attn_ssum = norm_pull(grad_norm)
    grad_attn = grad_one.astype(jnp.bfloat16)
    output_bsum = jnp.sum(grad_attn.astype(jnp.float32), axis=0)
    output_wsum = contract_rows(mixed_low, grad_attn)
    early_small = jnp.stack(
        [output_bsum, attn_gsum, attn_ssum, outer_bsum, ffn_gsum, ffn_ssum], axis=1
    )
    early = jnp.concatenate([output_wsum, early_small], axis=1)
    early_cols = early.shape[1]
    bsum_rows = jnp.pad(
        inner_bsum.reshape(wide_n, bias_n), ((0, 0), (0, ffn_rows * bias_k - bias_n))
    ).reshape(wide_n * ffn_rows, bias_k)
    ffn_sums = jnp.concatenate(
        [inner_wsum, outer_wsum_t, bsum_rows, early.reshape(wide_n * ffn_rows, -1)], axis=1
    ).astype(jnp.bfloat16)
    ffn_mine = lax.psum_scatter(ffn_sums, "wide", scatter_dimension=0, tiled=True)
    ffn_mine = ffn_mine.astype(jnp.float32)
    inner_wgrad = ffn_mine[:, :ffn_cols]
    outer_wgrad = ffn_mine[:, ffn_cols : 2 * ffn_cols].T
    inner_bgrad = ffn_mine[:, 2 * ffn_cols : 2 * ffn_cols + bias_k].reshape(-1)[:bias_n]
    early_wide = ffn_mine[:, 2 * ffn_cols + bias_k :].reshape(narrow_n, share, early_cols)
    early_mine = narrow_sum_rows(early_wide)

    grad_mixed = heads_of(contract_cols(grad_attn, output_full).astype(jnp.bfloat16))
    grad_qrot, grad_kall, grad_vall = attend_back(
        query_rot, all_keys, all_values, own_docs, key_docs, logsum, grad_mixed
    )
    back_keys, back_values = swapped(
        (
            grad_kall[:, half_len:].astype(jnp.bfloat16),
            grad_vall[:, half_len:].astype(jnp.bfloat16),
        ),
        "narrow",
        0,
    )
    grad_krot = grad_kall[:, :half_len] + back_keys.astype(jnp.float32)
    grad_values = (grad_vall[:, :half_len] + back_values.astype(jnp.float32)).astype(jnp.bfloat16)
    grad_query = unrotate(grad_qrot, own_cos, own_sin).astype(jnp.bfloat16)
    grad_keys = unrotate(grad_krot, own_cos, own_sin).astype(jnp.bfloat16)
    grad_qkv = jnp.concatenate(
        [
            grad_query.reshape(rows_dev, D),
            grad_keys.reshape(rows_dev, D),
            grad_values.reshape(rows_dev, D),
        ],
        axis=1,
    )
    qkv_wsum = contract_rows(layer_in, grad_qkv)
    qkv_bsum = jnp.sum(grad_qkv.astype(jnp.float32), axis=0).reshape(3, D)
    input_grad = grad_one + contract_cols(grad_qkv, qkv_full)
    late = jnp.concatenate(
        [
            qkv_wsum.reshape(total, share, 3 * D),
            qkv_bsum.T.reshape(total, share, 3),
        ],
        axis=2,
    )
    late_mine = scatter_sum_all(late)
    query_wgrad = late_mine[:, :D]
    key_wgrad = late_mine[:, D : 2 * D]
    value_wgrad = late_mine[:, 2 * D : 3 * D]
    query_bgrad = late_mine[:, 3 * D]
    key_bgrad = late_mine[:, 3 * D + 1]
    value_bgrad = late_mine[:, 3 * D + 2]
    output_wgrad = early_mine[:, :D]
    output_bgrad = early_mine[:, D]
    attn_ggrad = early_mine[:, D + 1]
    attn_sgrad = early_mine[:, D + 2]
    outer_bgrad = early_mine[:, D + 3]
    ffn_ggrad = early_mine[:, D + 4]
    ffn_sgrad = early_mine[:, D + 5]
    return (
        layer_out,
        input_grad,
        query_wgrad,
        query_bgrad,
        key_wgrad,
        key_bgrad,
        value_wgrad,
        value_bgrad,
        output_wgrad,
        output_bgrad,
        attn_ggrad,
        attn_sgrad,
        inner_wgrad,
        inner_bgrad,
        outer_wgrad,
        outer_bgrad,
        ffn_ggrad,
        ffn_sgrad,
    )


def solution(mesh):
    return jax.shard_map(
        local,
        mesh=mesh,
        in_specs=(
            P(("wide", "narrow"), None),
            P("wide", None),
            P(("wide", "narrow"), None),
            P(("wide", "narrow")),
            P(("wide", "narrow"), None),
            P(("wide", "narrow")),
            P(("wide", "narrow"), None),
            P(("wide", "narrow")),
            P(("wide", "narrow"), None),
            P(("wide", "narrow")),
            P(("wide", "narrow")),
            P(("wide", "narrow")),
            P("wide", "narrow"),
            P(("narrow", "wide")),
            P("narrow", "wide"),
            P(("wide", "narrow")),
            P(("wide", "narrow")),
            P(("wide", "narrow")),
            P(("wide", "narrow"), None),
        ),
        out_specs=(
            P(("wide", "narrow"), None),
            P(("wide", "narrow"), None),
            P(("wide", "narrow"), None),
            P(("wide", "narrow")),
            P(("wide", "narrow"), None),
            P(("wide", "narrow")),
            P(("wide", "narrow"), None),
            P(("wide", "narrow")),
            P(("wide", "narrow"), None),
            P(("wide", "narrow")),
            P(("wide", "narrow")),
            P(("wide", "narrow")),
            P("wide", "narrow"),
            P(("narrow", "wide")),
            P("narrow", "wide"),
            P(("wide", "narrow")),
            P(("wide", "narrow")),
            P(("wide", "narrow")),
        ),
        check_vma=False,
    )
```

```python
import jax
import jax.numpy as jnp
from jax import lax
from jax.sharding import PartitionSpec as P

D = 768
HEADS = 12
HEAD_DIM = 64

ALL = ("wide", "narrow")
layer_eps = 1e-12
masked_score = -1e30


def swapped(shard, axis, bit):
    return lax.ppermute(shard, axis, [(i, i ^ 1 << bit) for i in range(lax.axis_size(axis))])


def part_orders(total, narrow_n, parts):
    bits = total.bit_length() - 1
    core_bit = narrow_n.bit_length() - 1
    narrow_bits = list(range(core_bit))
    wide_bits = [b for b in reversed(range(core_bit + 1, bits))]
    orders = []
    for p in range(parts):
        k = p % max(1, len(wide_bits))
        orders.append(narrow_bits + wide_bits[k:] + wide_bits[:k] + [core_bit])
    return orders


def is_pow2(n):
    return n & (n - 1) == 0


def column_splits(cols, parts):
    tiles = -(-cols // 128)
    parts = max(1, min(parts, tiles))
    edges = [min(cols, (tiles * i // parts) * 128) for i in range(parts)] + [cols]
    return [(a, b) for a, b in zip(edges[:-1], edges[1:]) if b > a]


def doubling_gather(shard, order, total):
    me = lax.axis_index(ALL)
    cur = shard
    for b in order:
        other = lax.ppermute(cur, ALL, [(i, i ^ (1 << b)) for i in range(total)])
        bit = (me >> b) & 1
        pick = (jnp.arange(2) == bit).reshape((2,) + (1,) * cur.ndim)
        cur = jnp.where(pick, cur[None], other[None])
    k = len(order)
    perm = [k - 1 - order.index(b) for b in reversed(range(k))]
    cur = cur.transpose(perm + list(range(k, cur.ndim)))
    return cur.reshape((total,) + shard.shape)


def gather_all(shard, parts=3):
    total = lax.axis_size("wide") * lax.axis_size("narrow")
    narrow_n = lax.axis_size("narrow")
    if not (is_pow2(total) and is_pow2(narrow_n)):
        return lax.all_gather(shard, ALL, axis=0, tiled=False)
    splits = column_splits(shard.shape[-1], parts)
    orders = part_orders(total, narrow_n, len(splits))
    pieces = [
        doubling_gather(shard[..., a:b], order, total) for (a, b), order in zip(splits, orders)
    ]
    return jnp.concatenate(pieces, axis=-1)


def halving_scatter(parts_in, order, total):
    me = lax.axis_index(ALL)
    nbits = total.bit_length() - 1
    cur = parts_in.reshape((2,) * nbits + parts_in.shape[1:])
    axes = list(reversed(range(nbits)))
    for b in order:
        a = axes.index(b)
        bit = (me >> b) & 1
        mine = lax.dynamic_index_in_dim(cur, bit, axis=a, keepdims=False)
        theirs = lax.dynamic_index_in_dim(cur, 1 - bit, axis=a, keepdims=False)
        got = lax.ppermute(
            theirs.astype(jnp.bfloat16), ALL, [(i, i ^ (1 << b)) for i in range(total)]
        )
        cur = mine + got.astype(jnp.float32)
        axes.pop(a)
    return cur


def scatter_sum_all(parts_in, parts=3):
    total = lax.axis_size("wide") * lax.axis_size("narrow")
    narrow_n = lax.axis_size("narrow")
    if not (is_pow2(total) and is_pow2(narrow_n)):
        return lax.psum_scatter(
            parts_in.astype(jnp.bfloat16), ALL, scatter_dimension=0, tiled=False
        ).astype(jnp.float32)
    splits = column_splits(parts_in.shape[-1], parts)
    orders = part_orders(total, narrow_n, len(splits))
    pieces = [
        halving_scatter(parts_in[..., a:b], list(reversed(order)), total)
        for (a, b), order in zip(splits, orders)
    ]
    return jnp.concatenate(pieces, axis=-1)


def narrow_gather(rows):
    n = lax.axis_size("narrow")
    if n != 2:
        return lax.all_gather(rows, "narrow", axis=0, tiled=True)
    other = swapped(rows, "narrow", 0)
    first = lax.axis_index("narrow") == 0
    return jnp.where(first, jnp.concatenate([rows, other]), jnp.concatenate([other, rows]))


def narrow_scatter_sum(part):
    n = lax.axis_size("narrow")
    if n != 2:
        return lax.psum_scatter(
            part.astype(jnp.bfloat16), "narrow", scatter_dimension=0, tiled=True
        ).astype(jnp.float32)
    rows = part.shape[0] // 2
    me = lax.axis_index("narrow")
    mine = lax.dynamic_slice_in_dim(part, me * rows, rows, 0)
    theirs = lax.dynamic_slice_in_dim(part, (1 - me) * rows, rows, 0)
    return mine + swapped(theirs.astype(jnp.bfloat16), "narrow", 0).astype(jnp.float32)


def layer_norm(values, gain_vec, shift_vec):
    center = values - jnp.mean(values, axis=-1, keepdims=True)
    spread = jnp.mean(center * center, axis=-1, keepdims=True)
    return center * lax.rsqrt(spread + layer_eps) * gain_vec + shift_vec


def gelu_exact(values):
    return jax.nn.gelu(values, approximate=False)


def rotary_tables(doc_row):
    places = jnp.arange(doc_row.shape[0], dtype=jnp.int32)
    before = jnp.sum((doc_row[None, :] < doc_row[:, None]).astype(jnp.int32), axis=1)
    position = (places - before).astype(jnp.float32)
    frequency = 10000.0 ** (-2.0 * jnp.arange(HEAD_DIM // 2, dtype=jnp.float32) / HEAD_DIM)
    angles = position[:, None] * frequency[None, :]
    return (jnp.cos(angles), jnp.sin(angles))


def rotate(values, cosine, sine_tab):
    half_dim = values.shape[-1] // 2
    first_half = values[..., :half_dim]
    second = values[..., half_dim:]
    return jnp.concatenate(
        [first_half * cosine - second * sine_tab, second * cosine + first_half * sine_tab], axis=-1
    )


def unrotate(values, cosine, sine_tab):
    half_dim = values.shape[-1] // 2
    first_half = values[..., :half_dim]
    second = values[..., half_dim:]
    return jnp.concatenate(
        [first_half * cosine + second * sine_tab, second * cosine - first_half * sine_tab], axis=-1
    )


def contract_rows(left_op, right_op):
    return lax.dot_general(
        left_op, right_op, (((0,), (0,)), ((), ())), preferred_element_type=jnp.float32
    )


def contract_cols(left_op, right_op):
    return lax.dot_general(
        left_op, right_op, (((1,), (1,)), ((), ())), preferred_element_type=jnp.float32
    )


def score_block(query_rot, key_rot, query_docs, key_docs):
    scores = jnp.einsum(
        "pqhd,pkhd->phqk", query_rot, key_rot, preferred_element_type=jnp.float32
    ) * HEAD_DIM ** (-0.5)
    same_doc = query_docs[:, :, None] == key_docs[:, None, :]
    return jnp.where(same_doc[:, None], scores, masked_score)


def attend(query_rot, key_rot, value_low, query_docs, key_docs):
    scores = score_block(query_rot, key_rot, query_docs, key_docs)
    row_peak = jnp.max(scores, axis=-1, keepdims=True)
    exponent = jnp.exp(scores - row_peak)
    totals = jnp.sum(exponent, axis=-1, keepdims=True)
    probability = (exponent / totals).astype(jnp.bfloat16)
    mixed_out = jnp.einsum(
        "phqk,pkhd->pqhd", probability, value_low, preferred_element_type=jnp.float32
    )
    return (mixed_out, row_peak + jnp.log(totals))


def attend_back(query_rot, key_rot, value_low, query_docs, key_docs, logsum, grad_mixed):
    probability = jnp.exp(score_block(query_rot, key_rot, query_docs, key_docs) - logsum)
    grad_values = jnp.einsum(
        "phqk,pqhd->pkhd",
        probability.astype(jnp.bfloat16),
        grad_mixed,
        preferred_element_type=jnp.float32,
    )
    grad_probs = jnp.einsum(
        "pqhd,pkhd->phqk", grad_mixed, value_low, preferred_element_type=jnp.float32
    )
    inner_sum = jnp.sum(probability * grad_probs, axis=-1, keepdims=True)
    grad_scores = (probability * (grad_probs - inner_sum)).astype(jnp.bfloat16)
    grad_query = jnp.einsum(
        "phqk,pkhd->pqhd", grad_scores, key_rot, preferred_element_type=jnp.float32
    ) * HEAD_DIM ** (-0.5)
    grad_keys = jnp.einsum(
        "phqk,pqhd->pkhd", grad_scores, query_rot, preferred_element_type=jnp.float32
    ) * HEAD_DIM ** (-0.5)
    return (grad_query, grad_keys, grad_values)


def ffn_forward(rows, inner_cols, inner_offset, outer_cols):
    inner_pre = jnp.dot(rows, inner_cols, preferred_element_type=jnp.float32) + inner_offset
    act_value, gelu_pull = jax.vjp(gelu_exact, inner_pre)
    act_low = act_value.astype(jnp.bfloat16)
    return act_low, gelu_pull, contract_cols(act_low, outer_cols)


def ffn_backward(grads, gelu_pull, inner_cols, outer_cols):
    grad_act = jnp.dot(grads, outer_cols, preferred_element_type=jnp.float32)
    grad_inner = gelu_pull(grad_act)[0].astype(jnp.bfloat16)
    return grad_inner, contract_cols(grad_inner, inner_cols)


def local(
    layer_in,
    doc_ids,
    query_weight,
    query_bias,
    key_weight,
    key_bias,
    value_weight,
    value_bias,
    output_weight,
    output_bias,
    attn_gain,
    attn_shift,
    inner_weight,
    inner_bias,
    outer_weight,
    outer_bias,
    ffn_gain,
    ffn_shift,
    cotangent,
):
    wide_n = lax.axis_size("wide")
    narrow_n = lax.axis_size("narrow")
    total = wide_n * narrow_n
    share = query_weight.shape[0]
    small_list = (
        query_bias,
        key_bias,
        value_bias,
        output_bias,
        attn_gain,
        attn_shift,
        outer_bias,
        ffn_gain,
        ffn_shift,
    )
    small = jnp.stack(small_list, axis=1)
    small = jnp.pad(small, ((0, 0), (0, 128 - len(small_list))))
    shard = jnp.concatenate([query_weight, key_weight, value_weight, output_weight, small], axis=1)
    full = gather_all(shard).reshape(total * share, shard.shape[1])
    qkv_full = full[:, : 3 * D]
    output_full = full[:, 3 * D : 4 * D]
    vecs = full[:, 4 * D :].astype(jnp.float32)
    (
        query_offset,
        key_offset,
        value_offset,
        output_offset,
        attn_scale,
        attn_offset,
        outer_offset,
        ffn_scale,
        ffn_offset,
    ) = [vecs[:, i] for i in range(len(small_list))]
    qkv_offset = jnp.concatenate([query_offset, key_offset, value_offset])

    ffn_rows, ffn_cols = inner_weight.shape
    bias_n = inner_bias.shape[0]
    bias_k = -(-bias_n // ffn_rows)
    bias_rows = jnp.pad(inner_bias, (0, ffn_rows * bias_k - bias_n)).reshape(ffn_rows, bias_k)
    ffn_shard = jnp.concatenate([inner_weight, outer_weight.T, bias_rows], axis=1)
    ffn_shard, full = lax.optimization_barrier((ffn_shard, full))
    ffn_all = lax.all_gather(ffn_shard, "wide", axis=0, tiled=True)
    inner_cols = ffn_all[:, :ffn_cols]
    outer_cols = ffn_all[:, ffn_cols : 2 * ffn_cols]
    inner_offset = ffn_all[:, 2 * ffn_cols :].reshape(wide_n, ffn_rows * bias_k)[:, :bias_n]
    inner_offset = inner_offset.reshape(-1).astype(jnp.float32)

    rows_dev = layer_in.shape[0]
    half_len = doc_ids.shape[1] // 2
    pack_count = rows_dev // half_len
    narrow_place = lax.axis_index("narrow")
    half_bit = narrow_place % 2
    pair_slot = narrow_place // 2
    pack_docs = lax.dynamic_slice_in_dim(doc_ids, pair_slot * pack_count, pack_count, 0)
    cosine, sine_tab = jax.vmap(rotary_tables)(pack_docs)
    cosine = cosine[:, :, None, :]
    sine_tab = sine_tab[:, :, None, :]
    own_start = half_bit * half_len
    far_start = (1 - half_bit) * half_len
    own_cos = lax.dynamic_slice_in_dim(cosine, own_start, half_len, 1)
    own_sin = lax.dynamic_slice_in_dim(sine_tab, own_start, half_len, 1)
    own_docs = lax.dynamic_slice_in_dim(pack_docs, own_start, half_len, 1)
    far_docs = lax.dynamic_slice_in_dim(pack_docs, far_start, half_len, 1)
    key_docs = jnp.concatenate([own_docs, far_docs], axis=1)

    def heads_of(values):
        return values.reshape(pack_count, half_len, HEADS, HEAD_DIM)

    qkv = jnp.dot(layer_in, qkv_full, preferred_element_type=jnp.float32) + qkv_offset
    query_rot = rotate(heads_of(qkv[:, :D]), own_cos, own_sin).astype(jnp.bfloat16)
    key_rot = rotate(heads_of(qkv[:, D : 2 * D]), own_cos, own_sin).astype(jnp.bfloat16)
    value_low = heads_of(qkv[:, 2 * D :]).astype(jnp.bfloat16)
    far_keys, far_values = swapped((key_rot, value_low), "narrow", 0)
    all_keys = jnp.concatenate([key_rot, far_keys], axis=1)
    all_values = jnp.concatenate([value_low, far_values], axis=1)
    mixed_out, logsum = attend(query_rot, all_keys, all_values, own_docs, key_docs)
    mixed_low = mixed_out.reshape(rows_dev, D).astype(jnp.bfloat16)
    attn_out = jnp.dot(mixed_low, output_full, preferred_element_type=jnp.float32) + output_offset
    res_one = layer_in.astype(jnp.float32) + attn_out
    norm_one, norm_pull = jax.vjp(layer_norm, res_one, attn_scale, attn_offset)
    norm_low = norm_one.astype(jnp.bfloat16)

    if narrow_n == 2:
        far_rows = swapped(norm_low, "narrow", 0)
        own_act, own_pull, own_part = ffn_forward(norm_low, inner_cols, inner_offset, outer_cols)
        far_act, far_pull, far_part = ffn_forward(far_rows, inner_cols, inner_offset, outer_cols)
        outer_sum = own_part + swapped(far_part.astype(jnp.bfloat16), "narrow", 0).astype(
            jnp.float32
        )
    else:
        group_rows = lax.all_gather(norm_low, "narrow", axis=0, tiled=True)
        all_act, all_pull, all_part = ffn_forward(group_rows, inner_cols, inner_offset, outer_cols)
        outer_sum = narrow_scatter_sum(all_part)
    outer_out = outer_sum + outer_offset
    res_two = norm_one + outer_out
    layer_out, ffn_pull = jax.vjp(layer_norm, res_two, ffn_scale, ffn_offset)
    grad_two, ffn_gsum, ffn_ssum = ffn_pull(cotangent.astype(jnp.float32))
    grad_outer = grad_two.astype(jnp.bfloat16)
    outer_bsum = jnp.sum(grad_outer.astype(jnp.float32), axis=0)
    if narrow_n == 2:
        far_grads = swapped(grad_outer, "narrow", 0)
        own_inner, own_back = ffn_backward(grad_outer, own_pull, inner_cols, outer_cols)
        far_inner, far_back = ffn_backward(far_grads, far_pull, inner_cols, outer_cols)
        grad_part = own_back + swapped(far_back.astype(jnp.bfloat16), "narrow", 0).astype(
            jnp.float32
        )
        outer_wsum_t = contract_rows(grad_outer, own_act) + contract_rows(far_grads, far_act)
        inner_wsum = contract_rows(norm_low, own_inner) + contract_rows(far_rows, far_inner)
        inner_bsum = jnp.sum(own_inner.astype(jnp.float32), axis=0) + jnp.sum(
            far_inner.astype(jnp.float32), axis=0
        )
    else:
        group_grads = lax.all_gather(grad_outer, "narrow", axis=0, tiled=True)
        all_inner, all_back = ffn_backward(group_grads, all_pull, inner_cols, outer_cols)
        grad_part = narrow_scatter_sum(all_back)
        outer_wsum_t = contract_rows(group_grads, all_act)
        inner_wsum = contract_rows(group_rows, all_inner)
        inner_bsum = jnp.sum(all_inner.astype(jnp.float32), axis=0)
    bsum_rows = jnp.pad(
        inner_bsum.reshape(wide_n, bias_n), ((0, 0), (0, ffn_rows * bias_k - bias_n))
    ).reshape(wide_n * ffn_rows, bias_k)
    ffn_sums = jnp.concatenate([inner_wsum, outer_wsum_t, bsum_rows], axis=1).astype(jnp.bfloat16)
    ffn_mine = lax.psum_scatter(ffn_sums, "wide", scatter_dimension=0, tiled=True)
    ffn_mine = ffn_mine.astype(jnp.float32)
    inner_wgrad = ffn_mine[:, :ffn_cols]
    outer_wgrad = ffn_mine[:, ffn_cols : 2 * ffn_cols].T
    inner_bgrad = ffn_mine[:, 2 * ffn_cols :].reshape(-1)[:bias_n]

    grad_norm = grad_two + grad_part
    grad_one, attn_gsum, attn_ssum = norm_pull(grad_norm)
    grad_attn = grad_one.astype(jnp.bfloat16)
    output_bsum = jnp.sum(grad_attn.astype(jnp.float32), axis=0)
    output_wsum = contract_rows(mixed_low, grad_attn)
    early_small = jnp.stack(
        [output_bsum, attn_gsum, attn_ssum, outer_bsum, ffn_gsum, ffn_ssum], axis=1
    )
    early = jnp.concatenate(
        [output_wsum.reshape(total, share, D), early_small.reshape(total, share, -1)], axis=2
    )

    grad_mixed = heads_of(contract_cols(grad_attn, output_full).astype(jnp.bfloat16))
    grad_qrot, grad_kall, grad_vall = attend_back(
        query_rot, all_keys, all_values, own_docs, key_docs, logsum, grad_mixed
    )
    back_keys, back_values = swapped(
        (
            grad_kall[:, half_len:].astype(jnp.bfloat16),
            grad_vall[:, half_len:].astype(jnp.bfloat16),
        ),
        "narrow",
        0,
    )
    grad_krot = grad_kall[:, :half_len] + back_keys.astype(jnp.float32)
    grad_values = (grad_vall[:, :half_len] + back_values.astype(jnp.float32)).astype(jnp.bfloat16)
    grad_query = unrotate(grad_qrot, own_cos, own_sin).astype(jnp.bfloat16)
    grad_keys = unrotate(grad_krot, own_cos, own_sin).astype(jnp.bfloat16)
    grad_qkv = jnp.concatenate(
        [
            grad_query.reshape(rows_dev, D),
            grad_keys.reshape(rows_dev, D),
            grad_values.reshape(rows_dev, D),
        ],
        axis=1,
    )
    qkv_wsum = contract_rows(layer_in, grad_qkv)
    qkv_bsum = jnp.sum(grad_qkv.astype(jnp.float32), axis=0).reshape(3, D)
    input_grad = grad_one + contract_cols(grad_qkv, qkv_full)
    late = jnp.concatenate(
        [
            qkv_wsum.reshape(total, share, 3 * D),
            qkv_bsum.T.reshape(total, share, 3),
            early,
        ],
        axis=2,
    )
    late_mine = scatter_sum_all(late)
    early_mine = late_mine[:, 3 * D + 3 :]
    query_wgrad = late_mine[:, :D]
    key_wgrad = late_mine[:, D : 2 * D]
    value_wgrad = late_mine[:, 2 * D : 3 * D]
    query_bgrad = late_mine[:, 3 * D]
    key_bgrad = late_mine[:, 3 * D + 1]
    value_bgrad = late_mine[:, 3 * D + 2]
    output_wgrad = early_mine[:, :D]
    output_bgrad = early_mine[:, D]
    attn_ggrad = early_mine[:, D + 1]
    attn_sgrad = early_mine[:, D + 2]
    outer_bgrad = early_mine[:, D + 3]
    ffn_ggrad = early_mine[:, D + 4]
    ffn_sgrad = early_mine[:, D + 5]
    return (
        layer_out,
        input_grad,
        query_wgrad,
        query_bgrad,
        key_wgrad,
        key_bgrad,
        value_wgrad,
        value_bgrad,
        output_wgrad,
        output_bgrad,
        attn_ggrad,
        attn_sgrad,
        inner_wgrad,
        inner_bgrad,
        outer_wgrad,
        outer_bgrad,
        ffn_ggrad,
        ffn_sgrad,
    )


def solution(mesh):
    return jax.shard_map(
        local,
        mesh=mesh,
        in_specs=(
            P(("wide", "narrow"), None),
            P("wide", None),
            P(("wide", "narrow"), None),
            P(("wide", "narrow")),
            P(("wide", "narrow"), None),
            P(("wide", "narrow")),
            P(("wide", "narrow"), None),
            P(("wide", "narrow")),
            P(("wide", "narrow"), None),
            P(("wide", "narrow")),
            P(("wide", "narrow")),
            P(("wide", "narrow")),
            P("wide", "narrow"),
            P(("narrow", "wide")),
            P("narrow", "wide"),
            P(("wide", "narrow")),
            P(("wide", "narrow")),
            P(("wide", "narrow")),
            P(("wide", "narrow"), None),
        ),
        out_specs=(
            P(("wide", "narrow"), None),
            P(("wide", "narrow"), None),
            P(("wide", "narrow"), None),
            P(("wide", "narrow")),
            P(("wide", "narrow"), None),
            P(("wide", "narrow")),
            P(("wide", "narrow"), None),
            P(("wide", "narrow")),
            P(("wide", "narrow"), None),
            P(("wide", "narrow")),
            P(("wide", "narrow")),
            P(("wide", "narrow")),
            P("wide", "narrow"),
            P(("narrow", "wide")),
            P("narrow", "wide"),
            P(("wide", "narrow")),
            P(("wide", "narrow")),
            P(("wide", "narrow")),
        ),
        check_vma=False,
    )
```

```python
import jax
import jax.numpy as jnp
from jax import lax
from jax.sharding import PartitionSpec as P

D = 768
HEADS = 12
HEAD_DIM = 64

ALL = ("wide", "narrow")
layer_eps = 1e-12
masked_score = -1e30


def swapped(shard, axis, bit):
    return lax.ppermute(shard, axis, [(i, i ^ 1 << bit) for i in range(lax.axis_size(axis))])


def part_orders(total, narrow_n, parts):
    bits = total.bit_length() - 1
    core_bit = narrow_n.bit_length() - 1
    narrow_bits = list(range(core_bit))
    wide_bits = [b for b in reversed(range(core_bit + 1, bits))]
    orders = []
    for p in range(parts):
        k = p % max(1, len(wide_bits))
        orders.append(narrow_bits + wide_bits[k:] + wide_bits[:k] + [core_bit])
    return orders


def is_pow2(n):
    return n & (n - 1) == 0


def column_splits(cols, parts):
    tiles = -(-cols // 128)
    parts = max(1, min(parts, tiles))
    edges = [min(cols, (tiles * i // parts) * 128) for i in range(parts)] + [cols]
    return [(a, b) for a, b in zip(edges[:-1], edges[1:]) if b > a]


def doubling_gather(shard, order, total):
    me = lax.axis_index(ALL)
    cur = shard
    for b in order:
        other = lax.ppermute(cur, ALL, [(i, i ^ (1 << b)) for i in range(total)])
        bit = (me >> b) & 1
        pick = (jnp.arange(2) == bit).reshape((2,) + (1,) * cur.ndim)
        cur = jnp.where(pick, cur[None], other[None])
    k = len(order)
    perm = [k - 1 - order.index(b) for b in reversed(range(k))]
    cur = cur.transpose(perm + list(range(k, cur.ndim)))
    return cur.reshape((total,) + shard.shape)


def gather_all(shard, parts=3):
    total = lax.axis_size("wide") * lax.axis_size("narrow")
    narrow_n = lax.axis_size("narrow")
    if not (is_pow2(total) and is_pow2(narrow_n)):
        return lax.all_gather(shard, ALL, axis=0, tiled=False)
    splits = column_splits(shard.shape[-1], parts)
    orders = part_orders(total, narrow_n, len(splits))
    pieces = [
        doubling_gather(shard[..., a:b], order, total) for (a, b), order in zip(splits, orders)
    ]
    return jnp.concatenate(pieces, axis=-1)


def halving_scatter(arrays, order, total):
    me = lax.axis_index(ALL)
    nbits = total.bit_length() - 1
    cur = [x.reshape((2,) * nbits + x.shape[1:]) for x in arrays]
    axes = list(reversed(range(nbits)))
    for b in order:
        a = axes.index(b)
        bit = (me >> b) & 1
        mine = [lax.dynamic_index_in_dim(x, bit, axis=a, keepdims=False) for x in cur]
        theirs = tuple(
            lax.dynamic_index_in_dim(x, 1 - bit, axis=a, keepdims=False).astype(jnp.bfloat16)
            for x in cur
        )
        got = lax.ppermute(theirs, ALL, [(i, i ^ (1 << b)) for i in range(total)])
        cur = [m + g.astype(jnp.float32) for m, g in zip(mine, got)]
        axes.pop(a)
    return cur


def scatter_sum_all(arrays, parts=3):
    total = lax.axis_size("wide") * lax.axis_size("narrow")
    narrow_n = lax.axis_size("narrow")
    if not (is_pow2(total) and is_pow2(narrow_n)):
        return [
            lax.psum_scatter(
                x.astype(jnp.bfloat16), ALL, scatter_dimension=0, tiled=False
            ).astype(jnp.float32)
            for x in arrays
        ]
    orders = part_orders(total, narrow_n, parts)
    chains = [[] for _ in orders]
    pieces = []
    for x in arrays:
        for (a, c), chain in zip(column_splits(x.shape[-1], parts), chains):
            chain.append(len(pieces))
            pieces.append(x[..., a:c])
    results = [None] * len(pieces)
    for chain, order in zip(chains, orders):
        if chain:
            out = halving_scatter([pieces[i] for i in chain], list(reversed(order)), total)
            for i, r in zip(chain, out):
                results[i] = r
    merged = []
    at = 0
    for x in arrays:
        n = len(column_splits(x.shape[-1], parts))
        merged.append(jnp.concatenate(results[at : at + n], axis=-1) if n > 1 else results[at])
        at += n
    return merged


def narrow_gather(rows):
    n = lax.axis_size("narrow")
    if n != 2:
        return lax.all_gather(rows, "narrow", axis=0, tiled=True)
    other = swapped(rows, "narrow", 0)
    first = lax.axis_index("narrow") == 0
    return jnp.where(first, jnp.concatenate([rows, other]), jnp.concatenate([other, rows]))


def narrow_scatter_sum(part):
    n = lax.axis_size("narrow")
    if n != 2:
        return lax.psum_scatter(
            part.astype(jnp.bfloat16), "narrow", scatter_dimension=0, tiled=True
        ).astype(jnp.float32)
    rows = part.shape[0] // 2
    me = lax.axis_index("narrow")
    mine = lax.dynamic_slice_in_dim(part, me * rows, rows, 0)
    theirs = lax.dynamic_slice_in_dim(part, (1 - me) * rows, rows, 0)
    return mine + swapped(theirs.astype(jnp.bfloat16), "narrow", 0).astype(jnp.float32)


def layer_norm(values, gain_vec, shift_vec):
    center = values - jnp.mean(values, axis=-1, keepdims=True)
    spread = jnp.mean(center * center, axis=-1, keepdims=True)
    return center * lax.rsqrt(spread + layer_eps) * gain_vec + shift_vec


def gelu_exact(values):
    return jax.nn.gelu(values, approximate=False)


def rotary_tables(doc_row):
    places = jnp.arange(doc_row.shape[0], dtype=jnp.int32)
    before = jnp.sum((doc_row[None, :] < doc_row[:, None]).astype(jnp.int32), axis=1)
    position = (places - before).astype(jnp.float32)
    frequency = 10000.0 ** (-2.0 * jnp.arange(HEAD_DIM // 2, dtype=jnp.float32) / HEAD_DIM)
    angles = position[:, None] * frequency[None, :]
    return (jnp.cos(angles), jnp.sin(angles))


def rotate(values, cosine, sine_tab):
    half_dim = values.shape[-1] // 2
    first_half = values[..., :half_dim]
    second = values[..., half_dim:]
    return jnp.concatenate(
        [first_half * cosine - second * sine_tab, second * cosine + first_half * sine_tab], axis=-1
    )


def unrotate(values, cosine, sine_tab):
    half_dim = values.shape[-1] // 2
    first_half = values[..., :half_dim]
    second = values[..., half_dim:]
    return jnp.concatenate(
        [first_half * cosine + second * sine_tab, second * cosine - first_half * sine_tab], axis=-1
    )


def contract_rows(left_op, right_op):
    return lax.dot_general(
        left_op, right_op, (((0,), (0,)), ((), ())), preferred_element_type=jnp.float32
    )


def contract_cols(left_op, right_op):
    return lax.dot_general(
        left_op, right_op, (((1,), (1,)), ((), ())), preferred_element_type=jnp.float32
    )


def score_block(query_rot, key_rot, query_docs, key_docs):
    scores = jnp.einsum(
        "pqhd,pkhd->phqk", query_rot, key_rot, preferred_element_type=jnp.float32
    ) * HEAD_DIM ** (-0.5)
    same_doc = query_docs[:, :, None] == key_docs[:, None, :]
    return jnp.where(same_doc[:, None], scores, masked_score)


def attend(query_rot, key_rot, value_low, query_docs, key_docs):
    scores = score_block(query_rot, key_rot, query_docs, key_docs)
    row_peak = jnp.max(scores, axis=-1, keepdims=True)
    exponent = jnp.exp(scores - row_peak)
    totals = jnp.sum(exponent, axis=-1, keepdims=True)
    probability = (exponent / totals).astype(jnp.bfloat16)
    mixed_out = jnp.einsum(
        "phqk,pkhd->pqhd", probability, value_low, preferred_element_type=jnp.float32
    )
    return (mixed_out, row_peak + jnp.log(totals))


def attend_back(query_rot, key_rot, value_low, query_docs, key_docs, logsum, grad_mixed):
    probability = jnp.exp(score_block(query_rot, key_rot, query_docs, key_docs) - logsum)
    grad_values = jnp.einsum(
        "phqk,pqhd->pkhd",
        probability.astype(jnp.bfloat16),
        grad_mixed,
        preferred_element_type=jnp.float32,
    )
    grad_probs = jnp.einsum(
        "pqhd,pkhd->phqk", grad_mixed, value_low, preferred_element_type=jnp.float32
    )
    inner_sum = jnp.sum(probability * grad_probs, axis=-1, keepdims=True)
    grad_scores = (probability * (grad_probs - inner_sum)).astype(jnp.bfloat16)
    grad_query = jnp.einsum(
        "phqk,pkhd->pqhd", grad_scores, key_rot, preferred_element_type=jnp.float32
    ) * HEAD_DIM ** (-0.5)
    grad_keys = jnp.einsum(
        "phqk,pqhd->pkhd", grad_scores, query_rot, preferred_element_type=jnp.float32
    ) * HEAD_DIM ** (-0.5)
    return (grad_query, grad_keys, grad_values)


def ffn_forward(rows, inner_cols, inner_offset, outer_cols):
    inner_pre = jnp.dot(rows, inner_cols, preferred_element_type=jnp.float32) + inner_offset
    act_value, gelu_pull = jax.vjp(gelu_exact, inner_pre)
    act_low = act_value.astype(jnp.bfloat16)
    return act_low, gelu_pull, contract_cols(act_low, outer_cols)


def ffn_backward(grads, gelu_pull, inner_cols, outer_cols):
    grad_act = jnp.dot(grads, outer_cols, preferred_element_type=jnp.float32)
    grad_inner = gelu_pull(grad_act)[0].astype(jnp.bfloat16)
    return grad_inner, contract_cols(grad_inner, inner_cols)


def local(
    layer_in,
    doc_ids,
    query_weight,
    query_bias,
    key_weight,
    key_bias,
    value_weight,
    value_bias,
    output_weight,
    output_bias,
    attn_gain,
    attn_shift,
    inner_weight,
    inner_bias,
    outer_weight,
    outer_bias,
    ffn_gain,
    ffn_shift,
    cotangent,
):
    wide_n = lax.axis_size("wide")
    narrow_n = lax.axis_size("narrow")
    total = wide_n * narrow_n
    share = query_weight.shape[0]
    small_list = (
        query_bias,
        key_bias,
        value_bias,
        output_bias,
        attn_gain,
        attn_shift,
        outer_bias,
        ffn_gain,
        ffn_shift,
    )
    small = jnp.stack(small_list, axis=1)
    small = jnp.pad(small, ((0, 0), (0, 128 - len(small_list))))
    first = jnp.concatenate([key_weight, value_weight, small], axis=1)
    first_full = gather_all(first).reshape(total * share, first.shape[1])
    second = jnp.concatenate([query_weight, output_weight], axis=1)
    second, first_full = lax.optimization_barrier((second, first_full))
    second_full = gather_all(second).reshape(total * share, second.shape[1])
    kv_full = first_full[:, : 2 * D]
    query_full = second_full[:, :D]
    output_full = second_full[:, D:]
    full = second_full
    vecs = first_full[:, 2 * D :].astype(jnp.float32)
    (
        query_offset,
        key_offset,
        value_offset,
        output_offset,
        attn_scale,
        attn_offset,
        outer_offset,
        ffn_scale,
        ffn_offset,
    ) = [vecs[:, i] for i in range(len(small_list))]
    kv_offset = jnp.concatenate([key_offset, value_offset])

    ffn_rows, ffn_cols = inner_weight.shape
    bias_n = inner_bias.shape[0]
    bias_k = -(-bias_n // ffn_rows)
    bias_rows = jnp.pad(inner_bias, (0, ffn_rows * bias_k - bias_n)).reshape(ffn_rows, bias_k)
    ffn_shard = jnp.concatenate([inner_weight, outer_weight.T, bias_rows], axis=1)
    ffn_shard, full = lax.optimization_barrier((ffn_shard, full))
    ffn_all = lax.all_gather(ffn_shard, "wide", axis=0, tiled=True)
    inner_cols = ffn_all[:, :ffn_cols]
    outer_cols = ffn_all[:, ffn_cols : 2 * ffn_cols]
    inner_offset = ffn_all[:, 2 * ffn_cols :].reshape(wide_n, ffn_rows * bias_k)[:, :bias_n]
    inner_offset = inner_offset.reshape(-1).astype(jnp.float32)

    rows_dev = layer_in.shape[0]
    half_len = doc_ids.shape[1] // 2
    pack_count = rows_dev // half_len
    narrow_place = lax.axis_index("narrow")
    half_bit = narrow_place % 2
    pair_slot = narrow_place // 2
    pack_docs = lax.dynamic_slice_in_dim(doc_ids, pair_slot * pack_count, pack_count, 0)
    cosine, sine_tab = jax.vmap(rotary_tables)(pack_docs)
    cosine = cosine[:, :, None, :]
    sine_tab = sine_tab[:, :, None, :]
    own_start = half_bit * half_len
    far_start = (1 - half_bit) * half_len
    own_cos = lax.dynamic_slice_in_dim(cosine, own_start, half_len, 1)
    own_sin = lax.dynamic_slice_in_dim(sine_tab, own_start, half_len, 1)
    own_docs = lax.dynamic_slice_in_dim(pack_docs, own_start, half_len, 1)
    far_docs = lax.dynamic_slice_in_dim(pack_docs, far_start, half_len, 1)
    key_docs = jnp.concatenate([own_docs, far_docs], axis=1)

    def heads_of(values):
        return values.reshape(pack_count, half_len, HEADS, HEAD_DIM)

    kv = jnp.dot(layer_in, kv_full, preferred_element_type=jnp.float32) + kv_offset
    key_rot = rotate(heads_of(kv[:, :D]), own_cos, own_sin).astype(jnp.bfloat16)
    value_low = heads_of(kv[:, D:]).astype(jnp.bfloat16)
    far_keys, far_values = swapped((key_rot, value_low), "narrow", 0)
    query_pre = jnp.dot(layer_in, query_full, preferred_element_type=jnp.float32) + query_offset
    query_rot = rotate(heads_of(query_pre), own_cos, own_sin).astype(jnp.bfloat16)
    all_keys = jnp.concatenate([key_rot, far_keys], axis=1)
    all_values = jnp.concatenate([value_low, far_values], axis=1)
    mixed_out, logsum = attend(query_rot, all_keys, all_values, own_docs, key_docs)
    mixed_low = mixed_out.reshape(rows_dev, D).astype(jnp.bfloat16)
    attn_out = jnp.dot(mixed_low, output_full, preferred_element_type=jnp.float32) + output_offset
    res_one = layer_in.astype(jnp.float32) + attn_out
    norm_one, norm_pull = jax.vjp(layer_norm, res_one, attn_scale, attn_offset)
    norm_low = norm_one.astype(jnp.bfloat16)

    if narrow_n == 2:
        far_rows = swapped(norm_low, "narrow", 0)
        own_act, own_pull, own_part = ffn_forward(norm_low, inner_cols, inner_offset, outer_cols)
        far_act, far_pull, far_part = ffn_forward(far_rows, inner_cols, inner_offset, outer_cols)
        outer_sum = own_part + swapped(far_part.astype(jnp.bfloat16), "narrow", 0).astype(
            jnp.float32
        )
    else:
        group_rows = lax.all_gather(norm_low, "narrow", axis=0, tiled=True)
        all_act, all_pull, all_part = ffn_forward(group_rows, inner_cols, inner_offset, outer_cols)
        outer_sum = narrow_scatter_sum(all_part)
    outer_out = outer_sum + outer_offset
    res_two = norm_one + outer_out
    layer_out, ffn_pull = jax.vjp(layer_norm, res_two, ffn_scale, ffn_offset)
    grad_two, ffn_gsum, ffn_ssum = ffn_pull(cotangent.astype(jnp.float32))
    grad_outer = grad_two.astype(jnp.bfloat16)
    outer_bsum = jnp.sum(grad_outer.astype(jnp.float32), axis=0)
    if narrow_n == 2:
        far_grads = swapped(grad_outer, "narrow", 0)
        own_inner, own_back = ffn_backward(grad_outer, own_pull, inner_cols, outer_cols)
        far_inner, far_back = ffn_backward(far_grads, far_pull, inner_cols, outer_cols)
        grad_part = own_back + swapped(far_back.astype(jnp.bfloat16), "narrow", 0).astype(
            jnp.float32
        )
        outer_wsum_t = contract_rows(grad_outer, own_act) + contract_rows(far_grads, far_act)
        inner_wsum = contract_rows(norm_low, own_inner) + contract_rows(far_rows, far_inner)
        inner_bsum = jnp.sum(own_inner.astype(jnp.float32), axis=0) + jnp.sum(
            far_inner.astype(jnp.float32), axis=0
        )
    else:
        group_grads = lax.all_gather(grad_outer, "narrow", axis=0, tiled=True)
        all_inner, all_back = ffn_backward(group_grads, all_pull, inner_cols, outer_cols)
        grad_part = narrow_scatter_sum(all_back)
        outer_wsum_t = contract_rows(group_grads, all_act)
        inner_wsum = contract_rows(group_rows, all_inner)
        inner_bsum = jnp.sum(all_inner.astype(jnp.float32), axis=0)
    bsum_rows = jnp.pad(
        inner_bsum.reshape(wide_n, bias_n), ((0, 0), (0, ffn_rows * bias_k - bias_n))
    ).reshape(wide_n * ffn_rows, bias_k)
    ffn_sums = jnp.concatenate([inner_wsum, outer_wsum_t, bsum_rows], axis=1).astype(jnp.bfloat16)
    ffn_mine = lax.psum_scatter(ffn_sums, "wide", scatter_dimension=0, tiled=True)
    ffn_mine = ffn_mine.astype(jnp.float32)
    inner_wgrad = ffn_mine[:, :ffn_cols]
    outer_wgrad = ffn_mine[:, ffn_cols : 2 * ffn_cols].T
    inner_bgrad = ffn_mine[:, 2 * ffn_cols :].reshape(-1)[:bias_n]

    grad_norm = grad_two + grad_part
    grad_one, attn_gsum, attn_ssum = norm_pull(grad_norm)
    grad_attn = grad_one.astype(jnp.bfloat16)
    output_bsum = jnp.sum(grad_attn.astype(jnp.float32), axis=0)
    output_wsum = contract_rows(mixed_low, grad_attn)
    early_small = jnp.stack(
        [output_bsum, attn_gsum, attn_ssum, outer_bsum, ffn_gsum, ffn_ssum], axis=1
    )

    grad_mixed = heads_of(contract_cols(grad_attn, output_full).astype(jnp.bfloat16))
    grad_qrot, grad_kall, grad_vall = attend_back(
        query_rot, all_keys, all_values, own_docs, key_docs, logsum, grad_mixed
    )
    back_keys, back_values = swapped(
        (
            grad_kall[:, half_len:].astype(jnp.bfloat16),
            grad_vall[:, half_len:].astype(jnp.bfloat16),
        ),
        "narrow",
        0,
    )
    grad_krot = grad_kall[:, :half_len] + back_keys.astype(jnp.float32)
    grad_values = (grad_vall[:, :half_len] + back_values.astype(jnp.float32)).astype(jnp.bfloat16)
    grad_query = unrotate(grad_qrot, own_cos, own_sin).astype(jnp.bfloat16)
    grad_keys = unrotate(grad_krot, own_cos, own_sin).astype(jnp.bfloat16)
    grad_qkv = jnp.concatenate(
        [
            grad_query.reshape(rows_dev, D),
            grad_keys.reshape(rows_dev, D),
            grad_values.reshape(rows_dev, D),
        ],
        axis=1,
    )
    qkv_wsum = contract_rows(layer_in, grad_qkv)
    qkv_bsum = jnp.sum(grad_qkv.astype(jnp.float32), axis=0).reshape(3, D)
    input_grad = (
        grad_one
        + contract_cols(grad_qkv[:, :D], query_full)
        + contract_cols(grad_qkv[:, D:], kv_full)
    )
    late_mine, bias_mine, output_wgrad, small_mine = scatter_sum_all(
        [
            qkv_wsum.reshape(total, share, 3 * D),
            qkv_bsum.T.reshape(total, share, 3),
            output_wsum.reshape(total, share, D),
            early_small.reshape(total, share, -1),
        ]
    )
    query_wgrad = late_mine[:, :D]
    key_wgrad = late_mine[:, D : 2 * D]
    value_wgrad = late_mine[:, 2 * D : 3 * D]
    query_bgrad = bias_mine[:, 0]
    key_bgrad = bias_mine[:, 1]
    value_bgrad = bias_mine[:, 2]
    output_bgrad = small_mine[:, 0]
    attn_ggrad = small_mine[:, 1]
    attn_sgrad = small_mine[:, 2]
    outer_bgrad = small_mine[:, 3]
    ffn_ggrad = small_mine[:, 4]
    ffn_sgrad = small_mine[:, 5]
    return (
        layer_out,
        input_grad,
        query_wgrad,
        query_bgrad,
        key_wgrad,
        key_bgrad,
        value_wgrad,
        value_bgrad,
        output_wgrad,
        output_bgrad,
        attn_ggrad,
        attn_sgrad,
        inner_wgrad,
        inner_bgrad,
        outer_wgrad,
        outer_bgrad,
        ffn_ggrad,
        ffn_sgrad,
    )


def solution(mesh):
    return jax.shard_map(
        local,
        mesh=mesh,
        in_specs=(
            P(("wide", "narrow"), None),
            P("wide", None),
            P(("wide", "narrow"), None),
            P(("wide", "narrow")),
            P(("wide", "narrow"), None),
            P(("wide", "narrow")),
            P(("wide", "narrow"), None),
            P(("wide", "narrow")),
            P(("wide", "narrow"), None),
            P(("wide", "narrow")),
            P(("wide", "narrow")),
            P(("wide", "narrow")),
            P("wide", "narrow"),
            P(("narrow", "wide")),
            P("narrow", "wide"),
            P(("wide", "narrow")),
            P(("wide", "narrow")),
            P(("wide", "narrow")),
            P(("wide", "narrow"), None),
        ),
        out_specs=(
            P(("wide", "narrow"), None),
            P(("wide", "narrow"), None),
            P(("wide", "narrow"), None),
            P(("wide", "narrow")),
            P(("wide", "narrow"), None),
            P(("wide", "narrow")),
            P(("wide", "narrow"), None),
            P(("wide", "narrow")),
            P(("wide", "narrow"), None),
            P(("wide", "narrow")),
            P(("wide", "narrow")),
            P(("wide", "narrow")),
            P("wide", "narrow"),
            P(("narrow", "wide")),
            P("narrow", "wide"),
            P(("wide", "narrow")),
            P(("wide", "narrow")),
            P(("wide", "narrow")),
        ),
        check_vma=False,
    )
```

```python
import jax
import jax.numpy as jnp
from jax import lax
from jax.sharding import PartitionSpec as P

D = 768
HEADS = 12
HEAD_DIM = 64

ALL = ("wide", "narrow")
layer_eps = 1e-12
masked_score = -1e30


def swapped(shard, axis, bit):
    return lax.ppermute(shard, axis, [(i, i ^ 1 << bit) for i in range(lax.axis_size(axis))])


def part_orders(total, narrow_n, parts):
    bits = total.bit_length() - 1
    core_bit = narrow_n.bit_length() - 1
    narrow_bits = list(range(core_bit))
    wide_bits = [b for b in reversed(range(core_bit + 1, bits))]
    orders = []
    for p in range(parts):
        k = p % max(1, len(wide_bits))
        orders.append(narrow_bits + wide_bits[k:] + wide_bits[:k] + [core_bit])
    return orders


def is_pow2(n):
    return n & (n - 1) == 0


def column_splits(cols, parts):
    tiles = -(-cols // 128)
    parts = max(1, min(parts, tiles))
    edges = [min(cols, (tiles * i // parts) * 128) for i in range(parts)] + [cols]
    return [(a, b) for a, b in zip(edges[:-1], edges[1:]) if b > a]


def doubling_gather(shard, order, total):
    me = lax.axis_index(ALL)
    cur = shard
    for b in order:
        other = lax.ppermute(cur, ALL, [(i, i ^ (1 << b)) for i in range(total)])
        bit = (me >> b) & 1
        pick = (jnp.arange(2) == bit).reshape((2,) + (1,) * cur.ndim)
        cur = jnp.where(pick, cur[None], other[None])
    k = len(order)
    perm = [k - 1 - order.index(b) for b in reversed(range(k))]
    cur = cur.transpose(perm + list(range(k, cur.ndim)))
    return cur.reshape((total,) + shard.shape)


def gather_all(shard, parts=3):
    total = lax.axis_size("wide") * lax.axis_size("narrow")
    narrow_n = lax.axis_size("narrow")
    if not (is_pow2(total) and is_pow2(narrow_n)):
        return lax.all_gather(shard, ALL, axis=0, tiled=False)
    splits = column_splits(shard.shape[-1], parts)
    orders = part_orders(total, narrow_n, len(splits))
    pieces = [
        doubling_gather(shard[..., a:b], order, total) for (a, b), order in zip(splits, orders)
    ]
    return jnp.concatenate(pieces, axis=-1)


def halving_scatter(parts_in, order, total):
    me = lax.axis_index(ALL)
    nbits = total.bit_length() - 1
    cur = parts_in.reshape((2,) * nbits + parts_in.shape[1:])
    axes = list(reversed(range(nbits)))
    for b in order:
        a = axes.index(b)
        bit = (me >> b) & 1
        mine = lax.dynamic_index_in_dim(cur, bit, axis=a, keepdims=False)
        theirs = lax.dynamic_index_in_dim(cur, 1 - bit, axis=a, keepdims=False)
        got = lax.ppermute(
            theirs.astype(jnp.bfloat16), ALL, [(i, i ^ (1 << b)) for i in range(total)]
        )
        cur = mine + got.astype(jnp.float32)
        axes.pop(a)
    return cur


def scatter_sum_all(parts_in, parts=3):
    total = lax.axis_size("wide") * lax.axis_size("narrow")
    narrow_n = lax.axis_size("narrow")
    if not (is_pow2(total) and is_pow2(narrow_n)):
        return lax.psum_scatter(
            parts_in.astype(jnp.bfloat16), ALL, scatter_dimension=0, tiled=False
        ).astype(jnp.float32)
    splits = column_splits(parts_in.shape[-1], parts)
    orders = part_orders(total, narrow_n, len(splits))
    pieces = [
        halving_scatter(parts_in[..., a:b], list(reversed(order)), total)
        for (a, b), order in zip(splits, orders)
    ]
    return jnp.concatenate(pieces, axis=-1)


def narrow_gather(rows):
    n = lax.axis_size("narrow")
    if n != 2:
        return lax.all_gather(rows, "narrow", axis=0, tiled=True)
    other = swapped(rows, "narrow", 0)
    first = lax.axis_index("narrow") == 0
    return jnp.where(first, jnp.concatenate([rows, other]), jnp.concatenate([other, rows]))


def narrow_scatter_sum(part):
    n = lax.axis_size("narrow")
    if n != 2:
        return lax.psum_scatter(
            part.astype(jnp.bfloat16), "narrow", scatter_dimension=0, tiled=True
        ).astype(jnp.float32)
    rows = part.shape[0] // 2
    me = lax.axis_index("narrow")
    mine = lax.dynamic_slice_in_dim(part, me * rows, rows, 0)
    theirs = lax.dynamic_slice_in_dim(part, (1 - me) * rows, rows, 0)
    return mine + swapped(theirs.astype(jnp.bfloat16), "narrow", 0).astype(jnp.float32)


def layer_norm(values, gain_vec, shift_vec):
    center = values - jnp.mean(values, axis=-1, keepdims=True)
    spread = jnp.mean(center * center, axis=-1, keepdims=True)
    return center * lax.rsqrt(spread + layer_eps) * gain_vec + shift_vec


def gelu_exact(values):
    return jax.nn.gelu(values, approximate=False)


def rotary_tables(doc_row):
    places = jnp.arange(doc_row.shape[0], dtype=jnp.int32)
    before = jnp.sum((doc_row[None, :] < doc_row[:, None]).astype(jnp.int32), axis=1)
    position = (places - before).astype(jnp.float32)
    frequency = 10000.0 ** (-2.0 * jnp.arange(HEAD_DIM // 2, dtype=jnp.float32) / HEAD_DIM)
    angles = position[:, None] * frequency[None, :]
    return (jnp.cos(angles), jnp.sin(angles))


def rotate(values, cosine, sine_tab):
    half_dim = values.shape[-1] // 2
    first_half = values[..., :half_dim]
    second = values[..., half_dim:]
    return jnp.concatenate(
        [first_half * cosine - second * sine_tab, second * cosine + first_half * sine_tab], axis=-1
    )


def unrotate(values, cosine, sine_tab):
    half_dim = values.shape[-1] // 2
    first_half = values[..., :half_dim]
    second = values[..., half_dim:]
    return jnp.concatenate(
        [first_half * cosine + second * sine_tab, second * cosine - first_half * sine_tab], axis=-1
    )


def contract_rows(left_op, right_op):
    return lax.dot_general(
        left_op, right_op, (((0,), (0,)), ((), ())), preferred_element_type=jnp.float32
    )


def contract_cols(left_op, right_op):
    return lax.dot_general(
        left_op, right_op, (((1,), (1,)), ((), ())), preferred_element_type=jnp.float32
    )


def score_block(query_rot, key_rot, query_docs, key_docs):
    scores = jnp.einsum(
        "pqhd,pkhd->phqk", query_rot, key_rot, preferred_element_type=jnp.float32
    ) * HEAD_DIM ** (-0.5)
    same_doc = query_docs[:, :, None] == key_docs[:, None, :]
    return jnp.where(same_doc[:, None], scores, masked_score)


def attend(query_rot, key_rot, value_low, query_docs, key_docs):
    scores = score_block(query_rot, key_rot, query_docs, key_docs)
    row_peak = jnp.max(scores, axis=-1, keepdims=True)
    exponent = jnp.exp(scores - row_peak)
    totals = jnp.sum(exponent, axis=-1, keepdims=True)
    probability = (exponent / totals).astype(jnp.bfloat16)
    mixed_out = jnp.einsum(
        "phqk,pkhd->pqhd", probability, value_low, preferred_element_type=jnp.float32
    )
    return (mixed_out, row_peak + jnp.log(totals))


def attend_back(query_rot, key_rot, value_low, query_docs, key_docs, logsum, grad_mixed):
    probability = jnp.exp(score_block(query_rot, key_rot, query_docs, key_docs) - logsum)
    grad_values = jnp.einsum(
        "phqk,pqhd->pkhd",
        probability.astype(jnp.bfloat16),
        grad_mixed,
        preferred_element_type=jnp.float32,
    )
    grad_probs = jnp.einsum(
        "pqhd,pkhd->phqk", grad_mixed, value_low, preferred_element_type=jnp.float32
    )
    inner_sum = jnp.sum(probability * grad_probs, axis=-1, keepdims=True)
    grad_scores = (probability * (grad_probs - inner_sum)).astype(jnp.bfloat16)
    grad_query = jnp.einsum(
        "phqk,pkhd->pqhd", grad_scores, key_rot, preferred_element_type=jnp.float32
    ) * HEAD_DIM ** (-0.5)
    grad_keys = jnp.einsum(
        "phqk,pqhd->pkhd", grad_scores, query_rot, preferred_element_type=jnp.float32
    ) * HEAD_DIM ** (-0.5)
    return (grad_query, grad_keys, grad_values)


def ffn_forward(rows, inner_cols, inner_offset, outer_cols):
    inner_pre = jnp.dot(rows, inner_cols, preferred_element_type=jnp.float32) + inner_offset
    act_value, gelu_pull = jax.vjp(gelu_exact, inner_pre)
    act_low = act_value.astype(jnp.bfloat16)
    return act_low, gelu_pull, contract_cols(act_low, outer_cols)


def ffn_backward(grads, gelu_pull, inner_cols, outer_cols):
    grad_act = jnp.dot(grads, outer_cols, preferred_element_type=jnp.float32)
    grad_inner = gelu_pull(grad_act)[0].astype(jnp.bfloat16)
    return grad_inner, contract_cols(grad_inner, inner_cols)


def local(
    layer_in,
    doc_ids,
    query_weight,
    query_bias,
    key_weight,
    key_bias,
    value_weight,
    value_bias,
    output_weight,
    output_bias,
    attn_gain,
    attn_shift,
    inner_weight,
    inner_bias,
    outer_weight,
    outer_bias,
    ffn_gain,
    ffn_shift,
    cotangent,
):
    wide_n = lax.axis_size("wide")
    narrow_n = lax.axis_size("narrow")
    total = wide_n * narrow_n
    share = query_weight.shape[0]
    small_list = (
        query_bias,
        key_bias,
        value_bias,
        output_bias,
        attn_gain,
        attn_shift,
        outer_bias,
        ffn_gain,
        ffn_shift,
    )
    small = jnp.stack(small_list, axis=1)
    small = jnp.pad(small, ((0, 0), (0, 128 - len(small_list))))
    shard = jnp.concatenate([query_weight, key_weight, value_weight, output_weight, small], axis=1)
    full = gather_all(shard).reshape(total * share, shard.shape[1])
    qkv_full = full[:, : 3 * D]
    output_full = full[:, 3 * D : 4 * D]
    vecs = full[:, 4 * D :].astype(jnp.float32)
    (
        query_offset,
        key_offset,
        value_offset,
        output_offset,
        attn_scale,
        attn_offset,
        outer_offset,
        ffn_scale,
        ffn_offset,
    ) = [vecs[:, i] for i in range(len(small_list))]
    qkv_offset = jnp.concatenate([query_offset, key_offset, value_offset])

    ffn_rows, ffn_cols = inner_weight.shape
    bias_n = inner_bias.shape[0]
    bias_k = -(-bias_n // ffn_rows)
    bias_rows = jnp.pad(inner_bias, (0, ffn_rows * bias_k - bias_n)).reshape(ffn_rows, bias_k)
    ffn_shard = jnp.concatenate([inner_weight, outer_weight.T, bias_rows], axis=1)
    ffn_shard, full = lax.optimization_barrier((ffn_shard, full))
    ffn_all = lax.all_gather(ffn_shard, "wide", axis=0, tiled=True)
    inner_cols = ffn_all[:, :ffn_cols]
    outer_cols = ffn_all[:, ffn_cols : 2 * ffn_cols]
    inner_offset = ffn_all[:, 2 * ffn_cols :].reshape(wide_n, ffn_rows * bias_k)[:, :bias_n]
    inner_offset = inner_offset.reshape(-1).astype(jnp.float32)

    rows_dev = layer_in.shape[0]
    half_len = doc_ids.shape[1] // 2
    pack_count = rows_dev // half_len
    narrow_place = lax.axis_index("narrow")
    half_bit = narrow_place % 2
    pair_slot = narrow_place // 2
    pack_docs = lax.dynamic_slice_in_dim(doc_ids, pair_slot * pack_count, pack_count, 0)
    my_docs = lax.dynamic_slice_in_dim(pack_docs, half_bit, 1, 0)
    cosine, sine_tab = jax.vmap(rotary_tables)(my_docs)
    cosine = cosine[:, :, None, :]
    sine_tab = sine_tab[:, :, None, :]

    def to_pack(rows):
        keep = lax.dynamic_slice_in_dim(rows, half_bit * half_len, half_len, 0)
        give = lax.dynamic_slice_in_dim(rows, (1 - half_bit) * half_len, half_len, 0)
        got = swapped(give, "narrow", 0)
        return jnp.where(
            half_bit == 0, jnp.concatenate([keep, got]), jnp.concatenate([got, keep])
        )

    def from_pack(rows):
        keep = lax.dynamic_slice_in_dim(rows, half_bit * half_len, half_len, 0)
        give = lax.dynamic_slice_in_dim(rows, (1 - half_bit) * half_len, half_len, 0)
        got = swapped(give, "narrow", 0)
        return jnp.where(
            half_bit == 0, jnp.concatenate([keep, got]), jnp.concatenate([got, keep])
        )

    pack_in = to_pack(layer_in)
    pack_cot = to_pack(cotangent)

    def heads_of(values):
        return values.reshape(1, rows_dev, HEADS, HEAD_DIM)

    qkv = jnp.dot(pack_in, qkv_full, preferred_element_type=jnp.float32) + qkv_offset
    query_rot = rotate(heads_of(qkv[:, :D]), cosine, sine_tab).astype(jnp.bfloat16)
    key_rot = rotate(heads_of(qkv[:, D : 2 * D]), cosine, sine_tab).astype(jnp.bfloat16)
    value_low = heads_of(qkv[:, 2 * D :]).astype(jnp.bfloat16)
    mixed_out, logsum = attend(query_rot, key_rot, value_low, my_docs, my_docs)
    mixed_low = mixed_out.reshape(rows_dev, D).astype(jnp.bfloat16)
    attn_out = jnp.dot(mixed_low, output_full, preferred_element_type=jnp.float32) + output_offset
    res_one = pack_in.astype(jnp.float32) + attn_out
    norm_one, norm_pull = jax.vjp(layer_norm, res_one, attn_scale, attn_offset)
    norm_low = norm_one.astype(jnp.bfloat16)

    if narrow_n == 2:
        far_rows = swapped(norm_low, "narrow", 0)
        own_act, own_pull, own_part = ffn_forward(norm_low, inner_cols, inner_offset, outer_cols)
        far_act, far_pull, far_part = ffn_forward(far_rows, inner_cols, inner_offset, outer_cols)
        outer_sum = own_part + swapped(far_part.astype(jnp.bfloat16), "narrow", 0).astype(
            jnp.float32
        )
    else:
        group_rows = lax.all_gather(norm_low, "narrow", axis=0, tiled=True)
        all_act, all_pull, all_part = ffn_forward(group_rows, inner_cols, inner_offset, outer_cols)
        outer_sum = narrow_scatter_sum(all_part)
    outer_out = outer_sum + outer_offset
    res_two = norm_one + outer_out
    pack_out, ffn_pull = jax.vjp(layer_norm, res_two, ffn_scale, ffn_offset)
    layer_out = from_pack(pack_out)
    grad_two, ffn_gsum, ffn_ssum = ffn_pull(pack_cot.astype(jnp.float32))
    grad_outer = grad_two.astype(jnp.bfloat16)
    outer_bsum = jnp.sum(grad_outer.astype(jnp.float32), axis=0)
    if narrow_n == 2:
        far_grads = swapped(grad_outer, "narrow", 0)
        own_inner, own_back = ffn_backward(grad_outer, own_pull, inner_cols, outer_cols)
        far_inner, far_back = ffn_backward(far_grads, far_pull, inner_cols, outer_cols)
        grad_part = own_back + swapped(far_back.astype(jnp.bfloat16), "narrow", 0).astype(
            jnp.float32
        )
        outer_wsum_t = contract_rows(grad_outer, own_act) + contract_rows(far_grads, far_act)
        inner_wsum = contract_rows(norm_low, own_inner) + contract_rows(far_rows, far_inner)
        inner_bsum = jnp.sum(own_inner.astype(jnp.float32), axis=0) + jnp.sum(
            far_inner.astype(jnp.float32), axis=0
        )
    else:
        group_grads = lax.all_gather(grad_outer, "narrow", axis=0, tiled=True)
        all_inner, all_back = ffn_backward(group_grads, all_pull, inner_cols, outer_cols)
        grad_part = narrow_scatter_sum(all_back)
        outer_wsum_t = contract_rows(group_grads, all_act)
        inner_wsum = contract_rows(group_rows, all_inner)
        inner_bsum = jnp.sum(all_inner.astype(jnp.float32), axis=0)
    bsum_rows = jnp.pad(
        inner_bsum.reshape(wide_n, bias_n), ((0, 0), (0, ffn_rows * bias_k - bias_n))
    ).reshape(wide_n * ffn_rows, bias_k)
    ffn_sums = jnp.concatenate([inner_wsum, outer_wsum_t, bsum_rows], axis=1).astype(jnp.bfloat16)
    ffn_mine = lax.psum_scatter(ffn_sums, "wide", scatter_dimension=0, tiled=True)
    ffn_mine = ffn_mine.astype(jnp.float32)
    inner_wgrad = ffn_mine[:, :ffn_cols]
    outer_wgrad = ffn_mine[:, ffn_cols : 2 * ffn_cols].T
    inner_bgrad = ffn_mine[:, 2 * ffn_cols :].reshape(-1)[:bias_n]

    grad_norm = grad_two + grad_part
    grad_one, attn_gsum, attn_ssum = norm_pull(grad_norm)
    grad_attn = grad_one.astype(jnp.bfloat16)
    output_bsum = jnp.sum(grad_attn.astype(jnp.float32), axis=0)
    output_wsum = contract_rows(mixed_low, grad_attn)
    early_small = jnp.stack(
        [output_bsum, attn_gsum, attn_ssum, outer_bsum, ffn_gsum, ffn_ssum], axis=1
    )
    early = jnp.concatenate(
        [output_wsum.reshape(total, share, D), early_small.reshape(total, share, -1)], axis=2
    )

    grad_mixed = heads_of(contract_cols(grad_attn, output_full).astype(jnp.bfloat16))
    grad_qrot, grad_krot, grad_values = attend_back(
        query_rot, key_rot, value_low, my_docs, my_docs, logsum, grad_mixed
    )
    grad_values = grad_values.astype(jnp.bfloat16)
    grad_query = unrotate(grad_qrot, cosine, sine_tab).astype(jnp.bfloat16)
    grad_keys = unrotate(grad_krot, cosine, sine_tab).astype(jnp.bfloat16)
    grad_qkv = jnp.concatenate(
        [
            grad_query.reshape(rows_dev, D),
            grad_keys.reshape(rows_dev, D),
            grad_values.reshape(rows_dev, D),
        ],
        axis=1,
    )
    qkv_wsum = contract_rows(pack_in, grad_qkv)
    qkv_bsum = jnp.sum(grad_qkv.astype(jnp.float32), axis=0).reshape(3, D)
    input_grad = from_pack(grad_one + contract_cols(grad_qkv, qkv_full))
    late = jnp.concatenate(
        [
            qkv_wsum.reshape(total, share, 3 * D),
            qkv_bsum.T.reshape(total, share, 3),
            early,
        ],
        axis=2,
    )
    late_mine = scatter_sum_all(late)
    early_mine = late_mine[:, 3 * D + 3 :]
    query_wgrad = late_mine[:, :D]
    key_wgrad = late_mine[:, D : 2 * D]
    value_wgrad = late_mine[:, 2 * D : 3 * D]
    query_bgrad = late_mine[:, 3 * D]
    key_bgrad = late_mine[:, 3 * D + 1]
    value_bgrad = late_mine[:, 3 * D + 2]
    output_wgrad = early_mine[:, :D]
    output_bgrad = early_mine[:, D]
    attn_ggrad = early_mine[:, D + 1]
    attn_sgrad = early_mine[:, D + 2]
    outer_bgrad = early_mine[:, D + 3]
    ffn_ggrad = early_mine[:, D + 4]
    ffn_sgrad = early_mine[:, D + 5]
    return (
        layer_out,
        input_grad,
        query_wgrad,
        query_bgrad,
        key_wgrad,
        key_bgrad,
        value_wgrad,
        value_bgrad,
        output_wgrad,
        output_bgrad,
        attn_ggrad,
        attn_sgrad,
        inner_wgrad,
        inner_bgrad,
        outer_wgrad,
        outer_bgrad,
        ffn_ggrad,
        ffn_sgrad,
    )


def solution(mesh):
    return jax.shard_map(
        local,
        mesh=mesh,
        in_specs=(
            P(("wide", "narrow"), None),
            P("wide", None),
            P(("wide", "narrow"), None),
            P(("wide", "narrow")),
            P(("wide", "narrow"), None),
            P(("wide", "narrow")),
            P(("wide", "narrow"), None),
            P(("wide", "narrow")),
            P(("wide", "narrow"), None),
            P(("wide", "narrow")),
            P(("wide", "narrow")),
            P(("wide", "narrow")),
            P("wide", "narrow"),
            P(("narrow", "wide")),
            P("narrow", "wide"),
            P(("wide", "narrow")),
            P(("wide", "narrow")),
            P(("wide", "narrow")),
            P(("wide", "narrow"), None),
        ),
        out_specs=(
            P(("wide", "narrow"), None),
            P(("wide", "narrow"), None),
            P(("wide", "narrow"), None),
            P(("wide", "narrow")),
            P(("wide", "narrow"), None),
            P(("wide", "narrow")),
            P(("wide", "narrow"), None),
            P(("wide", "narrow")),
            P(("wide", "narrow"), None),
            P(("wide", "narrow")),
            P(("wide", "narrow")),
            P(("wide", "narrow")),
            P("wide", "narrow"),
            P(("narrow", "wide")),
            P("narrow", "wide"),
            P(("wide", "narrow")),
            P(("wide", "narrow")),
            P(("wide", "narrow")),
        ),
        check_vma=False,
    )
```

```python
import jax
import jax.numpy as jnp
from jax import lax
from jax.sharding import PartitionSpec as P

D = 768
HEADS = 12
HEAD_DIM = 64

ALL = ("wide", "narrow")
layer_eps = 1e-12
masked_score = -1e30


def swapped(shard, axis, bit):
    return lax.ppermute(shard, axis, [(i, i ^ 1 << bit) for i in range(lax.axis_size(axis))])


def part_orders(total, narrow_n, parts):
    bits = total.bit_length() - 1
    core_bit = narrow_n.bit_length() - 1
    narrow_bits = list(range(core_bit))
    wide_bits = [b for b in reversed(range(core_bit + 1, bits))]
    orders = []
    for p in range(parts):
        k = p % max(1, len(wide_bits))
        orders.append(narrow_bits + wide_bits[k:] + wide_bits[:k] + [core_bit])
    return orders


def is_pow2(n):
    return n & (n - 1) == 0


def column_splits(cols, parts):
    tiles = -(-cols // 128)
    parts = max(1, min(parts, tiles))
    edges = [min(cols, (tiles * i // parts) * 128) for i in range(parts)] + [cols]
    return [(a, b) for a, b in zip(edges[:-1], edges[1:]) if b > a]


def doubling_gather(shard, order, total):
    me = lax.axis_index(ALL)
    cur = shard
    for b in order:
        other = lax.ppermute(cur, ALL, [(i, i ^ (1 << b)) for i in range(total)])
        bit = (me >> b) & 1
        pick = (jnp.arange(2) == bit).reshape((2,) + (1,) * cur.ndim)
        cur = jnp.where(pick, cur[None], other[None])
    k = len(order)
    perm = [k - 1 - order.index(b) for b in reversed(range(k))]
    cur = cur.transpose(perm + list(range(k, cur.ndim)))
    return cur.reshape((total,) + shard.shape)


def gather_all(shard, parts=3):
    total = lax.axis_size("wide") * lax.axis_size("narrow")
    narrow_n = lax.axis_size("narrow")
    if not (is_pow2(total) and is_pow2(narrow_n)):
        return lax.all_gather(shard, ALL, axis=0, tiled=False)
    splits = column_splits(shard.shape[-1], parts)
    orders = part_orders(total, narrow_n, len(splits))
    pieces = [
        doubling_gather(shard[..., a:b], order, total) for (a, b), order in zip(splits, orders)
    ]
    return jnp.concatenate(pieces, axis=-1)


def halving_scatter(parts_in, order, total):
    me = lax.axis_index(ALL)
    nbits = total.bit_length() - 1
    cur = parts_in.reshape((2,) * nbits + parts_in.shape[1:])
    axes = list(reversed(range(nbits)))
    for b in order:
        a = axes.index(b)
        bit = (me >> b) & 1
        mine = lax.dynamic_index_in_dim(cur, bit, axis=a, keepdims=False)
        theirs = lax.dynamic_index_in_dim(cur, 1 - bit, axis=a, keepdims=False)
        got = lax.ppermute(
            theirs.astype(jnp.bfloat16), ALL, [(i, i ^ (1 << b)) for i in range(total)]
        )
        cur = mine.astype(jnp.float32) + got.astype(jnp.float32)
        axes.pop(a)
    return cur


def scatter_sum_all(parts_in, parts=3):
    total = lax.axis_size("wide") * lax.axis_size("narrow")
    narrow_n = lax.axis_size("narrow")
    if not (is_pow2(total) and is_pow2(narrow_n)):
        return lax.psum_scatter(
            parts_in.astype(jnp.bfloat16), ALL, scatter_dimension=0, tiled=False
        ).astype(jnp.float32)
    splits = column_splits(parts_in.shape[-1], parts)
    orders = part_orders(total, narrow_n, len(splits))
    pieces = [
        halving_scatter(parts_in[..., a:b], list(reversed(order)), total)
        for (a, b), order in zip(splits, orders)
    ]
    return jnp.concatenate(pieces, axis=-1)


def narrow_gather(rows):
    n = lax.axis_size("narrow")
    if n != 2:
        return lax.all_gather(rows, "narrow", axis=0, tiled=True)
    other = swapped(rows, "narrow", 0)
    first = lax.axis_index("narrow") == 0
    return jnp.where(first, jnp.concatenate([rows, other]), jnp.concatenate([other, rows]))


def narrow_scatter_sum(part):
    n = lax.axis_size("narrow")
    if n != 2:
        return lax.psum_scatter(
            part.astype(jnp.bfloat16), "narrow", scatter_dimension=0, tiled=True
        ).astype(jnp.float32)
    rows = part.shape[0] // 2
    me = lax.axis_index("narrow")
    mine = lax.dynamic_slice_in_dim(part, me * rows, rows, 0)
    theirs = lax.dynamic_slice_in_dim(part, (1 - me) * rows, rows, 0)
    return mine + swapped(theirs.astype(jnp.bfloat16), "narrow", 0).astype(jnp.float32)


def layer_norm(values, gain_vec, shift_vec):
    center = values - jnp.mean(values, axis=-1, keepdims=True)
    spread = jnp.mean(center * center, axis=-1, keepdims=True)
    return center * lax.rsqrt(spread + layer_eps) * gain_vec + shift_vec


def gelu_exact(values):
    return jax.nn.gelu(values, approximate=False)


def rotary_tables(doc_row):
    places = jnp.arange(doc_row.shape[0], dtype=jnp.int32)
    before = jnp.sum((doc_row[None, :] < doc_row[:, None]).astype(jnp.int32), axis=1)
    position = (places - before).astype(jnp.float32)
    frequency = 10000.0 ** (-2.0 * jnp.arange(HEAD_DIM // 2, dtype=jnp.float32) / HEAD_DIM)
    angles = position[:, None] * frequency[None, :]
    return (jnp.cos(angles), jnp.sin(angles))


def rotate(values, cosine, sine_tab):
    half_dim = values.shape[-1] // 2
    first_half = values[..., :half_dim]
    second = values[..., half_dim:]
    return jnp.concatenate(
        [first_half * cosine - second * sine_tab, second * cosine + first_half * sine_tab], axis=-1
    )


def unrotate(values, cosine, sine_tab):
    half_dim = values.shape[-1] // 2
    first_half = values[..., :half_dim]
    second = values[..., half_dim:]
    return jnp.concatenate(
        [first_half * cosine + second * sine_tab, second * cosine - first_half * sine_tab], axis=-1
    )


def contract_rows(left_op, right_op):
    return lax.dot_general(
        left_op, right_op, (((0,), (0,)), ((), ())), preferred_element_type=jnp.float32
    )


def contract_cols(left_op, right_op):
    return lax.dot_general(
        left_op, right_op, (((1,), (1,)), ((), ())), preferred_element_type=jnp.float32
    )


def score_block(query_rot, key_rot, query_docs, key_docs):
    scores = jnp.einsum(
        "pqhd,pkhd->phqk", query_rot, key_rot, preferred_element_type=jnp.float32
    ) * HEAD_DIM ** (-0.5)
    same_doc = query_docs[:, :, None] == key_docs[:, None, :]
    return jnp.where(same_doc[:, None], scores, masked_score)


def attend(query_rot, key_rot, value_low, query_docs, key_docs):
    scores = score_block(query_rot, key_rot, query_docs, key_docs)
    row_peak = jnp.max(scores, axis=-1, keepdims=True)
    exponent = jnp.exp(scores - row_peak)
    totals = jnp.sum(exponent, axis=-1, keepdims=True)
    probability = (exponent / totals).astype(jnp.bfloat16)
    mixed_out = jnp.einsum(
        "phqk,pkhd->pqhd", probability, value_low, preferred_element_type=jnp.float32
    )
    return (mixed_out, row_peak + jnp.log(totals))


def attend_back(query_rot, key_rot, value_low, query_docs, key_docs, logsum, grad_mixed):
    probability = jnp.exp(score_block(query_rot, key_rot, query_docs, key_docs) - logsum)
    grad_values = jnp.einsum(
        "phqk,pqhd->pkhd",
        probability.astype(jnp.bfloat16),
        grad_mixed,
        preferred_element_type=jnp.float32,
    )
    grad_probs = jnp.einsum(
        "pqhd,pkhd->phqk", grad_mixed, value_low, preferred_element_type=jnp.float32
    )
    inner_sum = jnp.sum(probability * grad_probs, axis=-1, keepdims=True)
    grad_scores = (probability * (grad_probs - inner_sum)).astype(jnp.bfloat16)
    grad_query = jnp.einsum(
        "phqk,pkhd->pqhd", grad_scores, key_rot, preferred_element_type=jnp.float32
    ) * HEAD_DIM ** (-0.5)
    grad_keys = jnp.einsum(
        "phqk,pqhd->pkhd", grad_scores, query_rot, preferred_element_type=jnp.float32
    ) * HEAD_DIM ** (-0.5)
    return (grad_query, grad_keys, grad_values)


def ffn_forward(rows, inner_cols, inner_offset, outer_cols):
    inner_pre = jnp.dot(rows, inner_cols, preferred_element_type=jnp.float32) + inner_offset
    act_value, gelu_pull = jax.vjp(gelu_exact, inner_pre)
    act_low = act_value.astype(jnp.bfloat16)
    return act_low, gelu_pull, contract_cols(act_low, outer_cols)


def ffn_backward(grads, gelu_pull, inner_cols, outer_cols):
    grad_act = jnp.dot(grads, outer_cols, preferred_element_type=jnp.float32)
    grad_inner = gelu_pull(grad_act)[0].astype(jnp.bfloat16)
    return grad_inner, contract_cols(grad_inner, inner_cols)


def local(
    layer_in,
    doc_ids,
    query_weight,
    query_bias,
    key_weight,
    key_bias,
    value_weight,
    value_bias,
    output_weight,
    output_bias,
    attn_gain,
    attn_shift,
    inner_weight,
    inner_bias,
    outer_weight,
    outer_bias,
    ffn_gain,
    ffn_shift,
    cotangent,
):
    wide_n = lax.axis_size("wide")
    narrow_n = lax.axis_size("narrow")
    total = wide_n * narrow_n
    share = query_weight.shape[0]
    small_list = (
        query_bias,
        key_bias,
        value_bias,
        output_bias,
        attn_gain,
        attn_shift,
        outer_bias,
        ffn_gain,
        ffn_shift,
    )
    small = jnp.stack(small_list, axis=1)
    small = jnp.pad(small, ((0, 0), (0, 128 - len(small_list))))
    shard = jnp.concatenate([query_weight, key_weight, value_weight, output_weight, small], axis=1)
    full = gather_all(shard).reshape(total * share, shard.shape[1])
    qkv_full = full[:, : 3 * D]
    output_full = full[:, 3 * D : 4 * D]
    vecs = full[:, 4 * D :].astype(jnp.float32)
    (
        query_offset,
        key_offset,
        value_offset,
        output_offset,
        attn_scale,
        attn_offset,
        outer_offset,
        ffn_scale,
        ffn_offset,
    ) = [vecs[:, i] for i in range(len(small_list))]
    qkv_offset = jnp.concatenate([query_offset, key_offset, value_offset])

    ffn_rows, ffn_cols = inner_weight.shape
    bias_n = inner_bias.shape[0]
    bias_k = -(-bias_n // ffn_rows)
    bias_rows = jnp.pad(inner_bias, (0, ffn_rows * bias_k - bias_n)).reshape(ffn_rows, bias_k)
    inner_shard = jnp.concatenate([inner_weight, bias_rows], axis=1)
    inner_shard, full = lax.optimization_barrier((inner_shard, full))
    inner_all = lax.all_gather(inner_shard, "wide", axis=0, tiled=True)
    outer_shard, inner_all = lax.optimization_barrier((outer_weight.T, inner_all))
    outer_cols = lax.all_gather(outer_shard, "wide", axis=0, tiled=True)
    inner_cols = inner_all[:, :ffn_cols]
    inner_offset = inner_all[:, ffn_cols:].reshape(wide_n, ffn_rows * bias_k)[:, :bias_n]
    inner_offset = inner_offset.reshape(-1).astype(jnp.float32)

    rows_dev = layer_in.shape[0]
    half_len = doc_ids.shape[1] // 2
    pack_count = rows_dev // half_len
    narrow_place = lax.axis_index("narrow")
    half_bit = narrow_place % 2
    pair_slot = narrow_place // 2
    pack_docs = lax.dynamic_slice_in_dim(doc_ids, pair_slot * pack_count, pack_count, 0)
    my_docs = lax.dynamic_slice_in_dim(pack_docs, half_bit, 1, 0)
    cosine, sine_tab = jax.vmap(rotary_tables)(my_docs)
    cosine = cosine[:, :, None, :]
    sine_tab = sine_tab[:, :, None, :]

    def to_pack(rows):
        keep = lax.dynamic_slice_in_dim(rows, half_bit * half_len, half_len, 0)
        give = lax.dynamic_slice_in_dim(rows, (1 - half_bit) * half_len, half_len, 0)
        got = swapped(give, "narrow", 0)
        return jnp.where(
            half_bit == 0, jnp.concatenate([keep, got]), jnp.concatenate([got, keep])
        )

    def from_pack(rows):
        keep = lax.dynamic_slice_in_dim(rows, half_bit * half_len, half_len, 0)
        give = lax.dynamic_slice_in_dim(rows, (1 - half_bit) * half_len, half_len, 0)
        got = swapped(give, "narrow", 0)
        return jnp.where(
            half_bit == 0, jnp.concatenate([keep, got]), jnp.concatenate([got, keep])
        )

    pack_in = to_pack(layer_in)
    pack_cot = to_pack(cotangent)

    def heads_of(values):
        return values.reshape(1, rows_dev, HEADS, HEAD_DIM)

    qkv = jnp.dot(pack_in, qkv_full, preferred_element_type=jnp.float32) + qkv_offset
    query_rot = rotate(heads_of(qkv[:, :D]), cosine, sine_tab).astype(jnp.bfloat16)
    key_rot = rotate(heads_of(qkv[:, D : 2 * D]), cosine, sine_tab).astype(jnp.bfloat16)
    value_low = heads_of(qkv[:, 2 * D :]).astype(jnp.bfloat16)
    mixed_out, logsum = attend(query_rot, key_rot, value_low, my_docs, my_docs)
    mixed_low = mixed_out.reshape(rows_dev, D).astype(jnp.bfloat16)
    attn_out = jnp.dot(mixed_low, output_full, preferred_element_type=jnp.float32) + output_offset
    res_one = pack_in.astype(jnp.float32) + attn_out
    norm_one, norm_pull = jax.vjp(layer_norm, res_one, attn_scale, attn_offset)
    norm_low = norm_one.astype(jnp.bfloat16)

    if narrow_n == 2:
        far_rows = swapped(norm_low, "narrow", 0)
        own_act, own_pull, own_part = ffn_forward(norm_low, inner_cols, inner_offset, outer_cols)
        far_act, far_pull, far_part = ffn_forward(far_rows, inner_cols, inner_offset, outer_cols)
        outer_sum = own_part + swapped(far_part.astype(jnp.bfloat16), "narrow", 0).astype(
            jnp.float32
        )
    else:
        group_rows = lax.all_gather(norm_low, "narrow", axis=0, tiled=True)
        all_act, all_pull, all_part = ffn_forward(group_rows, inner_cols, inner_offset, outer_cols)
        outer_sum = narrow_scatter_sum(all_part)
    outer_out = outer_sum + outer_offset
    res_two = norm_one + outer_out
    pack_out, ffn_pull = jax.vjp(layer_norm, res_two, ffn_scale, ffn_offset)
    layer_out = from_pack(pack_out)
    grad_two, ffn_gsum, ffn_ssum = ffn_pull(pack_cot.astype(jnp.float32))
    grad_outer = grad_two.astype(jnp.bfloat16)
    outer_bsum = jnp.sum(grad_outer.astype(jnp.float32), axis=0)
    if narrow_n == 2:
        far_grads = swapped(grad_outer, "narrow", 0)
        own_inner, own_back = ffn_backward(grad_outer, own_pull, inner_cols, outer_cols)
        far_inner, far_back = ffn_backward(far_grads, far_pull, inner_cols, outer_cols)
        grad_part = own_back + swapped(far_back.astype(jnp.bfloat16), "narrow", 0).astype(
            jnp.float32
        )
        outer_wsum_t = contract_rows(grad_outer, own_act) + contract_rows(far_grads, far_act)
        inner_wsum = contract_rows(norm_low, own_inner) + contract_rows(far_rows, far_inner)
        inner_bsum = jnp.sum(own_inner.astype(jnp.float32), axis=0) + jnp.sum(
            far_inner.astype(jnp.float32), axis=0
        )
    else:
        group_grads = lax.all_gather(grad_outer, "narrow", axis=0, tiled=True)
        all_inner, all_back = ffn_backward(group_grads, all_pull, inner_cols, outer_cols)
        grad_part = narrow_scatter_sum(all_back)
        outer_wsum_t = contract_rows(group_grads, all_act)
        inner_wsum = contract_rows(group_rows, all_inner)
        inner_bsum = jnp.sum(all_inner.astype(jnp.float32), axis=0)
    bsum_rows = jnp.pad(
        inner_bsum.reshape(wide_n, bias_n), ((0, 0), (0, ffn_rows * bias_k - bias_n))
    ).reshape(wide_n * ffn_rows, bias_k)
    ffn_sums = jnp.concatenate([inner_wsum, outer_wsum_t, bsum_rows], axis=1).astype(jnp.bfloat16)
    ffn_mine = lax.psum_scatter(ffn_sums, "wide", scatter_dimension=0, tiled=True)
    ffn_mine = ffn_mine.astype(jnp.float32)
    inner_wgrad = ffn_mine[:, :ffn_cols]
    outer_wgrad = ffn_mine[:, ffn_cols : 2 * ffn_cols].T
    inner_bgrad = ffn_mine[:, 2 * ffn_cols :].reshape(-1)[:bias_n]

    grad_norm = grad_two + grad_part
    grad_one, attn_gsum, attn_ssum = norm_pull(grad_norm)
    grad_attn = grad_one.astype(jnp.bfloat16)
    output_bsum = jnp.sum(grad_attn.astype(jnp.float32), axis=0)
    output_wsum = contract_rows(mixed_low, grad_attn)
    early_small = jnp.stack(
        [output_bsum, attn_gsum, attn_ssum, outer_bsum, ffn_gsum, ffn_ssum], axis=1
    )
    early = jnp.concatenate(
        [output_wsum.reshape(total, share, D), early_small.reshape(total, share, -1)], axis=2
    )

    grad_mixed = heads_of(contract_cols(grad_attn, output_full).astype(jnp.bfloat16))
    grad_qrot, grad_krot, grad_values = attend_back(
        query_rot, key_rot, value_low, my_docs, my_docs, logsum, grad_mixed
    )
    grad_values = grad_values.astype(jnp.bfloat16)
    grad_query = unrotate(grad_qrot, cosine, sine_tab).astype(jnp.bfloat16)
    grad_keys = unrotate(grad_krot, cosine, sine_tab).astype(jnp.bfloat16)
    grad_qkv = jnp.concatenate(
        [
            grad_query.reshape(rows_dev, D),
            grad_keys.reshape(rows_dev, D),
            grad_values.reshape(rows_dev, D),
        ],
        axis=1,
    )
    qkv_wsum = contract_rows(pack_in, grad_qkv)
    qkv_bsum = jnp.sum(grad_qkv.astype(jnp.float32), axis=0).reshape(3, D)
    input_grad = from_pack(grad_one + contract_cols(grad_qkv, qkv_full))
    late = jnp.concatenate(
        [
            qkv_wsum.reshape(total, share, 3 * D).astype(jnp.bfloat16),
            qkv_bsum.T.reshape(total, share, 3).astype(jnp.bfloat16),
            early.astype(jnp.bfloat16),
        ],
        axis=2,
    )
    late_mine = scatter_sum_all(late)
    early_mine = late_mine[:, 3 * D + 3 :]
    query_wgrad = late_mine[:, :D]
    key_wgrad = late_mine[:, D : 2 * D]
    value_wgrad = late_mine[:, 2 * D : 3 * D]
    query_bgrad = late_mine[:, 3 * D]
    key_bgrad = late_mine[:, 3 * D + 1]
    value_bgrad = late_mine[:, 3 * D + 2]
    output_wgrad = early_mine[:, :D]
    output_bgrad = early_mine[:, D]
    attn_ggrad = early_mine[:, D + 1]
    attn_sgrad = early_mine[:, D + 2]
    outer_bgrad = early_mine[:, D + 3]
    ffn_ggrad = early_mine[:, D + 4]
    ffn_sgrad = early_mine[:, D + 5]
    return (
        layer_out,
        input_grad,
        query_wgrad,
        query_bgrad,
        key_wgrad,
        key_bgrad,
        value_wgrad,
        value_bgrad,
        output_wgrad,
        output_bgrad,
        attn_ggrad,
        attn_sgrad,
        inner_wgrad,
        inner_bgrad,
        outer_wgrad,
        outer_bgrad,
        ffn_ggrad,
        ffn_sgrad,
    )


def solution(mesh):
    return jax.shard_map(
        local,
        mesh=mesh,
        in_specs=(
            P(("wide", "narrow"), None),
            P("wide", None),
            P(("wide", "narrow"), None),
            P(("wide", "narrow")),
            P(("wide", "narrow"), None),
            P(("wide", "narrow")),
            P(("wide", "narrow"), None),
            P(("wide", "narrow")),
            P(("wide", "narrow"), None),
            P(("wide", "narrow")),
            P(("wide", "narrow")),
            P(("wide", "narrow")),
            P("wide", "narrow"),
            P(("narrow", "wide")),
            P("narrow", "wide"),
            P(("wide", "narrow")),
            P(("wide", "narrow")),
            P(("wide", "narrow")),
            P(("wide", "narrow"), None),
        ),
        out_specs=(
            P(("wide", "narrow"), None),
            P(("wide", "narrow"), None),
            P(("wide", "narrow"), None),
            P(("wide", "narrow")),
            P(("wide", "narrow"), None),
            P(("wide", "narrow")),
            P(("wide", "narrow"), None),
            P(("wide", "narrow")),
            P(("wide", "narrow"), None),
            P(("wide", "narrow")),
            P(("wide", "narrow")),
            P(("wide", "narrow")),
            P("wide", "narrow"),
            P(("narrow", "wide")),
            P("narrow", "wide"),
            P(("wide", "narrow")),
            P(("wide", "narrow")),
            P(("wide", "narrow")),
        ),
        check_vma=False,
    )
```

```python
import jax
import jax.numpy as jnp
from jax import lax
from jax.sharding import PartitionSpec as P

D = 768
HEADS = 12
HEAD_DIM = 64

ALL = ("wide", "narrow")
layer_eps = 1e-12
masked_score = -1e30


def swapped(shard, axis, bit):
    return lax.ppermute(shard, axis, [(i, i ^ 1 << bit) for i in range(lax.axis_size(axis))])


def part_orders(total, narrow_n, parts):
    bits = total.bit_length() - 1
    core_bit = narrow_n.bit_length() - 1
    narrow_bits = list(range(core_bit))
    wide_bits = [b for b in reversed(range(core_bit + 1, bits))]
    orders = []
    for p in range(parts):
        k = p % max(1, len(wide_bits))
        orders.append(narrow_bits + wide_bits[k:] + wide_bits[:k] + [core_bit])
    return orders


def is_pow2(n):
    return n & (n - 1) == 0


def column_splits(cols, parts):
    tiles = -(-cols // 128)
    parts = max(1, min(parts, tiles))
    edges = [min(cols, (tiles * i // parts) * 128) for i in range(parts)] + [cols]
    return [(a, b) for a, b in zip(edges[:-1], edges[1:]) if b > a]


def doubling_gather(shard, order, total):
    me = lax.axis_index(ALL)
    cur = shard
    for b in order:
        other = lax.ppermute(cur, ALL, [(i, i ^ (1 << b)) for i in range(total)])
        bit = (me >> b) & 1
        pick = (jnp.arange(2) == bit).reshape((2,) + (1,) * cur.ndim)
        cur = jnp.where(pick, cur[None], other[None])
    k = len(order)
    perm = [k - 1 - order.index(b) for b in reversed(range(k))]
    cur = cur.transpose(perm + list(range(k, cur.ndim)))
    return cur.reshape((total,) + shard.shape)


def gather_all(shard, parts=3):
    total = lax.axis_size("wide") * lax.axis_size("narrow")
    narrow_n = lax.axis_size("narrow")
    if not (is_pow2(total) and is_pow2(narrow_n)):
        return lax.all_gather(shard, ALL, axis=0, tiled=False)
    splits = column_splits(shard.shape[-1], parts)
    orders = part_orders(total, narrow_n, len(splits))
    pieces = [
        doubling_gather(shard[..., a:b], order, total) for (a, b), order in zip(splits, orders)
    ]
    return jnp.concatenate(pieces, axis=-1)


def halving_scatter(parts_in, order, total):
    me = lax.axis_index(ALL)
    nbits = total.bit_length() - 1
    cur = parts_in.reshape((2,) * nbits + parts_in.shape[1:])
    axes = list(reversed(range(nbits)))
    for b in order:
        a = axes.index(b)
        bit = (me >> b) & 1
        mine = lax.dynamic_index_in_dim(cur, bit, axis=a, keepdims=False)
        theirs = lax.dynamic_index_in_dim(cur, 1 - bit, axis=a, keepdims=False)
        got = lax.ppermute(
            theirs.astype(jnp.bfloat16), ALL, [(i, i ^ (1 << b)) for i in range(total)]
        )
        cur = mine.astype(jnp.float32) + got.astype(jnp.float32)
        axes.pop(a)
    return cur


def scatter_sum_all(parts_in, parts=3):
    total = lax.axis_size("wide") * lax.axis_size("narrow")
    narrow_n = lax.axis_size("narrow")
    if not (is_pow2(total) and is_pow2(narrow_n)):
        return lax.psum_scatter(
            parts_in.astype(jnp.bfloat16), ALL, scatter_dimension=0, tiled=False
        ).astype(jnp.float32)
    splits = column_splits(parts_in.shape[-1], parts)
    orders = part_orders(total, narrow_n, len(splits))
    pieces = [
        halving_scatter(parts_in[..., a:b], list(reversed(order)), total)
        for (a, b), order in zip(splits, orders)
    ]
    return jnp.concatenate(pieces, axis=-1)


def narrow_gather(rows):
    n = lax.axis_size("narrow")
    if n != 2:
        return lax.all_gather(rows, "narrow", axis=0, tiled=True)
    other = swapped(rows, "narrow", 0)
    first = lax.axis_index("narrow") == 0
    return jnp.where(first, jnp.concatenate([rows, other]), jnp.concatenate([other, rows]))


def narrow_scatter_sum(part):
    n = lax.axis_size("narrow")
    if n != 2:
        return lax.psum_scatter(
            part.astype(jnp.bfloat16), "narrow", scatter_dimension=0, tiled=True
        ).astype(jnp.float32)
    rows = part.shape[0] // 2
    me = lax.axis_index("narrow")
    mine = lax.dynamic_slice_in_dim(part, me * rows, rows, 0)
    theirs = lax.dynamic_slice_in_dim(part, (1 - me) * rows, rows, 0)
    return mine + swapped(theirs.astype(jnp.bfloat16), "narrow", 0).astype(jnp.float32)


def layer_norm(values, gain_vec, shift_vec):
    center = values - jnp.mean(values, axis=-1, keepdims=True)
    spread = jnp.mean(center * center, axis=-1, keepdims=True)
    return center * lax.rsqrt(spread + layer_eps) * gain_vec + shift_vec


def gelu_exact(values):
    return jax.nn.gelu(values, approximate=False)


def rotary_tables(doc_row):
    places = jnp.arange(doc_row.shape[0], dtype=jnp.int32)
    before = jnp.sum((doc_row[None, :] < doc_row[:, None]).astype(jnp.int32), axis=1)
    position = (places - before).astype(jnp.float32)
    frequency = 10000.0 ** (-2.0 * jnp.arange(HEAD_DIM // 2, dtype=jnp.float32) / HEAD_DIM)
    angles = position[:, None] * frequency[None, :]
    return (jnp.cos(angles), jnp.sin(angles))


def rotate(values, cosine, sine_tab):
    half_dim = values.shape[-1] // 2
    first_half = values[..., :half_dim]
    second = values[..., half_dim:]
    return jnp.concatenate(
        [first_half * cosine - second * sine_tab, second * cosine + first_half * sine_tab], axis=-1
    )


def unrotate(values, cosine, sine_tab):
    half_dim = values.shape[-1] // 2
    first_half = values[..., :half_dim]
    second = values[..., half_dim:]
    return jnp.concatenate(
        [first_half * cosine + second * sine_tab, second * cosine - first_half * sine_tab], axis=-1
    )


def contract_rows(left_op, right_op):
    return lax.dot_general(
        left_op, right_op, (((0,), (0,)), ((), ())), preferred_element_type=jnp.float32
    )


def contract_cols(left_op, right_op):
    return lax.dot_general(
        left_op, right_op, (((1,), (1,)), ((), ())), preferred_element_type=jnp.float32
    )


def score_block(query_rot, key_rot, query_docs, key_docs):
    scores = jnp.einsum(
        "pqhd,pkhd->phqk", query_rot, key_rot, preferred_element_type=jnp.float32
    ) * HEAD_DIM ** (-0.5)
    same_doc = query_docs[:, :, None] == key_docs[:, None, :]
    return jnp.where(same_doc[:, None], scores, masked_score)


def attend(query_rot, key_rot, value_low, query_docs, key_docs):
    scores = score_block(query_rot, key_rot, query_docs, key_docs)
    row_peak = jnp.max(scores, axis=-1, keepdims=True)
    exponent = jnp.exp(scores - row_peak)
    totals = jnp.sum(exponent, axis=-1, keepdims=True)
    probability = (exponent / totals).astype(jnp.bfloat16)
    mixed_out = jnp.einsum(
        "phqk,pkhd->pqhd", probability, value_low, preferred_element_type=jnp.float32
    )
    return (mixed_out, row_peak + jnp.log(totals))


def attend_back(query_rot, key_rot, value_low, query_docs, key_docs, logsum, grad_mixed):
    probability = jnp.exp(score_block(query_rot, key_rot, query_docs, key_docs) - logsum)
    grad_values = jnp.einsum(
        "phqk,pqhd->pkhd",
        probability.astype(jnp.bfloat16),
        grad_mixed,
        preferred_element_type=jnp.float32,
    )
    grad_probs = jnp.einsum(
        "pqhd,pkhd->phqk", grad_mixed, value_low, preferred_element_type=jnp.float32
    )
    inner_sum = jnp.sum(probability * grad_probs, axis=-1, keepdims=True)
    grad_scores = (probability * (grad_probs - inner_sum)).astype(jnp.bfloat16)
    grad_query = jnp.einsum(
        "phqk,pkhd->pqhd", grad_scores, key_rot, preferred_element_type=jnp.float32
    ) * HEAD_DIM ** (-0.5)
    grad_keys = jnp.einsum(
        "phqk,pqhd->pkhd", grad_scores, query_rot, preferred_element_type=jnp.float32
    ) * HEAD_DIM ** (-0.5)
    return (grad_query, grad_keys, grad_values)


def ffn_forward(rows, inner_cols, inner_offset, outer_cols):
    inner_pre = jnp.dot(rows, inner_cols, preferred_element_type=jnp.float32) + inner_offset
    act_value, gelu_pull = jax.vjp(gelu_exact, inner_pre)
    act_low = act_value.astype(jnp.bfloat16)
    return act_low, gelu_pull, contract_cols(act_low, outer_cols)


def ffn_backward(grads, gelu_pull, inner_cols, outer_cols):
    grad_act = jnp.dot(grads, outer_cols, preferred_element_type=jnp.float32)
    grad_inner = gelu_pull(grad_act)[0].astype(jnp.bfloat16)
    return grad_inner, contract_cols(grad_inner, inner_cols)


def local(
    layer_in,
    doc_ids,
    query_weight,
    query_bias,
    key_weight,
    key_bias,
    value_weight,
    value_bias,
    output_weight,
    output_bias,
    attn_gain,
    attn_shift,
    inner_weight,
    inner_bias,
    outer_weight,
    outer_bias,
    ffn_gain,
    ffn_shift,
    cotangent,
):
    wide_n = lax.axis_size("wide")
    narrow_n = lax.axis_size("narrow")
    total = wide_n * narrow_n
    share = query_weight.shape[0]
    small_list = (
        query_bias,
        key_bias,
        value_bias,
        output_bias,
        attn_gain,
        attn_shift,
        outer_bias,
        ffn_gain,
        ffn_shift,
    )
    small = jnp.stack(small_list, axis=1)
    small = jnp.pad(small, ((0, 0), (0, 128 - len(small_list))))
    shard = jnp.concatenate([query_weight, key_weight, value_weight, output_weight, small], axis=1)
    full = gather_all(shard).reshape(total * share, shard.shape[1])
    qkv_full = full[:, : 3 * D]
    output_full = full[:, 3 * D : 4 * D]
    vecs = full[:, 4 * D :].astype(jnp.float32)
    (
        query_offset,
        key_offset,
        value_offset,
        output_offset,
        attn_scale,
        attn_offset,
        outer_offset,
        ffn_scale,
        ffn_offset,
    ) = [vecs[:, i] for i in range(len(small_list))]
    qkv_offset = jnp.concatenate([query_offset, key_offset, value_offset])

    ffn_rows, ffn_cols = inner_weight.shape
    bias_n = inner_bias.shape[0]
    bias_k = -(-bias_n // ffn_rows)
    bias_rows = jnp.pad(inner_bias, (0, ffn_rows * bias_k - bias_n)).reshape(ffn_rows, bias_k)
    ffn_shard = jnp.concatenate([inner_weight, outer_weight.T, bias_rows], axis=1)
    ffn_shard, full = lax.optimization_barrier((ffn_shard, full))
    ffn_all = lax.all_gather(ffn_shard, "wide", axis=0, tiled=True)
    inner_cols = ffn_all[:, :ffn_cols]
    outer_cols = ffn_all[:, ffn_cols : 2 * ffn_cols]
    inner_offset = ffn_all[:, 2 * ffn_cols :].reshape(wide_n, ffn_rows * bias_k)[:, :bias_n]
    inner_offset = inner_offset.reshape(-1).astype(jnp.float32)

    rows_dev = layer_in.shape[0]
    half_len = doc_ids.shape[1] // 2
    pack_count = rows_dev // half_len
    narrow_place = lax.axis_index("narrow")
    half_bit = narrow_place % 2
    pair_slot = narrow_place // 2
    pack_docs = lax.dynamic_slice_in_dim(doc_ids, pair_slot * pack_count, pack_count, 0)
    my_docs = lax.dynamic_slice_in_dim(pack_docs, half_bit, 1, 0)
    cosine, sine_tab = jax.vmap(rotary_tables)(my_docs)
    cosine = cosine[:, :, None, :]
    sine_tab = sine_tab[:, :, None, :]

    def to_pack(rows):
        keep = lax.dynamic_slice_in_dim(rows, half_bit * half_len, half_len, 0)
        give = lax.dynamic_slice_in_dim(rows, (1 - half_bit) * half_len, half_len, 0)
        got = swapped(give, "narrow", 0)
        return jnp.where(
            half_bit == 0, jnp.concatenate([keep, got]), jnp.concatenate([got, keep])
        )

    def from_pack(rows):
        keep = lax.dynamic_slice_in_dim(rows, half_bit * half_len, half_len, 0)
        give = lax.dynamic_slice_in_dim(rows, (1 - half_bit) * half_len, half_len, 0)
        got = swapped(give, "narrow", 0)
        return jnp.where(
            half_bit == 0, jnp.concatenate([keep, got]), jnp.concatenate([got, keep])
        )

    pack_in = to_pack(layer_in)
    pack_cot = to_pack(cotangent)

    def heads_of(values):
        return values.reshape(1, rows_dev, HEADS, HEAD_DIM)

    qkv = jnp.dot(pack_in, qkv_full, preferred_element_type=jnp.float32) + qkv_offset
    query_rot = rotate(heads_of(qkv[:, :D]), cosine, sine_tab).astype(jnp.bfloat16)
    key_rot = rotate(heads_of(qkv[:, D : 2 * D]), cosine, sine_tab).astype(jnp.bfloat16)
    value_low = heads_of(qkv[:, 2 * D :]).astype(jnp.bfloat16)
    mixed_out, logsum = attend(query_rot, key_rot, value_low, my_docs, my_docs)
    mixed_low = mixed_out.reshape(rows_dev, D).astype(jnp.bfloat16)
    attn_out = jnp.dot(mixed_low, output_full, preferred_element_type=jnp.float32) + output_offset
    res_one = pack_in.astype(jnp.float32) + attn_out
    norm_one, norm_pull = jax.vjp(layer_norm, res_one, attn_scale, attn_offset)
    norm_low = norm_one.astype(jnp.bfloat16)

    if narrow_n == 2:
        far_rows = swapped(norm_low, "narrow", 0)
        own_act, own_pull, own_part = ffn_forward(norm_low, inner_cols, inner_offset, outer_cols)
        far_act, far_pull, far_part = ffn_forward(far_rows, inner_cols, inner_offset, outer_cols)
        outer_sum = own_part + swapped(far_part.astype(jnp.bfloat16), "narrow", 0).astype(
            jnp.float32
        )
    else:
        group_rows = lax.all_gather(norm_low, "narrow", axis=0, tiled=True)
        all_act, all_pull, all_part = ffn_forward(group_rows, inner_cols, inner_offset, outer_cols)
        outer_sum = narrow_scatter_sum(all_part)
    outer_out = outer_sum + outer_offset
    res_two = norm_one + outer_out
    pack_out, ffn_pull = jax.vjp(layer_norm, res_two, ffn_scale, ffn_offset)
    layer_out = from_pack(pack_out)
    grad_two, ffn_gsum, ffn_ssum = ffn_pull(pack_cot.astype(jnp.float32))
    grad_outer = grad_two.astype(jnp.bfloat16)
    outer_bsum = jnp.sum(grad_outer.astype(jnp.float32), axis=0)
    if narrow_n == 2:
        far_grads = swapped(grad_outer, "narrow", 0)
        own_inner, own_back = ffn_backward(grad_outer, own_pull, inner_cols, outer_cols)
        far_inner, far_back = ffn_backward(far_grads, far_pull, inner_cols, outer_cols)
        grad_part = own_back + swapped(far_back.astype(jnp.bfloat16), "narrow", 0).astype(
            jnp.float32
        )
        outer_wsum_t = contract_rows(grad_outer, own_act) + contract_rows(far_grads, far_act)
        inner_wsum = contract_rows(norm_low, own_inner) + contract_rows(far_rows, far_inner)
        inner_bsum = jnp.sum(own_inner.astype(jnp.float32), axis=0) + jnp.sum(
            far_inner.astype(jnp.float32), axis=0
        )
    else:
        group_grads = lax.all_gather(grad_outer, "narrow", axis=0, tiled=True)
        all_inner, all_back = ffn_backward(group_grads, all_pull, inner_cols, outer_cols)
        grad_part = narrow_scatter_sum(all_back)
        outer_wsum_t = contract_rows(group_grads, all_act)
        inner_wsum = contract_rows(group_rows, all_inner)
        inner_bsum = jnp.sum(all_inner.astype(jnp.float32), axis=0)
    bsum_rows = jnp.pad(
        inner_bsum.reshape(wide_n, bias_n), ((0, 0), (0, ffn_rows * bias_k - bias_n))
    ).reshape(wide_n * ffn_rows, bias_k)
    ffn_sums = jnp.concatenate([inner_wsum, outer_wsum_t, bsum_rows], axis=1).astype(jnp.bfloat16)
    ffn_mine = lax.psum_scatter(ffn_sums, "wide", scatter_dimension=0, tiled=True)
    ffn_mine = ffn_mine.astype(jnp.float32)
    inner_wgrad = ffn_mine[:, :ffn_cols]
    outer_wgrad = ffn_mine[:, ffn_cols : 2 * ffn_cols].T
    inner_bgrad = ffn_mine[:, 2 * ffn_cols :].reshape(-1)[:bias_n]

    grad_norm = grad_two + grad_part
    grad_one, attn_gsum, attn_ssum = norm_pull(grad_norm)
    grad_attn = grad_one.astype(jnp.bfloat16)
    output_bsum = jnp.sum(grad_attn.astype(jnp.float32), axis=0)
    output_wsum = contract_rows(mixed_low, grad_attn)
    early_small = jnp.stack(
        [output_bsum, attn_gsum, attn_ssum, outer_bsum, ffn_gsum, ffn_ssum], axis=1
    )
    early = jnp.concatenate(
        [output_wsum.reshape(total, share, D), early_small.reshape(total, share, -1)], axis=2
    )

    grad_mixed = heads_of(contract_cols(grad_attn, output_full).astype(jnp.bfloat16))
    grad_qrot, grad_krot, grad_values = attend_back(
        query_rot, key_rot, value_low, my_docs, my_docs, logsum, grad_mixed
    )
    grad_values = grad_values.astype(jnp.bfloat16)
    grad_query = unrotate(grad_qrot, cosine, sine_tab).astype(jnp.bfloat16)
    grad_keys = unrotate(grad_krot, cosine, sine_tab).astype(jnp.bfloat16)
    grad_qkv = jnp.concatenate(
        [
            grad_query.reshape(rows_dev, D),
            grad_keys.reshape(rows_dev, D),
            grad_values.reshape(rows_dev, D),
        ],
        axis=1,
    )
    pack_grad = grad_one + contract_cols(grad_qkv, qkv_full)
    keep_grad = lax.dynamic_slice_in_dim(pack_grad, half_bit * half_len, half_len, 0)
    give_grad = lax.dynamic_slice_in_dim(pack_grad, (1 - half_bit) * half_len, half_len, 0)
    give_grad, grad_qkv, pack_in = lax.optimization_barrier((give_grad, grad_qkv, pack_in))
    got_grad = swapped(give_grad, "narrow", 0)
    input_grad = jnp.where(
        half_bit == 0,
        jnp.concatenate([keep_grad, got_grad]),
        jnp.concatenate([got_grad, keep_grad]),
    )
    qkv_wsum = contract_rows(pack_in, grad_qkv)
    qkv_bsum = jnp.sum(grad_qkv.astype(jnp.float32), axis=0).reshape(3, D)
    late = jnp.concatenate(
        [
            qkv_wsum.reshape(total, share, 3 * D).astype(jnp.bfloat16),
            qkv_bsum.T.reshape(total, share, 3).astype(jnp.bfloat16),
            early.astype(jnp.bfloat16),
        ],
        axis=2,
    )
    late_mine = scatter_sum_all(late)
    early_mine = late_mine[:, 3 * D + 3 :]
    query_wgrad = late_mine[:, :D]
    key_wgrad = late_mine[:, D : 2 * D]
    value_wgrad = late_mine[:, 2 * D : 3 * D]
    query_bgrad = late_mine[:, 3 * D]
    key_bgrad = late_mine[:, 3 * D + 1]
    value_bgrad = late_mine[:, 3 * D + 2]
    output_wgrad = early_mine[:, :D]
    output_bgrad = early_mine[:, D]
    attn_ggrad = early_mine[:, D + 1]
    attn_sgrad = early_mine[:, D + 2]
    outer_bgrad = early_mine[:, D + 3]
    ffn_ggrad = early_mine[:, D + 4]
    ffn_sgrad = early_mine[:, D + 5]
    return (
        layer_out,
        input_grad,
        query_wgrad,
        query_bgrad,
        key_wgrad,
        key_bgrad,
        value_wgrad,
        value_bgrad,
        output_wgrad,
        output_bgrad,
        attn_ggrad,
        attn_sgrad,
        inner_wgrad,
        inner_bgrad,
        outer_wgrad,
        outer_bgrad,
        ffn_ggrad,
        ffn_sgrad,
    )


def solution(mesh):
    return jax.shard_map(
        local,
        mesh=mesh,
        in_specs=(
            P(("wide", "narrow"), None),
            P("wide", None),
            P(("wide", "narrow"), None),
            P(("wide", "narrow")),
            P(("wide", "narrow"), None),
            P(("wide", "narrow")),
            P(("wide", "narrow"), None),
            P(("wide", "narrow")),
            P(("wide", "narrow"), None),
            P(("wide", "narrow")),
            P(("wide", "narrow")),
            P(("wide", "narrow")),
            P("wide", "narrow"),
            P(("narrow", "wide")),
            P("narrow", "wide"),
            P(("wide", "narrow")),
            P(("wide", "narrow")),
            P(("wide", "narrow")),
            P(("wide", "narrow"), None),
        ),
        out_specs=(
            P(("wide", "narrow"), None),
            P(("wide", "narrow"), None),
            P(("wide", "narrow"), None),
            P(("wide", "narrow")),
            P(("wide", "narrow"), None),
            P(("wide", "narrow")),
            P(("wide", "narrow"), None),
            P(("wide", "narrow")),
            P(("wide", "narrow"), None),
            P(("wide", "narrow")),
            P(("wide", "narrow")),
            P(("wide", "narrow")),
            P("wide", "narrow"),
            P(("narrow", "wide")),
            P("narrow", "wide"),
            P(("wide", "narrow")),
            P(("wide", "narrow")),
            P(("wide", "narrow")),
        ),
        check_vma=False,
    )
```

```python
import jax
import jax.numpy as jnp
from jax import lax
from jax.sharding import PartitionSpec as P

D = 768
HEADS = 12
HEAD_DIM = 64

ALL = ("wide", "narrow")
layer_eps = 1e-12
masked_score = -1e30


def swapped(shard, axis, bit):
    return lax.ppermute(shard, axis, [(i, i ^ 1 << bit) for i in range(lax.axis_size(axis))])


def part_orders(total, narrow_n, parts):
    bits = total.bit_length() - 1
    core_bit = narrow_n.bit_length() - 1
    narrow_bits = list(range(core_bit))
    wide_bits = [b for b in reversed(range(core_bit + 1, bits))]
    orders = []
    for p in range(parts):
        k = p % max(1, len(wide_bits))
        orders.append(narrow_bits + wide_bits[k:] + wide_bits[:k] + [core_bit])
    return orders


def is_pow2(n):
    return n & (n - 1) == 0


def column_splits(cols, parts):
    tiles = -(-cols // 128)
    parts = max(1, min(parts, tiles))
    edges = [min(cols, (tiles * i // parts) * 128) for i in range(parts)] + [cols]
    return [(a, b) for a, b in zip(edges[:-1], edges[1:]) if b > a]


def doubling_gather(shard, order, total):
    me = lax.axis_index(ALL)
    cur = shard
    for b in order:
        other = lax.ppermute(cur, ALL, [(i, i ^ (1 << b)) for i in range(total)])
        bit = (me >> b) & 1
        pick = (jnp.arange(2) == bit).reshape((2,) + (1,) * cur.ndim)
        cur = jnp.where(pick, cur[None], other[None])
    k = len(order)
    perm = [k - 1 - order.index(b) for b in reversed(range(k))]
    cur = cur.transpose(perm + list(range(k, cur.ndim)))
    return cur.reshape((total,) + shard.shape)


def gather_all(shard, parts=3):
    total = lax.axis_size("wide") * lax.axis_size("narrow")
    narrow_n = lax.axis_size("narrow")
    if not (is_pow2(total) and is_pow2(narrow_n)):
        return lax.all_gather(shard, ALL, axis=0, tiled=False)
    splits = column_splits(shard.shape[-1], parts)
    orders = part_orders(total, narrow_n, len(splits))
    pieces = [
        doubling_gather(shard[..., a:b], order, total) for (a, b), order in zip(splits, orders)
    ]
    return jnp.concatenate(pieces, axis=-1)


def halving_scatter(parts_in, order, total):
    me = lax.axis_index(ALL)
    nbits = total.bit_length() - 1
    cur = parts_in.reshape((2,) * nbits + parts_in.shape[1:])
    axes = list(reversed(range(nbits)))
    for b in order:
        a = axes.index(b)
        bit = (me >> b) & 1
        mine = lax.dynamic_index_in_dim(cur, bit, axis=a, keepdims=False)
        theirs = lax.dynamic_index_in_dim(cur, 1 - bit, axis=a, keepdims=False)
        got = lax.ppermute(
            theirs.astype(jnp.bfloat16), ALL, [(i, i ^ (1 << b)) for i in range(total)]
        )
        cur = mine.astype(jnp.float32) + got.astype(jnp.float32)
        axes.pop(a)
    return cur


def scatter_sum_all(parts_in, parts=3):
    total = lax.axis_size("wide") * lax.axis_size("narrow")
    narrow_n = lax.axis_size("narrow")
    if not (is_pow2(total) and is_pow2(narrow_n)):
        return lax.psum_scatter(
            parts_in.astype(jnp.bfloat16), ALL, scatter_dimension=0, tiled=False
        ).astype(jnp.float32)
    splits = column_splits(parts_in.shape[-1], parts)
    orders = part_orders(total, narrow_n, len(splits))
    pieces = [
        halving_scatter(parts_in[..., a:b], list(reversed(order)), total)
        for (a, b), order in zip(splits, orders)
    ]
    return jnp.concatenate(pieces, axis=-1)


def narrow_gather(rows):
    n = lax.axis_size("narrow")
    if n != 2:
        return lax.all_gather(rows, "narrow", axis=0, tiled=True)
    other = swapped(rows, "narrow", 0)
    first = lax.axis_index("narrow") == 0
    return jnp.where(first, jnp.concatenate([rows, other]), jnp.concatenate([other, rows]))


def narrow_scatter_sum(part):
    n = lax.axis_size("narrow")
    if n != 2:
        return lax.psum_scatter(
            part.astype(jnp.bfloat16), "narrow", scatter_dimension=0, tiled=True
        ).astype(jnp.float32)
    rows = part.shape[0] // 2
    me = lax.axis_index("narrow")
    mine = lax.dynamic_slice_in_dim(part, me * rows, rows, 0)
    theirs = lax.dynamic_slice_in_dim(part, (1 - me) * rows, rows, 0)
    return mine + swapped(theirs.astype(jnp.bfloat16), "narrow", 0).astype(jnp.float32)


def layer_norm(values, gain_vec, shift_vec):
    center = values - jnp.mean(values, axis=-1, keepdims=True)
    spread = jnp.mean(center * center, axis=-1, keepdims=True)
    return center * lax.rsqrt(spread + layer_eps) * gain_vec + shift_vec


def gelu_exact(values):
    return jax.nn.gelu(values, approximate=False)


def rotary_tables(doc_row):
    places = jnp.arange(doc_row.shape[0], dtype=jnp.int32)
    before = jnp.sum((doc_row[None, :] < doc_row[:, None]).astype(jnp.int32), axis=1)
    position = (places - before).astype(jnp.float32)
    frequency = 10000.0 ** (-2.0 * jnp.arange(HEAD_DIM // 2, dtype=jnp.float32) / HEAD_DIM)
    angles = position[:, None] * frequency[None, :]
    return (jnp.cos(angles), jnp.sin(angles))


def rotate(values, cosine, sine_tab):
    half_dim = values.shape[-1] // 2
    first_half = values[..., :half_dim]
    second = values[..., half_dim:]
    return jnp.concatenate(
        [first_half * cosine - second * sine_tab, second * cosine + first_half * sine_tab], axis=-1
    )


def unrotate(values, cosine, sine_tab):
    half_dim = values.shape[-1] // 2
    first_half = values[..., :half_dim]
    second = values[..., half_dim:]
    return jnp.concatenate(
        [first_half * cosine + second * sine_tab, second * cosine - first_half * sine_tab], axis=-1
    )


def contract_rows(left_op, right_op):
    return lax.dot_general(
        left_op, right_op, (((0,), (0,)), ((), ())), preferred_element_type=jnp.float32
    )


def contract_cols(left_op, right_op):
    return lax.dot_general(
        left_op, right_op, (((1,), (1,)), ((), ())), preferred_element_type=jnp.float32
    )


def score_block(query_rot, key_rot, query_docs, key_docs):
    scores = jnp.einsum(
        "pqhd,pkhd->phqk", query_rot, key_rot, preferred_element_type=jnp.float32
    ) * HEAD_DIM ** (-0.5)
    same_doc = query_docs[:, :, None] == key_docs[:, None, :]
    return jnp.where(same_doc[:, None], scores, masked_score)


def attend(query_rot, key_rot, value_low, query_docs, key_docs):
    scores = score_block(query_rot, key_rot, query_docs, key_docs)
    row_peak = jnp.max(scores, axis=-1, keepdims=True)
    exponent = jnp.exp(scores - row_peak)
    totals = jnp.sum(exponent, axis=-1, keepdims=True)
    probability = (exponent / totals).astype(jnp.bfloat16)
    mixed_out = jnp.einsum(
        "phqk,pkhd->pqhd", probability, value_low, preferred_element_type=jnp.float32
    )
    return (mixed_out, row_peak + jnp.log(totals))


def attend_back(query_rot, key_rot, value_low, query_docs, key_docs, logsum, grad_mixed):
    probability = jnp.exp(score_block(query_rot, key_rot, query_docs, key_docs) - logsum)
    grad_values = jnp.einsum(
        "phqk,pqhd->pkhd",
        probability.astype(jnp.bfloat16),
        grad_mixed,
        preferred_element_type=jnp.float32,
    )
    grad_probs = jnp.einsum(
        "pqhd,pkhd->phqk", grad_mixed, value_low, preferred_element_type=jnp.float32
    )
    inner_sum = jnp.sum(probability * grad_probs, axis=-1, keepdims=True)
    grad_scores = (probability * (grad_probs - inner_sum)).astype(jnp.bfloat16)
    grad_query = jnp.einsum(
        "phqk,pkhd->pqhd", grad_scores, key_rot, preferred_element_type=jnp.float32
    ) * HEAD_DIM ** (-0.5)
    grad_keys = jnp.einsum(
        "phqk,pqhd->pkhd", grad_scores, query_rot, preferred_element_type=jnp.float32
    ) * HEAD_DIM ** (-0.5)
    return (grad_query, grad_keys, grad_values)


def ffn_forward(rows, inner_cols, inner_offset, outer_cols):
    inner_pre = jnp.dot(rows, inner_cols, preferred_element_type=jnp.float32) + inner_offset
    act_value, gelu_pull = jax.vjp(gelu_exact, inner_pre)
    act_low = act_value.astype(jnp.bfloat16)
    return act_low, gelu_pull, contract_cols(act_low, outer_cols)


def ffn_backward(grads, gelu_pull, inner_cols, outer_cols):
    grad_act = jnp.dot(grads, outer_cols, preferred_element_type=jnp.float32)
    grad_inner = gelu_pull(grad_act)[0].astype(jnp.bfloat16)
    return grad_inner, contract_cols(grad_inner, inner_cols)


def local(
    layer_in,
    doc_ids,
    query_weight,
    query_bias,
    key_weight,
    key_bias,
    value_weight,
    value_bias,
    output_weight,
    output_bias,
    attn_gain,
    attn_shift,
    inner_weight,
    inner_bias,
    outer_weight,
    outer_bias,
    ffn_gain,
    ffn_shift,
    cotangent,
):
    wide_n = lax.axis_size("wide")
    narrow_n = lax.axis_size("narrow")
    total = wide_n * narrow_n
    share = query_weight.shape[0]
    small_list = (
        query_bias,
        key_bias,
        value_bias,
        output_bias,
        attn_gain,
        attn_shift,
        outer_bias,
        ffn_gain,
        ffn_shift,
    )
    small = jnp.stack(small_list, axis=1)
    small = jnp.pad(small, ((0, 0), (0, 128 - len(small_list))))
    shard = jnp.concatenate([query_weight, key_weight, value_weight, output_weight, small], axis=1)
    full = gather_all(shard).reshape(total * share, shard.shape[1])
    qkv_full = full[:, : 3 * D]
    output_full = full[:, 3 * D : 4 * D]
    vecs = full[:, 4 * D :].astype(jnp.float32)
    (
        query_offset,
        key_offset,
        value_offset,
        output_offset,
        attn_scale,
        attn_offset,
        outer_offset,
        ffn_scale,
        ffn_offset,
    ) = [vecs[:, i] for i in range(len(small_list))]
    qkv_offset = jnp.concatenate([query_offset, key_offset, value_offset])

    ffn_rows, ffn_cols = inner_weight.shape
    bias_n = inner_bias.shape[0]
    bias_k = -(-bias_n // ffn_rows)
    bias_rows = jnp.pad(inner_bias, (0, ffn_rows * bias_k - bias_n)).reshape(ffn_rows, bias_k)
    ffn_shard = jnp.concatenate([inner_weight, outer_weight.T, bias_rows], axis=1)
    ffn_shard, full = lax.optimization_barrier((ffn_shard, full))
    ffn_all = lax.all_gather(ffn_shard, "wide", axis=0, tiled=True)
    inner_cols = ffn_all[:, :ffn_cols]
    outer_cols = ffn_all[:, ffn_cols : 2 * ffn_cols]
    inner_offset = ffn_all[:, 2 * ffn_cols :].reshape(wide_n, ffn_rows * bias_k)[:, :bias_n]
    inner_offset = inner_offset.reshape(-1).astype(jnp.float32)

    rows_dev = layer_in.shape[0]
    half_len = doc_ids.shape[1] // 2
    pack_count = rows_dev // half_len
    narrow_place = lax.axis_index("narrow")
    half_bit = narrow_place % 2
    pair_slot = narrow_place // 2
    pack_docs = lax.dynamic_slice_in_dim(doc_ids, pair_slot * pack_count, pack_count, 0)
    my_docs = lax.dynamic_slice_in_dim(pack_docs, half_bit, 1, 0)
    cosine, sine_tab = jax.vmap(rotary_tables)(my_docs)
    cosine = cosine[:, :, None, :]
    sine_tab = sine_tab[:, :, None, :]

    def to_pack(rows):
        keep = lax.dynamic_slice_in_dim(rows, half_bit * half_len, half_len, 0)
        give = lax.dynamic_slice_in_dim(rows, (1 - half_bit) * half_len, half_len, 0)
        got = swapped(give, "narrow", 0)
        return jnp.where(
            half_bit == 0, jnp.concatenate([keep, got]), jnp.concatenate([got, keep])
        )

    def from_pack(rows):
        keep = lax.dynamic_slice_in_dim(rows, half_bit * half_len, half_len, 0)
        give = lax.dynamic_slice_in_dim(rows, (1 - half_bit) * half_len, half_len, 0)
        got = swapped(give, "narrow", 0)
        return jnp.where(
            half_bit == 0, jnp.concatenate([keep, got]), jnp.concatenate([got, keep])
        )

    pack_in = to_pack(layer_in)
    pack_cot = to_pack(cotangent)

    def heads_of(values):
        return values.reshape(1, rows_dev, HEADS, HEAD_DIM)

    qkv = jnp.dot(pack_in, qkv_full, preferred_element_type=jnp.float32) + qkv_offset
    query_rot = rotate(heads_of(qkv[:, :D]), cosine, sine_tab).astype(jnp.bfloat16)
    key_rot = rotate(heads_of(qkv[:, D : 2 * D]), cosine, sine_tab).astype(jnp.bfloat16)
    value_low = heads_of(qkv[:, 2 * D :]).astype(jnp.bfloat16)
    mixed_out, logsum = attend(query_rot, key_rot, value_low, my_docs, my_docs)
    mixed_low = mixed_out.reshape(rows_dev, D).astype(jnp.bfloat16)
    attn_out = jnp.dot(mixed_low, output_full, preferred_element_type=jnp.float32) + output_offset
    res_one = pack_in.astype(jnp.float32) + attn_out
    norm_one, norm_pull = jax.vjp(layer_norm, res_one, attn_scale, attn_offset)
    norm_low = norm_one.astype(jnp.bfloat16)

    if narrow_n == 2:
        far_rows = swapped(norm_low, "narrow", 0)
        own_act, own_pull, own_part = ffn_forward(norm_low, inner_cols, inner_offset, outer_cols)
        far_act, far_pull, far_part = ffn_forward(far_rows, inner_cols, inner_offset, outer_cols)
        outer_sum = own_part + swapped(far_part.astype(jnp.bfloat16), "narrow", 0).astype(
            jnp.float32
        )
    else:
        group_rows = lax.all_gather(norm_low, "narrow", axis=0, tiled=True)
        all_act, all_pull, all_part = ffn_forward(group_rows, inner_cols, inner_offset, outer_cols)
        outer_sum = narrow_scatter_sum(all_part)
    outer_out = outer_sum + outer_offset
    res_two = norm_one + outer_out
    pack_out, ffn_pull = jax.vjp(layer_norm, res_two, ffn_scale, ffn_offset)
    grad_two, ffn_gsum, ffn_ssum = ffn_pull(pack_cot.astype(jnp.float32))
    grad_outer = grad_two.astype(jnp.bfloat16)
    outer_bsum = jnp.sum(grad_outer.astype(jnp.float32), axis=0)
    if narrow_n == 2:
        far_grads = swapped(grad_outer, "narrow", 0)
        own_inner, own_back = ffn_backward(grad_outer, own_pull, inner_cols, outer_cols)
        far_inner, far_back = ffn_backward(far_grads, far_pull, inner_cols, outer_cols)
        grad_part = own_back + swapped(far_back.astype(jnp.bfloat16), "narrow", 0).astype(
            jnp.float32
        )
        outer_wsum_t = contract_rows(grad_outer, own_act) + contract_rows(far_grads, far_act)
        inner_wsum = contract_rows(norm_low, own_inner) + contract_rows(far_rows, far_inner)
        inner_bsum = jnp.sum(own_inner.astype(jnp.float32), axis=0) + jnp.sum(
            far_inner.astype(jnp.float32), axis=0
        )
    else:
        group_grads = lax.all_gather(grad_outer, "narrow", axis=0, tiled=True)
        all_inner, all_back = ffn_backward(group_grads, all_pull, inner_cols, outer_cols)
        grad_part = narrow_scatter_sum(all_back)
        outer_wsum_t = contract_rows(group_grads, all_act)
        inner_wsum = contract_rows(group_rows, all_inner)
        inner_bsum = jnp.sum(all_inner.astype(jnp.float32), axis=0)
    bsum_rows = jnp.pad(
        inner_bsum.reshape(wide_n, bias_n), ((0, 0), (0, ffn_rows * bias_k - bias_n))
    ).reshape(wide_n * ffn_rows, bias_k)
    ffn_sums = jnp.concatenate([inner_wsum, outer_wsum_t, bsum_rows], axis=1).astype(jnp.bfloat16)
    ffn_mine = lax.psum_scatter(ffn_sums, "wide", scatter_dimension=0, tiled=True)
    ffn_mine = ffn_mine.astype(jnp.float32)
    inner_wgrad = ffn_mine[:, :ffn_cols]
    outer_wgrad = ffn_mine[:, ffn_cols : 2 * ffn_cols].T
    inner_bgrad = ffn_mine[:, 2 * ffn_cols :].reshape(-1)[:bias_n]

    pack_out, grad_part = lax.optimization_barrier((pack_out, grad_part))
    layer_out = from_pack(pack_out)
    grad_norm = grad_two + grad_part
    grad_one, attn_gsum, attn_ssum = norm_pull(grad_norm)
    grad_attn = grad_one.astype(jnp.bfloat16)
    output_bsum = jnp.sum(grad_attn.astype(jnp.float32), axis=0)
    output_wsum = contract_rows(mixed_low, grad_attn)
    early_small = jnp.stack(
        [output_bsum, attn_gsum, attn_ssum, outer_bsum, ffn_gsum, ffn_ssum], axis=1
    )
    early = jnp.concatenate(
        [output_wsum.reshape(total, share, D), early_small.reshape(total, share, -1)], axis=2
    )

    grad_mixed = heads_of(contract_cols(grad_attn, output_full).astype(jnp.bfloat16))
    grad_qrot, grad_krot, grad_values = attend_back(
        query_rot, key_rot, value_low, my_docs, my_docs, logsum, grad_mixed
    )
    grad_values = grad_values.astype(jnp.bfloat16)
    grad_query = unrotate(grad_qrot, cosine, sine_tab).astype(jnp.bfloat16)
    grad_keys = unrotate(grad_krot, cosine, sine_tab).astype(jnp.bfloat16)
    grad_qkv = jnp.concatenate(
        [
            grad_query.reshape(rows_dev, D),
            grad_keys.reshape(rows_dev, D),
            grad_values.reshape(rows_dev, D),
        ],
        axis=1,
    )
    pack_grad = grad_one + contract_cols(grad_qkv, qkv_full)
    keep_grad = lax.dynamic_slice_in_dim(pack_grad, half_bit * half_len, half_len, 0)
    give_grad = lax.dynamic_slice_in_dim(pack_grad, (1 - half_bit) * half_len, half_len, 0)
    give_grad, grad_qkv, pack_in = lax.optimization_barrier((give_grad, grad_qkv, pack_in))
    got_grad = swapped(give_grad, "narrow", 0)
    input_grad = jnp.where(
        half_bit == 0,
        jnp.concatenate([keep_grad, got_grad]),
        jnp.concatenate([got_grad, keep_grad]),
    )
    qkv_wsum = contract_rows(pack_in, grad_qkv)
    qkv_bsum = jnp.sum(grad_qkv.astype(jnp.float32), axis=0).reshape(3, D)
    late = jnp.concatenate(
        [
            qkv_wsum.reshape(total, share, 3 * D).astype(jnp.bfloat16),
            qkv_bsum.T.reshape(total, share, 3).astype(jnp.bfloat16),
            early.astype(jnp.bfloat16),
        ],
        axis=2,
    )
    late_mine = scatter_sum_all(late)
    early_mine = late_mine[:, 3 * D + 3 :]
    query_wgrad = late_mine[:, :D]
    key_wgrad = late_mine[:, D : 2 * D]
    value_wgrad = late_mine[:, 2 * D : 3 * D]
    query_bgrad = late_mine[:, 3 * D]
    key_bgrad = late_mine[:, 3 * D + 1]
    value_bgrad = late_mine[:, 3 * D + 2]
    output_wgrad = early_mine[:, :D]
    output_bgrad = early_mine[:, D]
    attn_ggrad = early_mine[:, D + 1]
    attn_sgrad = early_mine[:, D + 2]
    outer_bgrad = early_mine[:, D + 3]
    ffn_ggrad = early_mine[:, D + 4]
    ffn_sgrad = early_mine[:, D + 5]
    return (
        layer_out,
        input_grad,
        query_wgrad,
        query_bgrad,
        key_wgrad,
        key_bgrad,
        value_wgrad,
        value_bgrad,
        output_wgrad,
        output_bgrad,
        attn_ggrad,
        attn_sgrad,
        inner_wgrad,
        inner_bgrad,
        outer_wgrad,
        outer_bgrad,
        ffn_ggrad,
        ffn_sgrad,
    )


def solution(mesh):
    return jax.shard_map(
        local,
        mesh=mesh,
        in_specs=(
            P(("wide", "narrow"), None),
            P("wide", None),
            P(("wide", "narrow"), None),
            P(("wide", "narrow")),
            P(("wide", "narrow"), None),
            P(("wide", "narrow")),
            P(("wide", "narrow"), None),
            P(("wide", "narrow")),
            P(("wide", "narrow"), None),
            P(("wide", "narrow")),
            P(("wide", "narrow")),
            P(("wide", "narrow")),
            P("wide", "narrow"),
            P(("narrow", "wide")),
            P("narrow", "wide"),
            P(("wide", "narrow")),
            P(("wide", "narrow")),
            P(("wide", "narrow")),
            P(("wide", "narrow"), None),
        ),
        out_specs=(
            P(("wide", "narrow"), None),
            P(("wide", "narrow"), None),
            P(("wide", "narrow"), None),
            P(("wide", "narrow")),
            P(("wide", "narrow"), None),
            P(("wide", "narrow")),
            P(("wide", "narrow"), None),
            P(("wide", "narrow")),
            P(("wide", "narrow"), None),
            P(("wide", "narrow")),
            P(("wide", "narrow")),
            P(("wide", "narrow")),
            P("wide", "narrow"),
            P(("narrow", "wide")),
            P("narrow", "wide"),
            P(("wide", "narrow")),
            P(("wide", "narrow")),
            P(("wide", "narrow")),
        ),
        check_vma=False,
    )
```

```python
import jax
import jax.numpy as jnp
from jax import lax
from jax.sharding import PartitionSpec as P

D = 768
HEADS = 12
HEAD_DIM = 64

ALL = ("wide", "narrow")
layer_eps = 1e-12
masked_score = -1e30


def swapped(shard, axis, bit):
    return lax.ppermute(shard, axis, [(i, i ^ 1 << bit) for i in range(lax.axis_size(axis))])


def part_orders(total, narrow_n, parts):
    bits = total.bit_length() - 1
    core_bit = narrow_n.bit_length() - 1
    narrow_bits = list(range(core_bit))
    wide_bits = [b for b in reversed(range(core_bit + 1, bits))]
    orders = []
    for p in range(parts):
        k = p % max(1, len(wide_bits))
        orders.append(narrow_bits + wide_bits[k:] + wide_bits[:k] + [core_bit])
    return orders


def is_pow2(n):
    return n & (n - 1) == 0


def column_splits(cols, parts):
    tiles = -(-cols // 128)
    parts = max(1, min(parts, tiles))
    edges = [min(cols, (tiles * i // parts) * 128) for i in range(parts)] + [cols]
    return [(a, b) for a, b in zip(edges[:-1], edges[1:]) if b > a]


def doubling_gather(shard, order, total):
    me = lax.axis_index(ALL)
    cur = shard
    for b in order:
        other = lax.ppermute(cur, ALL, [(i, i ^ (1 << b)) for i in range(total)])
        bit = (me >> b) & 1
        pick = (jnp.arange(2) == bit).reshape((2,) + (1,) * cur.ndim)
        cur = jnp.where(pick, cur[None], other[None])
    k = len(order)
    perm = [k - 1 - order.index(b) for b in reversed(range(k))]
    cur = cur.transpose(perm + list(range(k, cur.ndim)))
    return cur.reshape((total,) + shard.shape)


def gather_all(shard, parts=3):
    total = lax.axis_size("wide") * lax.axis_size("narrow")
    narrow_n = lax.axis_size("narrow")
    if not (is_pow2(total) and is_pow2(narrow_n)):
        return lax.all_gather(shard, ALL, axis=0, tiled=False)
    splits = column_splits(shard.shape[-1], parts)
    orders = part_orders(total, narrow_n, len(splits))
    pieces = [
        doubling_gather(shard[..., a:b], order, total) for (a, b), order in zip(splits, orders)
    ]
    return jnp.concatenate(pieces, axis=-1)


def halving_scatter(parts_in, order, total):
    me = lax.axis_index(ALL)
    nbits = total.bit_length() - 1
    cur = parts_in.reshape((2,) * nbits + parts_in.shape[1:])
    axes = list(reversed(range(nbits)))
    for b in order:
        a = axes.index(b)
        bit = (me >> b) & 1
        mine = lax.dynamic_index_in_dim(cur, bit, axis=a, keepdims=False)
        theirs = lax.dynamic_index_in_dim(cur, 1 - bit, axis=a, keepdims=False)
        got = lax.ppermute(
            theirs.astype(jnp.bfloat16), ALL, [(i, i ^ (1 << b)) for i in range(total)]
        )
        cur = mine.astype(jnp.float32) + got.astype(jnp.float32)
        axes.pop(a)
    return cur


def scatter_sum_all(parts_in, parts=3):
    total = lax.axis_size("wide") * lax.axis_size("narrow")
    narrow_n = lax.axis_size("narrow")
    if not (is_pow2(total) and is_pow2(narrow_n)):
        return lax.psum_scatter(
            parts_in.astype(jnp.bfloat16), ALL, scatter_dimension=0, tiled=False
        ).astype(jnp.float32)
    splits = column_splits(parts_in.shape[-1], parts)
    orders = part_orders(total, narrow_n, len(splits))
    pieces = [
        halving_scatter(parts_in[..., a:b], list(reversed(order)), total)
        for (a, b), order in zip(splits, orders)
    ]
    return jnp.concatenate(pieces, axis=-1)


def narrow_scatter_sum(part):
    n = lax.axis_size("narrow")
    if n != 2:
        return lax.psum_scatter(
            part.astype(jnp.bfloat16), "narrow", scatter_dimension=0, tiled=True
        ).astype(jnp.float32)
    rows = part.shape[0] // 2
    me = lax.axis_index("narrow")
    mine = lax.dynamic_slice_in_dim(part, me * rows, rows, 0)
    theirs = lax.dynamic_slice_in_dim(part, (1 - me) * rows, rows, 0)
    return mine + swapped(theirs.astype(jnp.bfloat16), "narrow", 0).astype(jnp.float32)


def layer_norm(values, gain_vec, shift_vec):
    center = values - jnp.mean(values, axis=-1, keepdims=True)
    spread = jnp.mean(center * center, axis=-1, keepdims=True)
    return center * lax.rsqrt(spread + layer_eps) * gain_vec + shift_vec


def gelu_exact(values):
    return jax.nn.gelu(values, approximate=False)


def rotary_tables(doc_row):
    places = jnp.arange(doc_row.shape[0], dtype=jnp.int32)
    before = jnp.sum((doc_row[None, :] < doc_row[:, None]).astype(jnp.int32), axis=1)
    position = (places - before).astype(jnp.float32)
    frequency = 10000.0 ** (-2.0 * jnp.arange(HEAD_DIM // 2, dtype=jnp.float32) / HEAD_DIM)
    angles = position[:, None] * frequency[None, :]
    return (jnp.cos(angles), jnp.sin(angles))


def rotate(values, cosine, sine_tab):
    half_dim = values.shape[-1] // 2
    first_half = values[..., :half_dim]
    second = values[..., half_dim:]
    return jnp.concatenate(
        [first_half * cosine - second * sine_tab, second * cosine + first_half * sine_tab], axis=-1
    )


def unrotate(values, cosine, sine_tab):
    half_dim = values.shape[-1] // 2
    first_half = values[..., :half_dim]
    second = values[..., half_dim:]
    return jnp.concatenate(
        [first_half * cosine + second * sine_tab, second * cosine - first_half * sine_tab], axis=-1
    )


def contract_rows(left_op, right_op):
    return lax.dot_general(
        left_op, right_op, (((0,), (0,)), ((), ())), preferred_element_type=jnp.float32
    )


def contract_cols(left_op, right_op):
    return lax.dot_general(
        left_op, right_op, (((1,), (1,)), ((), ())), preferred_element_type=jnp.float32
    )


def score_block(query_rot, key_rot, query_docs, key_docs):
    scores = jnp.einsum(
        "pqhd,pkhd->phqk", query_rot, key_rot, preferred_element_type=jnp.float32
    ) * HEAD_DIM ** (-0.5)
    same_doc = query_docs[:, :, None] == key_docs[:, None, :]
    return jnp.where(same_doc[:, None], scores, masked_score)


def attend(query_rot, key_rot, value_low, query_docs, key_docs):
    scores = score_block(query_rot, key_rot, query_docs, key_docs)
    row_peak = jnp.max(scores, axis=-1, keepdims=True)
    exponent = jnp.exp(scores - row_peak)
    totals = jnp.sum(exponent, axis=-1, keepdims=True)
    probability = (exponent / totals).astype(jnp.bfloat16)
    mixed_out = jnp.einsum(
        "phqk,pkhd->pqhd", probability, value_low, preferred_element_type=jnp.float32
    )
    return (mixed_out, row_peak + jnp.log(totals))


def attend_back(query_rot, key_rot, value_low, query_docs, key_docs, logsum, grad_mixed):
    probability = jnp.exp(score_block(query_rot, key_rot, query_docs, key_docs) - logsum)
    grad_values = jnp.einsum(
        "phqk,pqhd->pkhd",
        probability.astype(jnp.bfloat16),
        grad_mixed,
        preferred_element_type=jnp.float32,
    )
    grad_probs = jnp.einsum(
        "pqhd,pkhd->phqk", grad_mixed, value_low, preferred_element_type=jnp.float32
    )
    inner_sum = jnp.sum(probability * grad_probs, axis=-1, keepdims=True)
    grad_scores = (probability * (grad_probs - inner_sum)).astype(jnp.bfloat16)
    grad_query = jnp.einsum(
        "phqk,pkhd->pqhd", grad_scores, key_rot, preferred_element_type=jnp.float32
    ) * HEAD_DIM ** (-0.5)
    grad_keys = jnp.einsum(
        "phqk,pqhd->pkhd", grad_scores, query_rot, preferred_element_type=jnp.float32
    ) * HEAD_DIM ** (-0.5)
    return (grad_query, grad_keys, grad_values)


def ffn_forward(rows, inner_cols, inner_offset, outer_cols):
    inner_pre = jnp.dot(rows, inner_cols, preferred_element_type=jnp.float32) + inner_offset
    act_value, gelu_pull = jax.vjp(gelu_exact, inner_pre)
    act_low = act_value.astype(jnp.bfloat16)
    return act_low, gelu_pull, contract_cols(act_low, outer_cols)


def ffn_backward(grads, gelu_pull, inner_cols, outer_cols):
    grad_act = jnp.dot(grads, outer_cols, preferred_element_type=jnp.float32)
    grad_inner = gelu_pull(grad_act)[0].astype(jnp.bfloat16)
    return grad_inner, contract_cols(grad_inner, inner_cols)


def local_body(
    layer_in,
    doc_ids,
    query_weight,
    query_bias,
    key_weight,
    key_bias,
    value_weight,
    value_bias,
    output_weight,
    output_bias,
    attn_gain,
    attn_shift,
    inner_weight,
    inner_bias,
    outer_weight,
    outer_bias,
    ffn_gain,
    ffn_shift,
    cotangent,
):
    wide_n = lax.axis_size("wide")
    narrow_n = lax.axis_size("narrow")
    total = wide_n * narrow_n
    share = query_weight.shape[0]
    small_list = (
        query_bias,
        key_bias,
        value_bias,
        output_bias,
        attn_gain,
        attn_shift,
        outer_bias,
        ffn_gain,
        ffn_shift,
    )
    small = jnp.stack(small_list, axis=1)
    small = jnp.pad(small, ((0, 0), (0, 128 - len(small_list))))
    shard = jnp.concatenate([query_weight, key_weight, value_weight, output_weight, small], axis=1)
    full = gather_all(shard).reshape(total * share, shard.shape[1])
    qkv_full = full[:, : 3 * D]
    output_full = full[:, 3 * D : 4 * D]
    vecs = full[:, 4 * D :].astype(jnp.float32)
    (
        query_offset,
        key_offset,
        value_offset,
        output_offset,
        attn_scale,
        attn_offset,
        outer_offset,
        ffn_scale,
        ffn_offset,
    ) = [vecs[:, i] for i in range(len(small_list))]
    qkv_offset = jnp.concatenate([query_offset, key_offset, value_offset])

    ffn_rows, ffn_cols = inner_weight.shape
    bias_n = inner_bias.shape[0]
    bias_k = -(-bias_n // ffn_rows)
    bias_rows = jnp.pad(inner_bias, (0, ffn_rows * bias_k - bias_n)).reshape(ffn_rows, bias_k)
    ffn_shard = jnp.concatenate([inner_weight, outer_weight.T, bias_rows], axis=1)
    ffn_shard, full = lax.optimization_barrier((ffn_shard, full))
    ffn_all = lax.all_gather(ffn_shard, "wide", axis=0, tiled=True)
    inner_cols = ffn_all[:, :ffn_cols]
    outer_cols = ffn_all[:, ffn_cols : 2 * ffn_cols]
    inner_offset = ffn_all[:, 2 * ffn_cols :].reshape(wide_n, ffn_rows * bias_k)[:, :bias_n]
    inner_offset = inner_offset.reshape(-1).astype(jnp.float32)

    rows_dev = layer_in.shape[0]
    half_len = doc_ids.shape[1] // 2
    pack_count = rows_dev // half_len
    narrow_place = lax.axis_index("narrow")
    half_bit = narrow_place % 2
    pair_slot = narrow_place // 2
    pack_docs = lax.dynamic_slice_in_dim(doc_ids, pair_slot * pack_count, pack_count, 0)
    my_docs = lax.dynamic_slice_in_dim(pack_docs, half_bit, 1, 0)
    cosine, sine_tab = jax.vmap(rotary_tables)(my_docs)
    cosine = cosine[:, :, None, :]
    sine_tab = sine_tab[:, :, None, :]

    def to_pack(rows):
        keep = lax.dynamic_slice_in_dim(rows, half_bit * half_len, half_len, 0)
        give = lax.dynamic_slice_in_dim(rows, (1 - half_bit) * half_len, half_len, 0)
        got = swapped(give, "narrow", 0)
        return jnp.where(
            half_bit == 0, jnp.concatenate([keep, got]), jnp.concatenate([got, keep])
        )

    def from_pack(rows):
        keep = lax.dynamic_slice_in_dim(rows, half_bit * half_len, half_len, 0)
        give = lax.dynamic_slice_in_dim(rows, (1 - half_bit) * half_len, half_len, 0)
        got = swapped(give, "narrow", 0)
        return jnp.where(
            half_bit == 0, jnp.concatenate([keep, got]), jnp.concatenate([got, keep])
        )

    pack_in = to_pack(layer_in)
    pack_cot = to_pack(cotangent)

    def heads_of(values):
        return values.reshape(1, rows_dev, HEADS, HEAD_DIM)

    qkv = jnp.dot(pack_in, qkv_full, preferred_element_type=jnp.float32) + qkv_offset
    query_rot = rotate(heads_of(qkv[:, :D]), cosine, sine_tab).astype(jnp.bfloat16)
    key_rot = rotate(heads_of(qkv[:, D : 2 * D]), cosine, sine_tab).astype(jnp.bfloat16)
    value_low = heads_of(qkv[:, 2 * D :]).astype(jnp.bfloat16)
    mixed_out, logsum = attend(query_rot, key_rot, value_low, my_docs, my_docs)
    mixed_low = mixed_out.reshape(rows_dev, D).astype(jnp.bfloat16)
    attn_out = jnp.dot(mixed_low, output_full, preferred_element_type=jnp.float32) + output_offset
    res_one = pack_in.astype(jnp.float32) + attn_out
    norm_one, norm_pull = jax.vjp(layer_norm, res_one, attn_scale, attn_offset)
    norm_low = norm_one.astype(jnp.bfloat16)

    if narrow_n == 2:
        far_rows = swapped(norm_low, "narrow", 0)
        own_act, own_pull, own_part = ffn_forward(norm_low, inner_cols, inner_offset, outer_cols)
        far_act, far_pull, far_part = ffn_forward(far_rows, inner_cols, inner_offset, outer_cols)
        outer_sum = own_part + swapped(far_part.astype(jnp.bfloat16), "narrow", 0).astype(
            jnp.float32
        )
    else:
        group_rows = lax.all_gather(norm_low, "narrow", axis=0, tiled=True)
        all_act, all_pull, all_part = ffn_forward(group_rows, inner_cols, inner_offset, outer_cols)
        outer_sum = narrow_scatter_sum(all_part)
    outer_out = outer_sum + outer_offset
    res_two = norm_one + outer_out
    pack_out, ffn_pull = jax.vjp(layer_norm, res_two, ffn_scale, ffn_offset)
    grad_two, ffn_gsum, ffn_ssum = ffn_pull(pack_cot.astype(jnp.float32))
    grad_outer = grad_two.astype(jnp.bfloat16)
    outer_bsum = jnp.sum(grad_outer.astype(jnp.float32), axis=0)
    if narrow_n == 2:
        far_grads = swapped(grad_outer, "narrow", 0)
        own_inner, own_back = ffn_backward(grad_outer, own_pull, inner_cols, outer_cols)
        far_inner, far_back = ffn_backward(far_grads, far_pull, inner_cols, outer_cols)
        grad_part = own_back + swapped(far_back.astype(jnp.bfloat16), "narrow", 0).astype(
            jnp.float32
        )
        outer_wsum_t = contract_rows(grad_outer, own_act) + contract_rows(far_grads, far_act)
        inner_wsum = contract_rows(norm_low, own_inner) + contract_rows(far_rows, far_inner)
        inner_bsum = jnp.sum(own_inner.astype(jnp.float32), axis=0) + jnp.sum(
            far_inner.astype(jnp.float32), axis=0
        )
    else:
        group_grads = lax.all_gather(grad_outer, "narrow", axis=0, tiled=True)
        all_inner, all_back = ffn_backward(group_grads, all_pull, inner_cols, outer_cols)
        grad_part = narrow_scatter_sum(all_back)
        outer_wsum_t = contract_rows(group_grads, all_act)
        inner_wsum = contract_rows(group_rows, all_inner)
        inner_bsum = jnp.sum(all_inner.astype(jnp.float32), axis=0)
    bsum_rows = jnp.pad(
        inner_bsum.reshape(wide_n, bias_n), ((0, 0), (0, ffn_rows * bias_k - bias_n))
    ).reshape(wide_n * ffn_rows, bias_k)
    ffn_sums = jnp.concatenate([inner_wsum, outer_wsum_t, bsum_rows], axis=1).astype(jnp.bfloat16)
    ffn_mine = lax.psum_scatter(ffn_sums, "wide", scatter_dimension=0, tiled=True)
    ffn_mine = ffn_mine.astype(jnp.float32)
    inner_wgrad = ffn_mine[:, :ffn_cols]
    outer_wgrad = ffn_mine[:, ffn_cols : 2 * ffn_cols].T
    inner_bgrad = ffn_mine[:, 2 * ffn_cols :].reshape(-1)[:bias_n]

    pack_out, grad_part = lax.optimization_barrier((pack_out, grad_part))
    layer_out = from_pack(pack_out)
    grad_norm = grad_two + grad_part
    grad_one, attn_gsum, attn_ssum = norm_pull(grad_norm)
    grad_attn = grad_one.astype(jnp.bfloat16)
    output_bsum = jnp.sum(grad_attn.astype(jnp.float32), axis=0)
    output_wsum = contract_rows(mixed_low, grad_attn)
    early_small = jnp.stack(
        [output_bsum, attn_gsum, attn_ssum, outer_bsum, ffn_gsum, ffn_ssum], axis=1
    )
    early = jnp.concatenate(
        [output_wsum.reshape(total, share, D), early_small.reshape(total, share, -1)], axis=2
    )

    grad_mixed = heads_of(contract_cols(grad_attn, output_full).astype(jnp.bfloat16))
    grad_qrot, grad_krot, grad_values = attend_back(
        query_rot, key_rot, value_low, my_docs, my_docs, logsum, grad_mixed
    )
    grad_values = grad_values.astype(jnp.bfloat16)
    grad_query = unrotate(grad_qrot, cosine, sine_tab).astype(jnp.bfloat16)
    grad_keys = unrotate(grad_krot, cosine, sine_tab).astype(jnp.bfloat16)
    grad_qkv = jnp.concatenate(
        [
            grad_query.reshape(rows_dev, D),
            grad_keys.reshape(rows_dev, D),
            grad_values.reshape(rows_dev, D),
        ],
        axis=1,
    )
    pack_grad = grad_one + contract_cols(grad_qkv, qkv_full)
    keep_grad = lax.dynamic_slice_in_dim(pack_grad, half_bit * half_len, half_len, 0)
    give_grad = lax.dynamic_slice_in_dim(pack_grad, (1 - half_bit) * half_len, half_len, 0)
    give_grad, grad_qkv, pack_in = lax.optimization_barrier((give_grad, grad_qkv, pack_in))
    got_grad = swapped(give_grad, "narrow", 0)
    input_grad = jnp.where(
        half_bit == 0,
        jnp.concatenate([keep_grad, got_grad]),
        jnp.concatenate([got_grad, keep_grad]),
    )
    qkv_wsum = contract_rows(pack_in, grad_qkv)
    qkv_bsum = jnp.sum(grad_qkv.astype(jnp.float32), axis=0).reshape(3, D)
    late = jnp.concatenate(
        [
            qkv_wsum.reshape(total, share, 3 * D).astype(jnp.bfloat16),
            qkv_bsum.T.reshape(total, share, 3).astype(jnp.bfloat16),
            early.astype(jnp.bfloat16),
        ],
        axis=2,
    )
    late_mine = scatter_sum_all(late)
    early_mine = late_mine[:, 3 * D + 3 :]
    query_wgrad = late_mine[:, :D]
    key_wgrad = late_mine[:, D : 2 * D]
    value_wgrad = late_mine[:, 2 * D : 3 * D]
    query_bgrad = late_mine[:, 3 * D]
    key_bgrad = late_mine[:, 3 * D + 1]
    value_bgrad = late_mine[:, 3 * D + 2]
    output_wgrad = early_mine[:, :D]
    output_bgrad = early_mine[:, D]
    attn_ggrad = early_mine[:, D + 1]
    attn_sgrad = early_mine[:, D + 2]
    outer_bgrad = early_mine[:, D + 3]
    ffn_ggrad = early_mine[:, D + 4]
    ffn_sgrad = early_mine[:, D + 5]
    return (
        layer_out,
        input_grad,
        query_wgrad,
        query_bgrad,
        key_wgrad,
        key_bgrad,
        value_wgrad,
        value_bgrad,
        output_wgrad,
        output_bgrad,
        attn_ggrad,
        attn_sgrad,
        inner_wgrad,
        inner_bgrad,
        outer_wgrad,
        outer_bgrad,
        ffn_ggrad,
        ffn_sgrad,
    )


def solution(mesh):
    return shard_solution(mesh)


def shard_solution(mesh):
    return jax.shard_map(
        local_body,
        mesh=mesh,
        in_specs=(
            P(("wide", "narrow"), None),
            P("wide", None),
            P(("wide", "narrow"), None),
            P(("wide", "narrow")),
            P(("wide", "narrow"), None),
            P(("wide", "narrow")),
            P(("wide", "narrow"), None),
            P(("wide", "narrow")),
            P(("wide", "narrow"), None),
            P(("wide", "narrow")),
            P(("wide", "narrow")),
            P(("wide", "narrow")),
            P("wide", "narrow"),
            P(("narrow", "wide")),
            P("narrow", "wide"),
            P(("wide", "narrow")),
            P(("wide", "narrow")),
            P(("wide", "narrow")),
            P(("wide", "narrow"), None),
        ),
        out_specs=(
            P(("wide", "narrow"), None),
            P(("wide", "narrow"), None),
            P(("wide", "narrow"), None),
            P(("wide", "narrow")),
            P(("wide", "narrow"), None),
            P(("wide", "narrow")),
            P(("wide", "narrow"), None),
            P(("wide", "narrow")),
            P(("wide", "narrow"), None),
            P(("wide", "narrow")),
            P(("wide", "narrow")),
            P(("wide", "narrow")),
            P("wide", "narrow"),
            P(("narrow", "wide")),
            P("narrow", "wide"),
            P(("wide", "narrow")),
            P(("wide", "narrow")),
            P(("wide", "narrow")),
        ),
        check_vma=False,
    )
```

```python
import jax
import jax.numpy as jnp
from jax import lax
from jax.sharding import PartitionSpec as P

D = 768
HEADS = 12
HEAD_DIM = 64

ALL = ("wide", "narrow")
layer_eps = 1e-12
masked_score = -1e30


def swapped(shard, axis, bit):
    return lax.ppermute(shard, axis, [(i, i ^ 1 << bit) for i in range(lax.axis_size(axis))])


def part_orders(total, narrow_n, parts):
    bits = total.bit_length() - 1
    core_bit = narrow_n.bit_length() - 1
    narrow_bits = list(range(core_bit))
    wide_bits = [b for b in reversed(range(core_bit + 1, bits))]
    orders = []
    for p in range(parts):
        k = p % max(1, len(wide_bits))
        orders.append(narrow_bits + wide_bits[k:] + wide_bits[:k] + [core_bit])
    return orders


def is_pow2(n):
    return n & (n - 1) == 0


def column_splits(cols, parts):
    tiles = -(-cols // 128)
    parts = max(1, min(parts, tiles))
    edges = [min(cols, (tiles * i // parts) * 128) for i in range(parts)] + [cols]
    return [(a, b) for a, b in zip(edges[:-1], edges[1:]) if b > a]


def doubling_gather(shard, order, total):
    me = lax.axis_index(ALL)
    cur = shard
    for b in order:
        other = lax.ppermute(cur, ALL, [(i, i ^ (1 << b)) for i in range(total)])
        bit = (me >> b) & 1
        pick = (jnp.arange(2) == bit).reshape((2,) + (1,) * cur.ndim)
        cur = jnp.where(pick, cur[None], other[None])
    k = len(order)
    perm = [k - 1 - order.index(b) for b in reversed(range(k))]
    cur = cur.transpose(perm + list(range(k, cur.ndim)))
    return cur.reshape((total,) + shard.shape)


def gather_all(shard, parts=3):
    total = lax.axis_size("wide") * lax.axis_size("narrow")
    narrow_n = lax.axis_size("narrow")
    if not (is_pow2(total) and is_pow2(narrow_n)):
        return lax.all_gather(shard, ALL, axis=0, tiled=False)
    splits = column_splits(shard.shape[-1], parts)
    orders = part_orders(total, narrow_n, len(splits))
    pieces = [
        doubling_gather(shard[..., a:b], order, total) for (a, b), order in zip(splits, orders)
    ]
    return jnp.concatenate(pieces, axis=-1)


def halving_scatter(parts_in, order, total):
    me = lax.axis_index(ALL)
    nbits = total.bit_length() - 1
    cur = parts_in.reshape((2,) * nbits + parts_in.shape[1:])
    axes = list(reversed(range(nbits)))
    for b in order:
        a = axes.index(b)
        bit = (me >> b) & 1
        mine = lax.dynamic_index_in_dim(cur, bit, axis=a, keepdims=False)
        theirs = lax.dynamic_index_in_dim(cur, 1 - bit, axis=a, keepdims=False)
        got = lax.ppermute(
            theirs.astype(jnp.bfloat16), ALL, [(i, i ^ (1 << b)) for i in range(total)]
        )
        cur = mine.astype(jnp.float32) + got.astype(jnp.float32)
        axes.pop(a)
    return cur


def scatter_sum_all(parts_in, parts=3):
    total = lax.axis_size("wide") * lax.axis_size("narrow")
    narrow_n = lax.axis_size("narrow")
    if not (is_pow2(total) and is_pow2(narrow_n)):
        return lax.psum_scatter(
            parts_in.astype(jnp.bfloat16), ALL, scatter_dimension=0, tiled=False
        ).astype(jnp.float32)
    splits = column_splits(parts_in.shape[-1], parts)
    orders = part_orders(total, narrow_n, len(splits))
    pieces = [
        halving_scatter(parts_in[..., a:b], list(reversed(order)), total)
        for (a, b), order in zip(splits, orders)
    ]
    return jnp.concatenate(pieces, axis=-1)


def narrow_gather(rows):
    n = lax.axis_size("narrow")
    if n != 2:
        return lax.all_gather(rows, "narrow", axis=0, tiled=True)
    other = swapped(rows, "narrow", 0)
    first = lax.axis_index("narrow") == 0
    return jnp.where(first, jnp.concatenate([rows, other]), jnp.concatenate([other, rows]))


def narrow_scatter_sum(part):
    n = lax.axis_size("narrow")
    if n != 2:
        return lax.psum_scatter(
            part.astype(jnp.bfloat16), "narrow", scatter_dimension=0, tiled=True
        ).astype(jnp.float32)
    rows = part.shape[0] // 2
    me = lax.axis_index("narrow")
    mine = lax.dynamic_slice_in_dim(part, me * rows, rows, 0)
    theirs = lax.dynamic_slice_in_dim(part, (1 - me) * rows, rows, 0)
    return mine + swapped(theirs.astype(jnp.bfloat16), "narrow", 0).astype(jnp.float32)


def layer_norm(values, gain_vec, shift_vec):
    center = values - jnp.mean(values, axis=-1, keepdims=True)
    spread = jnp.mean(center * center, axis=-1, keepdims=True)
    return center * lax.rsqrt(spread + layer_eps) * gain_vec + shift_vec


def gelu_exact(values):
    return jax.nn.gelu(values, approximate=False)


def rotary_tables(doc_row):
    places = jnp.arange(doc_row.shape[0], dtype=jnp.int32)
    before = jnp.sum((doc_row[None, :] < doc_row[:, None]).astype(jnp.int32), axis=1)
    position = (places - before).astype(jnp.float32)
    frequency = 10000.0 ** (-2.0 * jnp.arange(HEAD_DIM // 2, dtype=jnp.float32) / HEAD_DIM)
    angles = position[:, None] * frequency[None, :]
    return (jnp.cos(angles), jnp.sin(angles))


def rotate(values, cosine, sine_tab):
    half_dim = values.shape[-1] // 2
    first_half = values[..., :half_dim]
    second = values[..., half_dim:]
    return jnp.concatenate(
        [first_half * cosine - second * sine_tab, second * cosine + first_half * sine_tab], axis=-1
    )


def unrotate(values, cosine, sine_tab):
    half_dim = values.shape[-1] // 2
    first_half = values[..., :half_dim]
    second = values[..., half_dim:]
    return jnp.concatenate(
        [first_half * cosine + second * sine_tab, second * cosine - first_half * sine_tab], axis=-1
    )


def contract_rows(left_op, right_op):
    return lax.dot_general(
        left_op, right_op, (((0,), (0,)), ((), ())), preferred_element_type=jnp.float32
    )


def contract_cols(left_op, right_op):
    return lax.dot_general(
        left_op, right_op, (((1,), (1,)), ((), ())), preferred_element_type=jnp.float32
    )


def score_block(query_rot, key_rot, query_docs, key_docs):
    scores = jnp.einsum(
        "pqhd,pkhd->phqk", query_rot, key_rot, preferred_element_type=jnp.float32
    ) * HEAD_DIM ** (-0.5)
    same_doc = query_docs[:, :, None] == key_docs[:, None, :]
    return jnp.where(same_doc[:, None], scores, masked_score)


def attend(query_rot, key_rot, value_low, query_docs, key_docs):
    scores = score_block(query_rot, key_rot, query_docs, key_docs)
    row_peak = jnp.max(scores, axis=-1, keepdims=True)
    exponent = jnp.exp(scores - row_peak)
    totals = jnp.sum(exponent, axis=-1, keepdims=True)
    probability = (exponent / totals).astype(jnp.bfloat16)
    mixed_out = jnp.einsum(
        "phqk,pkhd->pqhd", probability, value_low, preferred_element_type=jnp.float32
    )
    return (mixed_out, row_peak + jnp.log(totals))


def attend_back(query_rot, key_rot, value_low, query_docs, key_docs, logsum, grad_mixed):
    probability = jnp.exp(score_block(query_rot, key_rot, query_docs, key_docs) - logsum)
    grad_values = jnp.einsum(
        "phqk,pqhd->pkhd",
        probability.astype(jnp.bfloat16),
        grad_mixed,
        preferred_element_type=jnp.float32,
    )
    grad_probs = jnp.einsum(
        "pqhd,pkhd->phqk", grad_mixed, value_low, preferred_element_type=jnp.float32
    )
    inner_sum = jnp.sum(probability * grad_probs, axis=-1, keepdims=True)
    grad_scores = (probability * (grad_probs - inner_sum)).astype(jnp.bfloat16)
    grad_query = jnp.einsum(
        "phqk,pkhd->pqhd", grad_scores, key_rot, preferred_element_type=jnp.float32
    ) * HEAD_DIM ** (-0.5)
    grad_keys = jnp.einsum(
        "phqk,pqhd->pkhd", grad_scores, query_rot, preferred_element_type=jnp.float32
    ) * HEAD_DIM ** (-0.5)
    return (grad_query, grad_keys, grad_values)


def ffn_forward(rows, inner_cols, inner_offset, outer_cols):
    inner_pre = jnp.dot(rows, inner_cols, preferred_element_type=jnp.float32) + inner_offset
    act_value, gelu_pull = jax.vjp(gelu_exact, inner_pre)
    act_low = act_value.astype(jnp.bfloat16)
    return act_low, gelu_pull, contract_cols(act_low, outer_cols)


def ffn_backward(grads, gelu_pull, inner_cols, outer_cols):
    grad_act = jnp.dot(grads, outer_cols, preferred_element_type=jnp.float32)
    grad_inner = gelu_pull(grad_act)[0].astype(jnp.bfloat16)
    return grad_inner, contract_cols(grad_inner, inner_cols)


def local(
    layer_in,
    doc_ids,
    query_weight,
    query_bias,
    key_weight,
    key_bias,
    value_weight,
    value_bias,
    output_weight,
    output_bias,
    attn_gain,
    attn_shift,
    inner_weight,
    inner_bias,
    outer_weight,
    outer_bias,
    ffn_gain,
    ffn_shift,
    cotangent,
):
    wide_n = lax.axis_size("wide")
    narrow_n = lax.axis_size("narrow")
    total = wide_n * narrow_n
    share = query_weight.shape[0]
    small_list = (
        query_bias,
        key_bias,
        value_bias,
        output_bias,
        attn_gain,
        attn_shift,
        outer_bias,
        ffn_gain,
        ffn_shift,
    )
    small = jnp.stack(small_list, axis=1)
    small = jnp.pad(small, ((0, 0), (0, 128 - len(small_list))))
    shard = jnp.concatenate([query_weight, key_weight, value_weight, output_weight, small], axis=1)
    full = gather_all(shard).reshape(total * share, shard.shape[1])
    qkv_full = full[:, : 3 * D]
    output_full = full[:, 3 * D : 4 * D]
    vecs = full[:, 4 * D :].astype(jnp.float32)
    (
        query_offset,
        key_offset,
        value_offset,
        output_offset,
        attn_scale,
        attn_offset,
        outer_offset,
        ffn_scale,
        ffn_offset,
    ) = [vecs[:, i] for i in range(len(small_list))]
    qkv_offset = jnp.concatenate([query_offset, key_offset, value_offset])

    ffn_rows, ffn_cols = inner_weight.shape
    bias_n = inner_bias.shape[0]
    bias_k = -(-bias_n // ffn_rows)
    bias_rows = jnp.pad(inner_bias, (0, ffn_rows * bias_k - bias_n)).reshape(ffn_rows, bias_k)
    ffn_shard = jnp.concatenate([inner_weight, outer_weight.T, bias_rows], axis=1)
    ffn_shard, full = lax.optimization_barrier((ffn_shard, full))
    ffn_all = lax.all_gather(ffn_shard, "wide", axis=0, tiled=True)
    inner_cols = ffn_all[:, :ffn_cols]
    outer_cols = ffn_all[:, ffn_cols : 2 * ffn_cols]
    inner_offset = ffn_all[:, 2 * ffn_cols :].reshape(wide_n, ffn_rows * bias_k)[:, :bias_n]
    inner_offset = inner_offset.reshape(-1).astype(jnp.float32)

    rows_dev = layer_in.shape[0]
    half_len = doc_ids.shape[1] // 2
    pack_count = rows_dev // half_len
    narrow_place = lax.axis_index("narrow")
    half_bit = narrow_place % 2
    pair_slot = narrow_place // 2
    pack_docs = lax.dynamic_slice_in_dim(doc_ids, pair_slot * pack_count, pack_count, 0)
    my_docs = lax.dynamic_slice_in_dim(pack_docs, half_bit, 1, 0)
    cosine, sine_tab = jax.vmap(rotary_tables)(my_docs)
    cosine = cosine[:, :, None, :]
    sine_tab = sine_tab[:, :, None, :]

    def to_pack(rows):
        keep = lax.dynamic_slice_in_dim(rows, half_bit * half_len, half_len, 0)
        give = lax.dynamic_slice_in_dim(rows, (1 - half_bit) * half_len, half_len, 0)
        got = swapped(give, "narrow", 0)
        return jnp.where(
            half_bit == 0, jnp.concatenate([keep, got]), jnp.concatenate([got, keep])
        )

    def from_pack(rows):
        keep = lax.dynamic_slice_in_dim(rows, half_bit * half_len, half_len, 0)
        give = lax.dynamic_slice_in_dim(rows, (1 - half_bit) * half_len, half_len, 0)
        got = swapped(give, "narrow", 0)
        return jnp.where(
            half_bit == 0, jnp.concatenate([keep, got]), jnp.concatenate([got, keep])
        )

    pack_in = to_pack(layer_in)
    late_cot, pack_in = lax.optimization_barrier((cotangent, pack_in))
    pack_cot = to_pack(late_cot)

    def heads_of(values):
        return values.reshape(1, rows_dev, HEADS, HEAD_DIM)

    qkv = jnp.dot(pack_in, qkv_full, preferred_element_type=jnp.float32) + qkv_offset
    query_rot = rotate(heads_of(qkv[:, :D]), cosine, sine_tab).astype(jnp.bfloat16)
    key_rot = rotate(heads_of(qkv[:, D : 2 * D]), cosine, sine_tab).astype(jnp.bfloat16)
    value_low = heads_of(qkv[:, 2 * D :]).astype(jnp.bfloat16)
    mixed_out, logsum = attend(query_rot, key_rot, value_low, my_docs, my_docs)
    mixed_low = mixed_out.reshape(rows_dev, D).astype(jnp.bfloat16)
    attn_out = jnp.dot(mixed_low, output_full, preferred_element_type=jnp.float32) + output_offset
    res_one = pack_in.astype(jnp.float32) + attn_out
    norm_one, norm_pull = jax.vjp(layer_norm, res_one, attn_scale, attn_offset)
    norm_low = norm_one.astype(jnp.bfloat16)

    if narrow_n == 2:
        far_rows = swapped(norm_low, "narrow", 0)
        own_act, own_pull, own_part = ffn_forward(norm_low, inner_cols, inner_offset, outer_cols)
        far_act, far_pull, far_part = ffn_forward(far_rows, inner_cols, inner_offset, outer_cols)
        outer_sum = own_part + swapped(far_part.astype(jnp.bfloat16), "narrow", 0).astype(
            jnp.float32
        )
    else:
        group_rows = lax.all_gather(norm_low, "narrow", axis=0, tiled=True)
        all_act, all_pull, all_part = ffn_forward(group_rows, inner_cols, inner_offset, outer_cols)
        outer_sum = narrow_scatter_sum(all_part)
    outer_out = outer_sum + outer_offset
    res_two = norm_one + outer_out
    pack_out, ffn_pull = jax.vjp(layer_norm, res_two, ffn_scale, ffn_offset)
    grad_two, ffn_gsum, ffn_ssum = ffn_pull(pack_cot.astype(jnp.float32))
    grad_outer = grad_two.astype(jnp.bfloat16)
    outer_bsum = jnp.sum(grad_outer.astype(jnp.float32), axis=0)
    if narrow_n == 2:
        far_grads = swapped(grad_outer, "narrow", 0)
        own_inner, own_back = ffn_backward(grad_outer, own_pull, inner_cols, outer_cols)
        far_inner, far_back = ffn_backward(far_grads, far_pull, inner_cols, outer_cols)
        grad_part = own_back + swapped(far_back.astype(jnp.bfloat16), "narrow", 0).astype(
            jnp.float32
        )
        outer_wsum_t = contract_rows(grad_outer, own_act) + contract_rows(far_grads, far_act)
        inner_wsum = contract_rows(norm_low, own_inner) + contract_rows(far_rows, far_inner)
        inner_bsum = jnp.sum(own_inner.astype(jnp.float32), axis=0) + jnp.sum(
            far_inner.astype(jnp.float32), axis=0
        )
    else:
        group_grads = lax.all_gather(grad_outer, "narrow", axis=0, tiled=True)
        all_inner, all_back = ffn_backward(group_grads, all_pull, inner_cols, outer_cols)
        grad_part = narrow_scatter_sum(all_back)
        outer_wsum_t = contract_rows(group_grads, all_act)
        inner_wsum = contract_rows(group_rows, all_inner)
        inner_bsum = jnp.sum(all_inner.astype(jnp.float32), axis=0)
    bsum_rows = jnp.pad(
        inner_bsum.reshape(wide_n, bias_n), ((0, 0), (0, ffn_rows * bias_k - bias_n))
    ).reshape(wide_n * ffn_rows, bias_k)
    ffn_sums = jnp.concatenate([inner_wsum, outer_wsum_t, bsum_rows], axis=1).astype(jnp.bfloat16)
    ffn_mine = lax.psum_scatter(ffn_sums, "wide", scatter_dimension=0, tiled=True)
    ffn_mine = ffn_mine.astype(jnp.float32)
    inner_wgrad = ffn_mine[:, :ffn_cols]
    outer_wgrad = ffn_mine[:, ffn_cols : 2 * ffn_cols].T
    inner_bgrad = ffn_mine[:, 2 * ffn_cols :].reshape(-1)[:bias_n]

    pack_out, grad_part = lax.optimization_barrier((pack_out, grad_part))
    layer_out = from_pack(pack_out)
    grad_norm = grad_two + grad_part
    grad_one, attn_gsum, attn_ssum = norm_pull(grad_norm)
    grad_attn = grad_one.astype(jnp.bfloat16)
    output_bsum = jnp.sum(grad_attn.astype(jnp.float32), axis=0)
    output_wsum = contract_rows(mixed_low, grad_attn)
    early_small = jnp.stack(
        [output_bsum, attn_gsum, attn_ssum, outer_bsum, ffn_gsum, ffn_ssum], axis=1
    )
    early = jnp.concatenate(
        [output_wsum.reshape(total, share, D), early_small.reshape(total, share, -1)], axis=2
    )

    grad_mixed = heads_of(contract_cols(grad_attn, output_full).astype(jnp.bfloat16))
    grad_qrot, grad_krot, grad_values = attend_back(
        query_rot, key_rot, value_low, my_docs, my_docs, logsum, grad_mixed
    )
    grad_values = grad_values.astype(jnp.bfloat16)
    grad_query = unrotate(grad_qrot, cosine, sine_tab).astype(jnp.bfloat16)
    grad_keys = unrotate(grad_krot, cosine, sine_tab).astype(jnp.bfloat16)
    grad_qkv = jnp.concatenate(
        [
            grad_query.reshape(rows_dev, D),
            grad_keys.reshape(rows_dev, D),
            grad_values.reshape(rows_dev, D),
        ],
        axis=1,
    )
    pack_grad = grad_one + contract_cols(grad_qkv, qkv_full)
    keep_grad = lax.dynamic_slice_in_dim(pack_grad, half_bit * half_len, half_len, 0)
    give_grad = lax.dynamic_slice_in_dim(pack_grad, (1 - half_bit) * half_len, half_len, 0)
    give_grad, grad_qkv, pack_in = lax.optimization_barrier((give_grad, grad_qkv, pack_in))
    got_grad = swapped(give_grad, "narrow", 0)
    input_grad = jnp.where(
        half_bit == 0,
        jnp.concatenate([keep_grad, got_grad]),
        jnp.concatenate([got_grad, keep_grad]),
    )
    qkv_wsum = contract_rows(pack_in, grad_qkv)
    qkv_bsum = jnp.sum(grad_qkv.astype(jnp.float32), axis=0).reshape(3, D)
    late = jnp.concatenate(
        [
            qkv_wsum.reshape(total, share, 3 * D).astype(jnp.bfloat16),
            qkv_bsum.T.reshape(total, share, 3).astype(jnp.bfloat16),
            early.astype(jnp.bfloat16),
        ],
        axis=2,
    )
    late_mine = scatter_sum_all(late)
    early_mine = late_mine[:, 3 * D + 3 :]
    query_wgrad = late_mine[:, :D]
    key_wgrad = late_mine[:, D : 2 * D]
    value_wgrad = late_mine[:, 2 * D : 3 * D]
    query_bgrad = late_mine[:, 3 * D]
    key_bgrad = late_mine[:, 3 * D + 1]
    value_bgrad = late_mine[:, 3 * D + 2]
    output_wgrad = early_mine[:, :D]
    output_bgrad = early_mine[:, D]
    attn_ggrad = early_mine[:, D + 1]
    attn_sgrad = early_mine[:, D + 2]
    outer_bgrad = early_mine[:, D + 3]
    ffn_ggrad = early_mine[:, D + 4]
    ffn_sgrad = early_mine[:, D + 5]
    return (
        layer_out,
        input_grad,
        query_wgrad,
        query_bgrad,
        key_wgrad,
        key_bgrad,
        value_wgrad,
        value_bgrad,
        output_wgrad,
        output_bgrad,
        attn_ggrad,
        attn_sgrad,
        inner_wgrad,
        inner_bgrad,
        outer_wgrad,
        outer_bgrad,
        ffn_ggrad,
        ffn_sgrad,
    )


def solution(mesh):
    return jax.shard_map(
        local,
        mesh=mesh,
        in_specs=(
            P(("wide", "narrow"), None),
            P("wide", None),
            P(("wide", "narrow"), None),
            P(("wide", "narrow")),
            P(("wide", "narrow"), None),
            P(("wide", "narrow")),
            P(("wide", "narrow"), None),
            P(("wide", "narrow")),
            P(("wide", "narrow"), None),
            P(("wide", "narrow")),
            P(("wide", "narrow")),
            P(("wide", "narrow")),
            P("wide", "narrow"),
            P(("narrow", "wide")),
            P("narrow", "wide"),
            P(("wide", "narrow")),
            P(("wide", "narrow")),
            P(("wide", "narrow")),
            P(("wide", "narrow"), None),
        ),
        out_specs=(
            P(("wide", "narrow"), None),
            P(("wide", "narrow"), None),
            P(("wide", "narrow"), None),
            P(("wide", "narrow")),
            P(("wide", "narrow"), None),
            P(("wide", "narrow")),
            P(("wide", "narrow"), None),
            P(("wide", "narrow")),
            P(("wide", "narrow"), None),
            P(("wide", "narrow")),
            P(("wide", "narrow")),
            P(("wide", "narrow")),
            P("wide", "narrow"),
            P(("narrow", "wide")),
            P("narrow", "wide"),
            P(("wide", "narrow")),
            P(("wide", "narrow")),
            P(("wide", "narrow")),
        ),
        check_vma=False,
    )
```

```python
import jax
import jax.numpy as jnp
from jax import lax
from jax.sharding import PartitionSpec as P

D = 768
HEADS = 12
HEAD_DIM = 64

ALL = ("wide", "narrow")
layer_eps = 1e-12
masked_score = -1e30


def swapped(shard, axis, bit):
    return lax.ppermute(shard, axis, [(i, i ^ 1 << bit) for i in range(lax.axis_size(axis))])


def part_orders(total, narrow_n, parts):
    bits = total.bit_length() - 1
    core_bit = narrow_n.bit_length() - 1
    narrow_bits = list(range(core_bit))
    wide_bits = [b for b in reversed(range(core_bit + 1, bits))]
    orders = []
    for p in range(parts):
        k = p % max(1, len(wide_bits))
        orders.append(narrow_bits + wide_bits[k:] + wide_bits[:k] + [core_bit])
    return orders


def is_pow2(n):
    return n & (n - 1) == 0


def column_splits(cols, parts):
    tiles = -(-cols // 128)
    parts = max(1, min(parts, tiles))
    edges = [min(cols, (tiles * i // parts) * 128) for i in range(parts)] + [cols]
    return [(a, b) for a, b in zip(edges[:-1], edges[1:]) if b > a]


def doubling_gather(shard, order, total):
    me = lax.axis_index(ALL)
    cur = shard
    for b in order:
        other = lax.ppermute(cur, ALL, [(i, i ^ (1 << b)) for i in range(total)])
        bit = (me >> b) & 1
        pick = (jnp.arange(2) == bit).reshape((2,) + (1,) * cur.ndim)
        cur = jnp.where(pick, cur[None], other[None])
    k = len(order)
    perm = [k - 1 - order.index(b) for b in reversed(range(k))]
    cur = cur.transpose(perm + list(range(k, cur.ndim)))
    return cur.reshape((total,) + shard.shape)


def gather_all(shard, parts=3):
    total = lax.axis_size("wide") * lax.axis_size("narrow")
    narrow_n = lax.axis_size("narrow")
    if not (is_pow2(total) and is_pow2(narrow_n)):
        return lax.all_gather(shard, ALL, axis=0, tiled=False)
    splits = column_splits(shard.shape[-1], parts)
    orders = part_orders(total, narrow_n, len(splits))
    pieces = [
        doubling_gather(shard[..., a:b], order, total) for (a, b), order in zip(splits, orders)
    ]
    return jnp.concatenate(pieces, axis=-1)


def halving_scatter(parts_in, order, total):
    me = lax.axis_index(ALL)
    nbits = total.bit_length() - 1
    cur = parts_in.reshape((2,) * nbits + parts_in.shape[1:])
    axes = list(reversed(range(nbits)))
    for b in order:
        a = axes.index(b)
        bit = (me >> b) & 1
        mine = lax.dynamic_index_in_dim(cur, bit, axis=a, keepdims=False)
        theirs = lax.dynamic_index_in_dim(cur, 1 - bit, axis=a, keepdims=False)
        got = lax.ppermute(
            theirs.astype(jnp.bfloat16), ALL, [(i, i ^ (1 << b)) for i in range(total)]
        )
        cur = mine.astype(jnp.float32) + got.astype(jnp.float32)
        axes.pop(a)
    return cur


def scatter_sum_all(parts_in, parts=3):
    total = lax.axis_size("wide") * lax.axis_size("narrow")
    narrow_n = lax.axis_size("narrow")
    if not (is_pow2(total) and is_pow2(narrow_n)):
        return lax.psum_scatter(
            parts_in.astype(jnp.bfloat16), ALL, scatter_dimension=0, tiled=False
        ).astype(jnp.float32)
    splits = column_splits(parts_in.shape[-1], parts)
    orders = part_orders(total, narrow_n, len(splits))
    pieces = [
        halving_scatter(parts_in[..., a:b], list(reversed(order)), total)
        for (a, b), order in zip(splits, orders)
    ]
    return jnp.concatenate(pieces, axis=-1)


def scatter_sum_parts(part_list):
    total = lax.axis_size("wide") * lax.axis_size("narrow")
    narrow_n = lax.axis_size("narrow")
    if not (is_pow2(total) and is_pow2(narrow_n)):
        return jnp.concatenate([scatter_sum_all(x, 1) for x in part_list], axis=-1)
    orders = part_orders(total, narrow_n, len(part_list))
    return jnp.concatenate(
        [halving_scatter(x, list(reversed(o)), total) for x, o in zip(part_list, orders)],
        axis=-1,
    )


def narrow_gather(rows):
    n = lax.axis_size("narrow")
    if n != 2:
        return lax.all_gather(rows, "narrow", axis=0, tiled=True)
    other = swapped(rows, "narrow", 0)
    first = lax.axis_index("narrow") == 0
    return jnp.where(first, jnp.concatenate([rows, other]), jnp.concatenate([other, rows]))


def narrow_scatter_sum(part):
    n = lax.axis_size("narrow")
    if n != 2:
        return lax.psum_scatter(
            part.astype(jnp.bfloat16), "narrow", scatter_dimension=0, tiled=True
        ).astype(jnp.float32)
    rows = part.shape[0] // 2
    me = lax.axis_index("narrow")
    mine = lax.dynamic_slice_in_dim(part, me * rows, rows, 0)
    theirs = lax.dynamic_slice_in_dim(part, (1 - me) * rows, rows, 0)
    return mine + swapped(theirs.astype(jnp.bfloat16), "narrow", 0).astype(jnp.float32)


def layer_norm(values, gain_vec, shift_vec):
    center = values - jnp.mean(values, axis=-1, keepdims=True)
    spread = jnp.mean(center * center, axis=-1, keepdims=True)
    return center * lax.rsqrt(spread + layer_eps) * gain_vec + shift_vec


def gelu_exact(values):
    return jax.nn.gelu(values, approximate=False)


def rotary_tables(doc_row):
    places = jnp.arange(doc_row.shape[0], dtype=jnp.int32)
    before = jnp.sum((doc_row[None, :] < doc_row[:, None]).astype(jnp.int32), axis=1)
    position = (places - before).astype(jnp.float32)
    frequency = 10000.0 ** (-2.0 * jnp.arange(HEAD_DIM // 2, dtype=jnp.float32) / HEAD_DIM)
    angles = position[:, None] * frequency[None, :]
    return (jnp.cos(angles), jnp.sin(angles))


def rotate(values, cosine, sine_tab):
    half_dim = values.shape[-1] // 2
    first_half = values[..., :half_dim]
    second = values[..., half_dim:]
    return jnp.concatenate(
        [first_half * cosine - second * sine_tab, second * cosine + first_half * sine_tab], axis=-1
    )


def unrotate(values, cosine, sine_tab):
    half_dim = values.shape[-1] // 2
    first_half = values[..., :half_dim]
    second = values[..., half_dim:]
    return jnp.concatenate(
        [first_half * cosine + second * sine_tab, second * cosine - first_half * sine_tab], axis=-1
    )


def contract_rows(left_op, right_op):
    return lax.dot_general(
        left_op, right_op, (((0,), (0,)), ((), ())), preferred_element_type=jnp.float32
    )


def contract_cols(left_op, right_op):
    return lax.dot_general(
        left_op, right_op, (((1,), (1,)), ((), ())), preferred_element_type=jnp.float32
    )


def score_block(query_rot, key_rot, query_docs, key_docs):
    scores = jnp.einsum(
        "pqhd,pkhd->phqk", query_rot, key_rot, preferred_element_type=jnp.float32
    ) * HEAD_DIM ** (-0.5)
    same_doc = query_docs[:, :, None] == key_docs[:, None, :]
    return jnp.where(same_doc[:, None], scores, masked_score)


def attend(query_rot, key_rot, value_low, query_docs, key_docs):
    scores = score_block(query_rot, key_rot, query_docs, key_docs)
    row_peak = jnp.max(scores, axis=-1, keepdims=True)
    exponent = jnp.exp(scores - row_peak)
    totals = jnp.sum(exponent, axis=-1, keepdims=True)
    probability = (exponent / totals).astype(jnp.bfloat16)
    mixed_out = jnp.einsum(
        "phqk,pkhd->pqhd", probability, value_low, preferred_element_type=jnp.float32
    )
    return (mixed_out, row_peak + jnp.log(totals))


def attend_back(query_rot, key_rot, value_low, query_docs, key_docs, logsum, grad_mixed):
    probability = jnp.exp(score_block(query_rot, key_rot, query_docs, key_docs) - logsum)
    grad_values = jnp.einsum(
        "phqk,pqhd->pkhd",
        probability.astype(jnp.bfloat16),
        grad_mixed,
        preferred_element_type=jnp.float32,
    )
    grad_probs = jnp.einsum(
        "pqhd,pkhd->phqk", grad_mixed, value_low, preferred_element_type=jnp.float32
    )
    inner_sum = jnp.sum(probability * grad_probs, axis=-1, keepdims=True)
    grad_scores = (probability * (grad_probs - inner_sum)).astype(jnp.bfloat16)
    grad_query = jnp.einsum(
        "phqk,pkhd->pqhd", grad_scores, key_rot, preferred_element_type=jnp.float32
    ) * HEAD_DIM ** (-0.5)
    grad_keys = jnp.einsum(
        "phqk,pqhd->pkhd", grad_scores, query_rot, preferred_element_type=jnp.float32
    ) * HEAD_DIM ** (-0.5)
    return (grad_query, grad_keys, grad_values)


def ffn_forward(rows, inner_cols, inner_offset, outer_cols):
    inner_pre = jnp.dot(rows, inner_cols, preferred_element_type=jnp.float32) + inner_offset
    act_value, gelu_pull = jax.vjp(gelu_exact, inner_pre)
    act_low = act_value.astype(jnp.bfloat16)
    return act_low, gelu_pull, contract_cols(act_low, outer_cols)


def ffn_backward(grads, gelu_pull, inner_cols, outer_cols):
    grad_act = jnp.dot(grads, outer_cols, preferred_element_type=jnp.float32)
    grad_inner = gelu_pull(grad_act)[0].astype(jnp.bfloat16)
    return grad_inner, contract_cols(grad_inner, inner_cols)


def local(
    layer_in,
    doc_ids,
    query_weight,
    query_bias,
    key_weight,
    key_bias,
    value_weight,
    value_bias,
    output_weight,
    output_bias,
    attn_gain,
    attn_shift,
    inner_weight,
    inner_bias,
    outer_weight,
    outer_bias,
    ffn_gain,
    ffn_shift,
    cotangent,
):
    wide_n = lax.axis_size("wide")
    narrow_n = lax.axis_size("narrow")
    total = wide_n * narrow_n
    share = query_weight.shape[0]
    small_list = (
        query_bias,
        key_bias,
        value_bias,
        output_bias,
        attn_gain,
        attn_shift,
        outer_bias,
        ffn_gain,
        ffn_shift,
    )
    small = jnp.stack(small_list, axis=1)
    small = jnp.pad(small, ((0, 0), (0, 128 - len(small_list))))
    shard = jnp.concatenate([query_weight, key_weight, value_weight, output_weight, small], axis=1)
    full = gather_all(shard).reshape(total * share, shard.shape[1])
    qkv_full = full[:, : 3 * D]
    output_full = full[:, 3 * D : 4 * D]
    vecs = full[:, 4 * D :].astype(jnp.float32)
    (
        query_offset,
        key_offset,
        value_offset,
        output_offset,
        attn_scale,
        attn_offset,
        outer_offset,
        ffn_scale,
        ffn_offset,
    ) = [vecs[:, i] for i in range(len(small_list))]
    qkv_offset = jnp.concatenate([query_offset, key_offset, value_offset])

    ffn_rows, ffn_cols = inner_weight.shape
    bias_n = inner_bias.shape[0]
    bias_k = -(-bias_n // ffn_rows)
    bias_rows = jnp.pad(inner_bias, (0, ffn_rows * bias_k - bias_n)).reshape(ffn_rows, bias_k)
    ffn_shard = jnp.concatenate([inner_weight, outer_weight.T, bias_rows], axis=1)
    ffn_shard, full = lax.optimization_barrier((ffn_shard, full))
    ffn_all = lax.all_gather(ffn_shard, "wide", axis=0, tiled=True)
    inner_cols = ffn_all[:, :ffn_cols]
    outer_cols = ffn_all[:, ffn_cols : 2 * ffn_cols]
    inner_offset = ffn_all[:, 2 * ffn_cols :].reshape(wide_n, ffn_rows * bias_k)[:, :bias_n]
    inner_offset = inner_offset.reshape(-1).astype(jnp.float32)

    rows_dev = layer_in.shape[0]
    half_len = doc_ids.shape[1] // 2
    pack_count = rows_dev // half_len
    narrow_place = lax.axis_index("narrow")
    half_bit = narrow_place % 2
    pair_slot = narrow_place // 2
    pack_docs = lax.dynamic_slice_in_dim(doc_ids, pair_slot * pack_count, pack_count, 0)
    my_docs = lax.dynamic_slice_in_dim(pack_docs, half_bit, 1, 0)
    cosine, sine_tab = jax.vmap(rotary_tables)(my_docs)
    cosine = cosine[:, :, None, :]
    sine_tab = sine_tab[:, :, None, :]

    def to_pack(rows):
        keep = lax.dynamic_slice_in_dim(rows, half_bit * half_len, half_len, 0)
        give = lax.dynamic_slice_in_dim(rows, (1 - half_bit) * half_len, half_len, 0)
        got = swapped(give, "narrow", 0)
        return jnp.where(
            half_bit == 0, jnp.concatenate([keep, got]), jnp.concatenate([got, keep])
        )

    def from_pack(rows):
        keep = lax.dynamic_slice_in_dim(rows, half_bit * half_len, half_len, 0)
        give = lax.dynamic_slice_in_dim(rows, (1 - half_bit) * half_len, half_len, 0)
        got = swapped(give, "narrow", 0)
        return jnp.where(
            half_bit == 0, jnp.concatenate([keep, got]), jnp.concatenate([got, keep])
        )

    pack_in = to_pack(layer_in)
    pack_cot = to_pack(cotangent)

    def heads_of(values):
        return values.reshape(1, rows_dev, HEADS, HEAD_DIM)

    qkv = jnp.dot(pack_in, qkv_full, preferred_element_type=jnp.float32) + qkv_offset
    query_rot = rotate(heads_of(qkv[:, :D]), cosine, sine_tab).astype(jnp.bfloat16)
    key_rot = rotate(heads_of(qkv[:, D : 2 * D]), cosine, sine_tab).astype(jnp.bfloat16)
    value_low = heads_of(qkv[:, 2 * D :]).astype(jnp.bfloat16)
    mixed_out, logsum = attend(query_rot, key_rot, value_low, my_docs, my_docs)
    mixed_low = mixed_out.reshape(rows_dev, D).astype(jnp.bfloat16)
    attn_out = jnp.dot(mixed_low, output_full, preferred_element_type=jnp.float32) + output_offset
    res_one = pack_in.astype(jnp.float32) + attn_out
    norm_one, norm_pull = jax.vjp(layer_norm, res_one, attn_scale, attn_offset)
    norm_low = norm_one.astype(jnp.bfloat16)

    if narrow_n == 2:
        far_rows = swapped(norm_low, "narrow", 0)
        own_act, own_pull, own_part = ffn_forward(norm_low, inner_cols, inner_offset, outer_cols)
        far_act, far_pull, far_part = ffn_forward(far_rows, inner_cols, inner_offset, outer_cols)
        outer_sum = own_part + swapped(far_part.astype(jnp.bfloat16), "narrow", 0).astype(
            jnp.float32
        )
    else:
        group_rows = lax.all_gather(norm_low, "narrow", axis=0, tiled=True)
        all_act, all_pull, all_part = ffn_forward(group_rows, inner_cols, inner_offset, outer_cols)
        outer_sum = narrow_scatter_sum(all_part)
    outer_out = outer_sum + outer_offset
    res_two = norm_one + outer_out
    pack_out, ffn_pull = jax.vjp(layer_norm, res_two, ffn_scale, ffn_offset)
    grad_two, ffn_gsum, ffn_ssum = ffn_pull(pack_cot.astype(jnp.float32))
    grad_outer = grad_two.astype(jnp.bfloat16)
    outer_bsum = jnp.sum(grad_outer.astype(jnp.float32), axis=0)
    if narrow_n == 2:
        far_grads = swapped(grad_outer, "narrow", 0)
        own_inner, own_back = ffn_backward(grad_outer, own_pull, inner_cols, outer_cols)
        far_inner, far_back = ffn_backward(far_grads, far_pull, inner_cols, outer_cols)
        grad_part = own_back + swapped(far_back.astype(jnp.bfloat16), "narrow", 0).astype(
            jnp.float32
        )
        outer_wsum_t = contract_rows(grad_outer, own_act) + contract_rows(far_grads, far_act)
        inner_wsum = contract_rows(norm_low, own_inner) + contract_rows(far_rows, far_inner)
        inner_bsum = jnp.sum(own_inner.astype(jnp.float32), axis=0) + jnp.sum(
            far_inner.astype(jnp.float32), axis=0
        )
    else:
        group_grads = lax.all_gather(grad_outer, "narrow", axis=0, tiled=True)
        all_inner, all_back = ffn_backward(group_grads, all_pull, inner_cols, outer_cols)
        grad_part = narrow_scatter_sum(all_back)
        outer_wsum_t = contract_rows(group_grads, all_act)
        inner_wsum = contract_rows(group_rows, all_inner)
        inner_bsum = jnp.sum(all_inner.astype(jnp.float32), axis=0)
    bsum_rows = jnp.pad(
        inner_bsum.reshape(wide_n, bias_n), ((0, 0), (0, ffn_rows * bias_k - bias_n))
    ).reshape(wide_n * ffn_rows, bias_k)
    ffn_sums = jnp.concatenate([inner_wsum, outer_wsum_t, bsum_rows], axis=1).astype(jnp.bfloat16)
    ffn_mine = lax.psum_scatter(ffn_sums, "wide", scatter_dimension=0, tiled=True)
    ffn_mine = ffn_mine.astype(jnp.float32)
    inner_wgrad = ffn_mine[:, :ffn_cols]
    outer_wgrad = ffn_mine[:, ffn_cols : 2 * ffn_cols].T
    inner_bgrad = ffn_mine[:, 2 * ffn_cols :].reshape(-1)[:bias_n]

    pack_out, grad_part = lax.optimization_barrier((pack_out, grad_part))
    layer_out = from_pack(pack_out)
    grad_norm = grad_two + grad_part
    grad_one, attn_gsum, attn_ssum = norm_pull(grad_norm)
    grad_attn = grad_one.astype(jnp.bfloat16)
    output_bsum = jnp.sum(grad_attn.astype(jnp.float32), axis=0)
    output_wsum = contract_rows(mixed_low, grad_attn)
    early_small = jnp.stack(
        [output_bsum, attn_gsum, attn_ssum, outer_bsum, ffn_gsum, ffn_ssum], axis=1
    )
    early = jnp.concatenate(
        [output_wsum.reshape(total, share, D), early_small.reshape(total, share, -1)], axis=2
    )

    grad_mixed = heads_of(contract_cols(grad_attn, output_full).astype(jnp.bfloat16))
    grad_qrot, grad_krot, grad_values = attend_back(
        query_rot, key_rot, value_low, my_docs, my_docs, logsum, grad_mixed
    )
    grad_values = grad_values.astype(jnp.bfloat16)
    grad_query = unrotate(grad_qrot, cosine, sine_tab).astype(jnp.bfloat16)
    grad_keys = unrotate(grad_krot, cosine, sine_tab).astype(jnp.bfloat16)
    grad_qkv = jnp.concatenate(
        [
            grad_query.reshape(rows_dev, D),
            grad_keys.reshape(rows_dev, D),
            grad_values.reshape(rows_dev, D),
        ],
        axis=1,
    )
    pack_grad = grad_one + contract_cols(grad_qkv, qkv_full)
    keep_grad = lax.dynamic_slice_in_dim(pack_grad, half_bit * half_len, half_len, 0)
    give_grad = lax.dynamic_slice_in_dim(pack_grad, (1 - half_bit) * half_len, half_len, 0)
    give_grad, grad_qkv, pack_in = lax.optimization_barrier((give_grad, grad_qkv, pack_in))
    got_grad = swapped(give_grad, "narrow", 0)
    input_grad = jnp.where(
        half_bit == 0,
        jnp.concatenate([keep_grad, got_grad]),
        jnp.concatenate([got_grad, keep_grad]),
    )
    qkv_wsum = contract_rows(pack_in, grad_qkv)
    qkv_bsum = jnp.sum(grad_qkv.astype(jnp.float32), axis=0).reshape(3, D)
    wsum_parts = qkv_wsum.reshape(total, share, 3 * D).astype(jnp.bfloat16)
    cut = 3 * D * 4 // 9 // 128 * 128
    late_mine = scatter_sum_parts(
        [
            wsum_parts[..., :cut],
            wsum_parts[..., cut : 2 * cut],
            jnp.concatenate(
                [
                    wsum_parts[..., 2 * cut :],
                    qkv_bsum.T.reshape(total, share, 3).astype(jnp.bfloat16),
                    early.astype(jnp.bfloat16),
                ],
                axis=2,
            ),
        ]
    )
    early_mine = late_mine[:, 3 * D + 3 :]
    query_wgrad = late_mine[:, :D]
    key_wgrad = late_mine[:, D : 2 * D]
    value_wgrad = late_mine[:, 2 * D : 3 * D]
    query_bgrad = late_mine[:, 3 * D]
    key_bgrad = late_mine[:, 3 * D + 1]
    value_bgrad = late_mine[:, 3 * D + 2]
    output_wgrad = early_mine[:, :D]
    output_bgrad = early_mine[:, D]
    attn_ggrad = early_mine[:, D + 1]
    attn_sgrad = early_mine[:, D + 2]
    outer_bgrad = early_mine[:, D + 3]
    ffn_ggrad = early_mine[:, D + 4]
    ffn_sgrad = early_mine[:, D + 5]
    return (
        layer_out,
        input_grad,
        query_wgrad,
        query_bgrad,
        key_wgrad,
        key_bgrad,
        value_wgrad,
        value_bgrad,
        output_wgrad,
        output_bgrad,
        attn_ggrad,
        attn_sgrad,
        inner_wgrad,
        inner_bgrad,
        outer_wgrad,
        outer_bgrad,
        ffn_ggrad,
        ffn_sgrad,
    )


def solution(mesh):
    return jax.shard_map(
        local,
        mesh=mesh,
        in_specs=(
            P(("wide", "narrow"), None),
            P("wide", None),
            P(("wide", "narrow"), None),
            P(("wide", "narrow")),
            P(("wide", "narrow"), None),
            P(("wide", "narrow")),
            P(("wide", "narrow"), None),
            P(("wide", "narrow")),
            P(("wide", "narrow"), None),
            P(("wide", "narrow")),
            P(("wide", "narrow")),
            P(("wide", "narrow")),
            P("wide", "narrow"),
            P(("narrow", "wide")),
            P("narrow", "wide"),
            P(("wide", "narrow")),
            P(("wide", "narrow")),
            P(("wide", "narrow")),
            P(("wide", "narrow"), None),
        ),
        out_specs=(
            P(("wide", "narrow"), None),
            P(("wide", "narrow"), None),
            P(("wide", "narrow"), None),
            P(("wide", "narrow")),
            P(("wide", "narrow"), None),
            P(("wide", "narrow")),
            P(("wide", "narrow"), None),
            P(("wide", "narrow")),
            P(("wide", "narrow"), None),
            P(("wide", "narrow")),
            P(("wide", "narrow")),
            P(("wide", "narrow")),
            P("wide", "narrow"),
            P(("narrow", "wide")),
            P("narrow", "wide"),
            P(("wide", "narrow")),
            P(("wide", "narrow")),
            P(("wide", "narrow")),
        ),
        check_vma=False,
    )
```

```python
import jax
import jax.numpy as jnp
from jax import lax
from jax.sharding import PartitionSpec as P

D = 768
HEADS = 12
HEAD_DIM = 64

ALL = ("wide", "narrow")
layer_eps = 1e-12
masked_score = -1e30


def swapped(shard, axis, bit):
    return lax.ppermute(shard, axis, [(i, i ^ 1 << bit) for i in range(lax.axis_size(axis))])


def part_orders(total, narrow_n, parts):
    bits = total.bit_length() - 1
    core_bit = narrow_n.bit_length() - 1
    narrow_bits = list(range(core_bit))
    wide_bits = [b for b in reversed(range(core_bit + 1, bits))]
    orders = []
    for p in range(parts):
        k = p % max(1, len(wide_bits))
        orders.append(narrow_bits + wide_bits[k:] + wide_bits[:k] + [core_bit])
    return orders


def is_pow2(n):
    return n & (n - 1) == 0


def column_splits(cols, parts):
    tiles = -(-cols // 128)
    parts = max(1, min(parts, tiles))
    edges = [min(cols, (tiles * i // parts) * 128) for i in range(parts)] + [cols]
    return [(a, b) for a, b in zip(edges[:-1], edges[1:]) if b > a]


def doubling_gather(shard, order, total):
    me = lax.axis_index(ALL)
    cur = shard
    for b in order:
        other = lax.ppermute(cur, ALL, [(i, i ^ (1 << b)) for i in range(total)])
        bit = (me >> b) & 1
        pick = (jnp.arange(2) == bit).reshape((2,) + (1,) * cur.ndim)
        cur = jnp.where(pick, cur[None], other[None])
    k = len(order)
    perm = [k - 1 - order.index(b) for b in reversed(range(k))]
    cur = cur.transpose(perm + list(range(k, cur.ndim)))
    return cur.reshape((total,) + shard.shape)


def gather_all(shard, parts=3):
    total = lax.axis_size("wide") * lax.axis_size("narrow")
    narrow_n = lax.axis_size("narrow")
    if not (is_pow2(total) and is_pow2(narrow_n)):
        return lax.all_gather(shard, ALL, axis=0, tiled=False)
    splits = column_splits(shard.shape[-1], parts)
    orders = part_orders(total, narrow_n, len(splits))
    pieces = [
        doubling_gather(shard[..., a:b], order, total) for (a, b), order in zip(splits, orders)
    ]
    return jnp.concatenate(pieces, axis=-1)


def halving_scatter(parts_in, order, total):
    me = lax.axis_index(ALL)
    nbits = total.bit_length() - 1
    cur = parts_in.reshape((2,) * nbits + parts_in.shape[1:])
    axes = list(reversed(range(nbits)))
    for b in order:
        a = axes.index(b)
        bit = (me >> b) & 1
        mine = lax.dynamic_index_in_dim(cur, bit, axis=a, keepdims=False)
        theirs = lax.dynamic_index_in_dim(cur, 1 - bit, axis=a, keepdims=False)
        got = lax.ppermute(
            theirs.astype(jnp.bfloat16), ALL, [(i, i ^ (1 << b)) for i in range(total)]
        )
        cur = mine.astype(jnp.float32) + got.astype(jnp.float32)
        axes.pop(a)
    return cur


def scatter_sum_all(parts_in, parts=3):
    total = lax.axis_size("wide") * lax.axis_size("narrow")
    narrow_n = lax.axis_size("narrow")
    if not (is_pow2(total) and is_pow2(narrow_n)):
        return lax.psum_scatter(
            parts_in.astype(jnp.bfloat16), ALL, scatter_dimension=0, tiled=False
        ).astype(jnp.float32)
    splits = column_splits(parts_in.shape[-1], parts)
    orders = part_orders(total, narrow_n, len(splits))
    pieces = [
        halving_scatter(parts_in[..., a:b], list(reversed(order)), total)
        for (a, b), order in zip(splits, orders)
    ]
    return jnp.concatenate(pieces, axis=-1)


def scatter_sum_parts(part_list):
    total = lax.axis_size("wide") * lax.axis_size("narrow")
    narrow_n = lax.axis_size("narrow")
    if not (is_pow2(total) and is_pow2(narrow_n)):
        return jnp.concatenate([scatter_sum_all(x, 1) for x in part_list], axis=-1)
    orders = part_orders(total, narrow_n, len(part_list))
    return jnp.concatenate(
        [halving_scatter(x, list(reversed(o)), total) for x, o in zip(part_list, orders)],
        axis=-1,
    )


def narrow_gather(rows):
    n = lax.axis_size("narrow")
    if n != 2:
        return lax.all_gather(rows, "narrow", axis=0, tiled=True)
    other = swapped(rows, "narrow", 0)
    first = lax.axis_index("narrow") == 0
    return jnp.where(first, jnp.concatenate([rows, other]), jnp.concatenate([other, rows]))


def narrow_scatter_sum(part):
    n = lax.axis_size("narrow")
    if n != 2:
        return lax.psum_scatter(
            part.astype(jnp.bfloat16), "narrow", scatter_dimension=0, tiled=True
        ).astype(jnp.float32)
    rows = part.shape[0] // 2
    me = lax.axis_index("narrow")
    mine = lax.dynamic_slice_in_dim(part, me * rows, rows, 0)
    theirs = lax.dynamic_slice_in_dim(part, (1 - me) * rows, rows, 0)
    return mine + swapped(theirs.astype(jnp.bfloat16), "narrow", 0).astype(jnp.float32)


def layer_norm(values, gain_vec, shift_vec):
    center = values - jnp.mean(values, axis=-1, keepdims=True)
    spread = jnp.mean(center * center, axis=-1, keepdims=True)
    return center * lax.rsqrt(spread + layer_eps) * gain_vec + shift_vec


def gelu_exact(values):
    return jax.nn.gelu(values, approximate=False)


def rotary_tables(doc_row):
    places = jnp.arange(doc_row.shape[0], dtype=jnp.int32)
    before = jnp.sum((doc_row[None, :] < doc_row[:, None]).astype(jnp.int32), axis=1)
    position = (places - before).astype(jnp.float32)
    frequency = 10000.0 ** (-2.0 * jnp.arange(HEAD_DIM // 2, dtype=jnp.float32) / HEAD_DIM)
    angles = position[:, None] * frequency[None, :]
    return (jnp.cos(angles), jnp.sin(angles))


def rotate(values, cosine, sine_tab):
    half_dim = values.shape[-1] // 2
    first_half = values[..., :half_dim]
    second = values[..., half_dim:]
    return jnp.concatenate(
        [first_half * cosine - second * sine_tab, second * cosine + first_half * sine_tab], axis=-1
    )


def unrotate(values, cosine, sine_tab):
    half_dim = values.shape[-1] // 2
    first_half = values[..., :half_dim]
    second = values[..., half_dim:]
    return jnp.concatenate(
        [first_half * cosine + second * sine_tab, second * cosine - first_half * sine_tab], axis=-1
    )


def contract_rows(left_op, right_op):
    return lax.dot_general(
        left_op, right_op, (((0,), (0,)), ((), ())), preferred_element_type=jnp.float32
    )


def contract_cols(left_op, right_op):
    return lax.dot_general(
        left_op, right_op, (((1,), (1,)), ((), ())), preferred_element_type=jnp.float32
    )


def score_block(query_rot, key_rot, query_docs, key_docs):
    scores = jnp.einsum(
        "pqhd,pkhd->phqk", query_rot, key_rot, preferred_element_type=jnp.float32
    ) * HEAD_DIM ** (-0.5)
    same_doc = query_docs[:, :, None] == key_docs[:, None, :]
    return jnp.where(same_doc[:, None], scores, masked_score)


def attend(query_rot, key_rot, value_low, query_docs, key_docs):
    scores = score_block(query_rot, key_rot, query_docs, key_docs)
    row_peak = jnp.max(scores, axis=-1, keepdims=True)
    exponent = jnp.exp(scores - row_peak)
    totals = jnp.sum(exponent, axis=-1, keepdims=True)
    probability = (exponent / totals).astype(jnp.bfloat16)
    mixed_out = jnp.einsum(
        "phqk,pkhd->pqhd", probability, value_low, preferred_element_type=jnp.float32
    )
    return (mixed_out, row_peak + jnp.log(totals))


def attend_back(query_rot, key_rot, value_low, query_docs, key_docs, logsum, grad_mixed):
    probability = jnp.exp(score_block(query_rot, key_rot, query_docs, key_docs) - logsum)
    grad_values = jnp.einsum(
        "phqk,pqhd->pkhd",
        probability.astype(jnp.bfloat16),
        grad_mixed,
        preferred_element_type=jnp.float32,
    )
    grad_probs = jnp.einsum(
        "pqhd,pkhd->phqk", grad_mixed, value_low, preferred_element_type=jnp.float32
    )
    inner_sum = jnp.sum(probability * grad_probs, axis=-1, keepdims=True)
    grad_scores = (probability * (grad_probs - inner_sum)).astype(jnp.bfloat16)
    grad_query = jnp.einsum(
        "phqk,pkhd->pqhd", grad_scores, key_rot, preferred_element_type=jnp.float32
    ) * HEAD_DIM ** (-0.5)
    grad_keys = jnp.einsum(
        "phqk,pqhd->pkhd", grad_scores, query_rot, preferred_element_type=jnp.float32
    ) * HEAD_DIM ** (-0.5)
    return (grad_query, grad_keys, grad_values)


def ffn_forward(rows, inner_cols, inner_offset, outer_cols):
    inner_pre = jnp.dot(rows, inner_cols, preferred_element_type=jnp.float32) + inner_offset
    act_value, gelu_pull = jax.vjp(gelu_exact, inner_pre)
    act_low = act_value.astype(jnp.bfloat16)
    return act_low, gelu_pull, contract_cols(act_low, outer_cols)


def ffn_backward(grads, gelu_pull, inner_cols, outer_cols):
    grad_act = jnp.dot(grads, outer_cols, preferred_element_type=jnp.float32)
    grad_inner = gelu_pull(grad_act)[0].astype(jnp.bfloat16)
    return grad_inner, contract_cols(grad_inner, inner_cols)


def local(
    layer_in,
    doc_ids,
    query_weight,
    query_bias,
    key_weight,
    key_bias,
    value_weight,
    value_bias,
    output_weight,
    output_bias,
    attn_gain,
    attn_shift,
    inner_weight,
    inner_bias,
    outer_weight,
    outer_bias,
    ffn_gain,
    ffn_shift,
    cotangent,
):
    wide_n = lax.axis_size("wide")
    narrow_n = lax.axis_size("narrow")
    total = wide_n * narrow_n
    share = query_weight.shape[0]
    small_list = (
        query_bias,
        key_bias,
        value_bias,
        output_bias,
        attn_gain,
        attn_shift,
        outer_bias,
        ffn_gain,
        ffn_shift,
    )
    small = jnp.stack(small_list, axis=1)
    small = jnp.pad(small, ((0, 0), (0, 128 - len(small_list))))
    shard = jnp.concatenate([query_weight, key_weight, value_weight, output_weight, small], axis=1)
    full = gather_all(shard).reshape(total * share, shard.shape[1])
    qkv_full = full[:, : 3 * D]
    output_full = full[:, 3 * D : 4 * D]
    vecs = full[:, 4 * D :].astype(jnp.float32)
    (
        query_offset,
        key_offset,
        value_offset,
        output_offset,
        attn_scale,
        attn_offset,
        outer_offset,
        ffn_scale,
        ffn_offset,
    ) = [vecs[:, i] for i in range(len(small_list))]
    qkv_offset = jnp.concatenate([query_offset, key_offset, value_offset])

    ffn_rows, ffn_cols = inner_weight.shape
    bias_n = inner_bias.shape[0]
    bias_k = -(-bias_n // ffn_rows)
    bias_rows = jnp.pad(inner_bias, (0, ffn_rows * bias_k - bias_n)).reshape(ffn_rows, bias_k)
    ffn_shard = jnp.concatenate([inner_weight, outer_weight.T, bias_rows], axis=1)
    ffn_shard, full = lax.optimization_barrier((ffn_shard, full))
    ffn_all = lax.all_gather(ffn_shard, "wide", axis=0, tiled=True)
    inner_cols = ffn_all[:, :ffn_cols]
    outer_cols = ffn_all[:, ffn_cols : 2 * ffn_cols]
    inner_offset = ffn_all[:, 2 * ffn_cols :].reshape(wide_n, ffn_rows * bias_k)[:, :bias_n]
    inner_offset = inner_offset.reshape(-1).astype(jnp.float32)

    rows_dev = layer_in.shape[0]
    half_len = doc_ids.shape[1] // 2
    pack_count = rows_dev // half_len
    narrow_place = lax.axis_index("narrow")
    half_bit = narrow_place % 2
    pair_slot = narrow_place // 2
    pack_docs = lax.dynamic_slice_in_dim(doc_ids, pair_slot * pack_count, pack_count, 0)
    my_docs = lax.dynamic_slice_in_dim(pack_docs, half_bit, 1, 0)
    cosine, sine_tab = jax.vmap(rotary_tables)(my_docs)
    cosine = cosine[:, :, None, :]
    sine_tab = sine_tab[:, :, None, :]

    def to_pack(rows):
        keep = lax.dynamic_slice_in_dim(rows, half_bit * half_len, half_len, 0)
        give = lax.dynamic_slice_in_dim(rows, (1 - half_bit) * half_len, half_len, 0)
        got = swapped(give, "narrow", 0)
        return jnp.where(
            half_bit == 0, jnp.concatenate([keep, got]), jnp.concatenate([got, keep])
        )

    def from_pack(rows):
        keep = lax.dynamic_slice_in_dim(rows, half_bit * half_len, half_len, 0)
        give = lax.dynamic_slice_in_dim(rows, (1 - half_bit) * half_len, half_len, 0)
        got = swapped(give, "narrow", 0)
        return jnp.where(
            half_bit == 0, jnp.concatenate([keep, got]), jnp.concatenate([got, keep])
        )

    pack_in = to_pack(layer_in)
    pack_cot = to_pack(cotangent)

    def heads_of(values):
        return values.reshape(1, rows_dev, HEADS, HEAD_DIM)

    qkv = jnp.dot(pack_in, qkv_full, preferred_element_type=jnp.float32) + qkv_offset
    query_rot = rotate(heads_of(qkv[:, :D]), cosine, sine_tab).astype(jnp.bfloat16)
    key_rot = rotate(heads_of(qkv[:, D : 2 * D]), cosine, sine_tab).astype(jnp.bfloat16)
    value_low = heads_of(qkv[:, 2 * D :]).astype(jnp.bfloat16)
    mixed_out, logsum = attend(query_rot, key_rot, value_low, my_docs, my_docs)
    mixed_low = mixed_out.reshape(rows_dev, D).astype(jnp.bfloat16)
    attn_out = jnp.dot(mixed_low, output_full, preferred_element_type=jnp.float32) + output_offset
    res_one = pack_in.astype(jnp.float32) + attn_out
    norm_one, norm_pull = jax.vjp(layer_norm, res_one, attn_scale, attn_offset)
    norm_low = norm_one.astype(jnp.bfloat16)

    if narrow_n == 2:
        far_rows = swapped(norm_low, "narrow", 0)
        own_act, own_pull, own_part = ffn_forward(norm_low, inner_cols, inner_offset, outer_cols)
        far_act, far_pull, far_part = ffn_forward(far_rows, inner_cols, inner_offset, outer_cols)
        outer_sum = own_part + swapped(far_part.astype(jnp.bfloat16), "narrow", 0).astype(
            jnp.float32
        )
    else:
        group_rows = lax.all_gather(norm_low, "narrow", axis=0, tiled=True)
        all_act, all_pull, all_part = ffn_forward(group_rows, inner_cols, inner_offset, outer_cols)
        outer_sum = narrow_scatter_sum(all_part)
    outer_out = outer_sum + outer_offset
    res_two = norm_one + outer_out
    pack_out, ffn_pull = jax.vjp(layer_norm, res_two, ffn_scale, ffn_offset)
    grad_two, ffn_gsum, ffn_ssum = ffn_pull(pack_cot.astype(jnp.float32))
    grad_outer = grad_two.astype(jnp.bfloat16)
    outer_bsum = jnp.sum(grad_outer.astype(jnp.float32), axis=0)
    if narrow_n == 2:
        far_grads = swapped(grad_outer, "narrow", 0)
        own_inner, own_back = ffn_backward(grad_outer, own_pull, inner_cols, outer_cols)
        far_inner, far_back = ffn_backward(far_grads, far_pull, inner_cols, outer_cols)
        grad_part = own_back + swapped(far_back.astype(jnp.bfloat16), "narrow", 0).astype(
            jnp.float32
        )
        outer_wsum_t = contract_rows(grad_outer, own_act) + contract_rows(far_grads, far_act)
        inner_wsum = contract_rows(norm_low, own_inner) + contract_rows(far_rows, far_inner)
        inner_bsum = jnp.sum(own_inner.astype(jnp.float32), axis=0) + jnp.sum(
            far_inner.astype(jnp.float32), axis=0
        )
    else:
        group_grads = lax.all_gather(grad_outer, "narrow", axis=0, tiled=True)
        all_inner, all_back = ffn_backward(group_grads, all_pull, inner_cols, outer_cols)
        grad_part = narrow_scatter_sum(all_back)
        outer_wsum_t = contract_rows(group_grads, all_act)
        inner_wsum = contract_rows(group_rows, all_inner)
        inner_bsum = jnp.sum(all_inner.astype(jnp.float32), axis=0)
    bsum_rows = jnp.pad(
        inner_bsum.reshape(wide_n, bias_n), ((0, 0), (0, ffn_rows * bias_k - bias_n))
    ).reshape(wide_n * ffn_rows, bias_k)
    ffn_sums = jnp.concatenate([inner_wsum, outer_wsum_t, bsum_rows], axis=1).astype(jnp.bfloat16)
    ffn_mine = lax.psum_scatter(ffn_sums, "wide", scatter_dimension=0, tiled=True)
    ffn_mine = ffn_mine.astype(jnp.float32)
    inner_wgrad = ffn_mine[:, :ffn_cols]
    outer_wgrad = ffn_mine[:, ffn_cols : 2 * ffn_cols].T
    inner_bgrad = ffn_mine[:, 2 * ffn_cols :].reshape(-1)[:bias_n]

    pack_out, grad_part = lax.optimization_barrier((pack_out, grad_part))
    layer_out = from_pack(pack_out)
    grad_norm = grad_two + grad_part
    grad_one, attn_gsum, attn_ssum = norm_pull(grad_norm)
    grad_attn = grad_one.astype(jnp.bfloat16)
    output_bsum = jnp.sum(grad_attn.astype(jnp.float32), axis=0)
    output_wsum = contract_rows(mixed_low, grad_attn)
    early_small = jnp.stack(
        [output_bsum, attn_gsum, attn_ssum, outer_bsum, ffn_gsum, ffn_ssum], axis=1
    )
    early = jnp.concatenate(
        [output_wsum.reshape(total, share, D), early_small.reshape(total, share, -1)], axis=2
    )

    grad_mixed = heads_of(contract_cols(grad_attn, output_full).astype(jnp.bfloat16))
    grad_qrot, grad_krot, grad_values = attend_back(
        query_rot, key_rot, value_low, my_docs, my_docs, logsum, grad_mixed
    )
    grad_qrot = grad_qrot + layer_out[0, 0] * 0.0
    grad_values = grad_values.astype(jnp.bfloat16)
    grad_query = unrotate(grad_qrot, cosine, sine_tab).astype(jnp.bfloat16)
    grad_keys = unrotate(grad_krot, cosine, sine_tab).astype(jnp.bfloat16)
    grad_qkv = jnp.concatenate(
        [
            grad_query.reshape(rows_dev, D),
            grad_keys.reshape(rows_dev, D),
            grad_values.reshape(rows_dev, D),
        ],
        axis=1,
    )
    pack_grad = grad_one + contract_cols(grad_qkv, qkv_full)
    keep_grad = lax.dynamic_slice_in_dim(pack_grad, half_bit * half_len, half_len, 0)
    give_grad = lax.dynamic_slice_in_dim(pack_grad, (1 - half_bit) * half_len, half_len, 0)
    give_grad, grad_qkv, pack_in = lax.optimization_barrier((give_grad, grad_qkv, pack_in))
    got_grad = swapped(give_grad, "narrow", 0)
    input_grad = jnp.where(
        half_bit == 0,
        jnp.concatenate([keep_grad, got_grad]),
        jnp.concatenate([got_grad, keep_grad]),
    )
    qkv_wsum = contract_rows(pack_in, grad_qkv)
    qkv_bsum = jnp.sum(grad_qkv.astype(jnp.float32), axis=0).reshape(3, D)
    wsum_parts = qkv_wsum.reshape(total, share, 3 * D).astype(jnp.bfloat16)
    cut = 3 * D * 4 // 9 // 128 * 128
    late_mine = scatter_sum_parts(
        [
            wsum_parts[..., :cut],
            wsum_parts[..., cut : 2 * cut],
            jnp.concatenate(
                [
                    wsum_parts[..., 2 * cut :],
                    qkv_bsum.T.reshape(total, share, 3).astype(jnp.bfloat16),
                    early.astype(jnp.bfloat16),
                ],
                axis=2,
            ),
        ]
    )
    early_mine = late_mine[:, 3 * D + 3 :]
    query_wgrad = late_mine[:, :D]
    key_wgrad = late_mine[:, D : 2 * D]
    value_wgrad = late_mine[:, 2 * D : 3 * D]
    query_bgrad = late_mine[:, 3 * D]
    key_bgrad = late_mine[:, 3 * D + 1]
    value_bgrad = late_mine[:, 3 * D + 2]
    output_wgrad = early_mine[:, :D]
    output_bgrad = early_mine[:, D]
    attn_ggrad = early_mine[:, D + 1]
    attn_sgrad = early_mine[:, D + 2]
    outer_bgrad = early_mine[:, D + 3]
    ffn_ggrad = early_mine[:, D + 4]
    ffn_sgrad = early_mine[:, D + 5]
    return (
        layer_out,
        input_grad,
        query_wgrad,
        query_bgrad,
        key_wgrad,
        key_bgrad,
        value_wgrad,
        value_bgrad,
        output_wgrad,
        output_bgrad,
        attn_ggrad,
        attn_sgrad,
        inner_wgrad,
        inner_bgrad,
        outer_wgrad,
        outer_bgrad,
        ffn_ggrad,
        ffn_sgrad,
    )


def solution(mesh):
    return jax.shard_map(
        local,
        mesh=mesh,
        in_specs=(
            P(("wide", "narrow"), None),
            P("wide", None),
            P(("wide", "narrow"), None),
            P(("wide", "narrow")),
            P(("wide", "narrow"), None),
            P(("wide", "narrow")),
            P(("wide", "narrow"), None),
            P(("wide", "narrow")),
            P(("wide", "narrow"), None),
            P(("wide", "narrow")),
            P(("wide", "narrow")),
            P(("wide", "narrow")),
            P("wide", "narrow"),
            P(("narrow", "wide")),
            P("narrow", "wide"),
            P(("wide", "narrow")),
            P(("wide", "narrow")),
            P(("wide", "narrow")),
            P(("wide", "narrow"), None),
        ),
        out_specs=(
            P(("wide", "narrow"), None),
            P(("wide", "narrow"), None),
            P(("wide", "narrow"), None),
            P(("wide", "narrow")),
            P(("wide", "narrow"), None),
            P(("wide", "narrow")),
            P(("wide", "narrow"), None),
            P(("wide", "narrow")),
            P(("wide", "narrow"), None),
            P(("wide", "narrow")),
            P(("wide", "narrow")),
            P(("wide", "narrow")),
            P("wide", "narrow"),
            P(("narrow", "wide")),
            P("narrow", "wide"),
            P(("wide", "narrow")),
            P(("wide", "narrow")),
            P(("wide", "narrow")),
        ),
        check_vma=False,
    )
```

```python
import jax
import jax.numpy as jnp
from jax import lax
from jax.sharding import PartitionSpec as P

D = 768
HEADS = 12
HEAD_DIM = 64

ALL = ("wide", "narrow")
layer_eps = 1e-12
masked_score = -1e30


def swapped(shard, axis, bit):
    return lax.ppermute(shard, axis, [(i, i ^ 1 << bit) for i in range(lax.axis_size(axis))])


def part_orders(total, narrow_n, parts):
    bits = total.bit_length() - 1
    core_bit = narrow_n.bit_length() - 1
    narrow_bits = list(range(core_bit))
    wide_bits = [b for b in reversed(range(core_bit + 1, bits))]
    orders = []
    for p in range(parts):
        k = p % max(1, len(wide_bits))
        orders.append(narrow_bits + wide_bits[k:] + wide_bits[:k] + [core_bit])
    return orders


def is_pow2(n):
    return n & (n - 1) == 0


def column_splits(cols, parts):
    tiles = -(-cols // 128)
    parts = max(1, min(parts, tiles))
    edges = [min(cols, (tiles * i // parts) * 128) for i in range(parts)] + [cols]
    return [(a, b) for a, b in zip(edges[:-1], edges[1:]) if b > a]


def doubling_gather(shard, order, total):
    me = lax.axis_index(ALL)
    cur = shard
    for b in order:
        other = lax.ppermute(cur, ALL, [(i, i ^ (1 << b)) for i in range(total)])
        bit = (me >> b) & 1
        pick = (jnp.arange(2) == bit).reshape((2,) + (1,) * cur.ndim)
        cur = jnp.where(pick, cur[None], other[None])
    k = len(order)
    perm = [k - 1 - order.index(b) for b in reversed(range(k))]
    cur = cur.transpose(perm + list(range(k, cur.ndim)))
    return cur.reshape((total,) + shard.shape)


def gather_all(shard, parts=3):
    total = lax.axis_size("wide") * lax.axis_size("narrow")
    narrow_n = lax.axis_size("narrow")
    if not (is_pow2(total) and is_pow2(narrow_n)):
        return lax.all_gather(shard, ALL, axis=0, tiled=False)
    splits = column_splits(shard.shape[-1], parts)
    orders = part_orders(total, narrow_n, len(splits))
    pieces = [
        doubling_gather(shard[..., a:b], order, total) for (a, b), order in zip(splits, orders)
    ]
    return jnp.concatenate(pieces, axis=-1)


def halving_scatter(parts_in, order, total):
    me = lax.axis_index(ALL)
    nbits = total.bit_length() - 1
    cur = parts_in.reshape((2,) * nbits + parts_in.shape[1:])
    axes = list(reversed(range(nbits)))
    for b in order:
        a = axes.index(b)
        bit = (me >> b) & 1
        mine = lax.dynamic_index_in_dim(cur, bit, axis=a, keepdims=False)
        theirs = lax.dynamic_index_in_dim(cur, 1 - bit, axis=a, keepdims=False)
        got = lax.ppermute(
            theirs.astype(jnp.bfloat16), ALL, [(i, i ^ (1 << b)) for i in range(total)]
        )
        cur = mine.astype(jnp.float32) + got.astype(jnp.float32)
        axes.pop(a)
    return cur


def scatter_sum_all(parts_in, parts=3):
    total = lax.axis_size("wide") * lax.axis_size("narrow")
    narrow_n = lax.axis_size("narrow")
    if not (is_pow2(total) and is_pow2(narrow_n)):
        return lax.psum_scatter(
            parts_in.astype(jnp.bfloat16), ALL, scatter_dimension=0, tiled=False
        ).astype(jnp.float32)
    splits = column_splits(parts_in.shape[-1], parts)
    orders = part_orders(total, narrow_n, len(splits))
    pieces = [
        halving_scatter(parts_in[..., a:b], list(reversed(order)), total)
        for (a, b), order in zip(splits, orders)
    ]
    return jnp.concatenate(pieces, axis=-1)


def scatter_sum_parts(part_list):
    total = lax.axis_size("wide") * lax.axis_size("narrow")
    narrow_n = lax.axis_size("narrow")
    if not (is_pow2(total) and is_pow2(narrow_n)):
        return jnp.concatenate([scatter_sum_all(x, 1) for x in part_list], axis=-1)
    orders = part_orders(total, narrow_n, len(part_list))
    return jnp.concatenate(
        [halving_scatter(x, list(reversed(o)), total) for x, o in zip(part_list, orders)],
        axis=-1,
    )


def narrow_gather(rows):
    n = lax.axis_size("narrow")
    if n != 2:
        return lax.all_gather(rows, "narrow", axis=0, tiled=True)
    other = swapped(rows, "narrow", 0)
    first = lax.axis_index("narrow") == 0
    return jnp.where(first, jnp.concatenate([rows, other]), jnp.concatenate([other, rows]))


def narrow_scatter_sum(part):
    n = lax.axis_size("narrow")
    if n != 2:
        return lax.psum_scatter(
            part.astype(jnp.bfloat16), "narrow", scatter_dimension=0, tiled=True
        ).astype(jnp.float32)
    rows = part.shape[0] // 2
    me = lax.axis_index("narrow")
    mine = lax.dynamic_slice_in_dim(part, me * rows, rows, 0)
    theirs = lax.dynamic_slice_in_dim(part, (1 - me) * rows, rows, 0)
    return mine + swapped(theirs.astype(jnp.bfloat16), "narrow", 0).astype(jnp.float32)


def layer_norm(values, gain_vec, shift_vec):
    center = values - jnp.mean(values, axis=-1, keepdims=True)
    spread = jnp.mean(center * center, axis=-1, keepdims=True)
    return center * lax.rsqrt(spread + layer_eps) * gain_vec + shift_vec


def gelu_exact(values):
    return jax.nn.gelu(values, approximate=False)


def rotary_tables(doc_row):
    places = jnp.arange(doc_row.shape[0], dtype=jnp.int32)
    before = jnp.sum((doc_row[None, :] < doc_row[:, None]).astype(jnp.int32), axis=1)
    position = (places - before).astype(jnp.float32)
    frequency = 10000.0 ** (-2.0 * jnp.arange(HEAD_DIM // 2, dtype=jnp.float32) / HEAD_DIM)
    angles = position[:, None] * frequency[None, :]
    return (jnp.cos(angles), jnp.sin(angles))


def rotate(values, cosine, sine_tab):
    half_dim = values.shape[-1] // 2
    first_half = values[..., :half_dim]
    second = values[..., half_dim:]
    return jnp.concatenate(
        [first_half * cosine - second * sine_tab, second * cosine + first_half * sine_tab], axis=-1
    )


def unrotate(values, cosine, sine_tab):
    half_dim = values.shape[-1] // 2
    first_half = values[..., :half_dim]
    second = values[..., half_dim:]
    return jnp.concatenate(
        [first_half * cosine + second * sine_tab, second * cosine - first_half * sine_tab], axis=-1
    )


def contract_rows(left_op, right_op):
    return lax.dot_general(
        left_op, right_op, (((0,), (0,)), ((), ())), preferred_element_type=jnp.float32
    )


def contract_cols(left_op, right_op):
    return lax.dot_general(
        left_op, right_op, (((1,), (1,)), ((), ())), preferred_element_type=jnp.float32
    )


def score_block(query_rot, key_rot, query_docs, key_docs):
    scores = jnp.einsum(
        "pqhd,pkhd->phqk", query_rot, key_rot, preferred_element_type=jnp.float32
    ) * HEAD_DIM ** (-0.5)
    same_doc = query_docs[:, :, None] == key_docs[:, None, :]
    return jnp.where(same_doc[:, None], scores, masked_score)


def attend(query_rot, key_rot, value_low, query_docs, key_docs):
    scores = score_block(query_rot, key_rot, query_docs, key_docs)
    row_peak = jnp.max(scores, axis=-1, keepdims=True)
    exponent = jnp.exp(scores - row_peak)
    totals = jnp.sum(exponent, axis=-1, keepdims=True)
    probability = (exponent / totals).astype(jnp.bfloat16)
    mixed_out = jnp.einsum(
        "phqk,pkhd->pqhd", probability, value_low, preferred_element_type=jnp.float32
    )
    return (mixed_out, row_peak + jnp.log(totals))


def attend_back(query_rot, key_rot, value_low, query_docs, key_docs, logsum, grad_mixed):
    probability = jnp.exp(score_block(query_rot, key_rot, query_docs, key_docs) - logsum)
    grad_values = jnp.einsum(
        "phqk,pqhd->pkhd",
        probability.astype(jnp.bfloat16),
        grad_mixed,
        preferred_element_type=jnp.float32,
    )
    grad_probs = jnp.einsum(
        "pqhd,pkhd->phqk", grad_mixed, value_low, preferred_element_type=jnp.float32
    )
    inner_sum = jnp.sum(probability * grad_probs, axis=-1, keepdims=True)
    grad_scores = (probability * (grad_probs - inner_sum)).astype(jnp.bfloat16)
    grad_query = jnp.einsum(
        "phqk,pkhd->pqhd", grad_scores, key_rot, preferred_element_type=jnp.float32
    ) * HEAD_DIM ** (-0.5)
    grad_keys = jnp.einsum(
        "phqk,pqhd->pkhd", grad_scores, query_rot, preferred_element_type=jnp.float32
    ) * HEAD_DIM ** (-0.5)
    return (grad_query, grad_keys, grad_values)


def ffn_forward(rows, inner_cols, inner_offset, outer_cols):
    inner_pre = jnp.dot(rows, inner_cols, preferred_element_type=jnp.float32) + inner_offset
    act_value, gelu_pull = jax.vjp(gelu_exact, inner_pre)
    act_low = act_value.astype(jnp.bfloat16)
    return act_low, gelu_pull, contract_cols(act_low, outer_cols)


def ffn_backward(grads, gelu_pull, inner_cols, outer_cols):
    grad_act = jnp.dot(grads, outer_cols, preferred_element_type=jnp.float32)
    grad_inner = gelu_pull(grad_act)[0].astype(jnp.bfloat16)
    return grad_inner, contract_cols(grad_inner, inner_cols)


def local(
    layer_in,
    doc_ids,
    query_weight,
    query_bias,
    key_weight,
    key_bias,
    value_weight,
    value_bias,
    output_weight,
    output_bias,
    attn_gain,
    attn_shift,
    inner_weight,
    inner_bias,
    outer_weight,
    outer_bias,
    ffn_gain,
    ffn_shift,
    cotangent,
):
    wide_n = lax.axis_size("wide")
    narrow_n = lax.axis_size("narrow")
    total = wide_n * narrow_n
    share = query_weight.shape[0]
    small_list = (
        query_bias,
        key_bias,
        value_bias,
        output_bias,
        attn_gain,
        attn_shift,
        outer_bias,
        ffn_gain,
        ffn_shift,
    )
    small = jnp.stack(small_list, axis=1)
    small = jnp.pad(small, ((0, 0), (0, 128 - len(small_list))))
    shard = jnp.concatenate([query_weight, key_weight, value_weight, output_weight, small], axis=1)
    full = gather_all(shard).reshape(total * share, shard.shape[1])
    qkv_full = full[:, : 3 * D]
    output_full = full[:, 3 * D : 4 * D]
    vecs = full[:, 4 * D :].astype(jnp.float32)
    (
        query_offset,
        key_offset,
        value_offset,
        output_offset,
        attn_scale,
        attn_offset,
        outer_offset,
        ffn_scale,
        ffn_offset,
    ) = [vecs[:, i] for i in range(len(small_list))]
    qkv_offset = jnp.concatenate([query_offset, key_offset, value_offset])

    ffn_rows, ffn_cols = inner_weight.shape
    bias_n = inner_bias.shape[0]
    bias_k = -(-bias_n // ffn_rows)
    bias_rows = jnp.pad(inner_bias, (0, ffn_rows * bias_k - bias_n)).reshape(ffn_rows, bias_k)
    ffn_shard = jnp.concatenate([inner_weight, outer_weight.T, bias_rows], axis=1)
    ffn_shard, full = lax.optimization_barrier((ffn_shard, full))
    ffn_all = lax.all_gather(ffn_shard, "wide", axis=0, tiled=True)
    inner_cols = ffn_all[:, :ffn_cols]
    outer_cols = ffn_all[:, ffn_cols : 2 * ffn_cols]
    inner_offset = ffn_all[:, 2 * ffn_cols :].reshape(wide_n, ffn_rows * bias_k)[:, :bias_n]
    inner_offset = inner_offset.reshape(-1).astype(jnp.float32)

    rows_dev = layer_in.shape[0]
    half_len = doc_ids.shape[1] // 2
    pack_count = rows_dev // half_len
    narrow_place = lax.axis_index("narrow")
    half_bit = narrow_place % 2
    pair_slot = narrow_place // 2
    pack_docs = lax.dynamic_slice_in_dim(doc_ids, pair_slot * pack_count, pack_count, 0)
    my_docs = lax.dynamic_slice_in_dim(pack_docs, half_bit, 1, 0)
    cosine, sine_tab = jax.vmap(rotary_tables)(my_docs)
    cosine = cosine[:, :, None, :]
    sine_tab = sine_tab[:, :, None, :]

    def to_pack(rows):
        keep = lax.dynamic_slice_in_dim(rows, half_bit * half_len, half_len, 0)
        give = lax.dynamic_slice_in_dim(rows, (1 - half_bit) * half_len, half_len, 0)
        got = swapped(give, "narrow", 0)
        return jnp.where(
            half_bit == 0, jnp.concatenate([keep, got]), jnp.concatenate([got, keep])
        )

    def from_pack(rows):
        keep = lax.dynamic_slice_in_dim(rows, half_bit * half_len, half_len, 0)
        give = lax.dynamic_slice_in_dim(rows, (1 - half_bit) * half_len, half_len, 0)
        got = swapped(give, "narrow", 0)
        return jnp.where(
            half_bit == 0, jnp.concatenate([keep, got]), jnp.concatenate([got, keep])
        )

    pack_in = to_pack(layer_in)
    pack_cot = to_pack(cotangent)

    def heads_of(values):
        return values.reshape(1, rows_dev, HEADS, HEAD_DIM)

    qkv = jnp.dot(pack_in, qkv_full, preferred_element_type=jnp.float32) + qkv_offset
    query_rot = rotate(heads_of(qkv[:, :D]), cosine, sine_tab).astype(jnp.bfloat16)
    key_rot = rotate(heads_of(qkv[:, D : 2 * D]), cosine, sine_tab).astype(jnp.bfloat16)
    value_low = heads_of(qkv[:, 2 * D :]).astype(jnp.bfloat16)
    mixed_out, logsum = attend(query_rot, key_rot, value_low, my_docs, my_docs)
    mixed_low = mixed_out.reshape(rows_dev, D).astype(jnp.bfloat16)
    attn_out = jnp.dot(mixed_low, output_full, preferred_element_type=jnp.float32) + output_offset
    res_one = pack_in.astype(jnp.float32) + attn_out
    norm_one, norm_pull = jax.vjp(layer_norm, res_one, attn_scale, attn_offset)
    norm_low = norm_one.astype(jnp.bfloat16)

    if narrow_n == 2:
        far_rows = swapped(norm_low, "narrow", 0)
        own_act, own_pull, own_part = ffn_forward(norm_low, inner_cols, inner_offset, outer_cols)
        far_act, far_pull, far_part = ffn_forward(far_rows, inner_cols, inner_offset, outer_cols)
        outer_sum = own_part + swapped(far_part.astype(jnp.bfloat16), "narrow", 0).astype(
            jnp.float32
        )
    else:
        group_rows = lax.all_gather(norm_low, "narrow", axis=0, tiled=True)
        all_act, all_pull, all_part = ffn_forward(group_rows, inner_cols, inner_offset, outer_cols)
        outer_sum = narrow_scatter_sum(all_part)
    outer_out = outer_sum + outer_offset
    res_two = norm_one + outer_out
    pack_out, ffn_pull = jax.vjp(layer_norm, res_two, ffn_scale, ffn_offset)
    grad_two, ffn_gsum, ffn_ssum = ffn_pull(pack_cot.astype(jnp.float32))
    grad_outer = grad_two.astype(jnp.bfloat16)
    outer_bsum = jnp.sum(grad_outer.astype(jnp.float32), axis=0)
    if narrow_n == 2:
        far_grads = swapped(grad_outer, "narrow", 0)
        own_inner, own_back = ffn_backward(grad_outer, own_pull, inner_cols, outer_cols)
        far_inner, far_back = ffn_backward(far_grads, far_pull, inner_cols, outer_cols)
        grad_part = own_back + swapped(far_back.astype(jnp.bfloat16), "narrow", 0).astype(
            jnp.float32
        )
        outer_wsum_t = contract_rows(grad_outer, own_act) + contract_rows(far_grads, far_act)
        inner_wsum = contract_rows(norm_low, own_inner) + contract_rows(far_rows, far_inner)
        inner_bsum = jnp.sum(own_inner.astype(jnp.float32), axis=0) + jnp.sum(
            far_inner.astype(jnp.float32), axis=0
        )
    else:
        group_grads = lax.all_gather(grad_outer, "narrow", axis=0, tiled=True)
        all_inner, all_back = ffn_backward(group_grads, all_pull, inner_cols, outer_cols)
        grad_part = narrow_scatter_sum(all_back)
        outer_wsum_t = contract_rows(group_grads, all_act)
        inner_wsum = contract_rows(group_rows, all_inner)
        inner_bsum = jnp.sum(all_inner.astype(jnp.float32), axis=0)
    bsum_rows = jnp.pad(
        inner_bsum.reshape(wide_n, bias_n), ((0, 0), (0, ffn_rows * bias_k - bias_n))
    ).reshape(wide_n * ffn_rows, bias_k)
    ffn_sums = jnp.concatenate([inner_wsum, outer_wsum_t, bsum_rows], axis=1).astype(jnp.bfloat16)
    ffn_mine = lax.psum_scatter(ffn_sums, "wide", scatter_dimension=0, tiled=True)
    ffn_mine = ffn_mine.astype(jnp.float32)
    inner_wgrad = ffn_mine[:, :ffn_cols]
    outer_wgrad = ffn_mine[:, ffn_cols : 2 * ffn_cols].T
    inner_bgrad = ffn_mine[:, 2 * ffn_cols :].reshape(-1)[:bias_n]

    pack_out, grad_part = lax.optimization_barrier((pack_out, grad_part))
    layer_out = from_pack(pack_out)
    grad_norm = grad_two + grad_part
    grad_one, attn_gsum, attn_ssum = norm_pull(grad_norm)
    grad_attn = grad_one.astype(jnp.bfloat16)
    output_bsum = jnp.sum(grad_attn.astype(jnp.float32), axis=0)
    output_wsum = contract_rows(mixed_low, grad_attn)
    early_small = jnp.stack(
        [output_bsum, attn_gsum, attn_ssum, outer_bsum, ffn_gsum, ffn_ssum], axis=1
    )
    early = jnp.concatenate(
        [output_wsum.reshape(total, share, D), early_small.reshape(total, share, -1)], axis=2
    )

    grad_mixed = heads_of(contract_cols(grad_attn, output_full).astype(jnp.bfloat16))
    grad_qrot, grad_krot, grad_values = attend_back(
        query_rot, key_rot, value_low, my_docs, my_docs, logsum, grad_mixed
    )
    grad_values = grad_values.astype(jnp.bfloat16)
    grad_query = unrotate(grad_qrot, cosine, sine_tab).astype(jnp.bfloat16)
    grad_keys = unrotate(grad_krot, cosine, sine_tab).astype(jnp.bfloat16)
    grad_qkv = jnp.concatenate(
        [
            grad_query.reshape(rows_dev, D),
            grad_keys.reshape(rows_dev, D),
            grad_values.reshape(rows_dev, D),
        ],
        axis=1,
    )
    pack_grad = grad_one + contract_cols(grad_qkv, qkv_full)
    keep_grad = lax.dynamic_slice_in_dim(pack_grad, half_bit * half_len, half_len, 0)
    give_grad = lax.dynamic_slice_in_dim(pack_grad, (1 - half_bit) * half_len, half_len, 0)
    give_grad, grad_qkv, pack_in = lax.optimization_barrier((give_grad, grad_qkv, pack_in))
    got_grad = swapped(give_grad, "narrow", 0)
    input_grad = jnp.where(
        half_bit == 0,
        jnp.concatenate([keep_grad, got_grad]),
        jnp.concatenate([got_grad, keep_grad]),
    )
    qkv_wsum = contract_rows(pack_in, grad_qkv)
    qkv_bsum = jnp.sum(grad_qkv.astype(jnp.float32), axis=0).reshape(3, D)
    wsum_parts = qkv_wsum.reshape(total, share, 3 * D).astype(jnp.bfloat16)
    cut = 3 * D * 2 // 3 // 128 * 128
    late_mine = scatter_sum_parts(
        [
            wsum_parts[..., :cut],
            jnp.concatenate(
                [
                    wsum_parts[..., cut:],
                    qkv_bsum.T.reshape(total, share, 3).astype(jnp.bfloat16),
                    early.astype(jnp.bfloat16),
                ],
                axis=2,
            ),
        ]
    )
    early_mine = late_mine[:, 3 * D + 3 :]
    query_wgrad = late_mine[:, :D]
    key_wgrad = late_mine[:, D : 2 * D]
    value_wgrad = late_mine[:, 2 * D : 3 * D]
    query_bgrad = late_mine[:, 3 * D]
    key_bgrad = late_mine[:, 3 * D + 1]
    value_bgrad = late_mine[:, 3 * D + 2]
    output_wgrad = early_mine[:, :D]
    output_bgrad = early_mine[:, D]
    attn_ggrad = early_mine[:, D + 1]
    attn_sgrad = early_mine[:, D + 2]
    outer_bgrad = early_mine[:, D + 3]
    ffn_ggrad = early_mine[:, D + 4]
    ffn_sgrad = early_mine[:, D + 5]
    return (
        layer_out,
        input_grad,
        query_wgrad,
        query_bgrad,
        key_wgrad,
        key_bgrad,
        value_wgrad,
        value_bgrad,
        output_wgrad,
        output_bgrad,
        attn_ggrad,
        attn_sgrad,
        inner_wgrad,
        inner_bgrad,
        outer_wgrad,
        outer_bgrad,
        ffn_ggrad,
        ffn_sgrad,
    )


def solution(mesh):
    return jax.shard_map(
        local,
        mesh=mesh,
        in_specs=(
            P(("wide", "narrow"), None),
            P("wide", None),
            P(("wide", "narrow"), None),
            P(("wide", "narrow")),
            P(("wide", "narrow"), None),
            P(("wide", "narrow")),
            P(("wide", "narrow"), None),
            P(("wide", "narrow")),
            P(("wide", "narrow"), None),
            P(("wide", "narrow")),
            P(("wide", "narrow")),
            P(("wide", "narrow")),
            P("wide", "narrow"),
            P(("narrow", "wide")),
            P("narrow", "wide"),
            P(("wide", "narrow")),
            P(("wide", "narrow")),
            P(("wide", "narrow")),
            P(("wide", "narrow"), None),
        ),
        out_specs=(
            P(("wide", "narrow"), None),
            P(("wide", "narrow"), None),
            P(("wide", "narrow"), None),
            P(("wide", "narrow")),
            P(("wide", "narrow"), None),
            P(("wide", "narrow")),
            P(("wide", "narrow"), None),
            P(("wide", "narrow")),
            P(("wide", "narrow"), None),
            P(("wide", "narrow")),
            P(("wide", "narrow")),
            P(("wide", "narrow")),
            P("wide", "narrow"),
            P(("narrow", "wide")),
            P("narrow", "wide"),
            P(("wide", "narrow")),
            P(("wide", "narrow")),
            P(("wide", "narrow")),
        ),
        check_vma=False,
    )
```

```python
import itertools

import jax
import jax.numpy as jnp
from jax import lax
from jax.sharding import PartitionSpec as P

D = 768
HEADS = 12
HEAD_DIM = 64

ALL = ("wide", "narrow")
layer_eps = 1e-12
masked_score = -1e30


def swapped(shard, axis, bit):
    return lax.ppermute(shard, axis, [(i, i ^ 1 << bit) for i in range(lax.axis_size(axis))])


def part_orders(total, narrow_n, parts):
    bits = total.bit_length() - 1
    core_bit = narrow_n.bit_length() - 1
    narrow_bits = list(range(core_bit))
    wide_bits = [b for b in reversed(range(core_bit + 1, bits))]
    rotations = [wide_bits[k:] + wide_bits[:k] for k in range(max(1, len(wide_bits)))]
    others = [list(p) for p in itertools.permutations(wide_bits) if list(p) not in rotations]
    choices = rotations + others
    return [narrow_bits + choices[p % len(choices)] + [core_bit] for p in range(parts)]


def is_pow2(n):
    return n & (n - 1) == 0


def column_splits(cols, parts):
    tiles = -(-cols // 128)
    parts = max(1, min(parts, tiles))
    edges = [min(cols, (tiles * i // parts) * 128) for i in range(parts)] + [cols]
    return [(a, b) for a, b in zip(edges[:-1], edges[1:]) if b > a]


def doubling_gather(shard, order, total):
    me = lax.axis_index(ALL)
    cur = shard
    for b in order:
        other = lax.ppermute(cur, ALL, [(i, i ^ (1 << b)) for i in range(total)])
        bit = (me >> b) & 1
        pick = (jnp.arange(2) == bit).reshape((2,) + (1,) * cur.ndim)
        cur = jnp.where(pick, cur[None], other[None])
    k = len(order)
    perm = [k - 1 - order.index(b) for b in reversed(range(k))]
    cur = cur.transpose(perm + list(range(k, cur.ndim)))
    return cur.reshape((total,) + shard.shape)


def gather_all(shard, parts=3):
    total = lax.axis_size("wide") * lax.axis_size("narrow")
    narrow_n = lax.axis_size("narrow")
    if not (is_pow2(total) and is_pow2(narrow_n)):
        return lax.all_gather(shard, ALL, axis=0, tiled=False)
    splits = column_splits(shard.shape[-1], parts)
    orders = part_orders(total, narrow_n, len(splits))
    pieces = [
        doubling_gather(shard[..., a:b], order, total) for (a, b), order in zip(splits, orders)
    ]
    return jnp.concatenate(pieces, axis=-1)


def halving_scatter(parts_in, order, total):
    me = lax.axis_index(ALL)
    nbits = total.bit_length() - 1
    cur = parts_in.reshape((2,) * nbits + parts_in.shape[1:])
    axes = list(reversed(range(nbits)))
    for b in order:
        a = axes.index(b)
        bit = (me >> b) & 1
        mine = lax.dynamic_index_in_dim(cur, bit, axis=a, keepdims=False)
        theirs = lax.dynamic_index_in_dim(cur, 1 - bit, axis=a, keepdims=False)
        got = lax.ppermute(
            theirs.astype(jnp.bfloat16), ALL, [(i, i ^ (1 << b)) for i in range(total)]
        )
        cur = mine.astype(jnp.float32) + got.astype(jnp.float32)
        axes.pop(a)
    return cur


def scatter_sum_all(parts_in, parts=3):
    total = lax.axis_size("wide") * lax.axis_size("narrow")
    narrow_n = lax.axis_size("narrow")
    if not (is_pow2(total) and is_pow2(narrow_n)):
        return lax.psum_scatter(
            parts_in.astype(jnp.bfloat16), ALL, scatter_dimension=0, tiled=False
        ).astype(jnp.float32)
    splits = column_splits(parts_in.shape[-1], parts)
    orders = part_orders(total, narrow_n, len(splits))
    pieces = [
        halving_scatter(parts_in[..., a:b], list(reversed(order)), total)
        for (a, b), order in zip(splits, orders)
    ]
    return jnp.concatenate(pieces, axis=-1)


def scatter_sum_parts(part_list):
    total = lax.axis_size("wide") * lax.axis_size("narrow")
    narrow_n = lax.axis_size("narrow")
    if not (is_pow2(total) and is_pow2(narrow_n)):
        return jnp.concatenate([scatter_sum_all(x, 1) for x in part_list], axis=-1)
    orders = part_orders(total, narrow_n, len(part_list))
    return jnp.concatenate(
        [halving_scatter(x, list(reversed(o)), total) for x, o in zip(part_list, orders)],
        axis=-1,
    )


def narrow_gather(rows):
    n = lax.axis_size("narrow")
    if n != 2:
        return lax.all_gather(rows, "narrow", axis=0, tiled=True)
    other = swapped(rows, "narrow", 0)
    first = lax.axis_index("narrow") == 0
    return jnp.where(first, jnp.concatenate([rows, other]), jnp.concatenate([other, rows]))


def narrow_scatter_sum(part):
    n = lax.axis_size("narrow")
    if n != 2:
        return lax.psum_scatter(
            part.astype(jnp.bfloat16), "narrow", scatter_dimension=0, tiled=True
        ).astype(jnp.float32)
    rows = part.shape[0] // 2
    me = lax.axis_index("narrow")
    mine = lax.dynamic_slice_in_dim(part, me * rows, rows, 0)
    theirs = lax.dynamic_slice_in_dim(part, (1 - me) * rows, rows, 0)
    return mine + swapped(theirs.astype(jnp.bfloat16), "narrow", 0).astype(jnp.float32)


def layer_norm(values, gain_vec, shift_vec):
    center = values - jnp.mean(values, axis=-1, keepdims=True)
    spread = jnp.mean(center * center, axis=-1, keepdims=True)
    return center * lax.rsqrt(spread + layer_eps) * gain_vec + shift_vec


def gelu_exact(values):
    return jax.nn.gelu(values, approximate=False)


def rotary_tables(doc_row):
    places = jnp.arange(doc_row.shape[0], dtype=jnp.int32)
    before = jnp.sum((doc_row[None, :] < doc_row[:, None]).astype(jnp.int32), axis=1)
    position = (places - before).astype(jnp.float32)
    frequency = 10000.0 ** (-2.0 * jnp.arange(HEAD_DIM // 2, dtype=jnp.float32) / HEAD_DIM)
    angles = position[:, None] * frequency[None, :]
    return (jnp.cos(angles), jnp.sin(angles))


def rotate(values, cosine, sine_tab):
    half_dim = values.shape[-1] // 2
    first_half = values[..., :half_dim]
    second = values[..., half_dim:]
    return jnp.concatenate(
        [first_half * cosine - second * sine_tab, second * cosine + first_half * sine_tab], axis=-1
    )


def unrotate(values, cosine, sine_tab):
    half_dim = values.shape[-1] // 2
    first_half = values[..., :half_dim]
    second = values[..., half_dim:]
    return jnp.concatenate(
        [first_half * cosine + second * sine_tab, second * cosine - first_half * sine_tab], axis=-1
    )


def contract_rows(left_op, right_op):
    return lax.dot_general(
        left_op, right_op, (((0,), (0,)), ((), ())), preferred_element_type=jnp.float32
    )


def contract_cols(left_op, right_op):
    return lax.dot_general(
        left_op, right_op, (((1,), (1,)), ((), ())), preferred_element_type=jnp.float32
    )


def score_block(query_rot, key_rot, query_docs, key_docs):
    scores = jnp.einsum(
        "pqhd,pkhd->phqk", query_rot, key_rot, preferred_element_type=jnp.float32
    ) * HEAD_DIM ** (-0.5)
    same_doc = query_docs[:, :, None] == key_docs[:, None, :]
    return jnp.where(same_doc[:, None], scores, masked_score)


def attend(query_rot, key_rot, value_low, query_docs, key_docs):
    scores = score_block(query_rot, key_rot, query_docs, key_docs)
    row_peak = jnp.max(scores, axis=-1, keepdims=True)
    exponent = jnp.exp(scores - row_peak)
    totals = jnp.sum(exponent, axis=-1, keepdims=True)
    probability = (exponent / totals).astype(jnp.bfloat16)
    mixed_out = jnp.einsum(
        "phqk,pkhd->pqhd", probability, value_low, preferred_element_type=jnp.float32
    )
    return (mixed_out, row_peak + jnp.log(totals))


def attend_back(query_rot, key_rot, value_low, query_docs, key_docs, logsum, grad_mixed):
    probability = jnp.exp(score_block(query_rot, key_rot, query_docs, key_docs) - logsum)
    grad_values = jnp.einsum(
        "phqk,pqhd->pkhd",
        probability.astype(jnp.bfloat16),
        grad_mixed,
        preferred_element_type=jnp.float32,
    )
    grad_probs = jnp.einsum(
        "pqhd,pkhd->phqk", grad_mixed, value_low, preferred_element_type=jnp.float32
    )
    inner_sum = jnp.sum(probability * grad_probs, axis=-1, keepdims=True)
    grad_scores = (probability * (grad_probs - inner_sum)).astype(jnp.bfloat16)
    grad_query = jnp.einsum(
        "phqk,pkhd->pqhd", grad_scores, key_rot, preferred_element_type=jnp.float32
    ) * HEAD_DIM ** (-0.5)
    grad_keys = jnp.einsum(
        "phqk,pqhd->pkhd", grad_scores, query_rot, preferred_element_type=jnp.float32
    ) * HEAD_DIM ** (-0.5)
    return (grad_query, grad_keys, grad_values)


def ffn_forward(rows, inner_cols, inner_offset, outer_cols):
    inner_pre = jnp.dot(rows, inner_cols, preferred_element_type=jnp.float32) + inner_offset
    act_value, gelu_pull = jax.vjp(gelu_exact, inner_pre)
    act_low = act_value.astype(jnp.bfloat16)
    return act_low, gelu_pull, contract_cols(act_low, outer_cols)


def ffn_backward(grads, gelu_pull, inner_cols, outer_cols):
    grad_act = jnp.dot(grads, outer_cols, preferred_element_type=jnp.float32)
    grad_inner = gelu_pull(grad_act)[0].astype(jnp.bfloat16)
    return grad_inner, contract_cols(grad_inner, inner_cols)


def local(
    layer_in,
    doc_ids,
    query_weight,
    query_bias,
    key_weight,
    key_bias,
    value_weight,
    value_bias,
    output_weight,
    output_bias,
    attn_gain,
    attn_shift,
    inner_weight,
    inner_bias,
    outer_weight,
    outer_bias,
    ffn_gain,
    ffn_shift,
    cotangent,
):
    wide_n = lax.axis_size("wide")
    narrow_n = lax.axis_size("narrow")
    total = wide_n * narrow_n
    share = query_weight.shape[0]
    small_list = (
        query_bias,
        key_bias,
        value_bias,
        output_bias,
        attn_gain,
        attn_shift,
        outer_bias,
        ffn_gain,
        ffn_shift,
    )
    small = jnp.stack(small_list, axis=1)
    small = jnp.pad(small, ((0, 0), (0, 128 - len(small_list))))
    shard = jnp.concatenate([query_weight, key_weight, value_weight, output_weight, small], axis=1)
    full = gather_all(shard).reshape(total * share, shard.shape[1])
    qkv_full = full[:, : 3 * D]
    output_full = full[:, 3 * D : 4 * D]
    vecs = full[:, 4 * D :].astype(jnp.float32)
    (
        query_offset,
        key_offset,
        value_offset,
        output_offset,
        attn_scale,
        attn_offset,
        outer_offset,
        ffn_scale,
        ffn_offset,
    ) = [vecs[:, i] for i in range(len(small_list))]
    qkv_offset = jnp.concatenate([query_offset, key_offset, value_offset])

    ffn_rows, ffn_cols = inner_weight.shape
    bias_n = inner_bias.shape[0]
    bias_k = -(-bias_n // ffn_rows)
    bias_rows = jnp.pad(inner_bias, (0, ffn_rows * bias_k - bias_n)).reshape(ffn_rows, bias_k)
    ffn_shard = jnp.concatenate([inner_weight, outer_weight.T, bias_rows], axis=1)
    ffn_shard, full = lax.optimization_barrier((ffn_shard, full))
    ffn_all = lax.all_gather(ffn_shard, "wide", axis=0, tiled=True)
    inner_cols = ffn_all[:, :ffn_cols]
    outer_cols = ffn_all[:, ffn_cols : 2 * ffn_cols]
    inner_offset = ffn_all[:, 2 * ffn_cols :].reshape(wide_n, ffn_rows * bias_k)[:, :bias_n]
    inner_offset = inner_offset.reshape(-1).astype(jnp.float32)

    rows_dev = layer_in.shape[0]
    half_len = doc_ids.shape[1] // 2
    pack_count = rows_dev // half_len
    narrow_place = lax.axis_index("narrow")
    half_bit = narrow_place % 2
    pair_slot = narrow_place // 2
    pack_docs = lax.dynamic_slice_in_dim(doc_ids, pair_slot * pack_count, pack_count, 0)
    my_docs = lax.dynamic_slice_in_dim(pack_docs, half_bit, 1, 0)
    cosine, sine_tab = jax.vmap(rotary_tables)(my_docs)
    cosine = cosine[:, :, None, :]
    sine_tab = sine_tab[:, :, None, :]

    def to_pack(rows):
        keep = lax.dynamic_slice_in_dim(rows, half_bit * half_len, half_len, 0)
        give = lax.dynamic_slice_in_dim(rows, (1 - half_bit) * half_len, half_len, 0)
        got = swapped(give, "narrow", 0)
        return jnp.where(
            half_bit == 0, jnp.concatenate([keep, got]), jnp.concatenate([got, keep])
        )

    def from_pack(rows):
        keep = lax.dynamic_slice_in_dim(rows, half_bit * half_len, half_len, 0)
        give = lax.dynamic_slice_in_dim(rows, (1 - half_bit) * half_len, half_len, 0)
        got = swapped(give, "narrow", 0)
        return jnp.where(
            half_bit == 0, jnp.concatenate([keep, got]), jnp.concatenate([got, keep])
        )

    pack_in = to_pack(layer_in)
    pack_cot = to_pack(cotangent)

    def heads_of(values):
        return values.reshape(1, rows_dev, HEADS, HEAD_DIM)

    qkv = jnp.dot(pack_in, qkv_full, preferred_element_type=jnp.float32) + qkv_offset
    query_rot = rotate(heads_of(qkv[:, :D]), cosine, sine_tab).astype(jnp.bfloat16)
    key_rot = rotate(heads_of(qkv[:, D : 2 * D]), cosine, sine_tab).astype(jnp.bfloat16)
    value_low = heads_of(qkv[:, 2 * D :]).astype(jnp.bfloat16)
    mixed_out, logsum = attend(query_rot, key_rot, value_low, my_docs, my_docs)
    mixed_low = mixed_out.reshape(rows_dev, D).astype(jnp.bfloat16)
    attn_out = jnp.dot(mixed_low, output_full, preferred_element_type=jnp.float32) + output_offset
    res_one = pack_in.astype(jnp.float32) + attn_out
    norm_one, norm_pull = jax.vjp(layer_norm, res_one, attn_scale, attn_offset)
    norm_low = norm_one.astype(jnp.bfloat16)

    if narrow_n == 2:
        far_rows = swapped(norm_low, "narrow", 0)
        own_act, own_pull, own_part = ffn_forward(norm_low, inner_cols, inner_offset, outer_cols)
        far_act, far_pull, far_part = ffn_forward(far_rows, inner_cols, inner_offset, outer_cols)
        outer_sum = own_part + swapped(far_part.astype(jnp.bfloat16), "narrow", 0).astype(
            jnp.float32
        )
    else:
        group_rows = lax.all_gather(norm_low, "narrow", axis=0, tiled=True)
        all_act, all_pull, all_part = ffn_forward(group_rows, inner_cols, inner_offset, outer_cols)
        outer_sum = narrow_scatter_sum(all_part)
    outer_out = outer_sum + outer_offset
    res_two = norm_one + outer_out
    pack_out, ffn_pull = jax.vjp(layer_norm, res_two, ffn_scale, ffn_offset)
    grad_two, ffn_gsum, ffn_ssum = ffn_pull(pack_cot.astype(jnp.float32))
    grad_outer = grad_two.astype(jnp.bfloat16)
    outer_bsum = jnp.sum(grad_outer.astype(jnp.float32), axis=0)
    if narrow_n == 2:
        far_grads = swapped(grad_outer, "narrow", 0)
        own_inner, own_back = ffn_backward(grad_outer, own_pull, inner_cols, outer_cols)
        far_inner, far_back = ffn_backward(far_grads, far_pull, inner_cols, outer_cols)
        grad_part = own_back + swapped(far_back.astype(jnp.bfloat16), "narrow", 0).astype(
            jnp.float32
        )
        outer_wsum_t = contract_rows(grad_outer, own_act) + contract_rows(far_grads, far_act)
        inner_wsum = contract_rows(norm_low, own_inner) + contract_rows(far_rows, far_inner)
        inner_bsum = jnp.sum(own_inner.astype(jnp.float32), axis=0) + jnp.sum(
            far_inner.astype(jnp.float32), axis=0
        )
    else:
        group_grads = lax.all_gather(grad_outer, "narrow", axis=0, tiled=True)
        all_inner, all_back = ffn_backward(group_grads, all_pull, inner_cols, outer_cols)
        grad_part = narrow_scatter_sum(all_back)
        outer_wsum_t = contract_rows(group_grads, all_act)
        inner_wsum = contract_rows(group_rows, all_inner)
        inner_bsum = jnp.sum(all_inner.astype(jnp.float32), axis=0)
    bsum_rows = jnp.pad(
        inner_bsum.reshape(wide_n, bias_n), ((0, 0), (0, ffn_rows * bias_k - bias_n))
    ).reshape(wide_n * ffn_rows, bias_k)
    ffn_sums = jnp.concatenate([inner_wsum, outer_wsum_t, bsum_rows], axis=1).astype(jnp.bfloat16)
    ffn_mine = lax.psum_scatter(ffn_sums, "wide", scatter_dimension=0, tiled=True)
    ffn_mine = ffn_mine.astype(jnp.float32)
    inner_wgrad = ffn_mine[:, :ffn_cols]
    outer_wgrad = ffn_mine[:, ffn_cols : 2 * ffn_cols].T
    inner_bgrad = ffn_mine[:, 2 * ffn_cols :].reshape(-1)[:bias_n]

    pack_out, grad_part = lax.optimization_barrier((pack_out, grad_part))
    layer_out = from_pack(pack_out)
    grad_norm = grad_two + grad_part
    grad_one, attn_gsum, attn_ssum = norm_pull(grad_norm)
    grad_attn = grad_one.astype(jnp.bfloat16)
    output_bsum = jnp.sum(grad_attn.astype(jnp.float32), axis=0)
    output_wsum = contract_rows(mixed_low, grad_attn)
    early_small = jnp.stack(
        [output_bsum, attn_gsum, attn_ssum, outer_bsum, ffn_gsum, ffn_ssum], axis=1
    )
    early = jnp.concatenate(
        [output_wsum.reshape(total, share, D), early_small.reshape(total, share, -1)], axis=2
    )

    grad_mixed = heads_of(contract_cols(grad_attn, output_full).astype(jnp.bfloat16))
    grad_qrot, grad_krot, grad_values = attend_back(
        query_rot, key_rot, value_low, my_docs, my_docs, logsum, grad_mixed
    )
    grad_values = grad_values.astype(jnp.bfloat16)
    grad_query = unrotate(grad_qrot, cosine, sine_tab).astype(jnp.bfloat16)
    grad_keys = unrotate(grad_krot, cosine, sine_tab).astype(jnp.bfloat16)
    grad_qkv = jnp.concatenate(
        [
            grad_query.reshape(rows_dev, D),
            grad_keys.reshape(rows_dev, D),
            grad_values.reshape(rows_dev, D),
        ],
        axis=1,
    )
    pack_grad = grad_one + contract_cols(grad_qkv, qkv_full)
    keep_grad = lax.dynamic_slice_in_dim(pack_grad, half_bit * half_len, half_len, 0)
    give_grad = lax.dynamic_slice_in_dim(pack_grad, (1 - half_bit) * half_len, half_len, 0)
    give_grad, grad_qkv, pack_in = lax.optimization_barrier((give_grad, grad_qkv, pack_in))
    got_grad = swapped(give_grad, "narrow", 0)
    input_grad = jnp.where(
        half_bit == 0,
        jnp.concatenate([keep_grad, got_grad]),
        jnp.concatenate([got_grad, keep_grad]),
    )
    qkv_wsum = contract_rows(pack_in, grad_qkv)
    qkv_bsum = jnp.sum(grad_qkv.astype(jnp.float32), axis=0).reshape(3, D)
    wsum_parts = qkv_wsum.reshape(total, share, 3 * D).astype(jnp.bfloat16)
    late_mine = scatter_sum_parts(
        [
            wsum_parts[..., :D],
            wsum_parts[..., D : 2 * D],
            wsum_parts[..., 2 * D :],
            jnp.concatenate(
                [
                    qkv_bsum.T.reshape(total, share, 3).astype(jnp.bfloat16),
                    early.astype(jnp.bfloat16),
                ],
                axis=2,
            ),
        ]
    )
    early_mine = late_mine[:, 3 * D + 3 :]
    query_wgrad = late_mine[:, :D]
    key_wgrad = late_mine[:, D : 2 * D]
    value_wgrad = late_mine[:, 2 * D : 3 * D]
    query_bgrad = late_mine[:, 3 * D]
    key_bgrad = late_mine[:, 3 * D + 1]
    value_bgrad = late_mine[:, 3 * D + 2]
    output_wgrad = early_mine[:, :D]
    output_bgrad = early_mine[:, D]
    attn_ggrad = early_mine[:, D + 1]
    attn_sgrad = early_mine[:, D + 2]
    outer_bgrad = early_mine[:, D + 3]
    ffn_ggrad = early_mine[:, D + 4]
    ffn_sgrad = early_mine[:, D + 5]
    return (
        layer_out,
        input_grad,
        query_wgrad,
        query_bgrad,
        key_wgrad,
        key_bgrad,
        value_wgrad,
        value_bgrad,
        output_wgrad,
        output_bgrad,
        attn_ggrad,
        attn_sgrad,
        inner_wgrad,
        inner_bgrad,
        outer_wgrad,
        outer_bgrad,
        ffn_ggrad,
        ffn_sgrad,
    )


def solution(mesh):
    return jax.shard_map(
        local,
        mesh=mesh,
        in_specs=(
            P(("wide", "narrow"), None),
            P("wide", None),
            P(("wide", "narrow"), None),
            P(("wide", "narrow")),
            P(("wide", "narrow"), None),
            P(("wide", "narrow")),
            P(("wide", "narrow"), None),
            P(("wide", "narrow")),
            P(("wide", "narrow"), None),
            P(("wide", "narrow")),
            P(("wide", "narrow")),
            P(("wide", "narrow")),
            P("wide", "narrow"),
            P(("narrow", "wide")),
            P("narrow", "wide"),
            P(("wide", "narrow")),
            P(("wide", "narrow")),
            P(("wide", "narrow")),
            P(("wide", "narrow"), None),
        ),
        out_specs=(
            P(("wide", "narrow"), None),
            P(("wide", "narrow"), None),
            P(("wide", "narrow"), None),
            P(("wide", "narrow")),
            P(("wide", "narrow"), None),
            P(("wide", "narrow")),
            P(("wide", "narrow"), None),
            P(("wide", "narrow")),
            P(("wide", "narrow"), None),
            P(("wide", "narrow")),
            P(("wide", "narrow")),
            P(("wide", "narrow")),
            P("wide", "narrow"),
            P(("narrow", "wide")),
            P("narrow", "wide"),
            P(("wide", "narrow")),
            P(("wide", "narrow")),
            P(("wide", "narrow")),
        ),
        check_vma=False,
    )
```

```python
import itertools

import jax
import jax.numpy as jnp
from jax import lax
from jax.sharding import PartitionSpec as P

D = 768
HEADS = 12
HEAD_DIM = 64

ALL = ("wide", "narrow")
layer_eps = 1e-12
masked_score = -1e30


def swapped(shard, axis, bit):
    return lax.ppermute(shard, axis, [(i, i ^ 1 << bit) for i in range(lax.axis_size(axis))])


def part_orders(total, narrow_n, parts):
    bits = total.bit_length() - 1
    core_bit = narrow_n.bit_length() - 1
    narrow_bits = list(range(core_bit))
    wide_bits = [b for b in reversed(range(core_bit + 1, bits))]
    rotations = [wide_bits[k:] + wide_bits[:k] for k in range(max(1, len(wide_bits)))]
    others = [list(p) for p in itertools.permutations(wide_bits) if list(p) not in rotations]
    choices = rotations + others
    return [narrow_bits + choices[p % len(choices)] + [core_bit] for p in range(parts)]


def is_pow2(n):
    return n & (n - 1) == 0


def column_splits(cols, parts):
    tiles = -(-cols // 128)
    parts = max(1, min(parts, tiles))
    edges = [min(cols, (tiles * i // parts) * 128) for i in range(parts)] + [cols]
    return [(a, b) for a, b in zip(edges[:-1], edges[1:]) if b > a]


def doubling_gather(shard, order, total):
    me = lax.axis_index(ALL)
    cur = shard
    for b in order:
        other = lax.ppermute(cur, ALL, [(i, i ^ (1 << b)) for i in range(total)])
        bit = (me >> b) & 1
        pick = (jnp.arange(2) == bit).reshape((2,) + (1,) * cur.ndim)
        cur = jnp.where(pick, cur[None], other[None])
    k = len(order)
    perm = [k - 1 - order.index(b) for b in reversed(range(k))]
    cur = cur.transpose(perm + list(range(k, cur.ndim)))
    return cur.reshape((total,) + shard.shape)


def gather_all(shard, parts=3):
    total = lax.axis_size("wide") * lax.axis_size("narrow")
    narrow_n = lax.axis_size("narrow")
    if not (is_pow2(total) and is_pow2(narrow_n)):
        return lax.all_gather(shard, ALL, axis=0, tiled=False)
    splits = column_splits(shard.shape[-1], parts)
    orders = part_orders(total, narrow_n, len(splits))
    pieces = [
        doubling_gather(shard[..., a:b], order, total) for (a, b), order in zip(splits, orders)
    ]
    return jnp.concatenate(pieces, axis=-1)


def halving_scatter(parts_in, order, total):
    me = lax.axis_index(ALL)
    nbits = total.bit_length() - 1
    cur = parts_in.reshape((2,) * nbits + parts_in.shape[1:])
    axes = list(reversed(range(nbits)))
    for b in order:
        a = axes.index(b)
        bit = (me >> b) & 1
        mine = lax.dynamic_index_in_dim(cur, bit, axis=a, keepdims=False)
        theirs = lax.dynamic_index_in_dim(cur, 1 - bit, axis=a, keepdims=False)
        got = lax.ppermute(
            theirs.astype(jnp.bfloat16), ALL, [(i, i ^ (1 << b)) for i in range(total)]
        )
        cur = mine.astype(jnp.float32) + got.astype(jnp.float32)
        axes.pop(a)
    return cur


def scatter_sum_all(parts_in, parts=3):
    total = lax.axis_size("wide") * lax.axis_size("narrow")
    narrow_n = lax.axis_size("narrow")
    if not (is_pow2(total) and is_pow2(narrow_n)):
        return lax.psum_scatter(
            parts_in.astype(jnp.bfloat16), ALL, scatter_dimension=0, tiled=False
        ).astype(jnp.float32)
    splits = column_splits(parts_in.shape[-1], parts)
    orders = part_orders(total, narrow_n, len(splits))
    pieces = [
        halving_scatter(parts_in[..., a:b], list(reversed(order)), total)
        for (a, b), order in zip(splits, orders)
    ]
    return jnp.concatenate(pieces, axis=-1)


def scatter_sum_parts(part_list):
    total = lax.axis_size("wide") * lax.axis_size("narrow")
    narrow_n = lax.axis_size("narrow")
    if not (is_pow2(total) and is_pow2(narrow_n)):
        return jnp.concatenate([scatter_sum_all(x, 1) for x in part_list], axis=-1)
    orders = part_orders(total, narrow_n, len(part_list))
    return jnp.concatenate(
        [halving_scatter(x, list(reversed(o)), total) for x, o in zip(part_list, orders)],
        axis=-1,
    )


def narrow_gather(rows):
    n = lax.axis_size("narrow")
    if n != 2:
        return lax.all_gather(rows, "narrow", axis=0, tiled=True)
    other = swapped(rows, "narrow", 0)
    first = lax.axis_index("narrow") == 0
    return jnp.where(first, jnp.concatenate([rows, other]), jnp.concatenate([other, rows]))


def narrow_scatter_sum(part):
    n = lax.axis_size("narrow")
    if n != 2:
        return lax.psum_scatter(
            part.astype(jnp.bfloat16), "narrow", scatter_dimension=0, tiled=True
        ).astype(jnp.float32)
    rows = part.shape[0] // 2
    me = lax.axis_index("narrow")
    mine = lax.dynamic_slice_in_dim(part, me * rows, rows, 0)
    theirs = lax.dynamic_slice_in_dim(part, (1 - me) * rows, rows, 0)
    return mine + swapped(theirs.astype(jnp.bfloat16), "narrow", 0).astype(jnp.float32)


def layer_norm(values, gain_vec, shift_vec):
    center = values - jnp.mean(values, axis=-1, keepdims=True)
    spread = jnp.mean(center * center, axis=-1, keepdims=True)
    return center * lax.rsqrt(spread + layer_eps) * gain_vec + shift_vec


def gelu_exact(values):
    return jax.nn.gelu(values, approximate=False)


def rotary_tables(doc_row):
    places = jnp.arange(doc_row.shape[0], dtype=jnp.int32)
    before = jnp.sum((doc_row[None, :] < doc_row[:, None]).astype(jnp.int32), axis=1)
    position = (places - before).astype(jnp.float32)
    frequency = 10000.0 ** (-2.0 * jnp.arange(HEAD_DIM // 2, dtype=jnp.float32) / HEAD_DIM)
    angles = position[:, None] * frequency[None, :]
    return (jnp.cos(angles), jnp.sin(angles))


def rotate(values, cosine, sine_tab):
    half_dim = values.shape[-1] // 2
    first_half = values[..., :half_dim]
    second = values[..., half_dim:]
    return jnp.concatenate(
        [first_half * cosine - second * sine_tab, second * cosine + first_half * sine_tab], axis=-1
    )


def unrotate(values, cosine, sine_tab):
    half_dim = values.shape[-1] // 2
    first_half = values[..., :half_dim]
    second = values[..., half_dim:]
    return jnp.concatenate(
        [first_half * cosine + second * sine_tab, second * cosine - first_half * sine_tab], axis=-1
    )


def contract_rows(left_op, right_op):
    return lax.dot_general(
        left_op, right_op, (((0,), (0,)), ((), ())), preferred_element_type=jnp.float32
    )


def contract_cols(left_op, right_op):
    return lax.dot_general(
        left_op, right_op, (((1,), (1,)), ((), ())), preferred_element_type=jnp.float32
    )


def score_block(query_rot, key_rot, query_docs, key_docs):
    scores = jnp.einsum(
        "pqhd,pkhd->phqk", query_rot, key_rot, preferred_element_type=jnp.float32
    ) * HEAD_DIM ** (-0.5)
    same_doc = query_docs[:, :, None] == key_docs[:, None, :]
    return jnp.where(same_doc[:, None], scores, masked_score)


def attend(query_rot, key_rot, value_low, query_docs, key_docs):
    scores = score_block(query_rot, key_rot, query_docs, key_docs)
    row_peak = jnp.max(scores, axis=-1, keepdims=True)
    exponent = jnp.exp(scores - row_peak)
    totals = jnp.sum(exponent, axis=-1, keepdims=True)
    probability = (exponent / totals).astype(jnp.bfloat16)
    mixed_out = jnp.einsum(
        "phqk,pkhd->pqhd", probability, value_low, preferred_element_type=jnp.float32
    )
    return (mixed_out, row_peak + jnp.log(totals))


def attend_back(query_rot, key_rot, value_low, query_docs, key_docs, logsum, grad_mixed):
    probability = jnp.exp(score_block(query_rot, key_rot, query_docs, key_docs) - logsum)
    grad_values = jnp.einsum(
        "phqk,pqhd->pkhd",
        probability.astype(jnp.bfloat16),
        grad_mixed,
        preferred_element_type=jnp.float32,
    )
    grad_probs = jnp.einsum(
        "pqhd,pkhd->phqk", grad_mixed, value_low, preferred_element_type=jnp.float32
    )
    inner_sum = jnp.sum(probability * grad_probs, axis=-1, keepdims=True)
    grad_scores = (probability * (grad_probs - inner_sum)).astype(jnp.bfloat16)
    grad_query = jnp.einsum(
        "phqk,pkhd->pqhd", grad_scores, key_rot, preferred_element_type=jnp.float32
    ) * HEAD_DIM ** (-0.5)
    grad_keys = jnp.einsum(
        "phqk,pqhd->pkhd", grad_scores, query_rot, preferred_element_type=jnp.float32
    ) * HEAD_DIM ** (-0.5)
    return (grad_query, grad_keys, grad_values)


def ffn_forward(rows, inner_cols, inner_offset, outer_cols):
    inner_pre = jnp.dot(rows, inner_cols, preferred_element_type=jnp.float32) + inner_offset
    act_value, gelu_pull = jax.vjp(gelu_exact, inner_pre)
    act_low = act_value.astype(jnp.bfloat16)
    return act_low, gelu_pull, contract_cols(act_low, outer_cols)


def ffn_backward(grads, gelu_pull, inner_cols, outer_cols):
    grad_act = jnp.dot(grads, outer_cols, preferred_element_type=jnp.float32)
    grad_inner = gelu_pull(grad_act)[0].astype(jnp.bfloat16)
    return grad_inner, contract_cols(grad_inner, inner_cols)


def local(
    layer_in,
    doc_ids,
    query_weight,
    query_bias,
    key_weight,
    key_bias,
    value_weight,
    value_bias,
    output_weight,
    output_bias,
    attn_gain,
    attn_shift,
    inner_weight,
    inner_bias,
    outer_weight,
    outer_bias,
    ffn_gain,
    ffn_shift,
    cotangent,
):
    wide_n = lax.axis_size("wide")
    narrow_n = lax.axis_size("narrow")
    total = wide_n * narrow_n
    share = query_weight.shape[0]
    small_list = (
        query_bias,
        key_bias,
        value_bias,
        output_bias,
        attn_gain,
        attn_shift,
        outer_bias,
        ffn_gain,
        ffn_shift,
    )
    small = jnp.stack(small_list, axis=1)
    small = jnp.pad(small, ((0, 0), (0, 128 - len(small_list))))
    shard = jnp.concatenate([query_weight, key_weight, value_weight, output_weight, small], axis=1)
    full = gather_all(shard).reshape(total * share, shard.shape[1])
    qkv_full = full[:, : 3 * D]
    output_full = full[:, 3 * D : 4 * D]
    vecs = full[:, 4 * D :].astype(jnp.float32)
    (
        query_offset,
        key_offset,
        value_offset,
        output_offset,
        attn_scale,
        attn_offset,
        outer_offset,
        ffn_scale,
        ffn_offset,
    ) = [vecs[:, i] for i in range(len(small_list))]
    qkv_offset = jnp.concatenate([query_offset, key_offset, value_offset])

    ffn_rows, ffn_cols = inner_weight.shape
    bias_n = inner_bias.shape[0]
    bias_k = -(-bias_n // ffn_rows)
    bias_rows = jnp.pad(inner_bias, (0, ffn_rows * bias_k - bias_n)).reshape(ffn_rows, bias_k)
    ffn_shard = jnp.concatenate([inner_weight, outer_weight.T, bias_rows], axis=1)
    ffn_shard, full = lax.optimization_barrier((ffn_shard, full))
    ffn_all = lax.all_gather(ffn_shard, "wide", axis=0, tiled=True)
    inner_cols = ffn_all[:, :ffn_cols]
    outer_cols = ffn_all[:, ffn_cols : 2 * ffn_cols]
    inner_offset = ffn_all[:, 2 * ffn_cols :].reshape(wide_n, ffn_rows * bias_k)[:, :bias_n]
    inner_offset = inner_offset.reshape(-1).astype(jnp.float32)

    rows_dev = layer_in.shape[0]
    half_len = doc_ids.shape[1] // 2
    pack_count = rows_dev // half_len
    narrow_place = lax.axis_index("narrow")
    half_bit = narrow_place % 2
    pair_slot = narrow_place // 2
    pack_docs = lax.dynamic_slice_in_dim(doc_ids, pair_slot * pack_count, pack_count, 0)
    my_docs = lax.dynamic_slice_in_dim(pack_docs, half_bit, 1, 0)
    cosine, sine_tab = jax.vmap(rotary_tables)(my_docs)
    cosine = cosine[:, :, None, :]
    sine_tab = sine_tab[:, :, None, :]

    def to_pack(rows):
        keep = lax.dynamic_slice_in_dim(rows, half_bit * half_len, half_len, 0)
        give = lax.dynamic_slice_in_dim(rows, (1 - half_bit) * half_len, half_len, 0)
        got = swapped(give, "narrow", 0)
        return jnp.where(
            half_bit == 0, jnp.concatenate([keep, got]), jnp.concatenate([got, keep])
        )

    def from_pack(rows):
        keep = lax.dynamic_slice_in_dim(rows, half_bit * half_len, half_len, 0)
        give = lax.dynamic_slice_in_dim(rows, (1 - half_bit) * half_len, half_len, 0)
        got = swapped(give, "narrow", 0)
        return jnp.where(
            half_bit == 0, jnp.concatenate([keep, got]), jnp.concatenate([got, keep])
        )

    pack_in = to_pack(layer_in)
    pack_cot = to_pack(cotangent)

    def heads_of(values):
        return values.reshape(1, rows_dev, HEADS, HEAD_DIM)

    qkv = jnp.dot(pack_in, qkv_full, preferred_element_type=jnp.float32) + qkv_offset
    query_rot = rotate(heads_of(qkv[:, :D]), cosine, sine_tab).astype(jnp.bfloat16)
    key_rot = rotate(heads_of(qkv[:, D : 2 * D]), cosine, sine_tab).astype(jnp.bfloat16)
    value_low = heads_of(qkv[:, 2 * D :]).astype(jnp.bfloat16)
    mixed_out, logsum = attend(query_rot, key_rot, value_low, my_docs, my_docs)
    mixed_low = mixed_out.reshape(rows_dev, D).astype(jnp.bfloat16)
    attn_out = jnp.dot(mixed_low, output_full, preferred_element_type=jnp.float32) + output_offset
    res_one = pack_in.astype(jnp.float32) + attn_out
    norm_one, norm_pull = jax.vjp(layer_norm, res_one, attn_scale, attn_offset)
    norm_low = norm_one.astype(jnp.bfloat16)

    if narrow_n == 2:
        far_rows = swapped(norm_low, "narrow", 0)
        own_act, own_pull, own_part = ffn_forward(norm_low, inner_cols, inner_offset, outer_cols)
        far_act, far_pull, far_part = ffn_forward(far_rows, inner_cols, inner_offset, outer_cols)
        outer_sum = own_part + swapped(far_part.astype(jnp.bfloat16), "narrow", 0).astype(
            jnp.float32
        )
    else:
        group_rows = lax.all_gather(norm_low, "narrow", axis=0, tiled=True)
        all_act, all_pull, all_part = ffn_forward(group_rows, inner_cols, inner_offset, outer_cols)
        outer_sum = narrow_scatter_sum(all_part)
    outer_out = outer_sum + outer_offset
    res_two = norm_one + outer_out
    pack_out, ffn_pull = jax.vjp(layer_norm, res_two, ffn_scale, ffn_offset)
    grad_two, ffn_gsum, ffn_ssum = ffn_pull(pack_cot.astype(jnp.float32))
    grad_outer = grad_two.astype(jnp.bfloat16)
    outer_bsum = jnp.sum(grad_outer.astype(jnp.float32), axis=0)
    if narrow_n == 2:
        far_grads = swapped(grad_outer, "narrow", 0)
        own_inner, own_back = ffn_backward(grad_outer, own_pull, inner_cols, outer_cols)
        far_inner, far_back = ffn_backward(far_grads, far_pull, inner_cols, outer_cols)
        grad_part = own_back + swapped(far_back.astype(jnp.bfloat16), "narrow", 0).astype(
            jnp.float32
        )
        outer_wsum_t = contract_rows(grad_outer, own_act) + contract_rows(far_grads, far_act)
        inner_wsum = contract_rows(norm_low, own_inner) + contract_rows(far_rows, far_inner)
        inner_bsum = jnp.sum(own_inner.astype(jnp.float32), axis=0) + jnp.sum(
            far_inner.astype(jnp.float32), axis=0
        )
    else:
        group_grads = lax.all_gather(grad_outer, "narrow", axis=0, tiled=True)
        all_inner, all_back = ffn_backward(group_grads, all_pull, inner_cols, outer_cols)
        grad_part = narrow_scatter_sum(all_back)
        outer_wsum_t = contract_rows(group_grads, all_act)
        inner_wsum = contract_rows(group_rows, all_inner)
        inner_bsum = jnp.sum(all_inner.astype(jnp.float32), axis=0)
    bsum_rows = jnp.pad(
        inner_bsum.reshape(wide_n, bias_n), ((0, 0), (0, ffn_rows * bias_k - bias_n))
    ).reshape(wide_n * ffn_rows, bias_k)
    ffn_sums = jnp.concatenate([inner_wsum, outer_wsum_t, bsum_rows], axis=1).astype(jnp.bfloat16)
    ffn_mine = lax.psum_scatter(ffn_sums, "wide", scatter_dimension=0, tiled=True)
    ffn_mine = ffn_mine.astype(jnp.float32)
    inner_wgrad = ffn_mine[:, :ffn_cols]
    outer_wgrad = ffn_mine[:, ffn_cols : 2 * ffn_cols].T
    inner_bgrad = ffn_mine[:, 2 * ffn_cols :].reshape(-1)[:bias_n]

    pack_out, grad_part = lax.optimization_barrier((pack_out, grad_part))
    layer_out = from_pack(pack_out)
    grad_norm = grad_two + grad_part
    grad_one, attn_gsum, attn_ssum = norm_pull(grad_norm)
    grad_attn = grad_one.astype(jnp.bfloat16)
    output_bsum = jnp.sum(grad_attn.astype(jnp.float32), axis=0)
    output_wsum = contract_rows(mixed_low, grad_attn)
    early_small = jnp.stack(
        [output_bsum, attn_gsum, attn_ssum, outer_bsum, ffn_gsum, ffn_ssum], axis=1
    )
    early = jnp.concatenate(
        [output_wsum.reshape(total, share, D), early_small.reshape(total, share, -1)], axis=2
    )

    grad_mixed = heads_of(contract_cols(grad_attn, output_full).astype(jnp.bfloat16))
    grad_qrot, grad_krot, grad_values = attend_back(
        query_rot, key_rot, value_low, my_docs, my_docs, logsum, grad_mixed
    )
    grad_values = grad_values.astype(jnp.bfloat16)
    grad_query = unrotate(grad_qrot, cosine, sine_tab).astype(jnp.bfloat16)
    grad_keys = unrotate(grad_krot, cosine, sine_tab).astype(jnp.bfloat16)
    grad_qkv = jnp.concatenate(
        [
            grad_query.reshape(rows_dev, D),
            grad_keys.reshape(rows_dev, D),
            grad_values.reshape(rows_dev, D),
        ],
        axis=1,
    )
    pack_grad = grad_one + contract_cols(grad_qkv, qkv_full)
    keep_grad = lax.dynamic_slice_in_dim(pack_grad, half_bit * half_len, half_len, 0)
    give_grad = lax.dynamic_slice_in_dim(pack_grad, (1 - half_bit) * half_len, half_len, 0)
    give_grad, grad_qkv, pack_in = lax.optimization_barrier((give_grad, grad_qkv, pack_in))
    got_grad = swapped(give_grad, "narrow", 0)
    input_grad = jnp.where(
        half_bit == 0,
        jnp.concatenate([keep_grad, got_grad]),
        jnp.concatenate([got_grad, keep_grad]),
    )
    qkv_wsum = contract_rows(pack_in, grad_qkv)
    qkv_bsum = jnp.sum(grad_qkv.astype(jnp.float32), axis=0).reshape(3, D)
    wsum_parts = qkv_wsum.reshape(total, share, 3 * D).astype(jnp.bfloat16)
    segments = [
        wsum_parts,
        qkv_bsum.T.reshape(total, share, 3).astype(jnp.bfloat16),
        early.astype(jnp.bfloat16),
    ]
    starts = [0]
    for seg in segments:
        starts.append(starts[-1] + seg.shape[-1])
    chunks = []
    for a, c in column_splits(starts[-1], 6):
        bits_of = [
            seg[..., max(a, lo) - lo : min(c, hi) - lo]
            for seg, lo, hi in zip(segments, starts[:-1], starts[1:])
            if min(c, hi) > max(a, lo)
        ]
        chunks.append(bits_of[0] if len(bits_of) == 1 else jnp.concatenate(bits_of, axis=2))
    late_mine = scatter_sum_parts(chunks)
    early_mine = late_mine[:, 3 * D + 3 :]
    query_wgrad = late_mine[:, :D]
    key_wgrad = late_mine[:, D : 2 * D]
    value_wgrad = late_mine[:, 2 * D : 3 * D]
    query_bgrad = late_mine[:, 3 * D]
    key_bgrad = late_mine[:, 3 * D + 1]
    value_bgrad = late_mine[:, 3 * D + 2]
    output_wgrad = early_mine[:, :D]
    output_bgrad = early_mine[:, D]
    attn_ggrad = early_mine[:, D + 1]
    attn_sgrad = early_mine[:, D + 2]
    outer_bgrad = early_mine[:, D + 3]
    ffn_ggrad = early_mine[:, D + 4]
    ffn_sgrad = early_mine[:, D + 5]
    return (
        layer_out,
        input_grad,
        query_wgrad,
        query_bgrad,
        key_wgrad,
        key_bgrad,
        value_wgrad,
        value_bgrad,
        output_wgrad,
        output_bgrad,
        attn_ggrad,
        attn_sgrad,
        inner_wgrad,
        inner_bgrad,
        outer_wgrad,
        outer_bgrad,
        ffn_ggrad,
        ffn_sgrad,
    )


def solution(mesh):
    return jax.shard_map(
        local,
        mesh=mesh,
        in_specs=(
            P(("wide", "narrow"), None),
            P("wide", None),
            P(("wide", "narrow"), None),
            P(("wide", "narrow")),
            P(("wide", "narrow"), None),
            P(("wide", "narrow")),
            P(("wide", "narrow"), None),
            P(("wide", "narrow")),
            P(("wide", "narrow"), None),
            P(("wide", "narrow")),
            P(("wide", "narrow")),
            P(("wide", "narrow")),
            P("wide", "narrow"),
            P(("narrow", "wide")),
            P("narrow", "wide"),
            P(("wide", "narrow")),
            P(("wide", "narrow")),
            P(("wide", "narrow")),
            P(("wide", "narrow"), None),
        ),
        out_specs=(
            P(("wide", "narrow"), None),
            P(("wide", "narrow"), None),
            P(("wide", "narrow"), None),
            P(("wide", "narrow")),
            P(("wide", "narrow"), None),
            P(("wide", "narrow")),
            P(("wide", "narrow"), None),
            P(("wide", "narrow")),
            P(("wide", "narrow"), None),
            P(("wide", "narrow")),
            P(("wide", "narrow")),
            P(("wide", "narrow")),
            P("wide", "narrow"),
            P(("narrow", "wide")),
            P("narrow", "wide"),
            P(("wide", "narrow")),
            P(("wide", "narrow")),
            P(("wide", "narrow")),
        ),
        check_vma=False,
    )
```

```python
import itertools

import jax
import jax.numpy as jnp
from jax import lax
from jax.sharding import PartitionSpec as P

D = 768
HEADS = 12
HEAD_DIM = 64

ALL = ("wide", "narrow")
layer_eps = 1e-12
masked_score = -1e30


def swapped(shard, axis, bit):
    return lax.ppermute(shard, axis, [(i, i ^ 1 << bit) for i in range(lax.axis_size(axis))])


def part_orders(total, narrow_n, parts):
    bits = total.bit_length() - 1
    core_bit = narrow_n.bit_length() - 1
    narrow_bits = list(range(core_bit))
    wide_bits = [b for b in reversed(range(core_bit + 1, bits))]
    rotations = [wide_bits[k:] + wide_bits[:k] for k in range(max(1, len(wide_bits)))]
    others = [list(p) for p in itertools.permutations(wide_bits) if list(p) not in rotations]
    choices = rotations + others
    return [narrow_bits + choices[p % len(choices)] + [core_bit] for p in range(parts)]


def is_pow2(n):
    return n & (n - 1) == 0


def column_splits(cols, parts):
    tiles = -(-cols // 128)
    parts = max(1, min(parts, tiles))
    edges = [min(cols, (tiles * i // parts) * 128) for i in range(parts)] + [cols]
    return [(a, b) for a, b in zip(edges[:-1], edges[1:]) if b > a]


def doubling_gather(shard, order, total):
    me = lax.axis_index(ALL)
    cur = shard
    for b in order:
        other = lax.ppermute(cur, ALL, [(i, i ^ (1 << b)) for i in range(total)])
        bit = (me >> b) & 1
        pick = (jnp.arange(2) == bit).reshape((2,) + (1,) * cur.ndim)
        cur = jnp.where(pick, cur[None], other[None])
    k = len(order)
    perm = [k - 1 - order.index(b) for b in reversed(range(k))]
    cur = cur.transpose(perm + list(range(k, cur.ndim)))
    return cur.reshape((total,) + shard.shape)


def gather_all(shard, parts=4):
    total = lax.axis_size("wide") * lax.axis_size("narrow")
    narrow_n = lax.axis_size("narrow")
    if not (is_pow2(total) and is_pow2(narrow_n)):
        return lax.all_gather(shard, ALL, axis=0, tiled=False)
    splits = column_splits(shard.shape[-1], parts)
    orders = part_orders(total, narrow_n, len(splits))
    pieces = [
        doubling_gather(shard[..., a:b], order, total) for (a, b), order in zip(splits, orders)
    ]
    return jnp.concatenate(pieces, axis=-1)


def halving_scatter(parts_in, order, total):
    me = lax.axis_index(ALL)
    nbits = total.bit_length() - 1
    cur = parts_in.reshape((2,) * nbits + parts_in.shape[1:])
    axes = list(reversed(range(nbits)))
    for b in order:
        a = axes.index(b)
        bit = (me >> b) & 1
        mine = lax.dynamic_index_in_dim(cur, bit, axis=a, keepdims=False)
        theirs = lax.dynamic_index_in_dim(cur, 1 - bit, axis=a, keepdims=False)
        got = lax.ppermute(
            theirs.astype(jnp.bfloat16), ALL, [(i, i ^ (1 << b)) for i in range(total)]
        )
        cur = mine.astype(jnp.float32) + got.astype(jnp.float32)
        axes.pop(a)
    return cur


def scatter_sum_all(parts_in, parts=3):
    total = lax.axis_size("wide") * lax.axis_size("narrow")
    narrow_n = lax.axis_size("narrow")
    if not (is_pow2(total) and is_pow2(narrow_n)):
        return lax.psum_scatter(
            parts_in.astype(jnp.bfloat16), ALL, scatter_dimension=0, tiled=False
        ).astype(jnp.float32)
    splits = column_splits(parts_in.shape[-1], parts)
    orders = part_orders(total, narrow_n, len(splits))
    pieces = [
        halving_scatter(parts_in[..., a:b], list(reversed(order)), total)
        for (a, b), order in zip(splits, orders)
    ]
    return jnp.concatenate(pieces, axis=-1)


def scatter_sum_parts(part_list):
    total = lax.axis_size("wide") * lax.axis_size("narrow")
    narrow_n = lax.axis_size("narrow")
    if not (is_pow2(total) and is_pow2(narrow_n)):
        return jnp.concatenate([scatter_sum_all(x, 1) for x in part_list], axis=-1)
    orders = part_orders(total, narrow_n, len(part_list))
    return jnp.concatenate(
        [halving_scatter(x, list(reversed(o)), total) for x, o in zip(part_list, orders)],
        axis=-1,
    )


def narrow_gather(rows):
    n = lax.axis_size("narrow")
    if n != 2:
        return lax.all_gather(rows, "narrow", axis=0, tiled=True)
    other = swapped(rows, "narrow", 0)
    first = lax.axis_index("narrow") == 0
    return jnp.where(first, jnp.concatenate([rows, other]), jnp.concatenate([other, rows]))


def narrow_scatter_sum(part):
    n = lax.axis_size("narrow")
    if n != 2:
        return lax.psum_scatter(
            part.astype(jnp.bfloat16), "narrow", scatter_dimension=0, tiled=True
        ).astype(jnp.float32)
    rows = part.shape[0] // 2
    me = lax.axis_index("narrow")
    mine = lax.dynamic_slice_in_dim(part, me * rows, rows, 0)
    theirs = lax.dynamic_slice_in_dim(part, (1 - me) * rows, rows, 0)
    return mine + swapped(theirs.astype(jnp.bfloat16), "narrow", 0).astype(jnp.float32)


def layer_norm(values, gain_vec, shift_vec):
    center = values - jnp.mean(values, axis=-1, keepdims=True)
    spread = jnp.mean(center * center, axis=-1, keepdims=True)
    return center * lax.rsqrt(spread + layer_eps) * gain_vec + shift_vec


def gelu_exact(values):
    return jax.nn.gelu(values, approximate=False)


def rotary_tables(doc_row):
    places = jnp.arange(doc_row.shape[0], dtype=jnp.int32)
    before = jnp.sum((doc_row[None, :] < doc_row[:, None]).astype(jnp.int32), axis=1)
    position = (places - before).astype(jnp.float32)
    frequency = 10000.0 ** (-2.0 * jnp.arange(HEAD_DIM // 2, dtype=jnp.float32) / HEAD_DIM)
    angles = position[:, None] * frequency[None, :]
    return (jnp.cos(angles), jnp.sin(angles))


def rotate(values, cosine, sine_tab):
    half_dim = values.shape[-1] // 2
    first_half = values[..., :half_dim]
    second = values[..., half_dim:]
    return jnp.concatenate(
        [first_half * cosine - second * sine_tab, second * cosine + first_half * sine_tab], axis=-1
    )


def unrotate(values, cosine, sine_tab):
    half_dim = values.shape[-1] // 2
    first_half = values[..., :half_dim]
    second = values[..., half_dim:]
    return jnp.concatenate(
        [first_half * cosine + second * sine_tab, second * cosine - first_half * sine_tab], axis=-1
    )


def contract_rows(left_op, right_op):
    return lax.dot_general(
        left_op, right_op, (((0,), (0,)), ((), ())), preferred_element_type=jnp.float32
    )


def contract_cols(left_op, right_op):
    return lax.dot_general(
        left_op, right_op, (((1,), (1,)), ((), ())), preferred_element_type=jnp.float32
    )


def score_block(query_rot, key_rot, query_docs, key_docs):
    scores = jnp.einsum(
        "pqhd,pkhd->phqk", query_rot, key_rot, preferred_element_type=jnp.float32
    ) * HEAD_DIM ** (-0.5)
    same_doc = query_docs[:, :, None] == key_docs[:, None, :]
    return jnp.where(same_doc[:, None], scores, masked_score)


def attend(query_rot, key_rot, value_low, query_docs, key_docs):
    scores = score_block(query_rot, key_rot, query_docs, key_docs)
    row_peak = jnp.max(scores, axis=-1, keepdims=True)
    exponent = jnp.exp(scores - row_peak)
    totals = jnp.sum(exponent, axis=-1, keepdims=True)
    probability = (exponent / totals).astype(jnp.bfloat16)
    mixed_out = jnp.einsum(
        "phqk,pkhd->pqhd", probability, value_low, preferred_element_type=jnp.float32
    )
    return (mixed_out, row_peak + jnp.log(totals))


def attend_back(query_rot, key_rot, value_low, query_docs, key_docs, logsum, grad_mixed):
    probability = jnp.exp(score_block(query_rot, key_rot, query_docs, key_docs) - logsum)
    grad_values = jnp.einsum(
        "phqk,pqhd->pkhd",
        probability.astype(jnp.bfloat16),
        grad_mixed,
        preferred_element_type=jnp.float32,
    )
    grad_probs = jnp.einsum(
        "pqhd,pkhd->phqk", grad_mixed, value_low, preferred_element_type=jnp.float32
    )
    inner_sum = jnp.sum(probability * grad_probs, axis=-1, keepdims=True)
    grad_scores = (probability * (grad_probs - inner_sum)).astype(jnp.bfloat16)
    grad_query = jnp.einsum(
        "phqk,pkhd->pqhd", grad_scores, key_rot, preferred_element_type=jnp.float32
    ) * HEAD_DIM ** (-0.5)
    grad_keys = jnp.einsum(
        "phqk,pqhd->pkhd", grad_scores, query_rot, preferred_element_type=jnp.float32
    ) * HEAD_DIM ** (-0.5)
    return (grad_query, grad_keys, grad_values)


def ffn_forward(rows, inner_cols, inner_offset, outer_cols):
    inner_pre = jnp.dot(rows, inner_cols, preferred_element_type=jnp.float32) + inner_offset
    act_value, gelu_pull = jax.vjp(gelu_exact, inner_pre)
    act_low = act_value.astype(jnp.bfloat16)
    return act_low, gelu_pull, contract_cols(act_low, outer_cols)


def ffn_backward(grads, gelu_pull, inner_cols, outer_cols):
    grad_act = jnp.dot(grads, outer_cols, preferred_element_type=jnp.float32)
    grad_inner = gelu_pull(grad_act)[0].astype(jnp.bfloat16)
    return grad_inner, contract_cols(grad_inner, inner_cols)


def local(
    layer_in,
    doc_ids,
    query_weight,
    query_bias,
    key_weight,
    key_bias,
    value_weight,
    value_bias,
    output_weight,
    output_bias,
    attn_gain,
    attn_shift,
    inner_weight,
    inner_bias,
    outer_weight,
    outer_bias,
    ffn_gain,
    ffn_shift,
    cotangent,
):
    wide_n = lax.axis_size("wide")
    narrow_n = lax.axis_size("narrow")
    total = wide_n * narrow_n
    share = query_weight.shape[0]
    small_list = (
        query_bias,
        key_bias,
        value_bias,
        output_bias,
        attn_gain,
        attn_shift,
        outer_bias,
        ffn_gain,
        ffn_shift,
    )
    small = jnp.stack(small_list, axis=1)
    small = jnp.pad(small, ((0, 0), (0, 128 - len(small_list))))
    shard = jnp.concatenate([query_weight, key_weight, value_weight, output_weight, small], axis=1)
    full = gather_all(shard).reshape(total * share, shard.shape[1])
    qkv_full = full[:, : 3 * D]
    output_full = full[:, 3 * D : 4 * D]
    vecs = full[:, 4 * D :].astype(jnp.float32)
    (
        query_offset,
        key_offset,
        value_offset,
        output_offset,
        attn_scale,
        attn_offset,
        outer_offset,
        ffn_scale,
        ffn_offset,
    ) = [vecs[:, i] for i in range(len(small_list))]
    qkv_offset = jnp.concatenate([query_offset, key_offset, value_offset])

    ffn_rows, ffn_cols = inner_weight.shape
    bias_n = inner_bias.shape[0]
    bias_k = -(-bias_n // ffn_rows)
    bias_rows = jnp.pad(inner_bias, (0, ffn_rows * bias_k - bias_n)).reshape(ffn_rows, bias_k)
    ffn_shard = jnp.concatenate([inner_weight, outer_weight.T, bias_rows], axis=1)
    ffn_shard, full = lax.optimization_barrier((ffn_shard, full))
    ffn_all = lax.all_gather(ffn_shard, "wide", axis=0, tiled=True)
    inner_cols = ffn_all[:, :ffn_cols]
    outer_cols = ffn_all[:, ffn_cols : 2 * ffn_cols]
    inner_offset = ffn_all[:, 2 * ffn_cols :].reshape(wide_n, ffn_rows * bias_k)[:, :bias_n]
    inner_offset = inner_offset.reshape(-1).astype(jnp.float32)

    rows_dev = layer_in.shape[0]
    half_len = doc_ids.shape[1] // 2
    pack_count = rows_dev // half_len
    narrow_place = lax.axis_index("narrow")
    half_bit = narrow_place % 2
    pair_slot = narrow_place // 2
    pack_docs = lax.dynamic_slice_in_dim(doc_ids, pair_slot * pack_count, pack_count, 0)
    my_docs = lax.dynamic_slice_in_dim(pack_docs, half_bit, 1, 0)
    cosine, sine_tab = jax.vmap(rotary_tables)(my_docs)
    cosine = cosine[:, :, None, :]
    sine_tab = sine_tab[:, :, None, :]

    def to_pack(rows):
        keep = lax.dynamic_slice_in_dim(rows, half_bit * half_len, half_len, 0)
        give = lax.dynamic_slice_in_dim(rows, (1 - half_bit) * half_len, half_len, 0)
        got = swapped(give, "narrow", 0)
        return jnp.where(
            half_bit == 0, jnp.concatenate([keep, got]), jnp.concatenate([got, keep])
        )

    def from_pack(rows):
        keep = lax.dynamic_slice_in_dim(rows, half_bit * half_len, half_len, 0)
        give = lax.dynamic_slice_in_dim(rows, (1 - half_bit) * half_len, half_len, 0)
        got = swapped(give, "narrow", 0)
        return jnp.where(
            half_bit == 0, jnp.concatenate([keep, got]), jnp.concatenate([got, keep])
        )

    pack_in = to_pack(layer_in)
    pack_cot = to_pack(cotangent)

    def heads_of(values):
        return values.reshape(1, rows_dev, HEADS, HEAD_DIM)

    qkv = jnp.dot(pack_in, qkv_full, preferred_element_type=jnp.float32) + qkv_offset
    query_rot = rotate(heads_of(qkv[:, :D]), cosine, sine_tab).astype(jnp.bfloat16)
    key_rot = rotate(heads_of(qkv[:, D : 2 * D]), cosine, sine_tab).astype(jnp.bfloat16)
    value_low = heads_of(qkv[:, 2 * D :]).astype(jnp.bfloat16)
    mixed_out, logsum = attend(query_rot, key_rot, value_low, my_docs, my_docs)
    mixed_low = mixed_out.reshape(rows_dev, D).astype(jnp.bfloat16)
    attn_out = jnp.dot(mixed_low, output_full, preferred_element_type=jnp.float32) + output_offset
    res_one = pack_in.astype(jnp.float32) + attn_out
    norm_one, norm_pull = jax.vjp(layer_norm, res_one, attn_scale, attn_offset)
    norm_low = norm_one.astype(jnp.bfloat16)

    if narrow_n == 2:
        far_rows = swapped(norm_low, "narrow", 0)
        own_act, own_pull, own_part = ffn_forward(norm_low, inner_cols, inner_offset, outer_cols)
        far_act, far_pull, far_part = ffn_forward(far_rows, inner_cols, inner_offset, outer_cols)
        outer_sum = own_part + swapped(far_part.astype(jnp.bfloat16), "narrow", 0).astype(
            jnp.float32
        )
    else:
        group_rows = lax.all_gather(norm_low, "narrow", axis=0, tiled=True)
        all_act, all_pull, all_part = ffn_forward(group_rows, inner_cols, inner_offset, outer_cols)
        outer_sum = narrow_scatter_sum(all_part)
    outer_out = outer_sum + outer_offset
    res_two = norm_one + outer_out
    pack_out, ffn_pull = jax.vjp(layer_norm, res_two, ffn_scale, ffn_offset)
    grad_two, ffn_gsum, ffn_ssum = ffn_pull(pack_cot.astype(jnp.float32))
    grad_outer = grad_two.astype(jnp.bfloat16)
    outer_bsum = jnp.sum(grad_outer.astype(jnp.float32), axis=0)
    if narrow_n == 2:
        far_grads = swapped(grad_outer, "narrow", 0)
        own_inner, own_back = ffn_backward(grad_outer, own_pull, inner_cols, outer_cols)
        far_inner, far_back = ffn_backward(far_grads, far_pull, inner_cols, outer_cols)
        grad_part = own_back + swapped(far_back.astype(jnp.bfloat16), "narrow", 0).astype(
            jnp.float32
        )
        outer_wsum_t = contract_rows(grad_outer, own_act) + contract_rows(far_grads, far_act)
        inner_wsum = contract_rows(norm_low, own_inner) + contract_rows(far_rows, far_inner)
        inner_bsum = jnp.sum(own_inner.astype(jnp.float32), axis=0) + jnp.sum(
            far_inner.astype(jnp.float32), axis=0
        )
    else:
        group_grads = lax.all_gather(grad_outer, "narrow", axis=0, tiled=True)
        all_inner, all_back = ffn_backward(group_grads, all_pull, inner_cols, outer_cols)
        grad_part = narrow_scatter_sum(all_back)
        outer_wsum_t = contract_rows(group_grads, all_act)
        inner_wsum = contract_rows(group_rows, all_inner)
        inner_bsum = jnp.sum(all_inner.astype(jnp.float32), axis=0)
    bsum_rows = jnp.pad(
        inner_bsum.reshape(wide_n, bias_n), ((0, 0), (0, ffn_rows * bias_k - bias_n))
    ).reshape(wide_n * ffn_rows, bias_k)
    ffn_sums = jnp.concatenate([inner_wsum, outer_wsum_t, bsum_rows], axis=1).astype(jnp.bfloat16)
    ffn_mine = lax.psum_scatter(ffn_sums, "wide", scatter_dimension=0, tiled=True)
    ffn_mine = ffn_mine.astype(jnp.float32)
    inner_wgrad = ffn_mine[:, :ffn_cols]
    outer_wgrad = ffn_mine[:, ffn_cols : 2 * ffn_cols].T
    inner_bgrad = ffn_mine[:, 2 * ffn_cols :].reshape(-1)[:bias_n]

    pack_out, grad_part = lax.optimization_barrier((pack_out, grad_part))
    layer_out = from_pack(pack_out)
    grad_norm = grad_two + grad_part
    grad_one, attn_gsum, attn_ssum = norm_pull(grad_norm)
    grad_attn = grad_one.astype(jnp.bfloat16)
    output_bsum = jnp.sum(grad_attn.astype(jnp.float32), axis=0)
    output_wsum = contract_rows(mixed_low, grad_attn)
    early_small = jnp.stack(
        [output_bsum, attn_gsum, attn_ssum, outer_bsum, ffn_gsum, ffn_ssum], axis=1
    )
    early = jnp.concatenate(
        [output_wsum.reshape(total, share, D), early_small.reshape(total, share, -1)], axis=2
    )

    grad_mixed = heads_of(contract_cols(grad_attn, output_full).astype(jnp.bfloat16))
    grad_qrot, grad_krot, grad_values = attend_back(
        query_rot, key_rot, value_low, my_docs, my_docs, logsum, grad_mixed
    )
    grad_values = grad_values.astype(jnp.bfloat16)
    grad_query = unrotate(grad_qrot, cosine, sine_tab).astype(jnp.bfloat16)
    grad_keys = unrotate(grad_krot, cosine, sine_tab).astype(jnp.bfloat16)
    grad_qkv = jnp.concatenate(
        [
            grad_query.reshape(rows_dev, D),
            grad_keys.reshape(rows_dev, D),
            grad_values.reshape(rows_dev, D),
        ],
        axis=1,
    )
    pack_grad = grad_one + contract_cols(grad_qkv, qkv_full)
    keep_grad = lax.dynamic_slice_in_dim(pack_grad, half_bit * half_len, half_len, 0)
    give_grad = lax.dynamic_slice_in_dim(pack_grad, (1 - half_bit) * half_len, half_len, 0)
    give_grad, grad_qkv, pack_in = lax.optimization_barrier((give_grad, grad_qkv, pack_in))
    got_grad = swapped(give_grad, "narrow", 0)
    input_grad = jnp.where(
        half_bit == 0,
        jnp.concatenate([keep_grad, got_grad]),
        jnp.concatenate([got_grad, keep_grad]),
    )
    qkv_wsum = contract_rows(pack_in, grad_qkv)
    qkv_bsum = jnp.sum(grad_qkv.astype(jnp.float32), axis=0).reshape(3, D)
    wsum_parts = qkv_wsum.reshape(total, share, 3 * D).astype(jnp.bfloat16)
    late_mine = scatter_sum_parts(
        [
            wsum_parts[..., :D],
            wsum_parts[..., D : 2 * D],
            wsum_parts[..., 2 * D :],
            jnp.concatenate(
                [
                    qkv_bsum.T.reshape(total, share, 3).astype(jnp.bfloat16),
                    early.astype(jnp.bfloat16),
                ],
                axis=2,
            ),
        ]
    )
    early_mine = late_mine[:, 3 * D + 3 :]
    query_wgrad = late_mine[:, :D]
    key_wgrad = late_mine[:, D : 2 * D]
    value_wgrad = late_mine[:, 2 * D : 3 * D]
    query_bgrad = late_mine[:, 3 * D]
    key_bgrad = late_mine[:, 3 * D + 1]
    value_bgrad = late_mine[:, 3 * D + 2]
    output_wgrad = early_mine[:, :D]
    output_bgrad = early_mine[:, D]
    attn_ggrad = early_mine[:, D + 1]
    attn_sgrad = early_mine[:, D + 2]
    outer_bgrad = early_mine[:, D + 3]
    ffn_ggrad = early_mine[:, D + 4]
    ffn_sgrad = early_mine[:, D + 5]
    return (
        layer_out,
        input_grad,
        query_wgrad,
        query_bgrad,
        key_wgrad,
        key_bgrad,
        value_wgrad,
        value_bgrad,
        output_wgrad,
        output_bgrad,
        attn_ggrad,
        attn_sgrad,
        inner_wgrad,
        inner_bgrad,
        outer_wgrad,
        outer_bgrad,
        ffn_ggrad,
        ffn_sgrad,
    )


def solution(mesh):
    return jax.shard_map(
        local,
        mesh=mesh,
        in_specs=(
            P(("wide", "narrow"), None),
            P("wide", None),
            P(("wide", "narrow"), None),
            P(("wide", "narrow")),
            P(("wide", "narrow"), None),
            P(("wide", "narrow")),
            P(("wide", "narrow"), None),
            P(("wide", "narrow")),
            P(("wide", "narrow"), None),
            P(("wide", "narrow")),
            P(("wide", "narrow")),
            P(("wide", "narrow")),
            P("wide", "narrow"),
            P(("narrow", "wide")),
            P("narrow", "wide"),
            P(("wide", "narrow")),
            P(("wide", "narrow")),
            P(("wide", "narrow")),
            P(("wide", "narrow"), None),
        ),
        out_specs=(
            P(("wide", "narrow"), None),
            P(("wide", "narrow"), None),
            P(("wide", "narrow"), None),
            P(("wide", "narrow")),
            P(("wide", "narrow"), None),
            P(("wide", "narrow")),
            P(("wide", "narrow"), None),
            P(("wide", "narrow")),
            P(("wide", "narrow"), None),
            P(("wide", "narrow")),
            P(("wide", "narrow")),
            P(("wide", "narrow")),
            P("wide", "narrow"),
            P(("narrow", "wide")),
            P("narrow", "wide"),
            P(("wide", "narrow")),
            P(("wide", "narrow")),
            P(("wide", "narrow")),
        ),
        check_vma=False,
    )
```

```python
import itertools

import jax
import jax.numpy as jnp
from jax import lax
from jax.sharding import PartitionSpec as P

D = 768
HEADS = 12
HEAD_DIM = 64

ALL = ("wide", "narrow")
layer_eps = 1e-12
masked_score = -1e30


def swapped(shard, axis, bit):
    return lax.ppermute(shard, axis, [(i, i ^ 1 << bit) for i in range(lax.axis_size(axis))])


def part_orders(total, narrow_n, parts):
    bits = total.bit_length() - 1
    core_bit = narrow_n.bit_length() - 1
    narrow_bits = list(range(core_bit))
    wide_bits = [b for b in reversed(range(core_bit + 1, bits))]
    rotations = [wide_bits[k:] + wide_bits[:k] for k in range(max(1, len(wide_bits)))]
    others = [list(p) for p in itertools.permutations(wide_bits) if list(p) not in rotations]
    choices = rotations + others
    return [narrow_bits + choices[p % len(choices)] + [core_bit] for p in range(parts)]


def is_pow2(n):
    return n & (n - 1) == 0


def column_splits(cols, parts):
    tiles = -(-cols // 128)
    parts = max(1, min(parts, tiles))
    edges = [min(cols, (tiles * i // parts) * 128) for i in range(parts)] + [cols]
    return [(a, b) for a, b in zip(edges[:-1], edges[1:]) if b > a]


def doubling_gather(shard, order, total):
    me = lax.axis_index(ALL)
    cur = shard
    for b in order:
        other = lax.ppermute(cur, ALL, [(i, i ^ (1 << b)) for i in range(total)])
        bit = (me >> b) & 1
        pick = (jnp.arange(2) == bit).reshape((2,) + (1,) * cur.ndim)
        cur = jnp.where(pick, cur[None], other[None])
    k = len(order)
    perm = [k - 1 - order.index(b) for b in reversed(range(k))]
    cur = cur.transpose(perm + list(range(k, cur.ndim)))
    return cur.reshape((total,) + shard.shape)


def gather_all(shard, parts=3):
    total = lax.axis_size("wide") * lax.axis_size("narrow")
    narrow_n = lax.axis_size("narrow")
    if not (is_pow2(total) and is_pow2(narrow_n)):
        return lax.all_gather(shard, ALL, axis=0, tiled=False)
    splits = column_splits(shard.shape[-1], parts)
    orders = part_orders(total, narrow_n, len(splits))
    pieces = [
        doubling_gather(shard[..., a:b], order, total) for (a, b), order in zip(splits, orders)
    ]
    return jnp.concatenate(pieces, axis=-1)


def halving_scatter(parts_in, order, total):
    me = lax.axis_index(ALL)
    nbits = total.bit_length() - 1
    cur = parts_in.reshape((2,) * nbits + parts_in.shape[1:])
    axes = list(reversed(range(nbits)))
    for b in order:
        a = axes.index(b)
        bit = (me >> b) & 1
        mine = lax.dynamic_index_in_dim(cur, bit, axis=a, keepdims=False)
        theirs = lax.dynamic_index_in_dim(cur, 1 - bit, axis=a, keepdims=False)
        got = lax.ppermute(
            theirs.astype(jnp.bfloat16), ALL, [(i, i ^ (1 << b)) for i in range(total)]
        )
        cur = mine.astype(jnp.float32) + got.astype(jnp.float32)
        axes.pop(a)
    return cur


def scatter_sum_all(parts_in, parts=3):
    total = lax.axis_size("wide") * lax.axis_size("narrow")
    narrow_n = lax.axis_size("narrow")
    if not (is_pow2(total) and is_pow2(narrow_n)):
        return lax.psum_scatter(
            parts_in.astype(jnp.bfloat16), ALL, scatter_dimension=0, tiled=False
        ).astype(jnp.float32)
    splits = column_splits(parts_in.shape[-1], parts)
    orders = part_orders(total, narrow_n, len(splits))
    pieces = [
        halving_scatter(parts_in[..., a:b], list(reversed(order)), total)
        for (a, b), order in zip(splits, orders)
    ]
    return jnp.concatenate(pieces, axis=-1)


def scatter_sum_parts(part_list):
    total = lax.axis_size("wide") * lax.axis_size("narrow")
    narrow_n = lax.axis_size("narrow")
    if not (is_pow2(total) and is_pow2(narrow_n)):
        return jnp.concatenate([scatter_sum_all(x, 1) for x in part_list], axis=-1)
    orders = part_orders(total, narrow_n, len(part_list))
    return jnp.concatenate(
        [halving_scatter(x, list(reversed(o)), total) for x, o in zip(part_list, orders)],
        axis=-1,
    )


def narrow_gather(rows):
    n = lax.axis_size("narrow")
    if n != 2:
        return lax.all_gather(rows, "narrow", axis=0, tiled=True)
    other = swapped(rows, "narrow", 0)
    first = lax.axis_index("narrow") == 0
    return jnp.where(first, jnp.concatenate([rows, other]), jnp.concatenate([other, rows]))


def narrow_scatter_sum(part):
    n = lax.axis_size("narrow")
    if n != 2:
        return lax.psum_scatter(
            part.astype(jnp.bfloat16), "narrow", scatter_dimension=0, tiled=True
        ).astype(jnp.float32)
    rows = part.shape[0] // 2
    me = lax.axis_index("narrow")
    mine = lax.dynamic_slice_in_dim(part, me * rows, rows, 0)
    theirs = lax.dynamic_slice_in_dim(part, (1 - me) * rows, rows, 0)
    return mine + swapped(theirs.astype(jnp.bfloat16), "narrow", 0).astype(jnp.float32)


def layer_norm(values, gain_vec, shift_vec):
    center = values - jnp.mean(values, axis=-1, keepdims=True)
    spread = jnp.mean(center * center, axis=-1, keepdims=True)
    return center * lax.rsqrt(spread + layer_eps) * gain_vec + shift_vec


def gelu_exact(values):
    return jax.nn.gelu(values, approximate=False)


def rotary_tables(doc_row):
    places = jnp.arange(doc_row.shape[0], dtype=jnp.int32)
    before = jnp.sum((doc_row[None, :] < doc_row[:, None]).astype(jnp.int32), axis=1)
    position = (places - before).astype(jnp.float32)
    frequency = 10000.0 ** (-2.0 * jnp.arange(HEAD_DIM // 2, dtype=jnp.float32) / HEAD_DIM)
    angles = position[:, None] * frequency[None, :]
    return (jnp.cos(angles), jnp.sin(angles))


def rotate(values, cosine, sine_tab):
    half_dim = values.shape[-1] // 2
    first_half = values[..., :half_dim]
    second = values[..., half_dim:]
    return jnp.concatenate(
        [first_half * cosine - second * sine_tab, second * cosine + first_half * sine_tab], axis=-1
    )


def unrotate(values, cosine, sine_tab):
    half_dim = values.shape[-1] // 2
    first_half = values[..., :half_dim]
    second = values[..., half_dim:]
    return jnp.concatenate(
        [first_half * cosine + second * sine_tab, second * cosine - first_half * sine_tab], axis=-1
    )


def contract_rows(left_op, right_op):
    return lax.dot_general(
        left_op, right_op, (((0,), (0,)), ((), ())), preferred_element_type=jnp.float32
    )


def contract_cols(left_op, right_op):
    return lax.dot_general(
        left_op, right_op, (((1,), (1,)), ((), ())), preferred_element_type=jnp.float32
    )


def score_block(query_rot, key_rot, query_docs, key_docs):
    scores = jnp.einsum(
        "pqhd,pkhd->phqk", query_rot, key_rot, preferred_element_type=jnp.float32
    ) * HEAD_DIM ** (-0.5)
    same_doc = query_docs[:, :, None] == key_docs[:, None, :]
    return jnp.where(same_doc[:, None], scores, masked_score)


def attend(query_rot, key_rot, value_low, query_docs, key_docs):
    scores = score_block(query_rot, key_rot, query_docs, key_docs)
    row_peak = jnp.max(scores, axis=-1, keepdims=True)
    exponent = jnp.exp(scores - row_peak)
    totals = jnp.sum(exponent, axis=-1, keepdims=True)
    probability = (exponent / totals).astype(jnp.bfloat16)
    mixed_out = jnp.einsum(
        "phqk,pkhd->pqhd", probability, value_low, preferred_element_type=jnp.float32
    )
    return (mixed_out, row_peak + jnp.log(totals))


def attend_back(query_rot, key_rot, value_low, query_docs, key_docs, logsum, grad_mixed):
    probability = jnp.exp(score_block(query_rot, key_rot, query_docs, key_docs) - logsum)
    grad_values = jnp.einsum(
        "phqk,pqhd->pkhd",
        probability.astype(jnp.bfloat16),
        grad_mixed,
        preferred_element_type=jnp.float32,
    )
    grad_probs = jnp.einsum(
        "pqhd,pkhd->phqk", grad_mixed, value_low, preferred_element_type=jnp.float32
    )
    inner_sum = jnp.sum(probability * grad_probs, axis=-1, keepdims=True)
    grad_scores = (probability * (grad_probs - inner_sum)).astype(jnp.bfloat16)
    grad_query = jnp.einsum(
        "phqk,pkhd->pqhd", grad_scores, key_rot, preferred_element_type=jnp.float32
    ) * HEAD_DIM ** (-0.5)
    grad_keys = jnp.einsum(
        "phqk,pqhd->pkhd", grad_scores, query_rot, preferred_element_type=jnp.float32
    ) * HEAD_DIM ** (-0.5)
    return (grad_query, grad_keys, grad_values)


def ffn_forward(rows, inner_cols, inner_offset, outer_cols):
    inner_pre = jnp.dot(rows, inner_cols, preferred_element_type=jnp.float32) + inner_offset
    act_value, gelu_pull = jax.vjp(gelu_exact, inner_pre)
    act_low = act_value.astype(jnp.bfloat16)
    return act_low, gelu_pull, contract_cols(act_low, outer_cols)


def ffn_backward(grads, gelu_pull, inner_cols, outer_cols):
    grad_act = jnp.dot(grads, outer_cols, preferred_element_type=jnp.float32)
    grad_inner = gelu_pull(grad_act)[0].astype(jnp.bfloat16)
    return grad_inner, contract_cols(grad_inner, inner_cols)


def local(
    layer_in,
    doc_ids,
    query_weight,
    query_bias,
    key_weight,
    key_bias,
    value_weight,
    value_bias,
    output_weight,
    output_bias,
    attn_gain,
    attn_shift,
    inner_weight,
    inner_bias,
    outer_weight,
    outer_bias,
    ffn_gain,
    ffn_shift,
    cotangent,
):
    wide_n = lax.axis_size("wide")
    narrow_n = lax.axis_size("narrow")
    total = wide_n * narrow_n
    share = query_weight.shape[0]
    small_list = (
        query_bias,
        key_bias,
        value_bias,
        output_bias,
        attn_gain,
        attn_shift,
        outer_bias,
        ffn_gain,
        ffn_shift,
    )
    small = jnp.stack(small_list, axis=1)
    small = jnp.pad(small, ((0, 0), (0, 128 - len(small_list))))
    shard = jnp.concatenate([query_weight, key_weight, value_weight, output_weight, small], axis=1)
    full = gather_all(shard).reshape(total * share, shard.shape[1])
    qkv_full = full[:, : 3 * D]
    output_full = full[:, 3 * D : 4 * D]
    vecs = full[:, 4 * D :].astype(jnp.float32)
    (
        query_offset,
        key_offset,
        value_offset,
        output_offset,
        attn_scale,
        attn_offset,
        outer_offset,
        ffn_scale,
        ffn_offset,
    ) = [vecs[:, i] for i in range(len(small_list))]
    qkv_offset = jnp.concatenate([query_offset, key_offset, value_offset])

    ffn_rows, ffn_cols = inner_weight.shape
    bias_n = inner_bias.shape[0]
    bias_k = -(-bias_n // ffn_rows)
    bias_rows = jnp.pad(inner_bias, (0, ffn_rows * bias_k - bias_n)).reshape(ffn_rows, bias_k)
    ffn_shard = jnp.concatenate([inner_weight, outer_weight.T, bias_rows], axis=1)
    ffn_shard, full = lax.optimization_barrier((ffn_shard, full))
    ffn_all = lax.all_gather(ffn_shard, "wide", axis=0, tiled=True)
    inner_cols = ffn_all[:, :ffn_cols]
    outer_cols = ffn_all[:, ffn_cols : 2 * ffn_cols]
    inner_offset = ffn_all[:, 2 * ffn_cols :].reshape(wide_n, ffn_rows * bias_k)[:, :bias_n]
    inner_offset = inner_offset.reshape(-1).astype(jnp.float32)

    rows_dev = layer_in.shape[0]
    half_len = doc_ids.shape[1] // 2
    pack_count = rows_dev // half_len
    narrow_place = lax.axis_index("narrow")
    half_bit = narrow_place % 2
    pair_slot = narrow_place // 2
    pack_docs = lax.dynamic_slice_in_dim(doc_ids, pair_slot * pack_count, pack_count, 0)
    my_docs = lax.dynamic_slice_in_dim(pack_docs, half_bit, 1, 0)
    cosine, sine_tab = jax.vmap(rotary_tables)(my_docs)
    cosine = cosine[:, :, None, :]
    sine_tab = sine_tab[:, :, None, :]

    def to_pack(rows):
        keep = lax.dynamic_slice_in_dim(rows, half_bit * half_len, half_len, 0)
        give = lax.dynamic_slice_in_dim(rows, (1 - half_bit) * half_len, half_len, 0)
        got = swapped(give, "narrow", 0)
        return jnp.where(
            half_bit == 0, jnp.concatenate([keep, got]), jnp.concatenate([got, keep])
        )

    def from_pack(rows):
        keep = lax.dynamic_slice_in_dim(rows, half_bit * half_len, half_len, 0)
        give = lax.dynamic_slice_in_dim(rows, (1 - half_bit) * half_len, half_len, 0)
        got = swapped(give, "narrow", 0)
        return jnp.where(
            half_bit == 0, jnp.concatenate([keep, got]), jnp.concatenate([got, keep])
        )

    pack_in = to_pack(layer_in)
    pack_cot = to_pack(cotangent)

    def heads_of(values):
        return values.reshape(1, rows_dev, HEADS, HEAD_DIM)

    qkv = jnp.dot(pack_in, qkv_full, preferred_element_type=jnp.float32) + qkv_offset
    query_rot = rotate(heads_of(qkv[:, :D]), cosine, sine_tab).astype(jnp.bfloat16)
    key_rot = rotate(heads_of(qkv[:, D : 2 * D]), cosine, sine_tab).astype(jnp.bfloat16)
    value_low = heads_of(qkv[:, 2 * D :]).astype(jnp.bfloat16)
    mixed_out, logsum = attend(query_rot, key_rot, value_low, my_docs, my_docs)
    mixed_low = mixed_out.reshape(rows_dev, D).astype(jnp.bfloat16)
    attn_out = jnp.dot(mixed_low, output_full, preferred_element_type=jnp.float32) + output_offset
    res_one = pack_in.astype(jnp.float32) + attn_out
    norm_one, norm_pull = jax.vjp(layer_norm, res_one, attn_scale, attn_offset)
    norm_low = norm_one.astype(jnp.bfloat16)

    if narrow_n == 2:
        far_rows = swapped(norm_low, "narrow", 0)
        own_act, own_pull, own_part = ffn_forward(norm_low, inner_cols, inner_offset, outer_cols)
        far_act, far_pull, far_part = ffn_forward(far_rows, inner_cols, inner_offset, outer_cols)
        outer_sum = own_part + swapped(far_part.astype(jnp.bfloat16), "narrow", 0).astype(
            jnp.float32
        )
    else:
        group_rows = lax.all_gather(norm_low, "narrow", axis=0, tiled=True)
        all_act, all_pull, all_part = ffn_forward(group_rows, inner_cols, inner_offset, outer_cols)
        outer_sum = narrow_scatter_sum(all_part)
    outer_out = outer_sum + outer_offset
    res_two = norm_one + outer_out
    pack_out, ffn_pull = jax.vjp(layer_norm, res_two, ffn_scale, ffn_offset)
    grad_two, ffn_gsum, ffn_ssum = ffn_pull(pack_cot.astype(jnp.float32))
    grad_outer = grad_two.astype(jnp.bfloat16)
    outer_bsum = jnp.sum(grad_outer.astype(jnp.float32), axis=0)
    if narrow_n == 2:
        far_grads = swapped(grad_outer, "narrow", 0)
        own_inner, own_back = ffn_backward(grad_outer, own_pull, inner_cols, outer_cols)
        far_inner, far_back = ffn_backward(far_grads, far_pull, inner_cols, outer_cols)
        grad_part = own_back + swapped(far_back.astype(jnp.bfloat16), "narrow", 0).astype(
            jnp.float32
        )
        outer_wsum_t = contract_rows(grad_outer, own_act) + contract_rows(far_grads, far_act)
        inner_wsum = contract_rows(norm_low, own_inner) + contract_rows(far_rows, far_inner)
        inner_bsum = jnp.sum(own_inner.astype(jnp.float32), axis=0) + jnp.sum(
            far_inner.astype(jnp.float32), axis=0
        )
    else:
        group_grads = lax.all_gather(grad_outer, "narrow", axis=0, tiled=True)
        all_inner, all_back = ffn_backward(group_grads, all_pull, inner_cols, outer_cols)
        grad_part = narrow_scatter_sum(all_back)
        outer_wsum_t = contract_rows(group_grads, all_act)
        inner_wsum = contract_rows(group_rows, all_inner)
        inner_bsum = jnp.sum(all_inner.astype(jnp.float32), axis=0)
    bsum_rows = jnp.pad(
        inner_bsum.reshape(wide_n, bias_n), ((0, 0), (0, ffn_rows * bias_k - bias_n))
    ).reshape(wide_n * ffn_rows, bias_k)
    ffn_sums = jnp.concatenate([inner_wsum, outer_wsum_t, bsum_rows], axis=1).astype(jnp.bfloat16)
    ffn_mine = lax.psum_scatter(ffn_sums, "wide", scatter_dimension=0, tiled=True)
    ffn_mine = ffn_mine.astype(jnp.float32)
    inner_wgrad = ffn_mine[:, :ffn_cols]
    outer_wgrad = ffn_mine[:, ffn_cols : 2 * ffn_cols].T
    inner_bgrad = ffn_mine[:, 2 * ffn_cols :].reshape(-1)[:bias_n]

    pack_out, grad_part = lax.optimization_barrier((pack_out, grad_part))
    layer_out = from_pack(pack_out)
    grad_norm = grad_two + grad_part
    grad_one, attn_gsum, attn_ssum = norm_pull(grad_norm)
    grad_attn = grad_one.astype(jnp.bfloat16)
    output_bsum = jnp.sum(grad_attn.astype(jnp.float32), axis=0)
    output_wsum = contract_rows(mixed_low, grad_attn)
    early_small = jnp.stack(
        [output_bsum, attn_gsum, attn_ssum, outer_bsum, ffn_gsum, ffn_ssum], axis=1
    )
    early = jnp.concatenate(
        [output_wsum.reshape(total, share, D), early_small.reshape(total, share, -1)], axis=2
    )

    grad_mixed = heads_of(contract_cols(grad_attn, output_full).astype(jnp.bfloat16))
    grad_qrot, grad_krot, grad_values = attend_back(
        query_rot, key_rot, value_low, my_docs, my_docs, logsum, grad_mixed
    )
    grad_values = grad_values.astype(jnp.bfloat16)
    grad_query = unrotate(grad_qrot, cosine, sine_tab).astype(jnp.bfloat16)
    grad_keys = unrotate(grad_krot, cosine, sine_tab).astype(jnp.bfloat16)
    grad_qkv = jnp.concatenate(
        [
            grad_query.reshape(rows_dev, D),
            grad_keys.reshape(rows_dev, D),
            grad_values.reshape(rows_dev, D),
        ],
        axis=1,
    )
    pack_grad = grad_one + contract_cols(grad_qkv, qkv_full)
    keep_grad = lax.dynamic_slice_in_dim(pack_grad, half_bit * half_len, half_len, 0)
    give_grad = lax.dynamic_slice_in_dim(pack_grad, (1 - half_bit) * half_len, half_len, 0)
    give_grad, grad_qkv, pack_in = lax.optimization_barrier((give_grad, grad_qkv, pack_in))
    got_grad = swapped(give_grad, "narrow", 0)
    input_grad = jnp.where(
        half_bit == 0,
        jnp.concatenate([keep_grad, got_grad]),
        jnp.concatenate([got_grad, keep_grad]),
    )
    qkv_bsum = jnp.sum(grad_qkv.astype(jnp.float32), axis=0).reshape(3, D)
    late_mine = scatter_sum_parts(
        [
            *[
                contract_rows(pack_in, grad_qkv[:, k * D : (k + 1) * D])
                .reshape(total, share, D)
                .astype(jnp.bfloat16)
                for k in range(3)
            ],
            jnp.concatenate(
                [
                    qkv_bsum.T.reshape(total, share, 3).astype(jnp.bfloat16),
                    early.astype(jnp.bfloat16),
                ],
                axis=2,
            ),
        ]
    )
    early_mine = late_mine[:, 3 * D + 3 :]
    query_wgrad = late_mine[:, :D]
    key_wgrad = late_mine[:, D : 2 * D]
    value_wgrad = late_mine[:, 2 * D : 3 * D]
    query_bgrad = late_mine[:, 3 * D]
    key_bgrad = late_mine[:, 3 * D + 1]
    value_bgrad = late_mine[:, 3 * D + 2]
    output_wgrad = early_mine[:, :D]
    output_bgrad = early_mine[:, D]
    attn_ggrad = early_mine[:, D + 1]
    attn_sgrad = early_mine[:, D + 2]
    outer_bgrad = early_mine[:, D + 3]
    ffn_ggrad = early_mine[:, D + 4]
    ffn_sgrad = early_mine[:, D + 5]
    return (
        layer_out,
        input_grad,
        query_wgrad,
        query_bgrad,
        key_wgrad,
        key_bgrad,
        value_wgrad,
        value_bgrad,
        output_wgrad,
        output_bgrad,
        attn_ggrad,
        attn_sgrad,
        inner_wgrad,
        inner_bgrad,
        outer_wgrad,
        outer_bgrad,
        ffn_ggrad,
        ffn_sgrad,
    )


def solution(mesh):
    return jax.shard_map(
        local,
        mesh=mesh,
        in_specs=(
            P(("wide", "narrow"), None),
            P("wide", None),
            P(("wide", "narrow"), None),
            P(("wide", "narrow")),
            P(("wide", "narrow"), None),
            P(("wide", "narrow")),
            P(("wide", "narrow"), None),
            P(("wide", "narrow")),
            P(("wide", "narrow"), None),
            P(("wide", "narrow")),
            P(("wide", "narrow")),
            P(("wide", "narrow")),
            P("wide", "narrow"),
            P(("narrow", "wide")),
            P("narrow", "wide"),
            P(("wide", "narrow")),
            P(("wide", "narrow")),
            P(("wide", "narrow")),
            P(("wide", "narrow"), None),
        ),
        out_specs=(
            P(("wide", "narrow"), None),
            P(("wide", "narrow"), None),
            P(("wide", "narrow"), None),
            P(("wide", "narrow")),
            P(("wide", "narrow"), None),
            P(("wide", "narrow")),
            P(("wide", "narrow"), None),
            P(("wide", "narrow")),
            P(("wide", "narrow"), None),
            P(("wide", "narrow")),
            P(("wide", "narrow")),
            P(("wide", "narrow")),
            P("wide", "narrow"),
            P(("narrow", "wide")),
            P("narrow", "wide"),
            P(("wide", "narrow")),
            P(("wide", "narrow")),
            P(("wide", "narrow")),
        ),
        check_vma=False,
    )
```
